32 devices in a mesh: section: 2 (over core), fsdp: 4 (over z), replica: 4 (over y, x).
Axes of the slice: x: 2, y: 2, z: 4, core: 2. Of those that a mesh axis runs over, the one named last changes fastest.
Arguments:
- tokens_in: bfloat16 [2048, 2048], P(('fsdp', 'replica')), may hold values from -6 to 6
- cotangent: bfloat16 [2048, 2048], P(('fsdp', 'replica')), may hold values from -6 to 6
- ln1: bfloat16 [2, 2048], P('section', 'fsdp'), may hold values from 0.25 to 1.75
- wq: bfloat16 [2, 2048, 2048], P('section', 'fsdp'), may hold values from -0.125 to 0.125
- wk: bfloat16 [2, 2048, 1024], P('section', 'fsdp'), may hold values from -0.125 to 0.125
- wv: bfloat16 [2, 2048, 1024], P('section', 'fsdp'), may hold values from -0.125 to 0.125
- qn: bfloat16 [2, 128], P('section', 'fsdp'), may hold values from 0.5 to 2
- kn: bfloat16 [2, 128], P('section', 'fsdp'), may hold values from 0.5 to 2
- wo: bfloat16 [2, 2048, 2048], P('section', 'fsdp'), may hold values from -0.375 to 0.375
- ln2: bfloat16 [2, 2048], P('section', 'fsdp'), may hold values from 0.25 to 1.75
- wg: bfloat16 [2, 2048, 6144], P('section', 'fsdp'), may hold values from -0.125 to 0.125
- wu: bfloat16 [2, 2048, 6144], P('section', 'fsdp'), may hold values from -0.125 to 0.125
- wd: bfloat16 [2, 6144, 2048], P('section', 'fsdp'), may hold values from -0.078125 to 0.078125
Outputs:
- hidden_out: bfloat16 [2, 2048, 2048], P('section', ('fsdp', 'replica'))
- input_grad: float32 [2, 2048, 2048], P('section', ('fsdp', 'replica'))
- grad_ln1: float32 [2, 2048], P('section', 'fsdp')
- grad_wq: float32 [2, 2048, 2048], P('section', 'fsdp')
- grad_wk: float32 [2, 2048, 1024], P('section', 'fsdp')
- grad_wv: float32 [2, 2048, 1024], P('section', 'fsdp')
- grad_qn: float32 [2, 128], P('section', 'fsdp')
- grad_kn: float32 [2, 128], P('section', 'fsdp')
- grad_wo: float32 [2, 2048, 2048], P('section', 'fsdp')
- grad_ln2: float32 [2, 2048], P('section', 'fsdp')
- grad_wg: float32 [2, 2048, 6144], P('section', 'fsdp')
- up_weight_gradient: float32 [2, 2048, 6144], P('section', 'fsdp')
- grad_wd: float32 [2, 6144, 2048], P('section', 'fsdp')
The draws below stay inside these ranges and needn't reach their ends.
All inputs are finite; a program needn't handle non-finite values.
Results may differ from the reference program's by a relative error of at most 0.028.
Values may be sent and summed in bfloat16 or wider, within the bound.
A program may use at most 448 MiB of HBM per device.

```python
import math
import jax
import jax.numpy as jnp
from jax import lax

MODEL_WIDTH = 2048
HQ = 16
KEY_VALUE_HEADS = 8
HEAD_SIZE = 128
FF = 6144
LEN = 128
SEQS = 16
TOKENS = 2048


def levels(stream_key, dims, cuts, smallest, largest):
    level = 1.0
    for axis_at, parts in cuts:
        steps = jax.random.uniform(jax.random.fold_in(jax.random.fold_in(stream_key, 6), axis_at), (parts,), jnp.float32, smallest / len(cuts), largest / len(cuts))
        level = level * jnp.repeat(jnp.exp(steps), dims[axis_at] // parts).reshape((-1,) + (1,) * (len(dims) - 1 - axis_at))
    return level


def centred(own_key, extent, width, reach, shards=(), kind=jnp.bfloat16):
    result = width * jax.random.normal(own_key, extent, jnp.float32)
    if shards:
        result = result * levels(own_key, extent, shards, -0.22, 0.18)
    return jnp.clip(result, -reach, reach).astype(kind)


def setup_inputs(seed: int = 0) -> dict:
    splits = jax.random.split(jax.random.key(seed), 14)
    return {
        "tokens_in": centred(splits[0], (TOKENS, MODEL_WIDTH), 1.0, 6.0, ((0, 16),)),
        "cotangent": centred(splits[1], (TOKENS, MODEL_WIDTH), 1.0, 6.0, ((0, 16),)),
        "ln1": jnp.clip(1.0 + 0.15 * jax.random.normal(splits[2], (2, MODEL_WIDTH), jnp.float32), 0.25, 1.75).astype(jnp.bfloat16),
        "wq": centred(splits[3], (2, MODEL_WIDTH, HQ * HEAD_SIZE), MODEL_WIDTH ** -0.5, 0.125, ((0, 2), (1, 4))),
        "wk": centred(splits[4], (2, MODEL_WIDTH, KEY_VALUE_HEADS * HEAD_SIZE), MODEL_WIDTH ** -0.5, 0.125, ((0, 2), (1, 4))),
        "wv": centred(splits[5], (2, MODEL_WIDTH, KEY_VALUE_HEADS * HEAD_SIZE), MODEL_WIDTH ** -0.5, 0.125, ((0, 2), (1, 4))),
        "qn": jnp.clip(jnp.exp(math.log(2.0) - 1.3862944 * jax.random.uniform(splits[6], (2, HEAD_SIZE), jnp.float32) ** levels(splits[6], (2, HEAD_SIZE), ((0, 2), (1, 4)), -0.2, 0.2)), 0.5, 2.0).astype(jnp.bfloat16),
        "kn": jnp.clip(jnp.exp(math.log(2.0) - 1.3862944 * jax.random.uniform(splits[7], (2, HEAD_SIZE), jnp.float32) ** levels(splits[7], (2, HEAD_SIZE), ((0, 2), (1, 4)), -0.2, 0.2)), 0.5, 2.0).astype(jnp.bfloat16),
        "wo": centred(splits[8], (2, HQ * HEAD_SIZE, MODEL_WIDTH), (HQ * HEAD_SIZE // 8) ** -0.5, 0.375, ((0, 2), (1, 4))),
        "ln2": jnp.clip(1.0 + 0.15 * jax.random.normal(splits[9], (2, MODEL_WIDTH), jnp.float32), 0.25, 1.75).astype(jnp.bfloat16),
        "wg": centred(splits[10], (2, MODEL_WIDTH, FF), MODEL_WIDTH ** -0.5, 0.125, ((0, 2), (1, 4))),
        "wu": centred(splits[11], (2, MODEL_WIDTH, FF), MODEL_WIDTH ** -0.5, 0.125, ((0, 2), (1, 4))),
        "wd": centred(splits[12], (2, FF, MODEL_WIDTH), FF ** -0.5, 0.078125, ((0, 2), (1, 4))),
    }


EPS = 1e-06

def rope_tables(length, half_dim):
    freq = jnp.exp(jnp.arange(half_dim, dtype=jnp.float32) * (-math.log(1000000.0) / half_dim))
    angle = jnp.arange(length, dtype=jnp.float32)[:, None] * freq[None, :]
    return (jnp.cos(angle), jnp.sin(angle))

def rotate(field, cosine, sine, sign):
    half_dim = field.shape[-1] // 2
    first = field[..., :half_dim]
    second = field[..., half_dim:]
    cosine = cosine[None, :, None, :]
    sine = sign * sine[None, :, None, :]
    return jnp.concatenate([first * cosine - second * sine, second * cosine + first * sine], axis=-1)

def head_norm(field, gain):
    factor = lax.rsqrt(lax.optimization_barrier(jnp.mean(field * field, axis=-1, keepdims=True)) + EPS)
    return (field * factor * gain, factor)

def norm_back(field, factor, gain, grad, axes):
    scaled = grad * gain
    back = factor * scaled - field * factor * factor * factor * lax.optimization_barrier(jnp.mean(scaled * field, axis=-1, keepdims=True))
    return (back, lax.optimization_barrier(jnp.sum(grad * field * factor, axis=axes)))

def outer(left, right):
    return lax.dot_general(left, right, (((0,), (0,)), ((), ())), preferred_element_type=jnp.float32)

def against(left, right):
    return lax.dot_general(left, right, (((1,), (1,)), ((), ())), preferred_element_type=jnp.float32)

def scores_of(qrot, krot):
    length = qrot.shape[1]
    raw = jnp.einsum('sqkgd,smkd->skgqm', qrot.astype(jnp.float32), krot.astype(jnp.float32))
    raw = raw * (1.0 / math.sqrt(qrot.shape[-1]))
    causal = jnp.arange(length)[:, None] >= jnp.arange(length)[None, :]
    return jnp.where(causal, raw, -jnp.inf)

def forward_parts(x, weights, length):
    ln1, wq, wk, wv, qn, kn, wo, ln2, wg, wu, wd = weights
    rows = x.shape[0]
    seqs = rows // length
    head_dim = qn.shape[0]
    heads = wq.shape[1] // head_dim
    kv_heads = wk.shape[1] // head_dim
    group = heads // kv_heads
    cosine, sine = rope_tables(length, head_dim // 2)
    x32 = x.astype(jnp.float32)
    r1 = lax.rsqrt(lax.optimization_barrier(jnp.mean(x32 * x32, axis=-1, keepdims=True)) + EPS)
    xn = (x32 * r1 * ln1.astype(jnp.float32)).astype(jnp.bfloat16)
    query = jnp.dot(xn, wq, preferred_element_type=jnp.float32).reshape(seqs, length, heads, head_dim)
    keys = jnp.dot(xn, wk, preferred_element_type=jnp.float32).reshape(seqs, length, kv_heads, head_dim)
    values = jnp.dot(xn, wv, preferred_element_type=jnp.float32).astype(jnp.bfloat16)
    q_normed, q_factor = head_norm(query, qn.astype(jnp.float32))
    k_normed, k_factor = head_norm(keys, kn.astype(jnp.float32))
    qrot = rotate(q_normed, cosine, sine, 1.0).astype(jnp.bfloat16).reshape(seqs, length, kv_heads, group, head_dim)
    krot = rotate(k_normed, cosine, sine, 1.0).astype(jnp.bfloat16)
    vals = values.reshape(seqs, length, kv_heads, head_dim)
    scores = scores_of(qrot, krot)
    top = lax.optimization_barrier(jnp.max(scores, axis=-1, keepdims=True))
    lse = top + jnp.log(lax.optimization_barrier(jnp.sum(jnp.exp(scores - top), axis=-1, keepdims=True)))
    weights_p = jnp.exp(scores - lse).astype(jnp.bfloat16)
    attended = jnp.einsum('skgqm,smkd->sqkgd', weights_p.astype(jnp.float32), vals.astype(jnp.float32))
    attended = attended.astype(jnp.bfloat16).reshape(rows, heads * head_dim)
    hres = x32 + jnp.dot(attended, wo, preferred_element_type=jnp.float32)
    r2 = lax.rsqrt(lax.optimization_barrier(jnp.mean(hres * hres, axis=-1, keepdims=True)) + EPS)
    hn = (hres * r2 * ln2.astype(jnp.float32)).astype(jnp.bfloat16)
    gate = jnp.dot(hn, wg, preferred_element_type=jnp.float32)
    upper = jnp.dot(hn, wu, preferred_element_type=jnp.float32)
    active = (jax.nn.silu(gate) * upper).astype(jnp.bfloat16)
    output = (hres + jnp.dot(active, wd, preferred_element_type=jnp.float32)).astype(jnp.bfloat16)
    return (x32, r1, xn, query, q_factor, keys, k_factor, vals, qrot, krot, lse, attended, hres, r2, hn, gate, upper, active, output)

def forward(x, weights, length):
    return forward_parts(x, weights, length)[-1]

def act_backward(x, grad_out, weights, length):
    ln1, wq, wk, wv, qn, kn, wo, ln2, wg, wu, wd = weights
    x32, r1, xn, query, q_factor, keys, k_factor, vals, qrot, krot, lse, attended, hres, r2, hn, gate, upper, active, output = forward_parts(x, weights, length)
    rows = x.shape[0]
    seqs = rows // length
    head_dim = qn.shape[0]
    heads = wq.shape[1] // head_dim
    kv_heads = wk.shape[1] // head_dim
    group = heads // kv_heads
    cosine, sine = rope_tables(length, head_dim // 2)
    dact = against(grad_out, wd)
    sig = jax.nn.sigmoid(gate)
    d_up = (dact * gate * sig).astype(jnp.bfloat16)
    d_gate = (dact * upper * sig * (1.0 + gate * (1.0 - sig))).astype(jnp.bfloat16)
    d_hn = against(d_gate, wg) + against(d_up, wu)
    dh_norm, d_ln2 = norm_back(hres, r2, ln2.astype(jnp.float32), d_hn, 0)
    d_h = grad_out.astype(jnp.float32) + dh_norm
    d_ab = d_h.astype(jnp.bfloat16)
    d_out = against(d_ab, wo).astype(jnp.bfloat16).reshape(seqs, length, kv_heads, group, head_dim)
    scores = scores_of(qrot, krot)
    probs = jnp.exp(scores - lse)
    probs_b = probs.astype(jnp.bfloat16)
    d_v = jnp.einsum('skgqm,sqkgd->smkd', probs_b.astype(jnp.float32), d_out.astype(jnp.float32))
    d_vb = d_v.astype(jnp.bfloat16).reshape(rows, kv_heads * head_dim)
    d_p = jnp.einsum('sqkgd,smkd->skgqm', d_out.astype(jnp.float32), vals.astype(jnp.float32))
    delta = lax.optimization_barrier(jnp.sum(probs * d_p, axis=-1, keepdims=True))
    d_s = (probs * (d_p - delta) * (1.0 / math.sqrt(head_dim))).astype(jnp.bfloat16)
    d_qrot = jnp.einsum('skgqm,smkd->sqkgd', d_s.astype(jnp.float32), krot.astype(jnp.float32)).reshape(seqs, length, heads, head_dim)
    d_krot = jnp.einsum('skgqm,sqkgd->smkd', d_s.astype(jnp.float32), qrot.astype(jnp.float32))
    d_qh = rotate(d_qrot, cosine, sine, -1.0)
    d_kh = rotate(d_krot, cosine, sine, -1.0)
    d_q, d_qn = norm_back(query, q_factor, qn.astype(jnp.float32), d_qh, (0, 1, 2))
    d_k, d_kn = norm_back(keys, k_factor, kn.astype(jnp.float32), d_kh, (0, 1, 2))
    d_qb = d_q.astype(jnp.bfloat16).reshape(rows, heads * head_dim)
    d_kb = d_k.astype(jnp.bfloat16).reshape(rows, kv_heads * head_dim)
    d_xn = against(d_qb, wq) + against(d_kb, wk) + against(d_vb, wv)
    dx_norm, d_ln1 = norm_back(x32, r1, ln1.astype(jnp.float32), d_xn, 0)
    d_x = d_h + dx_norm
    saved = (xn, d_qb, d_kb, d_vb, attended, d_ab, hn, d_gate, d_up, active, grad_out)
    return (d_x, saved, (d_ln1, d_qn, d_kn, d_ln2))

def weight_grads(saved, small):
    xn, d_qb, d_kb, d_vb, attended, d_ab, hn, d_gate, d_up, active, grad_out = saved
    d_ln1, d_qn, d_kn, d_ln2 = small
    return (d_ln1, outer(xn, d_qb), outer(xn, d_kb), outer(xn, d_vb), d_qn, d_kn, outer(attended, d_ab), d_ln2, outer(hn, d_gate), outer(hn, d_up), outer(active, grad_out))

def reference(tokens_in, cotangent, ln1, wq, wk, wv, qn, kn, wo, ln2, wg, wu, wd):
    params = (ln1, wq, wk, wv, qn, kn, wo, ln2, wg, wu, wd)
    first_w = tuple((item[0] for item in params))
    second_weights_set = tuple((item[1] for item in params))
    inputs = tokens_in.reshape(SEQS, LEN, MODEL_WIDTH)
    cots = cotangent.reshape(SEQS, LEN, MODEL_WIDTH)

    def step(carry, item):
        x, grad_out = item
        y_first = forward(x, first_w, LEN)
        y_second = forward(y_first, second_weights_set, LEN)
        dx_second, saved_b, small_b = act_backward(y_first, grad_out, second_weights_set, LEN)
        first_input_gradient, saved_a, small_a = act_backward(x, dx_second.astype(jnp.bfloat16), first_w, LEN)
        grads_a = weight_grads(saved_a, small_a)
        grads_b = weight_grads(saved_b, small_b)
        carry = tuple((total + jnp.stack([left, right]) for total, left, right in zip(carry, grads_a, grads_b)))
        return (carry, (y_first, y_second, first_input_gradient, dx_second))
    zeros = tuple((jnp.zeros(item.shape, jnp.float32) for item in params))
    grads, outs = lax.scan(step, zeros, (inputs, cots))
    y_first, y_second, first_input_gradient, dx_second = outs
    hidden_out = jnp.stack([y_first.reshape(TOKENS, MODEL_WIDTH), y_second.reshape(TOKENS, MODEL_WIDTH)])
    input_grad = jnp.stack([first_input_gradient.reshape(TOKENS, MODEL_WIDTH), dx_second.reshape(TOKENS, MODEL_WIDTH)])
    return (hidden_out, input_grad, grads[0], grads[1], grads[2], grads[3], grads[4], grads[5], grads[6], grads[7], grads[8], grads[9], grads[10])
```

```python
import functools
import math

import jax
import jax.numpy as jnp
from jax import lax
from jax.experimental import pallas as pl
from jax.experimental.pallas import tpu as pltpu
from jax.sharding import PartitionSpec as P

LEN = 128
EPS = 1e-06
F32 = jnp.float32
BF16 = jnp.bfloat16
MESH = pl.DeviceIdType.MESH
TILE = 512


def rope_tables(length, half_dim):
    freq = jnp.exp(jnp.arange(half_dim, dtype=F32) * (-math.log(1000000.0) / half_dim))
    angle = jnp.arange(length, dtype=F32)[:, None] * freq[None, :]
    cosine, sine = jnp.cos(angle), jnp.sin(angle)
    return (
        jnp.concatenate([cosine, cosine], axis=1),
        jnp.concatenate([-sine, sine], axis=1),
    )


def nn(left, right):
    return jnp.dot(left, right, preferred_element_type=F32)


def nt(left, right):
    return lax.dot_general(left, right, (((1,), (1,)), ((), ())), preferred_element_type=F32)


def tn(left, right):
    return lax.dot_general(left, right, (((0,), (0,)), ((), ())), preferred_element_type=F32)


def mean_last(value):
    return jnp.mean(value, axis=-1, keepdims=True)


def tiles(total):
    return [(at, min(TILE, total - at)) for at in range(0, total, TILE)]


def layer_kernel(
    n,
    hd,
    tok, cot, ln1, ln2, qn, kn, cosine, sine, wqkv_h, wgu_h, wo_h, wd_h,
    y_h, dx_h, xn_h, hn_h, dy_h, dab_h, att_h, act_h, dgu_h, dqkv_h, dln1, dln2, dqn, dkn,
    wqkv, wgu, wo, wd,
    xin, dyin, xn_all, hn_all, dy_all, dab_all, qkv, qkvb, att, hres, gate, up, act, dgu, dqkv,
    dres, yv, sbuf, rbuf,
    w_sem, out_sem, ag_send, ag_recv, rs_send, rs_recv, hand_send, hand_recv,
):
    sec = lax.axis_index("section")
    me = lax.axis_index("fsdp")
    rows, width = tok.shape
    qcols = att.shape[-1]
    kcols = (qkvb.shape[-1] - qcols) // 2
    hidden = act.shape[-1]
    rep = wqkv.shape[1]
    kfold = wqkv.shape[1] * wqkv.shape[2]
    scale = 1.0 / math.sqrt(hd)

    barrier = pltpu.get_barrier_semaphore()
    for d in range(1, n):
        pl.semaphore_signal(
            barrier, inc=1, device_id={"fsdp": lax.rem(me + d, n)}, device_id_type=MESH
        )
    pl.semaphore_signal(barrier, inc=1, device_id={"section": 1 - sec}, device_id_type=MESH)

    loads = []
    for r in range(rep):
        loads.append(pltpu.make_async_copy(wqkv_h.at[r], wqkv.at[:, r], w_sem.at[r]))
    for r in range(rep):
        loads.append(pltpu.make_async_copy(wgu_h.at[r], wgu.at[:, r], w_sem.at[rep + r]))
    load_o = pltpu.make_async_copy(wo_h, wo, w_sem.at[2 * rep])
    load_d = pltpu.make_async_copy(wd_h, wd, w_sem.at[2 * rep + 1])
    for load in loads[:rep] + [load_o] + loads[rep:] + [load_d]:
        load.start()
    pl.semaphore_wait(barrier, n)

    def spread(buf, c, d):
        return pltpu.make_async_remote_copy(
            src_ref=buf.at[me],
            dst_ref=buf.at[me],
            send_sem=ag_send.at[c, d - 1],
            recv_sem=ag_recv.at[c, d - 1],
            device_id={"fsdp": lax.rem(me + d, n)},
            device_id_type=MESH,
        )

    def partial_to(c, d):
        return pltpu.make_async_remote_copy(
            src_ref=sbuf.at[d],
            dst_ref=rbuf.at[c % 2, d - 1],
            send_sem=rs_send.at[c, d - 1],
            recv_sem=rs_recv.at[c, d - 1],
            device_id={"fsdp": lax.rem(me - d + n, n)},
            device_id_type=MESH,
        )

    def spread_start(buf, c):
        for d in range(1, n):
            spread(buf, c, d).start()

    def spread_done(buf, c):
        for d in range(1, n):
            spread(buf, c, d).wait_send()

    def each_block(buf, c, work):
        def step(d, carry):
            @pl.when(d > 0)
            def _():
                spread(buf, c, d).wait_recv()

            work(d, lax.rem(me - d + n, n))

            @pl.when(d > 0)
            def _():
                partial_to(c, d).start()

            return carry

        lax.fori_loop(0, n, step, 0)

    def gathered_sum(c):
        for d in range(1, n):
            partial_to(c, d).wait()
        total = sbuf[0].astype(F32)
        for d in range(1, n):
            total = total + rbuf[c % 2, d - 1].astype(F32)
        return total

    outs = []

    def put(src, dst):
        copy = pltpu.make_async_copy(src, dst, out_sem.at[len(outs)])
        copy.start()
        outs.append(copy)

    def swap(value):
        return pltpu.roll(value, hd // 2, 1)

    def hand(src, dst, to, k):
        return pltpu.make_async_remote_copy(
            src_ref=src,
            dst_ref=dst,
            send_sem=hand_send.at[k],
            recv_sem=hand_recv.at[k],
            device_id={"section": to},
            device_id_type=MESH,
        )

    @pl.when(sec == 0)
    def _():
        xin[...] = tok[...]

    @pl.when(sec == 1)
    def _():
        hand(yv, xin, 0, 0).wait_recv()

    x32 = xin[...].astype(F32)
    r1 = lax.rsqrt(mean_last(x32 * x32) + EPS)
    xn_all[me] = (x32 * r1 * ln1[...]).astype(BF16)
    spread_start(xn_all, 0)
    for load in loads[:rep]:
        load.wait()
    load_o.wait()

    def masked_scores(qh, kh):
        raw = nt(qh, kh) * scale
        at_row = lax.broadcasted_iota(jnp.int32, raw.shape, 0)
        at_col = lax.broadcasted_iota(jnp.int32, raw.shape, 1)
        raw = jnp.where(at_row >= at_col, raw, -jnp.inf)
        top = jnp.max(raw, axis=-1, keepdims=True)
        lse = top + jnp.log(jnp.sum(jnp.exp(raw - top), axis=-1, keepdims=True))
        return jnp.exp(raw - lse)

    def attend(d, s):
        a = xn_all[s]
        for at, size in tiles(wqkv.shape[-1]):
            w = wqkv[:, :, :, at : at + size].reshape(width, size)
            qkv[s, :, at : at + size] = nn(a, w)
        for at in range(0, qcols + kcols, hd):
            field = qkv[s, :, at : at + hd]
            gain = qn[...] if at < qcols else kn[...]
            factor = lax.rsqrt(mean_last(field * field) + EPS)
            normed = field * factor * gain
            turned = normed * cosine[...] + swap(normed) * sine[...]
            qkvb[s, :, at : at + hd] = turned.astype(BF16)
        qkvb[s, :, qcols + kcols :] = qkv[s, :, qcols + kcols :].astype(BF16)
        for j in range(qcols // hd):
            kv = j * kcols // qcols
            kat = qcols + kv * hd
            vat = qcols + kcols + kv * hd
            probs = masked_scores(qkvb[s, :, j * hd : (j + 1) * hd], qkvb[s, :, kat : kat + hd])
            attended = nn(probs.astype(BF16), qkvb[s, :, vat : vat + hd])
            att[s, :, j * hd : (j + 1) * hd] = attended.astype(BF16)
        a = att[s]
        for at, size in tiles(width):
            sbuf[d, :, at : at + size] = nn(a, wo[:, at : at + size]).astype(BF16)

    each_block(xn_all, 0, attend)
    h = x32 + gathered_sum(0)
    hres[...] = h
    r2 = lax.rsqrt(mean_last(h * h) + EPS)
    hn_all[me] = (h * r2 * ln2[...]).astype(BF16)
    spread_start(hn_all, 1)
    put(xn_all, xn_h)
    put(att, att_h)
    for load in loads[rep:]:
        load.wait()
    load_d.wait()

    def feed(d, s):
        a = hn_all[s]
        for at, size in tiles(hidden):
            g = nn(a, wgu[:, :, :, at : at + size].reshape(width, size))
            u = nn(a, wgu[:, :, :, hidden + at : hidden + at + size].reshape(width, size))
            gate[s, :, at : at + size] = g
            up[s, :, at : at + size] = u
            act[s, :, at : at + size] = (g * jax.nn.sigmoid(g) * u).astype(BF16)
        a = act[s]
        for at, size in tiles(width):
            sbuf[d, :, at : at + size] = nn(a, wd[:, at : at + size]).astype(BF16)

    each_block(hn_all, 1, feed)
    yv[...] = (hres[...] + gathered_sum(1)).astype(BF16)

    @pl.when(sec == 0)
    def _():
        hand(yv, xin, 1, 0).start()

    put(yv, y_h)
    put(hn_all, hn_h)
    put(act, act_h)

    @pl.when(sec == 0)
    def _():
        hand(yv, dyin, 1, 1).wait_recv()

    @pl.when(sec == 1)
    def _():
        dyin[...] = cot[...]

    dy_all[me] = dyin[...]
    spread_start(dy_all, 2)

    def feed_back(d, s):
        a = dy_all[s]
        for at, size in tiles(hidden):
            dact = nt(a, wd[at : at + size, :])
            g = gate[s, :, at : at + size]
            u = up[s, :, at : at + size]
            sig = jax.nn.sigmoid(g)
            dgu[s, :, at : at + size] = (dact * u * sig * (1.0 + g * (1.0 - sig))).astype(BF16)
            dgu[s, :, hidden + at : hidden + at + size] = (dact * g * sig).astype(BF16)
        a = dgu[s]
        for f in range(n):
            w = wgu[f].reshape(kfold, wgu.shape[-1])
            sbuf[d, :, f * kfold : (f + 1) * kfold] = nt(a, w).astype(BF16)

    each_block(dy_all, 2, feed_back)
    dhn = gathered_sum(2)
    h = hres[...]
    r2 = lax.rsqrt(mean_last(h * h) + EPS)
    u = dhn * ln2[...]
    dh = dyin[...].astype(F32) + (r2 * u - h * r2 * r2 * r2 * mean_last(u * h))
    dln2[...] = jnp.sum(dhn * h * r2, axis=0, keepdims=True)
    dres[...] = dh
    dab_all[me] = dh.astype(BF16)
    spread_start(dab_all, 3)
    put(dy_all, dy_h)
    put(dgu, dgu_h)

    dqn[...] = jnp.zeros_like(dqn)
    dkn[...] = jnp.zeros_like(dkn)

    def head_back(s, at, grad, gain, dgain):
        field = qkv[s, :, at : at + hd]
        factor = lax.rsqrt(mean_last(field * field) + EPS)
        grad = grad * cosine[...] - swap(grad) * sine[...]
        v = grad * gain
        back = factor * v - field * factor * factor * factor * mean_last(v * field)
        dgain[...] += jnp.sum(grad * field * factor, axis=0, keepdims=True)
        dqkv[s, :, at : at + hd] = back.astype(BF16)

    def attend_back(d, s):
        a = dab_all[s]
        for at, size in tiles(qcols):
            dout = nt(a, wo[at : at + size, :]).astype(BF16)
            for kv in range(at * kcols // (qcols * hd), (at + size) * kcols // (qcols * hd)):
                kat = qcols + kv * hd
                vat = qcols + kcols + kv * hd
                kh = qkvb[s, :, kat : kat + hd]
                vh = qkvb[s, :, vat : vat + hd]
                dk = jnp.zeros((rows, hd), F32)
                dv = jnp.zeros((rows, hd), F32)
                for j in range(kv * qcols // kcols, (kv + 1) * qcols // kcols):
                    qh = qkvb[s, :, j * hd : (j + 1) * hd]
                    dh_out = dout[:, j * hd - at : (j + 1) * hd - at]
                    probs = masked_scores(qh, kh)
                    dv = dv + tn(probs.astype(BF16), dh_out)
                    dp = nt(dh_out, vh)
                    delta = jnp.sum(probs * dp, axis=-1, keepdims=True)
                    ds = (probs * (dp - delta) * scale).astype(BF16)
                    dk = dk + tn(ds, qh)
                    head_back(s, j * hd, nn(ds, kh), qn[...], dqn)
                head_back(s, kat, dk, kn[...], dkn)
                dqkv[s, :, vat : vat + hd] = dv.astype(BF16)
        a = dqkv[s]
        for f in range(n):
            w = wqkv[f].reshape(kfold, wqkv.shape[-1])
            sbuf[d, :, f * kfold : (f + 1) * kfold] = nt(a, w).astype(BF16)

    each_block(dab_all, 3, attend_back)
    dxn = gathered_sum(3)
    x32 = xin[...].astype(F32)
    r1 = lax.rsqrt(mean_last(x32 * x32) + EPS)
    u = dxn * ln1[...]
    dx = dres[...] + (r1 * u - x32 * r1 * r1 * r1 * mean_last(u * x32))
    dln1[...] = jnp.sum(dxn * x32 * r1, axis=0, keepdims=True)
    outs[2].wait()

    @pl.when(sec == 0)
    def _():
        hand(yv, xin, 1, 0).wait_send()

    yv[...] = dx.astype(BF16)

    @pl.when(sec == 1)
    def _():
        hand(yv, dyin, 0, 1).start()

    dres[...] = dx
    put(dres, dx_h)
    put(dab_all, dab_h)
    put(dqkv, dqkv_h)
    for c, buf in enumerate((xn_all, hn_all, dy_all, dab_all)):
        spread_done(buf, c)

    @pl.when(sec == 1)
    def _():
        hand(yv, dyin, 0, 1).wait_send()

    for k, copy in enumerate(outs):
        if k != 2:
            copy.wait()


def run_layer(n, rep, tok, cot, ln1, ln2, qn, kn, wqkv, wgu, wo, wd):
    rows, width = tok.shape
    hd = qn.shape[-1]
    qcols = wo.shape[0]
    qkvcols = wqkv.shape[-1]
    hidden = wd.shape[0]
    cosine, sine = rope_tables(rows, hd // 2)
    vm = pl.BlockSpec(memory_space=pltpu.VMEM)
    hbm = pl.BlockSpec(memory_space=pltpu.HBM)

    def wide(columns, kind):
        return (n, rows, columns), kind

    shaped = [
        ((rows, width), BF16),
        ((rows, width), F32),
        wide(width, BF16), wide(width, BF16), wide(width, BF16), wide(width, BF16),
        wide(qcols, BF16), wide(hidden, BF16), wide(2 * hidden, BF16), wide(qkvcols, BF16),
        ((1, width), F32), ((1, width), F32), ((1, hd), F32), ((1, hd), F32),
    ]
    scratch = [
        (wqkv.shape[1], rep, *wqkv.shape[2:]), (wgu.shape[1], rep, *wgu.shape[2:]), wo.shape, wd.shape,
    ]
    scratch = [pltpu.VMEM(shape, BF16) for shape in scratch] + [
        pltpu.VMEM((rows, width), BF16),
        pltpu.VMEM((rows, width), BF16),
        *[pltpu.VMEM(*wide(width, BF16)) for _ in range(4)],
        pltpu.VMEM(*wide(qkvcols, F32)),
        pltpu.VMEM(*wide(qkvcols, BF16)),
        pltpu.VMEM(*wide(qcols, BF16)),
        pltpu.VMEM((rows, width), F32),
        pltpu.VMEM(*wide(hidden, F32)),
        pltpu.VMEM(*wide(hidden, F32)),
        pltpu.VMEM(*wide(hidden, BF16)),
        pltpu.VMEM(*wide(2 * hidden, BF16)),
        pltpu.VMEM(*wide(qkvcols, BF16)),
        pltpu.VMEM((rows, width), F32),
        pltpu.VMEM((rows, width), BF16),
        pltpu.VMEM((n, rows, width), BF16),
        pltpu.VMEM((2, n - 1, rows, width), BF16),
        pltpu.SemaphoreType.DMA((2 * rep + 2,)),
        pltpu.SemaphoreType.DMA((10,)),
        pltpu.SemaphoreType.DMA((4, n - 1)),
        pltpu.SemaphoreType.DMA((4, n - 1)),
        pltpu.SemaphoreType.DMA((4, n - 1)),
        pltpu.SemaphoreType.DMA((4, n - 1)),
        pltpu.SemaphoreType.DMA((2,)),
        pltpu.SemaphoreType.DMA((2,)),
    ]
    return pl.pallas_call(
        functools.partial(layer_kernel, n, hd),
        out_shape=[jax.ShapeDtypeStruct(shape, kind) for shape, kind in shaped],
        in_specs=[vm] * 8 + [hbm] * 4,
        out_specs=[hbm] * 10 + [vm] * 4,
        scratch_shapes=scratch,
        compiler_params=pltpu.CompilerParams(
            collective_id=0, has_side_effects=True, vmem_limit_bytes=67043328
        ),
        name="layer",
    )(tok, cot, ln1, ln2, qn, kn, cosine, sine, wqkv, wgu, wo, wd)


def outer(left, right):
    return tn(left, right).astype(BF16)


def per_device(tokens_in, cotangent, ln1, wq, wk, wv, qn, kn, wo, ln2, wg, wu, wd):
    n, rep = lax.axis_size("fsdp"), lax.axis_size("replica")
    me, mine = lax.axis_index("fsdp"), lax.axis_index("replica")

    gains = (ln1[0], ln2[0], qn[0], kn[0])
    packed = lax.all_gather(jnp.concatenate(gains).reshape(1, -1), "fsdp", axis=0, tiled=True)
    full, at = [], 0
    for gain in gains:
        full.append(packed[:, at : at + gain.shape[0]].reshape(1, -1).astype(F32))
        at += gain.shape[0]
    ln1_all, ln2_all, qn_all, kn_all = full

    def columns(*weights):
        parts = []
        for w in weights:
            fold = w.shape[0] // rep
            part = lax.dynamic_slice_in_dim(w, mine * fold, fold, 0)
            parts.append(part.reshape(fold, n, -1))
        part = jnp.concatenate(parts, axis=2).transpose(1, 0, 2)
        part = lax.all_to_all(part, "fsdp", split_axis=0, concat_axis=0, tiled=True)
        return lax.all_gather(part, "replica", axis=0, tiled=False)

    wqkv = columns(wq[0], wk[0], wv[0])
    wgu = columns(wg[0], wu[0])
    (
        y, dx, xn, hn, dy, dab, att, act, dgu, dqkv, dln1, dln2, dqn, dkn,
    ) = run_layer(
        n, rep, tokens_in, cotangent, ln1_all, ln2_all, qn_all, kn_all, wqkv, wgu, wo[0], wd[0]
    )

    def flat(value):
        return value.reshape(-1, value.shape[-1])

    xn, hn, dy, dab, att, act, dgu, dqkv = map(flat, (xn, hn, dy, dab, att, act, dgu, dqkv))

    def rows_of(grad):
        grad = lax.psum_scatter(grad, "replica", scatter_dimension=0, tiled=True)
        return lax.all_gather(grad, "replica", axis=0, tiled=True).astype(F32)

    def columns_back(grad, widths):
        cols = grad.shape[1]
        grad = grad.reshape(n, rep, -1, cols).transpose(1, 0, 2, 3).reshape(-1, cols)
        grad = lax.psum_scatter(grad, "replica", scatter_dimension=0, tiled=True)
        grad = grad.reshape(n, -1, cols)
        grad = lax.all_to_all(grad, "fsdp", split_axis=0, concat_axis=0, tiled=True)
        grad = lax.all_gather(grad, "replica", axis=0, tiled=False)
        grad = grad.transpose(0, 2, 1, 3)
        pieces, at = [], 0
        for size in widths:
            piece = grad[..., at : at + size].astype(F32)
            pieces.append(piece.reshape(piece.shape[0] * piece.shape[1], -1))
            at += size
        return pieces

    g_wd = rows_of(outer(act, dy))
    g_wg, g_wu = columns_back(outer(hn, dgu), (wg.shape[2] // n, wu.shape[2] // n))
    g_wo = rows_of(outer(att, dab))
    g_wq, g_wk, g_wv = columns_back(
        outer(xn, dqkv), (wq.shape[2] // n, wk.shape[2] // n, wv.shape[2] // n)
    )
    small = jnp.concatenate([dln1[0], dln2[0], dqn[0], dkn[0]])
    small = lax.psum(small, ("fsdp", "replica"))
    owned, at = [], 0
    for gain in gains:
        size = gain.shape[0]
        owned.append(lax.dynamic_slice_in_dim(small, at + me * size, size, 0))
        at += n * size
    g_ln1, g_ln2, g_qn, g_kn = owned
    results = (y, dx, g_ln1, g_wq, g_wk, g_wv, g_qn, g_kn, g_wo, g_ln2, g_wg, g_wu, g_wd)
    return tuple(value[None] for value in results)


def solution(mesh):
    rows = P("section", "fsdp", None)
    gain = P("section", "fsdp")
    tokens = P(("fsdp", "replica"), None)
    stacked = P("section", ("fsdp", "replica"), None)
    weights = (gain, rows, rows, rows, gain, gain, rows, gain, rows, rows, rows)
    return jax.shard_map(
        per_device,
        mesh=mesh,
        in_specs=(tokens, tokens, *weights),
        out_specs=(stacked, stacked, *weights),
        check_vma=False,
    )
```

```python
import functools
import math

import jax
import jax.numpy as jnp
from jax import lax
from jax.experimental import pallas as pl
from jax.experimental.pallas import tpu as pltpu
from jax.sharding import PartitionSpec as P

LEN = 128
EPS = 1e-06
F32 = jnp.float32
BF16 = jnp.bfloat16
MESH = pl.DeviceIdType.MESH
TILE = 512


def rope_tables(length, half_dim):
    freq = jnp.exp(jnp.arange(half_dim, dtype=F32) * (-math.log(1000000.0) / half_dim))
    angle = jnp.arange(length, dtype=F32)[:, None] * freq[None, :]
    cosine, sine = jnp.cos(angle), jnp.sin(angle)
    return (
        jnp.concatenate([cosine, cosine], axis=1),
        jnp.concatenate([-sine, sine], axis=1),
    )


def nn(left, right):
    return jnp.dot(left, right, preferred_element_type=F32)


def nt(left, right):
    return lax.dot_general(left, right, (((1,), (1,)), ((), ())), preferred_element_type=F32)


def tn(left, right):
    return lax.dot_general(left, right, (((0,), (0,)), ((), ())), preferred_element_type=F32)


def mean_last(value):
    return jnp.mean(value, axis=-1, keepdims=True)


def tiles(total):
    return [(at, min(TILE, total - at)) for at in range(0, total, TILE)]


def layer_kernel(
    n,
    hd,
    tok, cot, ln1, ln2, qn, kn, cosine, sine, wqkv_h, wgu_h, wo_h, wd_h,
    y_h, dx_h, xn_h, hn_h, dy_h, dab_h, att_h, act_h, dgu_h, dqkv_h, dln1, dln2, dqn, dkn,
    wqkv, wgu, wo, wd,
    xin, dyin, xn_all, hn_all, dy_all, dab_all, qkv, qkvb, att, hres, gate, up, act, dgu, dqkv,
    dres, yv, sbuf, rbuf,
    w_sem, out_sem, ag_send, ag_recv, rs_send, rs_recv, hand_send, hand_recv,
):
    sec = lax.axis_index("section")
    me = lax.axis_index("fsdp")
    rows, width = tok.shape
    qcols = att.shape[-1]
    kcols = (qkvb.shape[-1] - qcols) // 2
    hidden = act.shape[-1]
    rep = wqkv.shape[1]
    kfold = wqkv.shape[1] * wqkv.shape[2]
    scale = 1.0 / math.sqrt(hd)

    barrier = pltpu.get_barrier_semaphore()
    for d in range(1, n):
        pl.semaphore_signal(
            barrier, inc=1, device_id={"fsdp": lax.rem(me + d, n)}, device_id_type=MESH
        )
    pl.semaphore_signal(barrier, inc=1, device_id={"section": 1 - sec}, device_id_type=MESH)

    loads = []
    for r in range(rep):
        loads.append(pltpu.make_async_copy(wqkv_h.at[r], wqkv.at[:, r], w_sem.at[r]))
    for r in range(rep):
        loads.append(pltpu.make_async_copy(wgu_h.at[r], wgu.at[:, r], w_sem.at[rep + r]))
    load_o = pltpu.make_async_copy(wo_h, wo, w_sem.at[2 * rep])
    load_d = pltpu.make_async_copy(wd_h, wd, w_sem.at[2 * rep + 1])
    for load in loads[:rep] + [load_o] + loads[rep:] + [load_d]:
        load.start()
    pl.semaphore_wait(barrier, n)

    def spread(buf, c, d):
        return pltpu.make_async_remote_copy(
            src_ref=buf.at[me],
            dst_ref=buf.at[me],
            send_sem=ag_send.at[c, d - 1],
            recv_sem=ag_recv.at[c, d - 1],
            device_id={"fsdp": lax.rem(me + d, n)},
            device_id_type=MESH,
        )

    def partial_to(c, d):
        return pltpu.make_async_remote_copy(
            src_ref=sbuf.at[d],
            dst_ref=rbuf.at[c % 2, d - 1],
            send_sem=rs_send.at[c, d - 1],
            recv_sem=rs_recv.at[c, d - 1],
            device_id={"fsdp": lax.rem(me - d + n, n)},
            device_id_type=MESH,
        )

    def spread_start(buf, c):
        for d in range(1, n):
            spread(buf, c, d).start()

    def spread_done(buf, c):
        for d in range(1, n):
            spread(buf, c, d).wait_send()

    def each_block(buf, c, work):
        def step(d, carry):
            @pl.when(d > 0)
            def _():
                spread(buf, c, d).wait_recv()

            work(d, lax.rem(me - d + n, n))

            @pl.when(d > 0)
            def _():
                partial_to(c, d).start()

            return carry

        lax.fori_loop(0, n, step, 0)

    def gathered_sum(c):
        for d in range(1, n):
            partial_to(c, d).wait()
        total = sbuf[0].astype(F32)
        for d in range(1, n):
            total = total + rbuf[c % 2, d - 1].astype(F32)
        return total

    outs = []

    def put(src, dst):
        copy = pltpu.make_async_copy(src, dst, out_sem.at[len(outs)])
        copy.start()
        outs.append(copy)

    def swap(value):
        return pltpu.roll(value, hd // 2, 1)

    def hand(src, dst, to, k):
        return pltpu.make_async_remote_copy(
            src_ref=src,
            dst_ref=dst,
            send_sem=hand_send.at[k],
            recv_sem=hand_recv.at[k],
            device_id={"section": to},
            device_id_type=MESH,
        )

    @pl.when(sec == 0)
    def _():
        xin[...] = tok[...]

    @pl.when(sec == 1)
    def _():
        hand(yv, xin, 0, 0).wait_recv()

    x32 = xin[...].astype(F32)
    r1 = lax.rsqrt(mean_last(x32 * x32) + EPS)
    xn_all[me] = (x32 * r1 * ln1[...]).astype(BF16)
    spread_start(xn_all, 0)
    for load in loads[:rep]:
        load.wait()
    load_o.wait()

    def masked_scores(qh, kh):
        raw = nt(qh, kh) * scale
        at_row = lax.broadcasted_iota(jnp.int32, raw.shape, 0)
        at_col = lax.broadcasted_iota(jnp.int32, raw.shape, 1)
        raw = jnp.where(at_row >= at_col, raw, -jnp.inf)
        top = jnp.max(raw, axis=-1, keepdims=True)
        lse = top + jnp.log(jnp.sum(jnp.exp(raw - top), axis=-1, keepdims=True))
        return jnp.exp(raw - lse)

    def attend(d, s):
        a = xn_all[s]
        for at, size in tiles(wqkv.shape[-1]):
            w = wqkv[:, :, :, at : at + size].reshape(width, size)
            qkv[s, :, at : at + size] = nn(a, w)
        for at in range(0, qcols + kcols, hd):
            field = qkv[s, :, at : at + hd]
            gain = qn[...] if at < qcols else kn[...]
            factor = lax.rsqrt(mean_last(field * field) + EPS)
            normed = field * factor * gain
            turned = normed * cosine[...] + swap(normed) * sine[...]
            qkvb[s, :, at : at + hd] = turned.astype(BF16)
        qkvb[s, :, qcols + kcols :] = qkv[s, :, qcols + kcols :].astype(BF16)
        for j in range(qcols // hd):
            kv = j * kcols // qcols
            kat = qcols + kv * hd
            vat = qcols + kcols + kv * hd
            probs = masked_scores(qkvb[s, :, j * hd : (j + 1) * hd], qkvb[s, :, kat : kat + hd])
            attended = nn(probs.astype(BF16), qkvb[s, :, vat : vat + hd])
            att[s, :, j * hd : (j + 1) * hd] = attended.astype(BF16)
        a = att[s]
        for at, size in tiles(width):
            sbuf[d, :, at : at + size] = nn(a, wo[:, at : at + size]).astype(BF16)

    each_block(xn_all, 0, attend)
    h = x32 + gathered_sum(0)
    hres[...] = h
    r2 = lax.rsqrt(mean_last(h * h) + EPS)
    hn_all[me] = (h * r2 * ln2[...]).astype(BF16)
    spread_start(hn_all, 1)
    put(xn_all, xn_h)
    put(att, att_h)
    for load in loads[rep:]:
        load.wait()
    load_d.wait()

    def feed(d, s):
        a = hn_all[s]
        for at, size in tiles(hidden):
            g = nn(a, wgu[:, :, :, at : at + size].reshape(width, size))
            u = nn(a, wgu[:, :, :, hidden + at : hidden + at + size].reshape(width, size))
            gate[s, :, at : at + size] = g
            up[s, :, at : at + size] = u
            act[s, :, at : at + size] = (g * jax.nn.sigmoid(g) * u).astype(BF16)
        a = act[s]
        for at, size in tiles(width):
            sbuf[d, :, at : at + size] = nn(a, wd[:, at : at + size]).astype(BF16)

    each_block(hn_all, 1, feed)
    yv[...] = (hres[...] + gathered_sum(1)).astype(BF16)

    @pl.when(sec == 0)
    def _():
        hand(yv, xin, 1, 0).start()

    put(yv, y_h)
    put(hn_all, hn_h)
    put(act, act_h)

    @pl.when(sec == 0)
    def _():
        hand(yv, dyin, 1, 1).wait_recv()

    @pl.when(sec == 1)
    def _():
        dyin[...] = cot[...]

    dy_all[me] = dyin[...]
    spread_start(dy_all, 2)

    def feed_back(d, s):
        a = dy_all[s]
        for at, size in tiles(hidden):
            dact = nt(a, wd[at : at + size, :])
            g = gate[s, :, at : at + size]
            u = up[s, :, at : at + size]
            sig = jax.nn.sigmoid(g)
            dgu[s, :, at : at + size] = (dact * u * sig * (1.0 + g * (1.0 - sig))).astype(BF16)
            dgu[s, :, hidden + at : hidden + at + size] = (dact * g * sig).astype(BF16)
        a = dgu[s]
        for f in range(n):
            w = wgu[f].reshape(kfold, wgu.shape[-1])
            sbuf[d, :, f * kfold : (f + 1) * kfold] = nt(a, w).astype(BF16)

    each_block(dy_all, 2, feed_back)
    dhn = gathered_sum(2)
    h = hres[...]
    r2 = lax.rsqrt(mean_last(h * h) + EPS)
    u = dhn * ln2[...]
    dh = dyin[...].astype(F32) + (r2 * u - h * r2 * r2 * r2 * mean_last(u * h))
    dln2[...] = jnp.sum(dhn * h * r2, axis=0, keepdims=True)
    dres[...] = dh
    dab_all[me] = dh.astype(BF16)
    spread_start(dab_all, 3)
    put(dy_all, dy_h)
    put(dgu, dgu_h)

    dqn[...] = jnp.zeros_like(dqn)
    dkn[...] = jnp.zeros_like(dkn)

    def head_back(s, at, grad, gain, dgain):
        field = qkv[s, :, at : at + hd]
        factor = lax.rsqrt(mean_last(field * field) + EPS)
        grad = grad * cosine[...] - swap(grad) * sine[...]
        v = grad * gain
        back = factor * v - field * factor * factor * factor * mean_last(v * field)
        dgain[...] += jnp.sum(grad * field * factor, axis=0, keepdims=True)
        dqkv[s, :, at : at + hd] = back.astype(BF16)

    def attend_back(d, s):
        a = dab_all[s]
        for at, size in tiles(qcols):
            dout = nt(a, wo[at : at + size, :]).astype(BF16)
            for kv in range(at * kcols // (qcols * hd), (at + size) * kcols // (qcols * hd)):
                kat = qcols + kv * hd
                vat = qcols + kcols + kv * hd
                kh = qkvb[s, :, kat : kat + hd]
                vh = qkvb[s, :, vat : vat + hd]
                dk = jnp.zeros((rows, hd), F32)
                dv = jnp.zeros((rows, hd), F32)
                for j in range(kv * qcols // kcols, (kv + 1) * qcols // kcols):
                    qh = qkvb[s, :, j * hd : (j + 1) * hd]
                    dh_out = dout[:, j * hd - at : (j + 1) * hd - at]
                    probs = masked_scores(qh, kh)
                    dv = dv + tn(probs.astype(BF16), dh_out)
                    dp = nt(dh_out, vh)
                    delta = jnp.sum(probs * dp, axis=-1, keepdims=True)
                    ds = (probs * (dp - delta) * scale).astype(BF16)
                    dk = dk + tn(ds, qh)
                    head_back(s, j * hd, nn(ds, kh), qn[...], dqn)
                head_back(s, kat, dk, kn[...], dkn)
                dqkv[s, :, vat : vat + hd] = dv.astype(BF16)
        a = dqkv[s]
        for f in range(n):
            w = wqkv[f].reshape(kfold, wqkv.shape[-1])
            sbuf[d, :, f * kfold : (f + 1) * kfold] = nt(a, w).astype(BF16)

    each_block(dab_all, 3, attend_back)
    dxn = gathered_sum(3)
    x32 = xin[...].astype(F32)
    r1 = lax.rsqrt(mean_last(x32 * x32) + EPS)
    u = dxn * ln1[...]
    dx = dres[...] + (r1 * u - x32 * r1 * r1 * r1 * mean_last(u * x32))
    dln1[...] = jnp.sum(dxn * x32 * r1, axis=0, keepdims=True)
    outs[2].wait()

    @pl.when(sec == 0)
    def _():
        hand(yv, xin, 1, 0).wait_send()

    yv[...] = dx.astype(BF16)

    @pl.when(sec == 1)
    def _():
        hand(yv, dyin, 0, 1).start()

    dres[...] = dx
    put(dres, dx_h)
    put(dab_all, dab_h)
    put(dqkv, dqkv_h)
    for c, buf in enumerate((xn_all, hn_all, dy_all, dab_all)):
        spread_done(buf, c)

    @pl.when(sec == 1)
    def _():
        hand(yv, dyin, 0, 1).wait_send()

    for k, copy in enumerate(outs):
        if k != 2:
            copy.wait()


def run_layer(n, rep, tok, cot, ln1, ln2, qn, kn, wqkv, wgu, wo, wd):
    rows, width = tok.shape
    hd = qn.shape[-1]
    qcols = wo.shape[0]
    qkvcols = wqkv.shape[-1]
    hidden = wd.shape[0]
    cosine, sine = rope_tables(rows, hd // 2)
    vm = pl.BlockSpec(memory_space=pltpu.VMEM)
    hbm = pl.BlockSpec(memory_space=pltpu.HBM)

    def wide(columns, kind):
        return (n, rows, columns), kind

    shaped = [
        ((rows, width), BF16),
        ((rows, width), F32),
        wide(width, BF16), wide(width, BF16), wide(width, BF16), wide(width, BF16),
        wide(qcols, BF16), wide(hidden, BF16), wide(2 * hidden, BF16), wide(qkvcols, BF16),
        ((1, width), F32), ((1, width), F32), ((1, hd), F32), ((1, hd), F32),
    ]
    scratch = [
        (wqkv.shape[1], rep, *wqkv.shape[2:]), (wgu.shape[1], rep, *wgu.shape[2:]), wo.shape, wd.shape,
    ]
    scratch = [pltpu.VMEM(shape, BF16) for shape in scratch] + [
        pltpu.VMEM((rows, width), BF16),
        pltpu.VMEM((rows, width), BF16),
        *[pltpu.VMEM(*wide(width, BF16)) for _ in range(4)],
        pltpu.VMEM(*wide(qkvcols, F32)),
        pltpu.VMEM(*wide(qkvcols, BF16)),
        pltpu.VMEM(*wide(qcols, BF16)),
        pltpu.VMEM((rows, width), F32),
        pltpu.VMEM(*wide(hidden, F32)),
        pltpu.VMEM(*wide(hidden, F32)),
        pltpu.VMEM(*wide(hidden, BF16)),
        pltpu.VMEM(*wide(2 * hidden, BF16)),
        pltpu.VMEM(*wide(qkvcols, BF16)),
        pltpu.VMEM((rows, width), F32),
        pltpu.VMEM((rows, width), BF16),
        pltpu.VMEM((n, rows, width), BF16),
        pltpu.VMEM((2, n - 1, rows, width), BF16),
        pltpu.SemaphoreType.DMA((2 * rep + 2,)),
        pltpu.SemaphoreType.DMA((10,)),
        pltpu.SemaphoreType.DMA((4, n - 1)),
        pltpu.SemaphoreType.DMA((4, n - 1)),
        pltpu.SemaphoreType.DMA((4, n - 1)),
        pltpu.SemaphoreType.DMA((4, n - 1)),
        pltpu.SemaphoreType.DMA((2,)),
        pltpu.SemaphoreType.DMA((2,)),
    ]
    return pl.pallas_call(
        functools.partial(layer_kernel, n, hd),
        out_shape=[jax.ShapeDtypeStruct(shape, kind) for shape, kind in shaped],
        in_specs=[vm] * 8 + [hbm] * 4,
        out_specs=[hbm] * 10 + [vm] * 4,
        scratch_shapes=scratch,
        compiler_params=pltpu.CompilerParams(
            collective_id=0, has_side_effects=True, vmem_limit_bytes=67043328
        ),
        name="layer",
    )(tok, cot, ln1, ln2, qn, kn, cosine, sine, wqkv, wgu, wo, wd)


def flip(value, bit):
    return value + (1 - 2 * (value // 2**bit % 2)) * 2**bit


def flips(value, bits, subset):
    for at, bit in enumerate(bits):
        if subset >> at & 1:
            value = flip(value, bit)
    return value


def grad_plan(n, qcols, hidden, width):
    fold = width // n
    blocks = fold // 128
    thirds = hidden // qcols
    return blocks, thirds, (blocks * thirds, blocks, hidden // 256, qcols // 256)


def grad_kernel(
    n, rep,
    xn_h, hn_h, dy_h, dab_h, att_h, act_h, dgu_h, dqkv_h,
    gq_h, gk_h, gv_h, go_h, gg_h, gu_h, gd_h,
    xn, hn, dy, dab, att, act, dgu, dqkv, mine_g, reduced, whole, *rest,
):
    steps = rep.bit_length() - 1
    got = rest[:steps]
    in_sem, rs_send, rs_recv, z_send, z_recv, ag_send, ag_recv, out_sem = rest[steps:]
    me = lax.axis_index("fsdp")
    mine = lax.axis_index("replica")
    ch = mine_g.shape[-1]
    part = 128 // n
    width = xn.shape[-1]
    fold = width // n
    hidden = act.shape[-1]
    kcols = gk_h.shape[-1] // n
    blocks, thirds, counts = grad_plan(n, ch, hidden, width)
    starts = [sum(counts[:k]) for k in range(len(counts) + 1)]
    total = starts[-1]
    columns_end = starts[2]
    g_slots, slots = mine_g.shape[0], whole.shape[0]
    orders = (tuple(range(steps)), tuple(reversed(range(steps))))

    barrier = pltpu.get_barrier_semaphore()
    for d in range(1, n):
        pl.semaphore_signal(
            barrier, inc=1, device_id={"fsdp": lax.rem(me + d, n)}, device_id_type=MESH
        )
    for bit in range(steps):
        pl.semaphore_signal(
            barrier, inc=1, device_id={"replica": flip(mine, bit)}, device_id_type=MESH
        )
    loads = []
    for k, (src, dst) in enumerate(
        ((hn_h, hn), (dgu_h, dgu), (xn_h, xn), (dqkv_h, dqkv), (act_h, act), (dy_h, dy), (att_h, att), (dab_h, dab))
    ):
        loads.append(pltpu.make_async_copy(src, dst, in_sem.at[k]))
        loads[-1].start()
    pl.semaphore_wait(barrier, n - 1 + steps)
    for load in loads:
        load.wait()

    def remote(src, dst, send, recv, where):
        return pltpu.make_async_remote_copy(
            src_ref=src, dst_ref=dst, send_sem=send, recv_sem=recv,
            device_id=where, device_id_type=MESH,
        )

    def scatter_copies(c, j):
        slot, two = lax.rem(c, g_slots), lax.rem(c, 2)
        for h, bits in enumerate(orders):
            partner = flip(mine, bits[j])
            for i in range(rep >> (j + 1)):
                piece = flips(partner, bits[j + 1 :], i)
                yield h, i, remote(
                    mine_g.at[slot, h, piece], got[j].at[two, h, i],
                    rs_send.at[j, two, h, i], rs_recv.at[j, two, h, i], {"replica": partner},
                )

    def across_copies(c):
        slot, two = lax.rem(c, slots), lax.rem(c, 2)
        for d in range(1, n):
            to = lax.rem(me + d, n)
            yield remote(
                reduced.at[:, pl.ds(to * part, part), :],
                whole.at[slot, :, mine, pl.ds(me * part, part), :],
                z_send.at[two, d - 1], z_recv.at[two, d - 1], {"fsdp": to},
            )

    def gather_copies(c, j):
        slot, two = lax.rem(c, slots), lax.rem(c, 2)
        for h, order in enumerate(orders):
            bits = order[::-1]
            partner = flip(mine, bits[j])
            for i in range(1 << j):
                piece = flips(mine, bits[:j], i)
                yield remote(
                    whole.at[slot, h, piece], whole.at[slot, h, piece],
                    ag_send.at[j, two, h, i], ag_recv.at[j, two, h, i], {"replica": partner},
                )

    def aligned(at):
        return pl.multiple_of(at, 128)

    def out_copies(c, kind):
        slot, two = lax.rem(c, slots), lax.rem(c, 2)
        at = c - starts[kind]
        for f in range(n):
            rows = slice(f * part, (f + 1) * part)
            if kind == 0:
                k, j = at // thirds, lax.rem(at, thirds)
                cols = pl.ds(aligned(f * hidden + j * ch), ch)
                pairs = [
                    (whole.at[slot, h, :, rows, :], dst.at[k, :, :, cols])
                    for h, dst in enumerate((gg_h, gu_h))
                ]
            elif kind == 1:
                cols = pl.ds(f * kcols, kcols)
                pairs = [
                    (whole.at[slot, 0, :, rows, :], gq_h.at[at, :, :, pl.ds(f * ch, ch)]),
                    (whole.at[slot, 1, :, rows, pl.ds(0, kcols)], gk_h.at[at, :, :, cols]),
                    (whole.at[slot, 1, :, rows, pl.ds(kcols, kcols)], gv_h.at[at, :, :, cols]),
                ]
            else:
                dst = gd_h if kind == 2 else go_h
                pairs = [
                    (
                        whole.at[slot, h, f],
                        dst.at[pl.ds(aligned(at * 256 + h * 128), 128), pl.ds(f * ch, ch)],
                    )
                    for h in range(2)
                ]
            for i, (src, to) in enumerate(pairs):
                yield pltpu.make_async_copy(src, to, out_sem.at[two, f, i])

    def compute(c, kind):
        slot = lax.rem(c, g_slots)
        at = c - starts[kind]
        if kind < 2:
            left, right = (hn, dgu) if kind == 0 else (xn, dqkv)
            k, j = (at // thirds, lax.rem(at, thirds)) if kind == 0 else (at, 0)
            lefts = jnp.concatenate(
                [left[:, pl.ds(aligned(f * fold + k * 128), 128)] for f in range(n)], axis=1
            )
            for h in range(2):
                gap = hidden if kind == 0 else ch
                product = tn(lefts, right[:, pl.ds(aligned(h * gap + j * ch), ch)]).astype(BF16)
                for f in range(n):
                    block = product[f * 128 : (f + 1) * 128].reshape(rep, 128 // rep, ch)
                    mine_g[slot, h, :, f * part : (f + 1) * part, :] = block
        else:
            left, right = (act, dy) if kind == 2 else (att, dab)
            for q in range(rep):
                cols = left[:, pl.ds(aligned(at * 256), 256)]
                product = tn(cols, right[:, q * ch : (q + 1) * ch]).astype(BF16)
                for h in range(2):
                    mine_g[slot, h, q] = product[h * 128 : (h + 1) * 128]

    def within(c, low, high):
        return jnp.logical_and(c >= low, c < high)

    def tick(t, carry):
        c = t - (2 * steps + 2)
        for kind in range(4):
            @pl.when(within(c, starts[kind], starts[kind + 1]))
            def _():
                for copy in out_copies(c, kind):
                    copy.wait()

        c_out = t - (2 * steps + 1)

        @pl.when(within(c_out, 0, total))
        def _():
            for copy in gather_copies(c_out, steps - 1):
                copy.wait()

        for kind in range(4):
            @pl.when(within(c_out, starts[kind], starts[kind + 1]))
            def _():
                for copy in out_copies(c_out, kind):
                    copy.start()

        for j in reversed(range(1, steps)):
            c_ag = t - (steps + 1 + j)

            @pl.when(within(c_ag, 0, total))
            def _():
                for copy in gather_copies(c_ag, j - 1):
                    copy.wait()
                for copy in gather_copies(c_ag, j):
                    copy.start()

        c_z = t - (steps + 1)

        @pl.when(within(c_z, 0, columns_end))
        def _():
            for copy in across_copies(c_z):
                copy.wait()

        @pl.when(within(c_z, 0, total))
        def _():
            for copy in gather_copies(c_z, 0):
                copy.start()

        for j in reversed(range(steps)):
            c_rs = t - (j + 1)
            slot, two = lax.rem(c_rs, g_slots), lax.rem(c_rs, 2)

            @pl.when(within(c_rs, 0, total))
            def _():
                for h, i, copy in scatter_copies(c_rs, j):
                    copy.wait()
                for h, bits in enumerate(orders):
                    for i in range(rep >> (j + 1)):
                        piece = flips(mine, bits[j + 1 :], i)
                        value = mine_g[slot, h, piece].astype(F32) + got[j][two, h, i].astype(F32)
                        if j < steps - 1:
                            mine_g[slot, h, piece] = value.astype(BF16)
                        else:
                            reduced[h] = value.astype(BF16)
                if j < steps - 1:
                    for h, i, copy in scatter_copies(c_rs, j + 1):
                        copy.start()

            if j == steps - 1:
                at = lax.rem(c_rs, slots)

                @pl.when(within(c_rs, 0, columns_end))
                def _():
                    for copy in across_copies(c_rs):
                        copy.start()
                    rows = pl.ds(pl.multiple_of(me * part, part), part)
                    whole[at, :, mine, rows, :] = reduced[:, rows, :]

                @pl.when(within(c_rs, columns_end, total))
                def _():
                    whole[at, :, mine] = reduced[...]

        for kind in range(4):
            @pl.when(within(t, starts[kind], starts[kind + 1]))
            def _():
                compute(t, kind)

        @pl.when(t < total)
        def _():
            for h, i, copy in scatter_copies(t, 0):
                copy.start()

        return carry

    lax.fori_loop(0, total + 2 * steps + 3, tick, 0)


def run_grads(n, rep, xn, hn, dy, dab, att, act, dgu, dqkv):
    tokens, width = xn.shape
    ch = att.shape[-1]
    hidden = act.shape[-1]
    kcols = (dqkv.shape[-1] - ch) // 2
    fold = width // n
    steps = rep.bit_length() - 1
    hbm = pl.BlockSpec(memory_space=pltpu.HBM)

    def owned(columns):
        return jax.ShapeDtypeStruct((fold // 128, rep, 128 // rep, columns * n), BF16)

    shaped = [
        owned(ch), owned(kcols), owned(kcols), jax.ShapeDtypeStruct((ch, width), BF16),
        owned(hidden), owned(hidden), jax.ShapeDtypeStruct((hidden, width), BF16),
    ]
    operands = (xn, hn, dy, dab, att, act, dgu, dqkv)
    scratch = [pltpu.VMEM(value.shape, BF16) for value in operands] + [
        pltpu.VMEM((steps + 1, 2, rep, 128, ch), BF16),
        pltpu.VMEM((2, 128, ch), BF16),
        pltpu.VMEM((steps + 3, 2, rep, 128, ch), BF16),
        *[pltpu.VMEM((2, 2, rep >> (j + 1), 128, ch), BF16) for j in range(steps)],
        pltpu.SemaphoreType.DMA((len(operands),)),
        pltpu.SemaphoreType.DMA((steps, 2, 2, rep // 2)),
        pltpu.SemaphoreType.DMA((steps, 2, 2, rep // 2)),
        pltpu.SemaphoreType.DMA((2, n - 1)),
        pltpu.SemaphoreType.DMA((2, n - 1)),
        pltpu.SemaphoreType.DMA((steps, 2, 2, rep // 2)),
        pltpu.SemaphoreType.DMA((steps, 2, 2, rep // 2)),
        pltpu.SemaphoreType.DMA((2, n, 3)),
    ]
    results = pl.pallas_call(
        functools.partial(grad_kernel, n, rep),
        out_shape=shaped,
        in_specs=[hbm] * len(operands),
        out_specs=[hbm] * len(shaped),
        scratch_shapes=scratch,
        compiler_params=pltpu.CompilerParams(
            collective_id=1, has_side_effects=True, vmem_limit_bytes=67043328
        ),
        name="grads",
    )(*operands)
    return [value.reshape(-1, value.shape[-1]).astype(F32) for value in results]


def per_device(tokens_in, cotangent, ln1, wq, wk, wv, qn, kn, wo, ln2, wg, wu, wd):
    n, rep = lax.axis_size("fsdp"), lax.axis_size("replica")
    me, mine = lax.axis_index("fsdp"), lax.axis_index("replica")

    gains = (ln1[0], ln2[0], qn[0], kn[0])
    packed = lax.all_gather(jnp.concatenate(gains).reshape(1, -1), "fsdp", axis=0, tiled=True)
    full, at = [], 0
    for gain in gains:
        full.append(packed[:, at : at + gain.shape[0]].reshape(1, -1).astype(F32))
        at += gain.shape[0]
    ln1_all, ln2_all, qn_all, kn_all = full

    def columns(*weights):
        parts = []
        for w in weights:
            fold = w.shape[0] // rep
            part = lax.dynamic_slice_in_dim(w, mine * fold, fold, 0)
            parts.append(part.reshape(fold, n, -1))
        part = jnp.concatenate(parts, axis=2).transpose(1, 0, 2)
        part = lax.all_to_all(part, "fsdp", split_axis=0, concat_axis=0, tiled=True)
        return lax.all_gather(part, "replica", axis=0, tiled=False)

    wqkv = columns(wq[0], wk[0], wv[0])
    wgu = columns(wg[0], wu[0])
    (
        y, dx, xn, hn, dy, dab, att, act, dgu, dqkv, dln1, dln2, dqn, dkn,
    ) = run_layer(
        n, rep, tokens_in, cotangent, ln1_all, ln2_all, qn_all, kn_all, wqkv, wgu, wo[0], wd[0]
    )

    def flat(value):
        return value.reshape(-1, value.shape[-1])

    xn, hn, dy, dab, att, act, dgu, dqkv = map(flat, (xn, hn, dy, dab, att, act, dgu, dqkv))

    g_wq, g_wk, g_wv, g_wo, g_wg, g_wu, g_wd = run_grads(
        n, rep, xn, hn, dy, dab, att, act, dgu, dqkv
    )
    small = jnp.concatenate([dln1[0], dln2[0], dqn[0], dkn[0]])
    small = lax.psum(small, ("fsdp", "replica"))
    owned, at = [], 0
    for gain in gains:
        size = gain.shape[0]
        owned.append(lax.dynamic_slice_in_dim(small, at + me * size, size, 0))
        at += n * size
    g_ln1, g_ln2, g_qn, g_kn = owned
    results = (y, dx, g_ln1, g_wq, g_wk, g_wv, g_qn, g_kn, g_wo, g_ln2, g_wg, g_wu, g_wd)
    return tuple(value[None] for value in results)


def solution(mesh):
    rows = P("section", "fsdp", None)
    gain = P("section", "fsdp")
    tokens = P(("fsdp", "replica"), None)
    stacked = P("section", ("fsdp", "replica"), None)
    weights = (gain, rows, rows, rows, gain, gain, rows, gain, rows, rows, rows)
    return jax.shard_map(
        per_device,
        mesh=mesh,
        in_specs=(tokens, tokens, *weights),
        out_specs=(stacked, stacked, *weights),
        check_vma=False,
    )
```

```python
import functools
import math

import jax
import jax.numpy as jnp
from jax import lax
from jax.experimental import pallas as pl
from jax.experimental.pallas import tpu as pltpu
from jax.sharding import PartitionSpec as P

LEN = 128
EPS = 1e-06
F32 = jnp.float32
BF16 = jnp.bfloat16
MESH = pl.DeviceIdType.MESH
TILE = 512


def rope_tables(length, half_dim):
    freq = jnp.exp(jnp.arange(half_dim, dtype=F32) * (-math.log(1000000.0) / half_dim))
    angle = jnp.arange(length, dtype=F32)[:, None] * freq[None, :]
    cosine, sine = jnp.cos(angle), jnp.sin(angle)
    return (
        jnp.concatenate([cosine, cosine], axis=1),
        jnp.concatenate([-sine, sine], axis=1),
    )


def nn(left, right):
    return jnp.dot(left, right, preferred_element_type=F32)


def nt(left, right):
    return lax.dot_general(left, right, (((1,), (1,)), ((), ())), preferred_element_type=F32)


def tn(left, right):
    return lax.dot_general(left, right, (((0,), (0,)), ((), ())), preferred_element_type=F32)


def mean_last(value):
    return jnp.mean(value, axis=-1, keepdims=True)


def tiles(total):
    return [(at, min(TILE, total - at)) for at in range(0, total, TILE)]


def flip(value, bit):
    return value + (1 - 2 * (value // 2**bit % 2)) * 2**bit


def flips(value, bits, subset):
    for at, bit in enumerate(bits):
        if subset >> at & 1:
            value = flip(value, bit)
    return value


def layer_kernel(
    n,
    rep,
    hd,
    tok, cot, ln1_own, ln2_own, qn_own, kn_own, cosine, sine, wq_h, wk_h, wv_h, wg_h, wu_h, wo_h, wd_h,
    y_h, dx_h, xn_h, hn_h, dy_h, dab_h, att_h, act_h, dgu_h, dqkv_h, dln1, dln2, dqn, dkn,
    wall, wo, wd, ln1, ln2, qn, kn, gains,
    xin, dyin, xn_all, hn_all, dy_all, dab_all, qkv, qkvb, att, hres, gate, up, act, dgu, dqkv,
    dres, yv, sbuf, rbuf,
    w_sem, zw_send, zw_recv, gw_send, gw_recv, own_sem, gain_send, gain_recv, turn,
    out_sem, ag_send, ag_recv, rs_send, rs_recv, hand_send, hand_recv,
):
    sec = lax.axis_index("section")
    me = lax.axis_index("fsdp")
    mine = lax.axis_index("replica")
    steps = rep.bit_length() - 1
    rows, width = tok.shape
    ch = att.shape[-1]
    qcols = ch
    kcols = (qkvb.shape[-1] - qcols) // 2
    hidden = act.shape[-1]
    chunks = wall.shape[0]
    share = wall.shape[3]
    kfold = rep * share
    scale = 1.0 / math.sqrt(hd)
    orders = (tuple(range(steps)), tuple(reversed(range(steps))))

    barrier = pltpu.get_barrier_semaphore()
    for d in range(1, n):
        pl.semaphore_signal(
            barrier, inc=1, device_id={"fsdp": lax.rem(me + d, n)}, device_id_type=MESH
        )
    for bit in range(steps):
        pl.semaphore_signal(
            barrier, inc=1, device_id={"replica": flip(mine, bit)}, device_id_type=MESH
        )
    pl.semaphore_signal(barrier, inc=1, device_id={"section": 1 - sec}, device_id_type=MESH)
    load_o = pltpu.make_async_copy(wo_h, wo, w_sem.at[0])
    load_d = pltpu.make_async_copy(wd_h, wd, w_sem.at[1])
    load_o.start()
    load_d.start()

    def remote(src, dst, send, recv, where):
        return pltpu.make_async_remote_copy(
            src_ref=src, dst_ref=dst, send_sem=send, recv_sem=recv,
            device_id=where, device_id_type=MESH,
        )

    at = 0
    gain_at = []
    gains[me] = jnp.zeros_like(gains[me])
    for value in (ln1_own, ln2_own, qn_own, kn_own):
        size = value.shape[-1]
        gains[me, :, at : at + size] = value[...].astype(F32)
        gain_at.append((at, size))
        at += size
    pl.semaphore_wait(barrier, n + steps)

    def gain_copy(d):
        return remote(
            gains.at[me], gains.at[me], gain_send.at[d - 1], gain_recv.at[d - 1],
            {"fsdp": lax.rem(me + d, n)},
        )

    for d in range(1, n):
        gain_copy(d).start()

    def slabs(c, to):
        rows_in = pl.ds(pl.multiple_of(mine * share, share), share)
        if isinstance(c, int) and c == 0:
            return (
                (wq_h.at[rows_in, pl.ds(to * ch, ch)], pl.ds(0, ch)),
                (wk_h.at[rows_in, pl.ds(to * kcols, kcols)], pl.ds(ch, kcols)),
                (wv_h.at[rows_in, pl.ds(to * kcols, kcols)], pl.ds(ch + kcols, kcols)),
            )
        cols = pl.ds(pl.multiple_of(to * hidden + (c - 1) * ch, 128), ch)
        return (
            (wg_h.at[rows_in, cols], pl.ds(0, ch)),
            (wu_h.at[rows_in, cols], pl.ds(ch, ch)),
        )

    def slab_copies(c):
        for i, (src, lanes) in enumerate(slabs(c, me)):
            yield pltpu.make_async_copy(src, wall.at[c, me, mine, :, lanes], own_sem.at[c, i])
        for d in range(1, n):
            to = lax.rem(me + d, n)
            for i, (src, lanes) in enumerate(slabs(c, to)):
                yield remote(
                    src, wall.at[c, me, mine, :, lanes],
                    zw_send.at[c, d - 1, i], zw_recv.at[c, d - 1, i], {"fsdp": to},
                )

    def slab_gathers(c, j):
        for h, order in enumerate(orders):
            bits = order[::-1]
            partner = flip(mine, bits[j])
            for i in range(1 << j):
                piece = flips(mine, bits[:j], i)
                ref = wall.at[c, :, piece, :, pl.ds(h * ch, ch)]
                yield remote(
                    ref, ref, gw_send.at[j, c, h, i], gw_recv.at[j, c, h, i], {"replica": partner}
                )

    def prepare(t):
        for j in reversed(range(steps + 1)):
            c = t - (j + 1)

            def advance(c=c, j=j):
                for copy in slab_copies(c) if j == 0 else slab_gathers(c, j - 1):
                    copy.wait()
                if j < steps:
                    for copy in slab_gathers(c, j):
                        copy.start()

            if isinstance(t, int):
                if 0 <= c < chunks:
                    advance()
            elif j == 0:
                @pl.when(jnp.logical_and(c >= 1, c < chunks))
                def _():
                    advance()
            else:
                @pl.when(jnp.logical_and(c >= 0, c < chunks))
                def _():
                    advance()

        if isinstance(t, int):
            if t < chunks:
                for copy in slab_copies(t):
                    copy.start()
        else:
            @pl.when(t < chunks)
            def _():
                for copy in slab_copies(t):
                    copy.start()

    def spread(buf, c, d):
        return pltpu.make_async_remote_copy(
            src_ref=buf.at[me],
            dst_ref=buf.at[me],
            send_sem=ag_send.at[c, d - 1],
            recv_sem=ag_recv.at[c, d - 1],
            device_id={"fsdp": lax.rem(me + d, n)},
            device_id_type=MESH,
        )

    def partial_to(c, d):
        return pltpu.make_async_remote_copy(
            src_ref=sbuf.at[d],
            dst_ref=rbuf.at[c % 2, d - 1],
            send_sem=rs_send.at[c, d - 1],
            recv_sem=rs_recv.at[c, d - 1],
            device_id={"fsdp": lax.rem(me - d + n, n)},
            device_id_type=MESH,
        )

    def spread_start(buf, c):
        for d in range(1, n):
            spread(buf, c, d).start()

    def spread_done(buf, c):
        for d in range(1, n):
            spread(buf, c, d).wait_send()

    def each_block(buf, c, work):
        def step(d, carry):
            @pl.when(d > 0)
            def _():
                spread(buf, c, d).wait_recv()

            work(d, lax.rem(me - d + n, n))

            @pl.when(d > 0)
            def _():
                partial_to(c, d).start()

            return carry

        lax.fori_loop(0, n, step, 0)

    def gathered_sum(c):
        for d in range(1, n):
            partial_to(c, d).wait()
        total = sbuf[0].astype(F32)
        for d in range(1, n):
            total = total + rbuf[c % 2, d - 1].astype(F32)
        return total

    outs = []

    def put(src, dst):
        copy = pltpu.make_async_copy(src, dst, out_sem.at[len(outs)])
        copy.start()
        outs.append(copy)

    def swap(value):
        return pltpu.roll(value, hd // 2, 1)

    def hand(src, dst, to, k):
        return pltpu.make_async_remote_copy(
            src_ref=src,
            dst_ref=dst,
            send_sem=hand_send.at[k],
            recv_sem=hand_recv.at[k],
            device_id={"section": to},
            device_id_type=MESH,
        )

    ticks = chunks + steps + 1

    @pl.when(sec == 0)
    def _():
        prepare(0)

    for d in range(1, n):
        gain_copy(d).wait()
    for k, full in enumerate((ln1, ln2, qn, kn)):
        at, size = gain_at[k]
        for f in range(n):
            full[:, f * size : (f + 1) * size] = gains[f, :, at : at + size]

    @pl.when(sec == 1)
    def _():
        pl.semaphore_wait(turn, 1)
        for t in range(steps + 2):
            prepare(t)
        lax.fori_loop(steps + 2, ticks, lambda t, carry: prepare(t) or carry, 0)

    @pl.when(sec == 0)
    def _():
        xin[...] = tok[...]

    @pl.when(sec == 1)
    def _():
        hand(yv, xin, 0, 0).wait_recv()

    x32 = xin[...].astype(F32)
    r1 = lax.rsqrt(mean_last(x32 * x32) + EPS)
    xn_all[me] = (x32 * r1 * ln1[...]).astype(BF16)
    spread_start(xn_all, 0)

    @pl.when(sec == 0)
    def _():
        for t in range(1, steps + 2):
            prepare(t)

    load_o.wait()
    load_d.wait()

    def masked_scores(qh, kh):
        raw = nt(qh, kh) * scale
        at_row = lax.broadcasted_iota(jnp.int32, raw.shape, 0)
        at_col = lax.broadcasted_iota(jnp.int32, raw.shape, 1)
        raw = jnp.where(at_row >= at_col, raw, -jnp.inf)
        top = jnp.max(raw, axis=-1, keepdims=True)
        lse = top + jnp.log(jnp.sum(jnp.exp(raw - top), axis=-1, keepdims=True))
        return jnp.exp(raw - lse)

    def attend(d, s):
        @pl.when(sec == 0)
        def _():
            prepare(steps + 2 + d)

            @pl.when(d == 0)
            def _():
                pl.semaphore_signal(
                    turn, inc=1, device_id={"section": 1}, device_id_type=MESH
                )

        a = xn_all[s]
        for at, size in tiles(2 * ch):
            w = wall[0, :, :, :, at : at + size].reshape(width, size)
            qkv[s, :, at : at + size] = nn(a, w)
        for at in range(0, qcols + kcols, hd):
            field = qkv[s, :, at : at + hd]
            gain = qn[...] if at < qcols else kn[...]
            factor = lax.rsqrt(mean_last(field * field) + EPS)
            normed = field * factor * gain
            turned = normed * cosine[...] + swap(normed) * sine[...]
            qkvb[s, :, at : at + hd] = turned.astype(BF16)
        qkvb[s, :, qcols + kcols :] = qkv[s, :, qcols + kcols :].astype(BF16)
        for j in range(qcols // hd):
            kv = j * kcols // qcols
            kat = qcols + kv * hd
            vat = qcols + kcols + kv * hd
            probs = masked_scores(qkvb[s, :, j * hd : (j + 1) * hd], qkvb[s, :, kat : kat + hd])
            attended = nn(probs.astype(BF16), qkvb[s, :, vat : vat + hd])
            att[s, :, j * hd : (j + 1) * hd] = attended.astype(BF16)
        a = att[s]
        for at, size in tiles(width):
            sbuf[d, :, at : at + size] = nn(a, wo[:, at : at + size]).astype(BF16)

    each_block(xn_all, 0, attend)
    h = x32 + gathered_sum(0)
    hres[...] = h
    r2 = lax.rsqrt(mean_last(h * h) + EPS)
    hn_all[me] = (h * r2 * ln2[...]).astype(BF16)
    spread_start(hn_all, 1)
    put(xn_all, xn_h)
    put(att, att_h)

    @pl.when(sec == 0)
    def _():
        lax.fori_loop(steps + 2 + n, ticks, lambda t, carry: prepare(t) or carry, 0)

    def feed(d, s):
        a = hn_all[s]
        for at in range(0, hidden, ch):
            size, j = ch, 1 + at // ch
            g = nn(a, wall[j, :, :, :, :ch].reshape(width, ch))
            u = nn(a, wall[j, :, :, :, ch:].reshape(width, ch))
            gate[s, :, at : at + size] = g
            up[s, :, at : at + size] = u
            act[s, :, at : at + size] = (g * jax.nn.sigmoid(g) * u).astype(BF16)
        a = act[s]
        for at, size in tiles(width):
            sbuf[d, :, at : at + size] = nn(a, wd[:, at : at + size]).astype(BF16)

    each_block(hn_all, 1, feed)
    yv[...] = (hres[...] + gathered_sum(1)).astype(BF16)

    @pl.when(sec == 0)
    def _():
        hand(yv, xin, 1, 0).start()

    put(yv, y_h)
    put(hn_all, hn_h)
    put(act, act_h)

    @pl.when(sec == 0)
    def _():
        hand(yv, dyin, 1, 1).wait_recv()

    @pl.when(sec == 1)
    def _():
        dyin[...] = cot[...]

    dy_all[me] = dyin[...]
    spread_start(dy_all, 2)

    def feed_back(d, s):
        a = dy_all[s]
        for at in range(0, hidden, ch):
            size = ch
            dact = nt(a, wd[at : at + size, :])
            g = gate[s, :, at : at + size]
            u = up[s, :, at : at + size]
            sig = jax.nn.sigmoid(g)
            dgu[s, :, 2 * at : 2 * at + ch] = (dact * u * sig * (1.0 + g * (1.0 - sig))).astype(BF16)
            dgu[s, :, 2 * at + ch : 2 * at + 2 * ch] = (dact * g * sig).astype(BF16)
        a = dgu[s]
        for f in range(n):
            total = jnp.zeros((rows, kfold), F32)
            for j in range(1, chunks):
                w = wall[j, f].reshape(kfold, 2 * ch)
                total = total + nt(a[:, 2 * (j - 1) * ch : 2 * j * ch], w)
            sbuf[d, :, f * kfold : (f + 1) * kfold] = total.astype(BF16)

    each_block(dy_all, 2, feed_back)
    dhn = gathered_sum(2)
    h = hres[...]
    r2 = lax.rsqrt(mean_last(h * h) + EPS)
    u = dhn * ln2[...]
    dh = dyin[...].astype(F32) + (r2 * u - h * r2 * r2 * r2 * mean_last(u * h))
    dln2[...] = jnp.sum(dhn * h * r2, axis=0, keepdims=True)
    dres[...] = dh
    dab_all[me] = dh.astype(BF16)
    spread_start(dab_all, 3)
    put(dy_all, dy_h)
    put(dgu, dgu_h)

    dqn[...] = jnp.zeros_like(dqn)
    dkn[...] = jnp.zeros_like(dkn)

    def head_back(s, at, grad, gain, dgain):
        field = qkv[s, :, at : at + hd]
        factor = lax.rsqrt(mean_last(field * field) + EPS)
        grad = grad * cosine[...] - swap(grad) * sine[...]
        v = grad * gain
        back = factor * v - field * factor * factor * factor * mean_last(v * field)
        dgain[...] += jnp.sum(grad * field * factor, axis=0, keepdims=True)
        dqkv[s, :, at : at + hd] = back.astype(BF16)

    def attend_back(d, s):
        a = dab_all[s]
        for at, size in tiles(qcols):
            dout = nt(a, wo[at : at + size, :]).astype(BF16)
            for kv in range(at * kcols // (qcols * hd), (at + size) * kcols // (qcols * hd)):
                kat = qcols + kv * hd
                vat = qcols + kcols + kv * hd
                kh = qkvb[s, :, kat : kat + hd]
                vh = qkvb[s, :, vat : vat + hd]
                dk = jnp.zeros((rows, hd), F32)
                dv = jnp.zeros((rows, hd), F32)
                for j in range(kv * qcols // kcols, (kv + 1) * qcols // kcols):
                    qh = qkvb[s, :, j * hd : (j + 1) * hd]
                    dh_out = dout[:, j * hd - at : (j + 1) * hd - at]
                    probs = masked_scores(qh, kh)
                    dv = dv + tn(probs.astype(BF16), dh_out)
                    dp = nt(dh_out, vh)
                    delta = jnp.sum(probs * dp, axis=-1, keepdims=True)
                    ds = (probs * (dp - delta) * scale).astype(BF16)
                    dk = dk + tn(ds, qh)
                    head_back(s, j * hd, nn(ds, kh), qn[...], dqn)
                head_back(s, kat, dk, kn[...], dkn)
                dqkv[s, :, vat : vat + hd] = dv.astype(BF16)
        a = dqkv[s]
        for f in range(n):
            w = wall[0, f].reshape(kfold, 2 * ch)
            sbuf[d, :, f * kfold : (f + 1) * kfold] = nt(a, w).astype(BF16)

    each_block(dab_all, 3, attend_back)
    dxn = gathered_sum(3)
    x32 = xin[...].astype(F32)
    r1 = lax.rsqrt(mean_last(x32 * x32) + EPS)
    u = dxn * ln1[...]
    dx = dres[...] + (r1 * u - x32 * r1 * r1 * r1 * mean_last(u * x32))
    dln1[...] = jnp.sum(dxn * x32 * r1, axis=0, keepdims=True)
    outs[2].wait()

    @pl.when(sec == 0)
    def _():
        hand(yv, xin, 1, 0).wait_send()

    yv[...] = dx.astype(BF16)

    @pl.when(sec == 1)
    def _():
        hand(yv, dyin, 0, 1).start()

    dres[...] = dx
    put(dres, dx_h)
    put(dab_all, dab_h)
    put(dqkv, dqkv_h)
    for c, buf in enumerate((xn_all, hn_all, dy_all, dab_all)):
        spread_done(buf, c)

    @pl.when(sec == 1)
    def _():
        hand(yv, dyin, 0, 1).wait_send()

    for k, copy in enumerate(outs):
        if k != 2:
            copy.wait()


def run_layer(n, rep, tok, cot, ln1, ln2, qn, kn, wq, wk, wv, wg, wu, wo, wd):
    rows, width = tok.shape
    hd = n * qn.shape[-1]
    qcols = wo.shape[0]
    qkvcols = 2 * qcols
    steps = rep.bit_length() - 1
    chunks = 1 + wd.shape[0] // qcols
    lanes = -(-2 * (ln1.shape[-1] + qn.shape[-1]) // 128) * 128
    hidden = wd.shape[0]
    cosine, sine = rope_tables(rows, hd // 2)
    vm = pl.BlockSpec(memory_space=pltpu.VMEM)
    hbm = pl.BlockSpec(memory_space=pltpu.HBM)

    def wide(columns, kind):
        return (n, rows, columns), kind

    shaped = [
        ((rows, width), BF16),
        ((rows, width), F32),
        wide(width, BF16), wide(width, BF16), wide(width, BF16), wide(width, BF16),
        wide(qcols, BF16), wide(hidden, BF16), wide(2 * hidden, BF16), wide(qkvcols, BF16),
        ((1, width), F32), ((1, width), F32), ((1, hd), F32), ((1, hd), F32),
    ]
    scratch = [
        pltpu.VMEM((chunks, n, rep, width // (n * rep), qkvcols), BF16),
        pltpu.VMEM(wo.shape, BF16),
        pltpu.VMEM(wd.shape, BF16),
        pltpu.VMEM((1, width), F32),
        pltpu.VMEM((1, width), F32),
        pltpu.VMEM((1, hd), F32),
        pltpu.VMEM((1, hd), F32),
        pltpu.VMEM((n, 1, lanes), F32),
        pltpu.VMEM((rows, width), BF16),
        pltpu.VMEM((rows, width), BF16),
        *[pltpu.VMEM(*wide(width, BF16)) for _ in range(4)],
        pltpu.VMEM(*wide(qkvcols, F32)),
        pltpu.VMEM(*wide(qkvcols, BF16)),
        pltpu.VMEM(*wide(qcols, BF16)),
        pltpu.VMEM((rows, width), F32),
        pltpu.VMEM(*wide(hidden, F32)),
        pltpu.VMEM(*wide(hidden, F32)),
        pltpu.VMEM(*wide(hidden, BF16)),
        pltpu.VMEM(*wide(2 * hidden, BF16)),
        pltpu.VMEM(*wide(qkvcols, BF16)),
        pltpu.VMEM((rows, width), F32),
        pltpu.VMEM((rows, width), BF16),
        pltpu.VMEM((n, rows, width), BF16),
        pltpu.VMEM((2, n - 1, rows, width), BF16),
        pltpu.SemaphoreType.DMA((2,)),
        pltpu.SemaphoreType.DMA((chunks, n - 1, 3)),
        pltpu.SemaphoreType.DMA((chunks, n - 1, 3)),
        pltpu.SemaphoreType.DMA((steps, chunks, 2, rep // 2)),
        pltpu.SemaphoreType.DMA((steps, chunks, 2, rep // 2)),
        pltpu.SemaphoreType.DMA((chunks, 3)),
        pltpu.SemaphoreType.DMA((n - 1,)),
        pltpu.SemaphoreType.DMA((n - 1,)),
        pltpu.SemaphoreType.REGULAR,
        pltpu.SemaphoreType.DMA((10,)),
        pltpu.SemaphoreType.DMA((4, n - 1)),
        pltpu.SemaphoreType.DMA((4, n - 1)),
        pltpu.SemaphoreType.DMA((4, n - 1)),
        pltpu.SemaphoreType.DMA((4, n - 1)),
        pltpu.SemaphoreType.DMA((2,)),
        pltpu.SemaphoreType.DMA((2,)),
    ]
    return pl.pallas_call(
        functools.partial(layer_kernel, n, rep, hd),
        out_shape=[jax.ShapeDtypeStruct(shape, kind) for shape, kind in shaped],
        in_specs=[vm] * 8 + [hbm] * 7,
        out_specs=[hbm] * 10 + [vm] * 4,
        scratch_shapes=scratch,
        compiler_params=pltpu.CompilerParams(
            collective_id=0, has_side_effects=True, vmem_limit_bytes=67043328
        ),
        name="layer",
    )(tok, cot, ln1, ln2, qn, kn, cosine, sine, wq, wk, wv, wg, wu, wo, wd)


def grad_plan(n, qcols, hidden, width):
    fold = width // n
    blocks = fold // 128
    thirds = hidden // qcols
    return blocks, thirds, (blocks * thirds, blocks, hidden // 256, qcols // 256)


def grad_kernel(
    n, rep,
    xn_h, hn_h, dy_h, dab_h, att_h, act_h, dgu_h, dqkv_h, dln1, dln2, dqn, dkn,
    gq_h, gk_h, gv_h, go_h, gg_h, gu_h, gd_h, sums,
    xn, hn, dy, dab, att, act, dgu, dqkv, mine_g, reduced, whole, pack, pack_z, pack_r, pack_in, *rest,
):
    steps = rep.bit_length() - 1
    got = rest[:steps]
    (
        in_sem, rs_send, rs_recv, z_send, z_recv, ag_send, ag_recv, out_sem,
        pz_send, pz_recv, pr_send, pr_recv,
    ) = rest[steps:]
    me = lax.axis_index("fsdp")
    mine = lax.axis_index("replica")
    ch = mine_g.shape[-1]
    part = 128 // n
    width = xn.shape[-1]
    fold = width // n
    hidden = act.shape[-1]
    kcols = gk_h.shape[-1] // n
    blocks, thirds, counts = grad_plan(n, ch, hidden, width)
    starts = [sum(counts[:k]) for k in range(len(counts) + 1)]
    total = starts[-1]
    columns_end = starts[2]
    g_slots, slots = mine_g.shape[0], whole.shape[0]
    orders = (tuple(range(steps)), tuple(reversed(range(steps))))

    barrier = pltpu.get_barrier_semaphore()
    for d in range(1, n):
        pl.semaphore_signal(
            barrier, inc=1, device_id={"fsdp": lax.rem(me + d, n)}, device_id_type=MESH
        )
    for bit in range(steps):
        pl.semaphore_signal(
            barrier, inc=1, device_id={"replica": flip(mine, bit)}, device_id_type=MESH
        )
    loads = []
    for k, (src, dst) in enumerate(
        ((hn_h, hn), (dgu_h, dgu), (xn_h, xn), (dqkv_h, dqkv), (act_h, act), (dy_h, dy), (att_h, att), (dab_h, dab))
    ):
        loads.append(pltpu.make_async_copy(src, dst, in_sem.at[k]))
        loads[-1].start()
    pack[...] = jnp.zeros_like(pack)
    at = 0
    for value in (dln1, dln2, dqn, dkn):
        size = value.shape[-1] // n
        for f in range(n):
            pack[f, :, at : at + size] = value[:, f * size : (f + 1) * size]
        at += size
    pl.semaphore_wait(barrier, n - 1 + steps)
    for load in loads:
        load.wait()

    def remote(src, dst, send, recv, where):
        return pltpu.make_async_remote_copy(
            src_ref=src, dst_ref=dst, send_sem=send, recv_sem=recv,
            device_id=where, device_id_type=MESH,
        )

    def scatter_copies(c, j):
        slot, two = lax.rem(c, g_slots), lax.rem(c, 2)
        for h, bits in enumerate(orders):
            partner = flip(mine, bits[j])
            for i in range(rep >> (j + 1)):
                piece = flips(partner, bits[j + 1 :], i)
                yield h, i, remote(
                    mine_g.at[slot, h, piece], got[j].at[two, h, i],
                    rs_send.at[j, two, h, i], rs_recv.at[j, two, h, i], {"replica": partner},
                )

    def across_copies(c):
        slot, two = lax.rem(c, slots), lax.rem(c, 2)
        for d in range(1, n):
            to = lax.rem(me + d, n)
            yield remote(
                reduced.at[:, pl.ds(to * part, part), :],
                whole.at[slot, :, mine, pl.ds(me * part, part), :],
                z_send.at[two, d - 1], z_recv.at[two, d - 1], {"fsdp": to},
            )

    def gather_copies(c, j):
        slot, two = lax.rem(c, slots), lax.rem(c, 2)
        for h, order in enumerate(orders):
            bits = order[::-1]
            partner = flip(mine, bits[j])
            for i in range(1 << j):
                piece = flips(mine, bits[:j], i)
                yield remote(
                    whole.at[slot, h, piece], whole.at[slot, h, piece],
                    ag_send.at[j, two, h, i], ag_recv.at[j, two, h, i], {"replica": partner},
                )

    def pack_across(d):
        to = lax.rem(me + d, n)
        return remote(
            pack.at[to], pack_z.at[d - 1], pz_send.at[d - 1], pz_recv.at[d - 1], {"fsdp": to}
        )

    def pack_swap(j):
        return remote(
            pack_r.at[j], pack_in.at[j], pr_send.at[j], pr_recv.at[j], {"replica": flip(mine, j)}
        )

    for d in range(1, n):
        pack_across(d).start()

    def pack_tick(t):
        for j in range(steps + 1):
            @pl.when(t == 2 * j + 2)
            def _():
                if j == 0:
                    value = pack[me]
                    for d in range(1, n):
                        pack_across(d).wait()
                        value = value + pack_z[d - 1]
                else:
                    pack_swap(j - 1).wait()
                    value = pack_r[j - 1] + pack_in[j - 1]
                if j < steps:
                    pack_r[j] = value
                    pack_swap(j).start()
                else:
                    sums[...] = value

    def aligned(at):
        return pl.multiple_of(at, 128)

    def out_copies(c, kind):
        slot, two = lax.rem(c, slots), lax.rem(c, 2)
        at = c - starts[kind]
        for f in range(n):
            rows = slice(f * part, (f + 1) * part)
            if kind == 0:
                k, j = at // thirds, lax.rem(at, thirds)
                cols = pl.ds(aligned(f * hidden + j * ch), ch)
                pairs = [
                    (whole.at[slot, h, :, rows, :], dst.at[k, :, :, cols])
                    for h, dst in enumerate((gg_h, gu_h))
                ]
            elif kind == 1:
                cols = pl.ds(f * kcols, kcols)
                pairs = [
                    (whole.at[slot, 0, :, rows, :], gq_h.at[at, :, :, pl.ds(f * ch, ch)]),
                    (whole.at[slot, 1, :, rows, pl.ds(0, kcols)], gk_h.at[at, :, :, cols]),
                    (whole.at[slot, 1, :, rows, pl.ds(kcols, kcols)], gv_h.at[at, :, :, cols]),
                ]
            else:
                dst = gd_h if kind == 2 else go_h
                pairs = [
                    (
                        whole.at[slot, h, f],
                        dst.at[pl.ds(aligned(at * 256 + h * 128), 128), pl.ds(f * ch, ch)],
                    )
                    for h in range(2)
                ]
            for i, (src, to) in enumerate(pairs):
                yield pltpu.make_async_copy(src, to, out_sem.at[two, f, i])

    def compute(c, kind):
        slot = lax.rem(c, g_slots)
        at = c - starts[kind]
        if kind < 2:
            left, right = (hn, dgu) if kind == 0 else (xn, dqkv)
            k, j = (at // thirds, lax.rem(at, thirds)) if kind == 0 else (at, 0)
            lefts = jnp.concatenate(
                [left[:, pl.ds(aligned(f * fold + k * 128), 128)] for f in range(n)], axis=1
            )
            for h in range(2):
                product = tn(lefts, right[:, pl.ds(aligned((2 * j + h) * ch), ch)]).astype(BF16)
                for f in range(n):
                    block = product[f * 128 : (f + 1) * 128].reshape(rep, 128 // rep, ch)
                    mine_g[slot, h, :, f * part : (f + 1) * part, :] = block
        else:
            left, right = (act, dy) if kind == 2 else (att, dab)
            for q in range(rep):
                cols = left[:, pl.ds(aligned(at * 256), 256)]
                product = tn(cols, right[:, q * ch : (q + 1) * ch]).astype(BF16)
                for h in range(2):
                    mine_g[slot, h, q] = product[h * 128 : (h + 1) * 128]

    def within(c, low, high):
        return jnp.logical_and(c >= low, c < high)

    def tick(t, carry):
        c = t - (2 * steps + 2)
        for kind in range(4):
            @pl.when(within(c, starts[kind], starts[kind + 1]))
            def _():
                for copy in out_copies(c, kind):
                    copy.wait()

        c_out = t - (2 * steps + 1)

        @pl.when(within(c_out, 0, total))
        def _():
            for copy in gather_copies(c_out, steps - 1):
                copy.wait()

        for kind in range(4):
            @pl.when(within(c_out, starts[kind], starts[kind + 1]))
            def _():
                for copy in out_copies(c_out, kind):
                    copy.start()

        for j in reversed(range(1, steps)):
            c_ag = t - (steps + 1 + j)

            @pl.when(within(c_ag, 0, total))
            def _():
                for copy in gather_copies(c_ag, j - 1):
                    copy.wait()
                for copy in gather_copies(c_ag, j):
                    copy.start()

        c_z = t - (steps + 1)

        @pl.when(within(c_z, 0, columns_end))
        def _():
            for copy in across_copies(c_z):
                copy.wait()

        @pl.when(within(c_z, 0, total))
        def _():
            for copy in gather_copies(c_z, 0):
                copy.start()

        for j in reversed(range(steps)):
            c_rs = t - (j + 1)
            slot, two = lax.rem(c_rs, g_slots), lax.rem(c_rs, 2)

            @pl.when(within(c_rs, 0, total))
            def _():
                for h, i, copy in scatter_copies(c_rs, j):
                    copy.wait()
                for h, bits in enumerate(orders):
                    for i in range(rep >> (j + 1)):
                        piece = flips(mine, bits[j + 1 :], i)
                        value = mine_g[slot, h, piece].astype(F32) + got[j][two, h, i].astype(F32)
                        if j < steps - 1:
                            mine_g[slot, h, piece] = value.astype(BF16)
                        else:
                            reduced[h] = value.astype(BF16)
                if j < steps - 1:
                    for h, i, copy in scatter_copies(c_rs, j + 1):
                        copy.start()

            if j == steps - 1:
                at = lax.rem(c_rs, slots)

                @pl.when(within(c_rs, 0, columns_end))
                def _():
                    for copy in across_copies(c_rs):
                        copy.start()
                    rows = pl.ds(pl.multiple_of(me * part, part), part)
                    whole[at, :, mine, rows, :] = reduced[:, rows, :]

                @pl.when(within(c_rs, columns_end, total))
                def _():
                    whole[at, :, mine] = reduced[...]

        for kind in range(4):
            @pl.when(within(t, starts[kind], starts[kind + 1]))
            def _():
                compute(t, kind)

        @pl.when(t < total)
        def _():
            for h, i, copy in scatter_copies(t, 0):
                copy.start()

        pack_tick(t)
        return carry

    lax.fori_loop(0, total + 2 * steps + 3, tick, 0)


def run_grads(n, rep, xn, hn, dy, dab, att, act, dgu, dqkv, small):
    tokens, width = xn.shape
    ch = att.shape[-1]
    hidden = act.shape[-1]
    kcols = (dqkv.shape[-1] - ch) // 2
    fold = width // n
    steps = rep.bit_length() - 1
    hbm = pl.BlockSpec(memory_space=pltpu.HBM)

    def owned(columns):
        return jax.ShapeDtypeStruct((fold // 128, rep, 128 // rep, columns * n), BF16)

    shaped = [
        owned(ch), owned(kcols), owned(kcols), jax.ShapeDtypeStruct((ch, width), BF16),
        owned(hidden), owned(hidden), jax.ShapeDtypeStruct((hidden, width), BF16),
    ]
    lanes = -(-sum(value.shape[-1] for value in small) // (128 * n)) * 128
    vm = pl.BlockSpec(memory_space=pltpu.VMEM)
    operands = (xn, hn, dy, dab, att, act, dgu, dqkv)
    scratch = [pltpu.VMEM(value.shape, BF16) for value in operands] + [
        pltpu.VMEM((steps + 1, 2, rep, 128, ch), BF16),
        pltpu.VMEM((2, 128, ch), BF16),
        pltpu.VMEM((steps + 3, 2, rep, 128, ch), BF16),
        pltpu.VMEM((n, 1, lanes), F32),
        pltpu.VMEM((n - 1, 1, lanes), F32),
        pltpu.VMEM((steps, 1, lanes), F32),
        pltpu.VMEM((steps, 1, lanes), F32),
        *[pltpu.VMEM((2, 2, rep >> (j + 1), 128, ch), BF16) for j in range(steps)],
        pltpu.SemaphoreType.DMA((len(operands),)),
        pltpu.SemaphoreType.DMA((steps, 2, 2, rep // 2)),
        pltpu.SemaphoreType.DMA((steps, 2, 2, rep // 2)),
        pltpu.SemaphoreType.DMA((2, n - 1)),
        pltpu.SemaphoreType.DMA((2, n - 1)),
        pltpu.SemaphoreType.DMA((steps, 2, 2, rep // 2)),
        pltpu.SemaphoreType.DMA((steps, 2, 2, rep // 2)),
        pltpu.SemaphoreType.DMA((2, n, 3)),
        pltpu.SemaphoreType.DMA((n - 1,)),
        pltpu.SemaphoreType.DMA((n - 1,)),
        pltpu.SemaphoreType.DMA((steps,)),
        pltpu.SemaphoreType.DMA((steps,)),
    ]
    *results, sums = pl.pallas_call(
        functools.partial(grad_kernel, n, rep),
        out_shape=shaped + [jax.ShapeDtypeStruct((1, lanes), F32)],
        in_specs=[hbm] * len(operands) + [vm] * len(small),
        out_specs=[hbm] * len(shaped) + [vm],
        scratch_shapes=scratch,
        compiler_params=pltpu.CompilerParams(
            collective_id=1, has_side_effects=True, vmem_limit_bytes=67043328
        ),
        name="grads",
    )(*operands, *small)
    return [value.reshape(-1, value.shape[-1]).astype(F32) for value in results], sums


def per_device(tokens_in, cotangent, ln1, wq, wk, wv, qn, kn, wo, ln2, wg, wu, wd):
    n, rep = lax.axis_size("fsdp"), lax.axis_size("replica")

    (
        y, dx, xn, hn, dy, dab, att, act, dgu, dqkv, *small,
    ) = run_layer(
        n, rep, tokens_in, cotangent, ln1, ln2, qn, kn,
        wq[0], wk[0], wv[0], wg[0], wu[0], wo[0], wd[0],
    )

    def flat(value):
        return value.reshape(-1, value.shape[-1])

    xn, hn, dy, dab, att, act, dgu, dqkv = map(flat, (xn, hn, dy, dab, att, act, dgu, dqkv))

    grads, sums = run_grads(n, rep, xn, hn, dy, dab, att, act, dgu, dqkv, small)
    g_wq, g_wk, g_wv, g_wo, g_wg, g_wu, g_wd = grads
    owned, at = [], 0
    for gain in (ln1, ln2, qn, kn):
        owned.append(sums[0, at : at + gain.shape[1]])
        at += gain.shape[1]
    g_ln1, g_ln2, g_qn, g_kn = owned
    results = (y, dx, g_ln1, g_wq, g_wk, g_wv, g_qn, g_kn, g_wo, g_ln2, g_wg, g_wu, g_wd)
    return tuple(value[None] for value in results)


def solution(mesh):
    rows = P("section", "fsdp", None)
    gain = P("section", "fsdp")
    tokens = P(("fsdp", "replica"), None)
    stacked = P("section", ("fsdp", "replica"), None)
    weights = (gain, rows, rows, rows, gain, gain, rows, gain, rows, rows, rows)
    return jax.shard_map(
        per_device,
        mesh=mesh,
        in_specs=(tokens, tokens, *weights),
        out_specs=(stacked, stacked, *weights),
        check_vma=False,
    )
```

```python
import functools
import math

import jax
import jax.numpy as jnp
from jax import lax
from jax.experimental import pallas as pl
from jax.experimental.pallas import tpu as pltpu
from jax.sharding import PartitionSpec as P

LEN = 128
EPS = 1e-06
F32 = jnp.float32
BF16 = jnp.bfloat16
MESH = pl.DeviceIdType.MESH
TILE = 512


def rope_tables(length, half_dim):
    freq = jnp.exp(jnp.arange(half_dim, dtype=F32) * (-math.log(1000000.0) / half_dim))
    angle = jnp.arange(length, dtype=F32)[:, None] * freq[None, :]
    cosine, sine = jnp.cos(angle), jnp.sin(angle)
    return (
        jnp.concatenate([cosine, cosine], axis=1),
        jnp.concatenate([-sine, sine], axis=1),
    )


def nn(left, right):
    return jnp.dot(left, right, preferred_element_type=F32)


def nt(left, right):
    return lax.dot_general(left, right, (((1,), (1,)), ((), ())), preferred_element_type=F32)


def tn(left, right):
    return lax.dot_general(left, right, (((0,), (0,)), ((), ())), preferred_element_type=F32)


def mean_last(value):
    return jnp.mean(value, axis=-1, keepdims=True)


def tiles(total):
    return [(at, min(TILE, total - at)) for at in range(0, total, TILE)]


def flip(value, bit):
    return value + (1 - 2 * (value // 2**bit % 2)) * 2**bit


def flips(value, bits, subset):
    for at, bit in enumerate(bits):
        if subset >> at & 1:
            value = flip(value, bit)
    return value


def layer_kernel(
    n,
    rep,
    hd,
    tok, cot, ln1_own, ln2_own, qn_own, kn_own, cosine, sine, wq_h, wk_h, wv_h, wg_h, wu_h, wo_h, wd_h,
    y_h, dx_h, xn_h, hn_h, dy_h, dab_h, att_h, act_h, dgu_h, dqkv_h, dln1, dln2, dqn, dkn,
    wall, wo, wd, ln1, ln2, qn, kn, gains,
    xin, xn_all, hn_all, dy_all, qkv, qkvb, att, hres, gate, up, act, dgu, dqkv,
    yv, sbuf, rbuf,
    w_sem, zw_send, zw_recv, gw_send, gw_recv, own_sem, gain_send, gain_recv, turn,
    out_sem, ag_send, ag_recv, rs_send, rs_recv, hand_send, hand_recv,
):
    sec = lax.axis_index("section")
    me = lax.axis_index("fsdp")
    mine = lax.axis_index("replica")
    steps = rep.bit_length() - 1
    rows, width = tok.shape
    ch = att.shape[-1]
    qcols = ch
    kcols = (qkvb.shape[-1] - qcols) // 2
    hidden = act.shape[-1]
    chunks = wall.shape[0]
    share = wall.shape[3]
    kfold = rep * share
    scale = 1.0 / math.sqrt(hd)
    orders = (tuple(range(steps)), tuple(reversed(range(steps))))

    barrier = pltpu.get_barrier_semaphore()
    for d in range(1, n):
        pl.semaphore_signal(
            barrier, inc=1, device_id={"fsdp": lax.rem(me + d, n)}, device_id_type=MESH
        )
    for bit in range(steps):
        pl.semaphore_signal(
            barrier, inc=1, device_id={"replica": flip(mine, bit)}, device_id_type=MESH
        )
    pl.semaphore_signal(barrier, inc=1, device_id={"section": 1 - sec}, device_id_type=MESH)
    load_o = pltpu.make_async_copy(wo_h, wo, w_sem.at[0])
    load_d = pltpu.make_async_copy(wd_h, wd, w_sem.at[1])
    load_x = pltpu.make_async_copy(tok, xin, w_sem.at[2])
    load_y = pltpu.make_async_copy(cot, dy_all.at[me], w_sem.at[3])

    @pl.when(sec == 0)
    def _():
        load_x.start()

    @pl.when(sec == 1)
    def _():
        load_y.start()

    load_o.start()
    load_d.start()

    def remote(src, dst, send, recv, where):
        return pltpu.make_async_remote_copy(
            src_ref=src, dst_ref=dst, send_sem=send, recv_sem=recv,
            device_id=where, device_id_type=MESH,
        )

    at = 0
    gain_at = []
    gains[me] = jnp.zeros_like(gains[me])
    for value in (ln1_own, ln2_own, qn_own, kn_own):
        size = value.shape[-1]
        gains[me, :, at : at + size] = value[...].astype(F32)
        gain_at.append((at, size))
        at += size
    pl.semaphore_wait(barrier, n + steps)

    def gain_copy(d):
        return remote(
            gains.at[me], gains.at[me], gain_send.at[d - 1], gain_recv.at[d - 1],
            {"fsdp": lax.rem(me + d, n)},
        )

    for d in range(1, n):
        gain_copy(d).start()

    def slabs(c, to):
        rows_in = pl.ds(pl.multiple_of(mine * share, share), share)
        if isinstance(c, int) and c == 0:
            return (
                (wq_h.at[rows_in, pl.ds(to * ch, ch)], pl.ds(0, ch)),
                (wk_h.at[rows_in, pl.ds(to * kcols, kcols)], pl.ds(ch, kcols)),
                (wv_h.at[rows_in, pl.ds(to * kcols, kcols)], pl.ds(ch + kcols, kcols)),
            )
        cols = pl.ds(pl.multiple_of(to * hidden + (c - 1) * ch, 128), ch)
        return (
            (wg_h.at[rows_in, cols], pl.ds(0, ch)),
            (wu_h.at[rows_in, cols], pl.ds(ch, ch)),
        )

    def slab_copies(c):
        for i, (src, lanes) in enumerate(slabs(c, me)):
            yield pltpu.make_async_copy(src, wall.at[c, me, mine, :, lanes], own_sem.at[c, i])
        for d in range(1, n):
            to = lax.rem(me + d, n)
            for i, (src, lanes) in enumerate(slabs(c, to)):
                yield remote(
                    src, wall.at[c, me, mine, :, lanes],
                    zw_send.at[c, d - 1, i], zw_recv.at[c, d - 1, i], {"fsdp": to},
                )

    def slab_gathers(c, j):
        for h, order in enumerate(orders):
            bits = order[::-1]
            partner = flip(mine, bits[j])
            for i in range(1 << j):
                piece = flips(mine, bits[:j], i)
                ref = wall.at[c, :, piece, :, pl.ds(h * ch, ch)]
                yield remote(
                    ref, ref, gw_send.at[j, c, h, i], gw_recv.at[j, c, h, i], {"replica": partner}
                )

    def prepare(c, j):
        for copy in slab_copies(c) if j == 0 else slab_gathers(c, j - 1):
            copy.wait()
        if j < steps:
            for copy in slab_gathers(c, j):
                copy.start()

    def prepare_rest(t):
        for j in reversed(range(steps + 1)):
            c = t - j + 1

            @pl.when(jnp.logical_and(c >= 1, c < chunks))
            def _():
                prepare(c, j)

    bits = n.bit_length() - 1
    piece = width // n

    def low(m):
        return (m & -m).bit_length() - 1

    def across(s):
        return sum((me // 2**j + s // 2**j) % 2 * 2**j for j in range(bits))

    def spread(buf, c, m, j):
        ref = buf.at[flips(me, range(bits), m)]
        return remote(
            ref, ref, ag_send.at[c, m + 2**j], ag_recv.at[c, m + 2**j], {"fsdp": flip(me, j)}
        )

    def spread_start(buf, c):
        for j in range(bits):
            spread(buf, c, 0, j).start()

    def spread_done(buf, c):
        for m in range(n):
            for j in range(bits if m == 0 else low(m)):
                spread(buf, c, m, j).wait_send()

    def fold(c, m, k, j):
        cols = pl.ds(k * piece, piece)
        return remote(
            sbuf.at[c % 2, m, :, cols], rbuf.at[c % 2, m - 1, :, cols],
            rs_send.at[c, m, k], rs_recv.at[c, m, k], {"fsdp": flip(me, j)},
        )

    def each_block(buf, c, work):
        def step(s, carry):
            slot = across(s)

            @pl.when(s > 0)
            def _():
                ref = buf.at[slot]
                remote(
                    ref, ref, ag_send.at[c, s], ag_recv.at[c, s], {"fsdp": flip(me, 0)}
                ).wait_recv()

            for m in range(2, n, 2):
                @pl.when(s == m)
                def _():
                    for j in range(low(m)):
                        spread(buf, c, m, j).start()

            def ship(k, value):
                sbuf[c % 2, s, :, k * piece : (k + 1) * piece] = value.astype(BF16)

                @pl.when(s % 2 == 1)
                def _():
                    fold(c, s, k, 0).start()

            work(s, slot, ship)
            return carry

        lax.fori_loop(0, n, step, 0)

    def settle(c):
        own, heard = sbuf.at[c % 2], rbuf.at[c % 2]
        for m in sorted(range(2, n, 2), key=low):
            for k in range(n):
                cols = slice(k * piece, (k + 1) * piece)
                value = own[m, :, cols].astype(F32)
                for j in range(low(m)):
                    fold(c, m + 2**j, k, j).wait_recv()
                    value = value + heard[m + 2**j - 1, :, cols].astype(F32)
                own[m, :, cols] = value.astype(BF16)
                fold(c, m, k, low(m)).start()
        for j in range(bits):
            for k in range(n):
                fold(c, 2**j, k, j).wait_recv()
        for m in range(1, n):
            for k in range(n):
                fold(c, m, k, low(m)).wait_send()

    def summed(c, at):
        total = sbuf[c % 2, 0, at].astype(F32)
        for j in range(bits):
            total = total + rbuf[c % 2, 2**j - 1, at].astype(F32)
        return total

    def by_rows(work):
        height = 32

        def step(i, carry):
            work(pl.ds(pl.multiple_of(i * height, height), height))
            return carry

        lax.fori_loop(0, rows // height, step, 0)

    outs = []

    def put(src, dst):
        copy = pltpu.make_async_copy(src, dst, out_sem.at[len(outs)])
        copy.start()
        outs.append(copy)

    def swap(value):
        return pltpu.roll(value, hd // 2, 1)

    def hand(src, dst, to, k):
        return pltpu.make_async_remote_copy(
            src_ref=src,
            dst_ref=dst,
            send_sem=hand_send.at[k],
            recv_sem=hand_recv.at[k],
            device_id={"section": to},
            device_id_type=MESH,
        )

    ticks = chunks - 1 + steps
    ahead = 2

    @pl.when(sec == 1)
    def _():
        pl.semaphore_wait(turn, 1)

    for copy in slab_copies(0):
        copy.start()
    for d in range(1, n):
        gain_copy(d).wait()
    for k, full in enumerate((ln1, ln2, qn, kn)):
        at, size = gain_at[k]
        for f in range(n):
            full[:, f * size : (f + 1) * size] = gains[f, :, at : at + size]

    @pl.when(sec == 1)
    def _():
        for c in range(1, chunks):
            for copy in slab_copies(c):
                copy.start()
        for j in range(steps + 1):
            prepare(0, j)
        for t in range(ahead):
            prepare_rest(t)
        hand(yv, xin, 0, 0).wait_recv()

    @pl.when(sec == 0)
    def _():
        load_x.wait()

    @by_rows
    def _(at):
        x32 = xin[at].astype(F32)
        r1 = lax.rsqrt(mean_last(x32 * x32) + EPS)
        xn_all[me, at] = (x32 * r1 * ln1[...]).astype(BF16)

    spread_start(xn_all, 0)

    @pl.when(sec == 0)
    def _():
        for c in range(1, chunks):
            for copy in slab_copies(c):
                copy.start()
        for j in range(steps + 1):
            prepare(0, j)

    load_o.wait()
    load_d.wait()

    def masked_scores(qh, kh):
        raw = nt(qh, kh) * scale
        at_row = lax.broadcasted_iota(jnp.int32, raw.shape, 0)
        at_col = lax.broadcasted_iota(jnp.int32, raw.shape, 1)
        raw = jnp.where(at_row >= at_col, raw, -jnp.inf)
        top = jnp.max(raw, axis=-1, keepdims=True)
        lse = top + jnp.log(jnp.sum(jnp.exp(raw - top), axis=-1, keepdims=True))
        return jnp.exp(raw - lse)

    def attend(d, s, ship):
        prepare_rest(d + ahead * sec)

        @pl.when(jnp.logical_and(sec == 0, d == n - 1))
        def _():
            pl.semaphore_signal(turn, inc=1, device_id={"section": 1}, device_id_type=MESH)

        a = xn_all[s]
        for at, size in tiles(2 * ch):
            w = wall[0, :, :, :, at : at + size].reshape(width, size)
            qkv[s, :, at : at + size] = nn(a, w)
        for at in range(0, qcols + kcols, hd):
            field = qkv[s, :, at : at + hd]
            gain = qn[...] if at < qcols else kn[...]
            factor = lax.rsqrt(mean_last(field * field) + EPS)
            normed = field * factor * gain
            turned = normed * cosine[...] + swap(normed) * sine[...]
            qkvb[s, :, at : at + hd] = turned.astype(BF16)
        qkvb[s, :, qcols + kcols :] = qkv[s, :, qcols + kcols :].astype(BF16)
        for j in range(qcols // hd):
            kv = j * kcols // qcols
            kat = qcols + kv * hd
            vat = qcols + kcols + kv * hd
            probs = masked_scores(qkvb[s, :, j * hd : (j + 1) * hd], qkvb[s, :, kat : kat + hd])
            attended = nn(probs.astype(BF16), qkvb[s, :, vat : vat + hd])
            att[s, :, j * hd : (j + 1) * hd] = attended.astype(BF16)
        a = att[s]
        for k in range(n):
            ship(k, nn(a, wo[:, k * piece : (k + 1) * piece]))

    each_block(xn_all, 0, attend)
    settle(0)

    @by_rows
    def _(at):
        h = xin[at].astype(F32) + summed(0, at)
        hres[at] = h
        r2 = lax.rsqrt(mean_last(h * h) + EPS)
        hn_all[me, at] = (h * r2 * ln2[...]).astype(BF16)

    spread_start(hn_all, 1)
    put(xn_all, xn_h)
    put(att, att_h)

    lax.fori_loop(n + ahead * sec, ticks, lambda t, carry: prepare_rest(t) or carry, 0)

    @pl.when(sec == 1)
    def _():
        load_y.wait()
        spread_start(dy_all, 2)

    def feed(d, s, ship):
        a = hn_all[s]
        for at in range(0, hidden, ch):
            size, j = ch, 1 + at // ch
            g = nn(a, wall[j, :, :, :, :ch].reshape(width, ch))
            u = nn(a, wall[j, :, :, :, ch:].reshape(width, ch))
            gate[s, :, at : at + size] = g
            up[s, :, at : at + size] = u
            act[s, :, at : at + size] = (g * jax.nn.sigmoid(g) * u).astype(BF16)
        a = act[s]
        for k in range(n):
            ship(k, nn(a, wd[:, k * piece : (k + 1) * piece]))

    each_block(hn_all, 1, feed)
    put(hn_all, hn_h)
    put(act, act_h)

    @pl.when(sec == 0)
    def _():
        settle(1)

        @by_rows
        def _(at):
            yv[at] = (hres[at] + summed(1, at)).astype(BF16)

        hand(yv, xin, 1, 0).start()
        hand(yv, dy_all.at[me], 1, 1).wait_recv()
        spread_start(dy_all, 2)

    spread_done(hn_all, 1)
    outs[2].wait()

    def feed_back(d, s, ship):
        a = dy_all[s]
        for at in range(0, hidden, ch):
            size = ch
            dact = nt(a, wd[at : at + size, :])
            g = gate[s, :, at : at + size]
            u = up[s, :, at : at + size]
            sig = jax.nn.sigmoid(g)
            dgu[s, :, 2 * at : 2 * at + ch] = (dact * u * sig * (1.0 + g * (1.0 - sig))).astype(BF16)
            dgu[s, :, 2 * at + ch : 2 * at + 2 * ch] = (dact * g * sig).astype(BF16)
        a = dgu[s]
        for f in range(n):
            total = jnp.zeros((rows, kfold), F32)
            for j in range(1, chunks):
                w = wall[j, f].reshape(kfold, 2 * ch)
                total = total + nt(a[:, 2 * (j - 1) * ch : 2 * j * ch], w)
            ship(f, total)

    each_block(dy_all, 2, feed_back)

    @pl.when(sec == 1)
    def _():
        settle(1)

        @by_rows
        def _(at):
            yv[at] = (hres[at] + summed(1, at)).astype(BF16)


    put(yv, y_h)
    settle(2)
    dln2[...] = jnp.zeros_like(dln2)
    dln1[...] = jnp.zeros_like(dln1)

    @by_rows
    def _(at):
        dhn = summed(2, at)
        h = hres[at]
        r2 = lax.rsqrt(mean_last(h * h) + EPS)
        u = dhn * ln2[...]
        dh = dy_all[me, at].astype(F32) + (r2 * u - h * r2 * r2 * r2 * mean_last(u * h))
        dln2[...] += jnp.sum(dhn * h * r2, axis=0, keepdims=True)
        hres[at] = dh
        hn_all[me, at] = dh.astype(BF16)

    spread_start(hn_all, 3)
    put(dy_all, dy_h)
    put(dgu, dgu_h)

    dqn[...] = jnp.zeros_like(dqn)
    dkn[...] = jnp.zeros_like(dkn)

    def head_back(s, at, grad, gain, dgain):
        field = qkv[s, :, at : at + hd]
        factor = lax.rsqrt(mean_last(field * field) + EPS)
        grad = grad * cosine[...] - swap(grad) * sine[...]
        v = grad * gain
        back = factor * v - field * factor * factor * factor * mean_last(v * field)
        dgain[...] += jnp.sum(grad * field * factor, axis=0, keepdims=True)
        dqkv[s, :, at : at + hd] = back.astype(BF16)

    def attend_back(d, s, ship):
        a = hn_all[s]
        for at, size in tiles(qcols):
            dout = nt(a, wo[at : at + size, :]).astype(BF16)
            for kv in range(at * kcols // (qcols * hd), (at + size) * kcols // (qcols * hd)):
                kat = qcols + kv * hd
                vat = qcols + kcols + kv * hd
                kh = qkvb[s, :, kat : kat + hd]
                vh = qkvb[s, :, vat : vat + hd]
                dk = jnp.zeros((rows, hd), F32)
                dv = jnp.zeros((rows, hd), F32)
                for j in range(kv * qcols // kcols, (kv + 1) * qcols // kcols):
                    qh = qkvb[s, :, j * hd : (j + 1) * hd]
                    dh_out = dout[:, j * hd - at : (j + 1) * hd - at]
                    probs = masked_scores(qh, kh)
                    dv = dv + tn(probs.astype(BF16), dh_out)
                    dp = nt(dh_out, vh)
                    delta = jnp.sum(probs * dp, axis=-1, keepdims=True)
                    ds = (probs * (dp - delta) * scale).astype(BF16)
                    dk = dk + tn(ds, qh)
                    head_back(s, j * hd, nn(ds, kh), qn[...], dqn)
                head_back(s, kat, dk, kn[...], dkn)
                dqkv[s, :, vat : vat + hd] = dv.astype(BF16)
        a = dqkv[s]
        for f in range(n):
            w = wall[0, f].reshape(kfold, 2 * ch)
            ship(f, nt(a, w))

    each_block(hn_all, 3, attend_back)
    settle(3)
    outs[4].wait()

    @pl.when(sec == 0)
    def _():
        hand(yv, xin, 1, 0).wait_send()

    @by_rows
    def _(at):
        dxn = summed(3, at)
        x32 = xin[at].astype(F32)
        r1 = lax.rsqrt(mean_last(x32 * x32) + EPS)
        u = dxn * ln1[...]
        dx = hres[at] + (r1 * u - x32 * r1 * r1 * r1 * mean_last(u * x32))
        dln1[...] += jnp.sum(dxn * x32 * r1, axis=0, keepdims=True)
        yv[at] = dx.astype(BF16)
        hres[at] = dx

    @pl.when(sec == 1)
    def _():
        hand(yv, dy_all.at[me], 0, 1).start()

    put(hres, dx_h)
    put(hn_all, dab_h)
    put(dqkv, dqkv_h)
    for c, buf in ((0, xn_all), (2, dy_all), (3, hn_all)):
        spread_done(buf, c)

    @pl.when(sec == 1)
    def _():
        hand(yv, dy_all.at[me], 0, 1).wait_send()

    for k, copy in enumerate(outs):
        if k not in (2, 4):
            copy.wait()


def run_layer(n, rep, tok, cot, ln1, ln2, qn, kn, wq, wk, wv, wg, wu, wo, wd):
    rows, width = tok.shape
    hd = n * qn.shape[-1]
    qcols = wo.shape[0]
    qkvcols = 2 * qcols
    steps = rep.bit_length() - 1
    chunks = 1 + wd.shape[0] // qcols
    lanes = -(-2 * (ln1.shape[-1] + qn.shape[-1]) // 128) * 128
    hidden = wd.shape[0]
    cosine, sine = rope_tables(rows, hd // 2)
    vm = pl.BlockSpec(memory_space=pltpu.VMEM)
    hbm = pl.BlockSpec(memory_space=pltpu.HBM)

    def wide(columns, kind):
        return (n, rows, columns), kind

    shaped = [
        ((rows, width), BF16),
        ((rows, width), F32),
        wide(width, BF16), wide(width, BF16), wide(width, BF16), wide(width, BF16),
        wide(qcols, BF16), wide(hidden, BF16), wide(2 * hidden, BF16), wide(qkvcols, BF16),
        ((1, width), F32), ((1, width), F32), ((1, hd), F32), ((1, hd), F32),
    ]
    scratch = [
        pltpu.VMEM((chunks, n, rep, width // (n * rep), qkvcols), BF16),
        pltpu.VMEM(wo.shape, BF16),
        pltpu.VMEM(wd.shape, BF16),
        pltpu.VMEM((1, width), F32),
        pltpu.VMEM((1, width), F32),
        pltpu.VMEM((1, hd), F32),
        pltpu.VMEM((1, hd), F32),
        pltpu.VMEM((n, 1, lanes), F32),
        pltpu.VMEM((rows, width), BF16),
        *[pltpu.VMEM(*wide(width, BF16)) for _ in range(3)],
        pltpu.VMEM(*wide(qkvcols, F32)),
        pltpu.VMEM(*wide(qkvcols, BF16)),
        pltpu.VMEM(*wide(qcols, BF16)),
        pltpu.VMEM((rows, width), F32),
        pltpu.VMEM(*wide(hidden, F32)),
        pltpu.VMEM(*wide(hidden, F32)),
        pltpu.VMEM(*wide(hidden, BF16)),
        pltpu.VMEM(*wide(2 * hidden, BF16)),
        pltpu.VMEM(*wide(qkvcols, BF16)),
        pltpu.VMEM((rows, width), BF16),
        pltpu.VMEM((2, n, rows, width), BF16),
        pltpu.VMEM((2, n - 1, rows, width), BF16),
        pltpu.SemaphoreType.DMA((4,)),
        pltpu.SemaphoreType.DMA((chunks, n - 1, 3)),
        pltpu.SemaphoreType.DMA((chunks, n - 1, 3)),
        pltpu.SemaphoreType.DMA((steps, chunks, 2, rep // 2)),
        pltpu.SemaphoreType.DMA((steps, chunks, 2, rep // 2)),
        pltpu.SemaphoreType.DMA((chunks, 3)),
        pltpu.SemaphoreType.DMA((n - 1,)),
        pltpu.SemaphoreType.DMA((n - 1,)),
        pltpu.SemaphoreType.REGULAR,
        pltpu.SemaphoreType.DMA((10,)),
        pltpu.SemaphoreType.DMA((4, n)),
        pltpu.SemaphoreType.DMA((4, n)),
        pltpu.SemaphoreType.DMA((4, n, n)),
        pltpu.SemaphoreType.DMA((4, n, n)),
        pltpu.SemaphoreType.DMA((2,)),
        pltpu.SemaphoreType.DMA((2,)),
    ]
    return pl.pallas_call(
        functools.partial(layer_kernel, n, rep, hd),
        out_shape=[jax.ShapeDtypeStruct(shape, kind) for shape, kind in shaped],
        in_specs=[hbm] * 2 + [vm] * 6 + [hbm] * 7,
        out_specs=[hbm] * 10 + [vm] * 4,
        scratch_shapes=scratch,
        compiler_params=pltpu.CompilerParams(
            collective_id=0, has_side_effects=True, vmem_limit_bytes=67043328
        ),
        name="layer",
    )(tok, cot, ln1, ln2, qn, kn, cosine, sine, wq, wk, wv, wg, wu, wo, wd)


def grad_plan(n, qcols, hidden, width):
    fold = width // n
    blocks = fold // 128
    thirds = hidden // qcols
    return blocks, thirds, (blocks * thirds, blocks, hidden // 256, qcols // 256)


def grad_kernel(
    n, rep,
    xn_h, hn_h, dy_h, dab_h, att_h, act_h, dgu_h, dqkv_h, dln1, dln2, dqn, dkn,
    gq_h, gk_h, gv_h, go_h, gg_h, gu_h, gd_h, sums,
    xn, hn, dy, dab, att, act, dgu, dqkv, mine_g, reduced, whole, pack, pack_z, pack_r, pack_in, *rest,
):
    steps = rep.bit_length() - 1
    got = rest[:steps]
    (
        in_sem, rs_send, rs_recv, z_send, z_recv, ag_send, ag_recv, out_sem,
        pz_send, pz_recv, pr_send, pr_recv,
    ) = rest[steps:]
    me = lax.axis_index("fsdp")
    mine = lax.axis_index("replica")
    ch = mine_g.shape[-1]
    part = 128 // n
    width = xn.shape[-1]
    fold = width // n
    hidden = act.shape[-1]
    kcols = gk_h.shape[-1] // n
    blocks, thirds, counts = grad_plan(n, ch, hidden, width)
    starts = [sum(counts[:k]) for k in range(len(counts) + 1)]
    total = starts[-1]
    columns_end = starts[2]
    g_slots, slots = mine_g.shape[0], whole.shape[0]
    orders = (tuple(range(steps)), tuple(reversed(range(steps))))

    barrier = pltpu.get_barrier_semaphore()
    for d in range(1, n):
        pl.semaphore_signal(
            barrier, inc=1, device_id={"fsdp": lax.rem(me + d, n)}, device_id_type=MESH
        )
    for bit in range(steps):
        pl.semaphore_signal(
            barrier, inc=1, device_id={"replica": flip(mine, bit)}, device_id_type=MESH
        )
    loads = []
    for k, (src, dst) in enumerate(
        ((hn_h, hn), (dgu_h, dgu), (xn_h, xn), (dqkv_h, dqkv), (act_h, act), (dy_h, dy), (att_h, att), (dab_h, dab))
    ):
        loads.append(pltpu.make_async_copy(src, dst, in_sem.at[k]))
        loads[-1].start()
    pack[...] = jnp.zeros_like(pack)
    at = 0
    for value in (dln1, dln2, dqn, dkn):
        size = value.shape[-1] // n
        for f in range(n):
            pack[f, :, at : at + size] = value[:, f * size : (f + 1) * size]
        at += size
    pl.semaphore_wait(barrier, n - 1 + steps)
    for load in loads:
        load.wait()

    def remote(src, dst, send, recv, where):
        return pltpu.make_async_remote_copy(
            src_ref=src, dst_ref=dst, send_sem=send, recv_sem=recv,
            device_id=where, device_id_type=MESH,
        )

    def scatter_copies(c, j):
        slot, two = lax.rem(c, g_slots), lax.rem(c, 2)
        for h, bits in enumerate(orders):
            partner = flip(mine, bits[j])
            for i in range(rep >> (j + 1)):
                piece = flips(partner, bits[j + 1 :], i)
                yield h, i, remote(
                    mine_g.at[slot, h, piece], got[j].at[two, h, i],
                    rs_send.at[j, two, h, i], rs_recv.at[j, two, h, i], {"replica": partner},
                )

    def across_copies(c):
        slot, two = lax.rem(c, slots), lax.rem(c, 2)
        for d in range(1, n):
            to = lax.rem(me + d, n)
            yield remote(
                reduced.at[:, pl.ds(to * part, part), :],
                whole.at[slot, :, mine, pl.ds(me * part, part), :],
                z_send.at[two, d - 1], z_recv.at[two, d - 1], {"fsdp": to},
            )

    def gather_copies(c, j):
        slot, two = lax.rem(c, slots), lax.rem(c, 2)
        for h, order in enumerate(orders):
            bits = order[::-1]
            partner = flip(mine, bits[j])
            for i in range(1 << j):
                piece = flips(mine, bits[:j], i)
                yield remote(
                    whole.at[slot, h, piece], whole.at[slot, h, piece],
                    ag_send.at[j, two, h, i], ag_recv.at[j, two, h, i], {"replica": partner},
                )

    def pack_across(d):
        to = lax.rem(me + d, n)
        return remote(
            pack.at[to], pack_z.at[d - 1], pz_send.at[d - 1], pz_recv.at[d - 1], {"fsdp": to}
        )

    def pack_swap(j):
        return remote(
            pack_r.at[j], pack_in.at[j], pr_send.at[j], pr_recv.at[j], {"replica": flip(mine, j)}
        )

    for d in range(1, n):
        pack_across(d).start()

    def pack_tick(t):
        for j in range(steps + 1):
            @pl.when(t == 2 * j + 2)
            def _():
                if j == 0:
                    value = pack[me]
                    for d in range(1, n):
                        pack_across(d).wait()
                        value = value + pack_z[d - 1]
                else:
                    pack_swap(j - 1).wait()
                    value = pack_r[j - 1] + pack_in[j - 1]
                if j < steps:
                    pack_r[j] = value
                    pack_swap(j).start()
                else:
                    sums[...] = value

    def aligned(at):
        return pl.multiple_of(at, 128)

    def out_copies(c, kind):
        slot, two = lax.rem(c, slots), lax.rem(c, 2)
        at = c - starts[kind]
        for f in range(n):
            rows = slice(f * part, (f + 1) * part)
            if kind == 0:
                k, j = at // thirds, lax.rem(at, thirds)
                cols = pl.ds(aligned(f * hidden + j * ch), ch)
                pairs = [
                    (whole.at[slot, h, :, rows, :], dst.at[k, :, :, cols])
                    for h, dst in enumerate((gg_h, gu_h))
                ]
            elif kind == 1:
                cols = pl.ds(f * kcols, kcols)
                pairs = [
                    (whole.at[slot, 0, :, rows, :], gq_h.at[at, :, :, pl.ds(f * ch, ch)]),
                    (whole.at[slot, 1, :, rows, pl.ds(0, kcols)], gk_h.at[at, :, :, cols]),
                    (whole.at[slot, 1, :, rows, pl.ds(kcols, kcols)], gv_h.at[at, :, :, cols]),
                ]
            else:
                dst = gd_h if kind == 2 else go_h
                pairs = [
                    (
                        whole.at[slot, h, f],
                        dst.at[pl.ds(aligned(at * 256 + h * 128), 128), pl.ds(f * ch, ch)],
                    )
                    for h in range(2)
                ]
            for i, (src, to) in enumerate(pairs):
                yield pltpu.make_async_copy(src, to, out_sem.at[two, f, i])

    def compute(c, kind):
        slot = lax.rem(c, g_slots)
        at = c - starts[kind]
        if kind < 2:
            left, right = (hn, dgu) if kind == 0 else (xn, dqkv)
            k, j = (at // thirds, lax.rem(at, thirds)) if kind == 0 else (at, 0)
            lefts = jnp.concatenate(
                [left[:, pl.ds(aligned(f * fold + k * 128), 128)] for f in range(n)], axis=1
            )
            for h in range(2):
                product = tn(lefts, right[:, pl.ds(aligned((2 * j + h) * ch), ch)]).astype(BF16)
                for f in range(n):
                    block = product[f * 128 : (f + 1) * 128].reshape(rep, 128 // rep, ch)
                    mine_g[slot, h, :, f * part : (f + 1) * part, :] = block
        else:
            left, right = (act, dy) if kind == 2 else (att, dab)
            for q in range(rep):
                cols = left[:, pl.ds(aligned(at * 256), 256)]
                product = tn(cols, right[:, q * ch : (q + 1) * ch]).astype(BF16)
                for h in range(2):
                    mine_g[slot, h, q] = product[h * 128 : (h + 1) * 128]

    def within(c, low, high):
        return jnp.logical_and(c >= low, c < high)

    def tick(t, carry):
        c = t - (2 * steps + 2)
        for kind in range(4):
            @pl.when(within(c, starts[kind], starts[kind + 1]))
            def _():
                for copy in out_copies(c, kind):
                    copy.wait()

        c_out = t - (2 * steps + 1)

        @pl.when(within(c_out, 0, total))
        def _():
            for copy in gather_copies(c_out, steps - 1):
                copy.wait()

        for kind in range(4):
            @pl.when(within(c_out, starts[kind], starts[kind + 1]))
            def _():
                for copy in out_copies(c_out, kind):
                    copy.start()

        for j in reversed(range(1, steps)):
            c_ag = t - (steps + 1 + j)

            @pl.when(within(c_ag, 0, total))
            def _():
                for copy in gather_copies(c_ag, j - 1):
                    copy.wait()
                for copy in gather_copies(c_ag, j):
                    copy.start()

        c_z = t - (steps + 1)

        @pl.when(within(c_z, 0, columns_end))
        def _():
            for copy in across_copies(c_z):
                copy.wait()

        @pl.when(within(c_z, 0, total))
        def _():
            for copy in gather_copies(c_z, 0):
                copy.start()

        for j in reversed(range(steps)):
            c_rs = t - (j + 1)
            slot, two = lax.rem(c_rs, g_slots), lax.rem(c_rs, 2)

            @pl.when(within(c_rs, 0, total))
            def _():
                for h, i, copy in scatter_copies(c_rs, j):
                    copy.wait()
                for h, bits in enumerate(orders):
                    for i in range(rep >> (j + 1)):
                        piece = flips(mine, bits[j + 1 :], i)
                        value = mine_g[slot, h, piece].astype(F32) + got[j][two, h, i].astype(F32)
                        if j < steps - 1:
                            mine_g[slot, h, piece] = value.astype(BF16)
                        else:
                            reduced[h] = value.astype(BF16)
                if j < steps - 1:
                    for h, i, copy in scatter_copies(c_rs, j + 1):
                        copy.start()

            if j == steps - 1:
                at = lax.rem(c_rs, slots)

                @pl.when(within(c_rs, 0, columns_end))
                def _():
                    for copy in across_copies(c_rs):
                        copy.start()
                    rows = pl.ds(pl.multiple_of(me * part, part), part)
                    whole[at, :, mine, rows, :] = reduced[:, rows, :]

                @pl.when(within(c_rs, columns_end, total))
                def _():
                    whole[at, :, mine] = reduced[...]

        for kind in range(4):
            @pl.when(within(t, starts[kind], starts[kind + 1]))
            def _():
                compute(t, kind)

        @pl.when(t < total)
        def _():
            for h, i, copy in scatter_copies(t, 0):
                copy.start()

        pack_tick(t)
        return carry

    lax.fori_loop(0, total + 2 * steps + 3, tick, 0)


def run_grads(n, rep, xn, hn, dy, dab, att, act, dgu, dqkv, small):
    tokens, width = xn.shape
    ch = att.shape[-1]
    hidden = act.shape[-1]
    kcols = (dqkv.shape[-1] - ch) // 2
    fold = width // n
    steps = rep.bit_length() - 1
    hbm = pl.BlockSpec(memory_space=pltpu.HBM)

    def owned(columns):
        return jax.ShapeDtypeStruct((fold // 128, rep, 128 // rep, columns * n), BF16)

    shaped = [
        owned(ch), owned(kcols), owned(kcols), jax.ShapeDtypeStruct((ch, width), BF16),
        owned(hidden), owned(hidden), jax.ShapeDtypeStruct((hidden, width), BF16),
    ]
    lanes = -(-sum(value.shape[-1] for value in small) // (128 * n)) * 128
    vm = pl.BlockSpec(memory_space=pltpu.VMEM)
    operands = (xn, hn, dy, dab, att, act, dgu, dqkv)
    scratch = [pltpu.VMEM(value.shape, BF16) for value in operands] + [
        pltpu.VMEM((steps + 1, 2, rep, 128, ch), BF16),
        pltpu.VMEM((2, 128, ch), BF16),
        pltpu.VMEM((steps + 3, 2, rep, 128, ch), BF16),
        pltpu.VMEM((n, 1, lanes), F32),
        pltpu.VMEM((n - 1, 1, lanes), F32),
        pltpu.VMEM((steps, 1, lanes), F32),
        pltpu.VMEM((steps, 1, lanes), F32),
        *[pltpu.VMEM((2, 2, rep >> (j + 1), 128, ch), BF16) for j in range(steps)],
        pltpu.SemaphoreType.DMA((len(operands),)),
        pltpu.SemaphoreType.DMA((steps, 2, 2, rep // 2)),
        pltpu.SemaphoreType.DMA((steps, 2, 2, rep // 2)),
        pltpu.SemaphoreType.DMA((2, n - 1)),
        pltpu.SemaphoreType.DMA((2, n - 1)),
        pltpu.SemaphoreType.DMA((steps, 2, 2, rep // 2)),
        pltpu.SemaphoreType.DMA((steps, 2, 2, rep // 2)),
        pltpu.SemaphoreType.DMA((2, n, 3)),
        pltpu.SemaphoreType.DMA((n - 1,)),
        pltpu.SemaphoreType.DMA((n - 1,)),
        pltpu.SemaphoreType.DMA((steps,)),
        pltpu.SemaphoreType.DMA((steps,)),
    ]
    *results, sums = pl.pallas_call(
        functools.partial(grad_kernel, n, rep),
        out_shape=shaped + [jax.ShapeDtypeStruct((1, lanes), F32)],
        in_specs=[hbm] * len(operands) + [vm] * len(small),
        out_specs=[hbm] * len(shaped) + [vm],
        scratch_shapes=scratch,
        compiler_params=pltpu.CompilerParams(
            collective_id=1, has_side_effects=True, vmem_limit_bytes=67043328
        ),
        name="grads",
    )(*operands, *small)
    return [value.reshape(-1, value.shape[-1]).astype(F32) for value in results], sums


def per_device(tokens_in, cotangent, ln1, wq, wk, wv, qn, kn, wo, ln2, wg, wu, wd):
    n, rep = lax.axis_size("fsdp"), lax.axis_size("replica")

    (
        y, dx, xn, hn, dy, dab, att, act, dgu, dqkv, *small,
    ) = run_layer(
        n, rep, tokens_in, cotangent, ln1, ln2, qn, kn,
        wq[0], wk[0], wv[0], wg[0], wu[0], wo[0], wd[0],
    )

    def flat(value):
        return value.reshape(-1, value.shape[-1])

    xn, hn, dy, dab, att, act, dgu, dqkv = map(flat, (xn, hn, dy, dab, att, act, dgu, dqkv))

    grads, sums = run_grads(n, rep, xn, hn, dy, dab, att, act, dgu, dqkv, small)
    g_wq, g_wk, g_wv, g_wo, g_wg, g_wu, g_wd = grads
    owned, at = [], 0
    for gain in (ln1, ln2, qn, kn):
        owned.append(sums[0, at : at + gain.shape[1]])
        at += gain.shape[1]
    g_ln1, g_ln2, g_qn, g_kn = owned
    results = (y, dx, g_ln1, g_wq, g_wk, g_wv, g_qn, g_kn, g_wo, g_ln2, g_wg, g_wu, g_wd)
    return tuple(value[None] for value in results)


def solution(mesh):
    rows = P("section", "fsdp", None)
    gain = P("section", "fsdp")
    tokens = P(("fsdp", "replica"), None)
    stacked = P("section", ("fsdp", "replica"), None)
    weights = (gain, rows, rows, rows, gain, gain, rows, gain, rows, rows, rows)
    return jax.shard_map(
        per_device,
        mesh=mesh,
        in_specs=(tokens, tokens, *weights),
        out_specs=(stacked, stacked, *weights),
        check_vma=False,
    )
```

```python
import functools
import math

import jax
import jax.numpy as jnp
from jax import lax
from jax.experimental import pallas as pl
from jax.experimental.pallas import tpu as pltpu
from jax.sharding import PartitionSpec as P

LEN = 128
EPS = 1e-06
F32 = jnp.float32
BF16 = jnp.bfloat16
MESH = pl.DeviceIdType.MESH
TILE = 512


def rope_tables(length, half_dim):
    freq = jnp.exp(jnp.arange(half_dim, dtype=F32) * (-math.log(1000000.0) / half_dim))
    angle = jnp.arange(length, dtype=F32)[:, None] * freq[None, :]
    cosine, sine = jnp.cos(angle), jnp.sin(angle)
    return (
        jnp.concatenate([cosine, cosine], axis=1),
        jnp.concatenate([-sine, sine], axis=1),
    )


def nn(left, right):
    return jnp.dot(left, right, preferred_element_type=F32)


def nt(left, right):
    return lax.dot_general(left, right, (((1,), (1,)), ((), ())), preferred_element_type=F32)


def tn(left, right):
    return lax.dot_general(left, right, (((0,), (0,)), ((), ())), preferred_element_type=F32)


def mean_last(value):
    return jnp.mean(value, axis=-1, keepdims=True)


def tiles(total):
    return [(at, min(TILE, total - at)) for at in range(0, total, TILE)]


def flip(value, bit):
    return value + (1 - 2 * (value // 2**bit % 2)) * 2**bit


def flips(value, bits, subset):
    for at, bit in enumerate(bits):
        if subset >> at & 1:
            value = flip(value, bit)
    return value


def layer_kernel(
    n,
    rep,
    hd,
    tok, cot, ln1_own, ln2_own, qn_own, kn_own, cosine, sine, wq_h, wk_h, wv_h, wg_h, wu_h, wo_h, wd_h,
    y_h, dx_h, xn_h, hn_h, dy_h, dab_h, att_h, act_h, dgu_h, dqkv_h, dln1, dln2, dqn, dkn,
    wall, wo, wd, ln1, ln2, qn, kn, gains,
    xin, xn_all, hn_all, dy_all, qkv, qkvb, att, hres, gate, up, act, dgu, dqkv,
    dob, yv, sbuf, rbuf,
    w_sem, zw_send, zw_recv, gw_send, gw_recv, own_sem, gain_send, gain_recv, turn,
    out_sem, ag_send, ag_recv, rs_send, rs_recv, hand_send, hand_recv,
):
    sec = lax.axis_index("section")
    me = lax.axis_index("fsdp")
    mine = lax.axis_index("replica")
    steps = rep.bit_length() - 1
    rows, width = tok.shape
    ch = att.shape[-1]
    qcols = ch
    kcols = (qkvb.shape[-1] - qcols) // 2
    hidden = act.shape[-1]
    chunks = wall.shape[0]
    share = wall.shape[3]
    kfold = rep * share
    scale = 1.0 / math.sqrt(hd)
    orders = (tuple(range(steps)), tuple(reversed(range(steps))))

    barrier = pltpu.get_barrier_semaphore()
    for d in range(1, n):
        pl.semaphore_signal(
            barrier, inc=1, device_id={"fsdp": lax.rem(me + d, n)}, device_id_type=MESH
        )
    for bit in range(steps):
        pl.semaphore_signal(
            barrier, inc=1, device_id={"replica": flip(mine, bit)}, device_id_type=MESH
        )
    pl.semaphore_signal(barrier, inc=1, device_id={"section": 1 - sec}, device_id_type=MESH)
    load_o = pltpu.make_async_copy(wo_h, wo, w_sem.at[0])
    load_d = pltpu.make_async_copy(wd_h, wd, w_sem.at[1])
    load_x = pltpu.make_async_copy(tok, xin, w_sem.at[2])
    load_y = pltpu.make_async_copy(cot, dy_all.at[me], w_sem.at[3])

    @pl.when(sec == 0)
    def _():
        load_x.start()

    @pl.when(sec == 1)
    def _():
        load_y.start()

    load_o.start()
    load_d.start()

    def remote(src, dst, send, recv, where):
        return pltpu.make_async_remote_copy(
            src_ref=src, dst_ref=dst, send_sem=send, recv_sem=recv,
            device_id=where, device_id_type=MESH,
        )

    at = 0
    gain_at = []
    gains[me] = jnp.zeros_like(gains[me])
    for value in (ln1_own, ln2_own, qn_own, kn_own):
        size = value.shape[-1]
        gains[me, :, at : at + size] = value[...].astype(F32)
        gain_at.append((at, size))
        at += size
    pl.semaphore_wait(barrier, n + steps)

    def gain_copy(d):
        return remote(
            gains.at[me], gains.at[me], gain_send.at[d - 1], gain_recv.at[d - 1],
            {"fsdp": lax.rem(me + d, n)},
        )

    for d in range(1, n):
        gain_copy(d).start()

    def slabs(c, to):
        rows_in = pl.ds(pl.multiple_of(mine * share, share), share)
        if isinstance(c, int) and c == 0:
            return (
                (wq_h.at[rows_in, pl.ds(to * ch, ch)], pl.ds(0, ch)),
                (wk_h.at[rows_in, pl.ds(to * kcols, kcols)], pl.ds(ch, kcols)),
                (wv_h.at[rows_in, pl.ds(to * kcols, kcols)], pl.ds(ch + kcols, kcols)),
            )
        cols = pl.ds(pl.multiple_of(to * hidden + (c - 1) * ch, 128), ch)
        return (
            (wg_h.at[rows_in, cols], pl.ds(0, ch)),
            (wu_h.at[rows_in, cols], pl.ds(ch, ch)),
        )

    def slab_copies(c):
        for i, (src, lanes) in enumerate(slabs(c, me)):
            yield pltpu.make_async_copy(src, wall.at[c, me, mine, :, lanes], own_sem.at[c, i])
        for d in range(1, n):
            to = lax.rem(me + d, n)
            for i, (src, lanes) in enumerate(slabs(c, to)):
                yield remote(
                    src, wall.at[c, me, mine, :, lanes],
                    zw_send.at[c, d - 1, i], zw_recv.at[c, d - 1, i], {"fsdp": to},
                )

    def slab_gathers(c, j):
        for h, order in enumerate(orders):
            bits = order[::-1]
            partner = flip(mine, bits[j])
            for i in range(1 << j):
                piece = flips(mine, bits[:j], i)
                ref = wall.at[c, :, piece, :, pl.ds(h * ch, ch)]
                yield remote(
                    ref, ref, gw_send.at[j, c, h, i], gw_recv.at[j, c, h, i], {"replica": partner}
                )

    def prepare(c, j):
        for copy in slab_copies(c) if j == 0 else slab_gathers(c, j - 1):
            copy.wait()
        if j < steps:
            for copy in slab_gathers(c, j):
                copy.start()

    events = [
        (t - j, j) for t in range(1, chunks + steps) for j in range(steps) if 1 <= t - j < chunks
    ]
    events.sort(key=lambda event: (event[0] + event[1], -event[1]))
    places = n - 1
    ahead = 3

    def prepare_at(*at):
        for first in (0, 1):
            @pl.when(sec == first)
            def _():
                for k in at:
                    if k + ahead * first < len(events):
                        prepare(*events[k + ahead * first])

    bits = n.bit_length() - 1
    piece = width // n

    def low(m):
        return (m & -m).bit_length() - 1

    def across(s):
        return sum((me // 2**j + s // 2**j) % 2 * 2**j for j in range(bits))

    def spread(buf, c, m, j):
        ref = buf.at[flips(me, range(bits), m)]
        return remote(
            ref, ref, ag_send.at[c, m + 2**j], ag_recv.at[c, m + 2**j], {"fsdp": flip(me, j)}
        )

    def spread_start(buf, c):
        for j in range(bits):
            spread(buf, c, 0, j).start()

    def spread_done(buf, c):
        for m in range(n):
            for j in range(bits if m == 0 else low(m)):
                spread(buf, c, m, j).wait_send()

    def fold(c, m, k, j):
        cols = pl.ds(k * piece, piece)
        return remote(
            sbuf.at[c % 2, m, :, cols], rbuf.at[c % 2, m - 1, :, cols],
            rs_send.at[c, m, k], rs_recv.at[c, m, k], {"fsdp": flip(me, j)},
        )

    def each_pair(buf, c, work):
        def hear(s):
            ref = buf.at[across(s)]
            remote(
                ref, ref, ag_send.at[c, s], ag_recv.at[c, s], {"fsdp": flip(me, 0)}
            ).wait_recv()

        def step(q, carry):
            hear(2 * q + 1)

            def relay():
                for m in range(2, n, 2):
                    @pl.when(2 * q + 2 == m)
                    def _():
                        hear(m)
                        for j in range(low(m)):
                            spread(buf, c, m, j).start()

            def ship(k, value):
                for i in range(2):
                    part = value[i * rows : (i + 1) * rows].astype(BF16)
                    sbuf[c % 2, 2 * q + (me + i) % 2, :, k * piece : (k + 1) * piece] = part
                fold(c, 2 * q + 1, k, 0).start()

            work(q, across(2 * q) // 2 * 2, relay, ship)
            return carry

        lax.fori_loop(0, n // 2, step, 0)

    def settle_through(c):
        own, heard = sbuf.at[c % 2], rbuf.at[c % 2]
        for m in sorted(range(2, n, 2), key=low):
            for k in range(n):
                cols = slice(k * piece, (k + 1) * piece)
                value = own[m, :, cols].astype(F32)
                for j in range(low(m)):
                    fold(c, m + 2**j, k, j).wait_recv()
                    value = value + heard[m + 2**j - 1, :, cols].astype(F32)
                own[m, :, cols] = value.astype(BF16)
                fold(c, m, k, low(m)).start()

    def settle_own(c):
        for j in range(bits):
            for k in range(n):
                fold(c, 2**j, k, j).wait_recv()
        for m in range(1, n):
            for k in range(n):
                fold(c, m, k, low(m)).wait_send()

    def pair_of(buf, base):
        value = buf[pl.ds(base, 2)]
        return value.reshape(2 * rows, value.shape[-1])

    def summed(c, at):
        total = sbuf[c % 2, 0, at].astype(F32)
        for j in range(bits):
            total = total + rbuf[c % 2, 2**j - 1, at].astype(F32)
        return total

    def by_rows(work):
        height = 32

        def step(i, carry):
            work(pl.ds(pl.multiple_of(i * height, height), height))
            return carry

        lax.fori_loop(0, rows // height, step, 0)

    outs = []

    def put(src, dst):
        copy = pltpu.make_async_copy(src, dst, out_sem.at[len(outs)])
        copy.start()
        outs.append(copy)

    def swap(value):
        return pltpu.roll(value, hd // 2, 1)

    def hand(src, dst, to, k):
        return pltpu.make_async_remote_copy(
            src_ref=src,
            dst_ref=dst,
            send_sem=hand_send.at[k],
            recv_sem=hand_recv.at[k],
            device_id={"section": to},
            device_id_type=MESH,
        )

    @pl.when(sec == 1)
    def _():
        pl.semaphore_wait(turn, 1)

    for copy in slab_copies(0):
        copy.start()
    for d in range(1, n):
        gain_copy(d).wait()
    for k, full in enumerate((ln1, ln2, qn, kn)):
        at, size = gain_at[k]
        for f in range(n):
            full[:, f * size : (f + 1) * size] = gains[f, :, at : at + size]

    @pl.when(sec == 1)
    def _():
        for j in range(steps + 1):
            prepare(0, j)
            for c in [j + 1] if j < steps else range(j + 1, chunks):
                for copy in slab_copies(c):
                    copy.start()
        for event in events[:ahead]:
            prepare(*event)
        hand(yv, xin, 0, 0).wait_recv()

    @pl.when(sec == 0)
    def _():
        load_x.wait()

    @by_rows
    def _(at):
        x32 = xin[at].astype(F32)
        r1 = lax.rsqrt(mean_last(x32 * x32) + EPS)
        xn_all[me, at] = (x32 * r1 * ln1[...]).astype(BF16)

    spread_start(xn_all, 0)

    @pl.when(sec == 0)
    def _():
        for c in range(1, chunks):
            for copy in slab_copies(c):
                copy.start()
        for j in range(steps + 1):
            prepare(0, j)

    load_o.wait()
    load_d.wait()

    def masked_scores(qh, kh):
        raw = nt(qh, kh) * scale
        at_row = lax.broadcasted_iota(jnp.int32, raw.shape, 0)
        at_col = lax.broadcasted_iota(jnp.int32, raw.shape, 1)
        raw = jnp.where(at_row >= at_col, raw, -jnp.inf)
        top = jnp.max(raw, axis=-1, keepdims=True)
        lse = top + jnp.log(jnp.sum(jnp.exp(raw - top), axis=-1, keepdims=True))
        return jnp.exp(raw - lse)

    def attend_block(s):
        for at in range(0, qcols + kcols, hd):
            field = qkv[s, :, at : at + hd]
            gain = qn[...] if at < qcols else kn[...]
            factor = lax.rsqrt(mean_last(field * field) + EPS)
            normed = field * factor * gain
            turned = normed * cosine[...] + swap(normed) * sine[...]
            qkvb[s, :, at : at + hd] = turned.astype(BF16)
        qkvb[s, :, qcols + kcols :] = qkv[s, :, qcols + kcols :].astype(BF16)
        for j in range(qcols // hd):
            kv = j * kcols // qcols
            kat = qcols + kv * hd
            vat = qcols + kcols + kv * hd
            probs = masked_scores(qkvb[s, :, j * hd : (j + 1) * hd], qkvb[s, :, kat : kat + hd])
            attended = nn(probs.astype(BF16), qkvb[s, :, vat : vat + hd])
            att[s, :, j * hd : (j + 1) * hd] = attended.astype(BF16)
    def both(base, work):
        lax.fori_loop(0, 2, lambda i, carry: work(base + i) or carry, 0)

    def attend(q, base, relay, ship):
        for k in range(places):
            if k % 2 == 0:
                @pl.when(q == k // 2)
                def _():
                    prepare_at(k)

        a = pair_of(xn_all, base)
        for at, size in tiles(2 * ch):
            w = wall[0, :, :, :, at : at + size].reshape(width, size)
            qkv[pl.ds(base, 2), :, at : at + size] = nn(a, w).reshape(2, rows, size)
        relay()
        both(base, attend_block)
        for k in range(places):
            if k % 2 == 1:
                @pl.when(q == k // 2)
                def _():
                    prepare_at(k)

        a = pair_of(att, base)
        for k in range(n):
            ship(k, nn(a, wo[:, k * piece : (k + 1) * piece]))

    each_pair(xn_all, 0, attend)
    settle_through(0)
    prepare_at(places, places + 1)
    settle_own(0)

    @by_rows
    def _(at):
        h = xin[at].astype(F32) + summed(0, at)
        hres[at] = h
        r2 = lax.rsqrt(mean_last(h * h) + EPS)
        hn_all[me, at] = (h * r2 * ln2[...]).astype(BF16)

    spread_start(hn_all, 1)
    put(xn_all, xn_h)
    put(att, att_h)

    prepare_at(*range(places + 2, len(events)))
    for c in range(1, chunks):
        prepare(c, steps)

    @pl.when(sec == 0)
    def _():
        pl.semaphore_signal(turn, inc=1, device_id={"section": 1}, device_id_type=MESH)

    def feed(q, base, relay, ship):
        a = pair_of(hn_all, base)
        here = pl.ds(base, 2)
        for at in range(0, hidden, ch):
            j = 1 + at // ch
            g = nn(a, wall[j, :, :, :, :ch].reshape(width, ch))
            u = nn(a, wall[j, :, :, :, ch:].reshape(width, ch))
            gate[here, :, at : at + ch] = g.reshape(2, rows, ch)
            up[here, :, at : at + ch] = u.reshape(2, rows, ch)
            value = (g * jax.nn.sigmoid(g) * u).astype(BF16)
            act[here, :, at : at + ch] = value.reshape(2, rows, ch)
        relay()

        @pl.when(jnp.logical_and(sec == 1, q == 0))
        def _():
            load_y.wait()
            spread_start(dy_all, 2)

        a = pair_of(act, base)
        for k in range(n):
            ship(k, nn(a, wd[:, k * piece : (k + 1) * piece]))

    each_pair(hn_all, 1, feed)

    def write_y():
        @by_rows
        def _(at):
            yv[at] = (hres[at] + summed(1, at)).astype(BF16)

    put(hn_all, hn_h)
    put(act, act_h)

    @pl.when(sec == 0)
    def _():
        settle_through(1)
        settle_own(1)
        write_y()
        hand(yv, xin, 1, 0).start()
        hand(yv, dy_all.at[me], 1, 1).wait_recv()
        spread_start(dy_all, 2)

    spread_done(hn_all, 1)
    outs[2].wait()

    def feed_back(q, base, relay, ship):
        a = pair_of(dy_all, base)
        here = pl.ds(base, 2)
        for at in range(0, hidden, ch):
            dact = nt(a, wd[at : at + ch, :])
            g = gate[here, :, at : at + ch].reshape(2 * rows, ch)
            u = up[here, :, at : at + ch].reshape(2 * rows, ch)
            sig = jax.nn.sigmoid(g)
            dg = (dact * u * sig * (1.0 + g * (1.0 - sig))).astype(BF16)
            du = (dact * g * sig).astype(BF16)
            dgu[here, :, 2 * at : 2 * at + ch] = dg.reshape(2, rows, ch)
            dgu[here, :, 2 * at + ch : 2 * at + 2 * ch] = du.reshape(2, rows, ch)
        relay()

        @pl.when(jnp.logical_and(sec == 1, q == n // 2 - 1))
        def _():
            settle_through(1)

        a = pair_of(dgu, base)
        for f in range(n):
            total = jnp.zeros((2 * rows, kfold), F32)
            for j in range(1, chunks):
                w = wall[j, f].reshape(kfold, 2 * ch)
                total = total + nt(a[:, 2 * (j - 1) * ch : 2 * j * ch], w)
            ship(f, total)

    each_pair(dy_all, 2, feed_back)
    settle_through(2)

    @pl.when(sec == 1)
    def _():
        settle_own(1)
        write_y()

    settle_own(2)
    dln2[...] = jnp.zeros_like(dln2)
    dln1[...] = jnp.zeros_like(dln1)

    @by_rows
    def _(at):
        dhn = summed(2, at)
        h = hres[at]
        r2 = lax.rsqrt(mean_last(h * h) + EPS)
        u = dhn * ln2[...]
        dh = dy_all[me, at].astype(F32) + (r2 * u - h * r2 * r2 * r2 * mean_last(u * h))
        dln2[...] += jnp.sum(dhn * h * r2, axis=0, keepdims=True)
        hres[at] = dh
        hn_all[me, at] = dh.astype(BF16)

    spread_start(hn_all, 3)

    put(yv, y_h)
    put(dy_all, dy_h)
    put(dgu, dgu_h)

    dqn[...] = jnp.zeros_like(dqn)
    dkn[...] = jnp.zeros_like(dkn)

    def head_back(s, at, grad, gain, dgain):
        field = qkv[s, :, at : at + hd]
        factor = lax.rsqrt(mean_last(field * field) + EPS)
        grad = grad * cosine[...] - swap(grad) * sine[...]
        v = grad * gain
        back = factor * v - field * factor * factor * factor * mean_last(v * field)
        dgain[...] += jnp.sum(grad * field * factor, axis=0, keepdims=True)
        dqkv[s, :, at : at + hd] = back.astype(BF16)

    def attend_back_block(i, s):
        for kv in range(kcols // hd):
            kat = qcols + kv * hd
            vat = qcols + kcols + kv * hd
            kh = qkvb[s, :, kat : kat + hd]
            vh = qkvb[s, :, vat : vat + hd]
            dk = jnp.zeros((rows, hd), F32)
            dv = jnp.zeros((rows, hd), F32)
            for j in range(kv * qcols // kcols, (kv + 1) * qcols // kcols):
                qh = qkvb[s, :, j * hd : (j + 1) * hd]
                dh_out = dob[i, :, j * hd : (j + 1) * hd]
                probs = masked_scores(qh, kh)
                dv = dv + tn(probs.astype(BF16), dh_out)
                dp = nt(dh_out, vh)
                delta = jnp.sum(probs * dp, axis=-1, keepdims=True)
                ds = (probs * (dp - delta) * scale).astype(BF16)
                dk = dk + tn(ds, qh)
                head_back(s, j * hd, nn(ds, kh), qn[...], dqn)
            head_back(s, kat, dk, kn[...], dkn)
            dqkv[s, :, vat : vat + hd] = dv.astype(BF16)
    def attend_back(q, base, relay, ship):
        a = pair_of(hn_all, base)
        for at, size in tiles(qcols):
            dout = nt(a, wo[at : at + size, :]).astype(BF16)
            dob[:, :, at : at + size] = dout.reshape(2, rows, size)
        relay()
        lax.fori_loop(0, 2, lambda i, carry: attend_back_block(i, base + i) or carry, 0)
        a = pair_of(dqkv, base)
        for f in range(n):
            w = wall[0, f].reshape(kfold, 2 * ch)
            ship(f, nt(a, w))

    each_pair(hn_all, 3, attend_back)
    settle_through(3)
    settle_own(3)
    outs[4].wait()

    @pl.when(sec == 0)
    def _():
        hand(yv, xin, 1, 0).wait_send()

    @by_rows
    def _(at):
        dxn = summed(3, at)
        x32 = xin[at].astype(F32)
        r1 = lax.rsqrt(mean_last(x32 * x32) + EPS)
        u = dxn * ln1[...]
        dx = hres[at] + (r1 * u - x32 * r1 * r1 * r1 * mean_last(u * x32))
        dln1[...] += jnp.sum(dxn * x32 * r1, axis=0, keepdims=True)
        yv[at] = dx.astype(BF16)
        hres[at] = dx

    @pl.when(sec == 1)
    def _():
        hand(yv, dy_all.at[me], 0, 1).start()

    put(hres, dx_h)
    put(hn_all, dab_h)
    put(dqkv, dqkv_h)
    for c, buf in ((0, xn_all), (2, dy_all), (3, hn_all)):
        spread_done(buf, c)

    @pl.when(sec == 1)
    def _():
        hand(yv, dy_all.at[me], 0, 1).wait_send()

    for k, copy in enumerate(outs):
        if k not in (2, 4):
            copy.wait()


def run_layer(n, rep, tok, cot, ln1, ln2, qn, kn, wq, wk, wv, wg, wu, wo, wd):
    rows, width = tok.shape
    hd = n * qn.shape[-1]
    qcols = wo.shape[0]
    qkvcols = 2 * qcols
    steps = rep.bit_length() - 1
    chunks = 1 + wd.shape[0] // qcols
    lanes = -(-2 * (ln1.shape[-1] + qn.shape[-1]) // 128) * 128
    hidden = wd.shape[0]
    cosine, sine = rope_tables(rows, hd // 2)
    vm = pl.BlockSpec(memory_space=pltpu.VMEM)
    hbm = pl.BlockSpec(memory_space=pltpu.HBM)

    def wide(columns, kind):
        return (n, rows, columns), kind

    shaped = [
        ((rows, width), BF16),
        ((rows, width), F32),
        wide(width, BF16), wide(width, BF16), wide(width, BF16), wide(width, BF16),
        wide(qcols, BF16), wide(hidden, BF16), wide(2 * hidden, BF16), wide(qkvcols, BF16),
        ((1, width), F32), ((1, width), F32), ((1, hd), F32), ((1, hd), F32),
    ]
    scratch = [
        pltpu.VMEM((chunks, n, rep, width // (n * rep), qkvcols), BF16),
        pltpu.VMEM(wo.shape, BF16),
        pltpu.VMEM(wd.shape, BF16),
        pltpu.VMEM((1, width), F32),
        pltpu.VMEM((1, width), F32),
        pltpu.VMEM((1, hd), F32),
        pltpu.VMEM((1, hd), F32),
        pltpu.VMEM((n, 1, lanes), F32),
        pltpu.VMEM((rows, width), BF16),
        *[pltpu.VMEM(*wide(width, BF16)) for _ in range(3)],
        pltpu.VMEM(*wide(qkvcols, F32)),
        pltpu.VMEM(*wide(qkvcols, BF16)),
        pltpu.VMEM(*wide(qcols, BF16)),
        pltpu.VMEM((rows, width), F32),
        pltpu.VMEM(*wide(hidden, F32)),
        pltpu.VMEM(*wide(hidden, F32)),
        pltpu.VMEM(*wide(hidden, BF16)),
        pltpu.VMEM(*wide(2 * hidden, BF16)),
        pltpu.VMEM(*wide(qkvcols, BF16)),
        pltpu.VMEM((2, rows, qcols), BF16),
        pltpu.VMEM((rows, width), BF16),
        pltpu.VMEM((2, n, rows, width), BF16),
        pltpu.VMEM((2, n - 1, rows, width), BF16),
        pltpu.SemaphoreType.DMA((4,)),
        pltpu.SemaphoreType.DMA((chunks, n - 1, 3)),
        pltpu.SemaphoreType.DMA((chunks, n - 1, 3)),
        pltpu.SemaphoreType.DMA((steps, chunks, 2, rep // 2)),
        pltpu.SemaphoreType.DMA((steps, chunks, 2, rep // 2)),
        pltpu.SemaphoreType.DMA((chunks, 3)),
        pltpu.SemaphoreType.DMA((n - 1,)),
        pltpu.SemaphoreType.DMA((n - 1,)),
        pltpu.SemaphoreType.REGULAR,
        pltpu.SemaphoreType.DMA((10,)),
        pltpu.SemaphoreType.DMA((4, n)),
        pltpu.SemaphoreType.DMA((4, n)),
        pltpu.SemaphoreType.DMA((4, n, n)),
        pltpu.SemaphoreType.DMA((4, n, n)),
        pltpu.SemaphoreType.DMA((2,)),
        pltpu.SemaphoreType.DMA((2,)),
    ]
    return pl.pallas_call(
        functools.partial(layer_kernel, n, rep, hd),
        out_shape=[jax.ShapeDtypeStruct(shape, kind) for shape, kind in shaped],
        in_specs=[hbm] * 2 + [vm] * 6 + [hbm] * 7,
        out_specs=[hbm] * 10 + [vm] * 4,
        scratch_shapes=scratch,
        compiler_params=pltpu.CompilerParams(
            collective_id=0, has_side_effects=True, vmem_limit_bytes=67043328
        ),
        name="layer",
    )(tok, cot, ln1, ln2, qn, kn, cosine, sine, wq, wk, wv, wg, wu, wo, wd)


def grad_plan(n, qcols, hidden, width):
    fold = width // n
    blocks = fold // 128
    thirds = hidden // qcols
    return blocks, thirds, (blocks * thirds, blocks, hidden // 256, qcols // 256)


def grad_kernel(
    n, rep,
    xn_h, hn_h, dy_h, dab_h, att_h, act_h, dgu_h, dqkv_h, dln1, dln2, dqn, dkn,
    gq_h, gk_h, gv_h, go_h, gg_h, gu_h, gd_h, sums,
    xn, hn, dy, dab, att, act, dgu, dqkv, mine_g, reduced, whole, pack, pack_z, pack_r, pack_in, *rest,
):
    steps = rep.bit_length() - 1
    got = rest[:steps]
    (
        in_sem, rs_send, rs_recv, z_send, z_recv, ag_send, ag_recv, out_sem,
        pz_send, pz_recv, pr_send, pr_recv,
    ) = rest[steps:]
    me = lax.axis_index("fsdp")
    mine = lax.axis_index("replica")
    ch = mine_g.shape[-1]
    part = 128 // n
    width = xn.shape[-1]
    fold = width // n
    hidden = act.shape[-1]
    kcols = gk_h.shape[-1] // n
    blocks, thirds, counts = grad_plan(n, ch, hidden, width)
    starts = [sum(counts[:k]) for k in range(len(counts) + 1)]
    total = starts[-1]
    columns_end = starts[2]
    g_slots, slots = mine_g.shape[0], whole.shape[0]
    orders = (tuple(range(steps)), tuple(reversed(range(steps))))

    barrier = pltpu.get_barrier_semaphore()
    for d in range(1, n):
        pl.semaphore_signal(
            barrier, inc=1, device_id={"fsdp": lax.rem(me + d, n)}, device_id_type=MESH
        )
    for bit in range(steps):
        pl.semaphore_signal(
            barrier, inc=1, device_id={"replica": flip(mine, bit)}, device_id_type=MESH
        )
    loads = []
    for k, (src, dst) in enumerate(
        ((hn_h, hn), (dgu_h, dgu), (xn_h, xn), (dqkv_h, dqkv), (act_h, act), (dy_h, dy), (att_h, att), (dab_h, dab))
    ):
        loads.append(pltpu.make_async_copy(src, dst, in_sem.at[k]))
        loads[-1].start()
    pack[...] = jnp.zeros_like(pack)
    at = 0
    for value in (dln1, dln2, dqn, dkn):
        size = value.shape[-1] // n
        for f in range(n):
            pack[f, :, at : at + size] = value[:, f * size : (f + 1) * size]
        at += size
    pl.semaphore_wait(barrier, n - 1 + steps)
    for load in loads:
        load.wait()

    def remote(src, dst, send, recv, where):
        return pltpu.make_async_remote_copy(
            src_ref=src, dst_ref=dst, send_sem=send, recv_sem=recv,
            device_id=where, device_id_type=MESH,
        )

    def scatter_copies(c, j):
        slot, two = lax.rem(c, g_slots), lax.rem(c, 2)
        for h, bits in enumerate(orders):
            partner = flip(mine, bits[j])
            for i in range(rep >> (j + 1)):
                piece = flips(partner, bits[j + 1 :], i)
                yield h, i, remote(
                    mine_g.at[slot, h, piece], got[j].at[two, h, i],
                    rs_send.at[j, two, h, i], rs_recv.at[j, two, h, i], {"replica": partner},
                )

    def across_copies(c):
        slot, two = lax.rem(c, slots), lax.rem(c, 2)
        for d in range(1, n):
            to = lax.rem(me + d, n)
            yield remote(
                reduced.at[:, pl.ds(to * part, part), :],
                whole.at[slot, :, mine, pl.ds(me * part, part), :],
                z_send.at[two, d - 1], z_recv.at[two, d - 1], {"fsdp": to},
            )

    def gather_copies(c, j):
        slot, two = lax.rem(c, slots), lax.rem(c, 2)
        for h, order in enumerate(orders):
            bits = order[::-1]
            partner = flip(mine, bits[j])
            for i in range(1 << j):
                piece = flips(mine, bits[:j], i)
                yield remote(
                    whole.at[slot, h, piece], whole.at[slot, h, piece],
                    ag_send.at[j, two, h, i], ag_recv.at[j, two, h, i], {"replica": partner},
                )

    def pack_across(d):
        to = lax.rem(me + d, n)
        return remote(
            pack.at[to], pack_z.at[d - 1], pz_send.at[d - 1], pz_recv.at[d - 1], {"fsdp": to}
        )

    def pack_swap(j):
        return remote(
            pack_r.at[j], pack_in.at[j], pr_send.at[j], pr_recv.at[j], {"replica": flip(mine, j)}
        )

    for d in range(1, n):
        pack_across(d).start()

    def pack_tick(t):
        for j in range(steps + 1):
            @pl.when(t == 2 * j + 2)
            def _():
                if j == 0:
                    value = pack[me]
                    for d in range(1, n):
                        pack_across(d).wait()
                        value = value + pack_z[d - 1]
                else:
                    pack_swap(j - 1).wait()
                    value = pack_r[j - 1] + pack_in[j - 1]
                if j < steps:
                    pack_r[j] = value
                    pack_swap(j).start()
                else:
                    sums[...] = value

    def aligned(at):
        return pl.multiple_of(at, 128)

    def out_copies(c, kind):
        slot, two = lax.rem(c, slots), lax.rem(c, 2)
        at = c - starts[kind]
        for f in range(n):
            rows = slice(f * part, (f + 1) * part)
            if kind == 0:
                k, j = at // thirds, lax.rem(at, thirds)
                cols = pl.ds(aligned(f * hidden + j * ch), ch)
                pairs = [
                    (whole.at[slot, h, :, rows, :], dst.at[k, :, :, cols])
                    for h, dst in enumerate((gg_h, gu_h))
                ]
            elif kind == 1:
                cols = pl.ds(f * kcols, kcols)
                pairs = [
                    (whole.at[slot, 0, :, rows, :], gq_h.at[at, :, :, pl.ds(f * ch, ch)]),
                    (whole.at[slot, 1, :, rows, pl.ds(0, kcols)], gk_h.at[at, :, :, cols]),
                    (whole.at[slot, 1, :, rows, pl.ds(kcols, kcols)], gv_h.at[at, :, :, cols]),
                ]
            else:
                dst = gd_h if kind == 2 else go_h
                pairs = [
                    (
                        whole.at[slot, h, f],
                        dst.at[pl.ds(aligned(at * 256 + h * 128), 128), pl.ds(f * ch, ch)],
                    )
                    for h in range(2)
                ]
            for i, (src, to) in enumerate(pairs):
                yield pltpu.make_async_copy(src, to, out_sem.at[two, f, i])

    def compute(c, kind):
        slot = lax.rem(c, g_slots)
        at = c - starts[kind]
        if kind < 2:
            left, right = (hn, dgu) if kind == 0 else (xn, dqkv)
            k, j = (at // thirds, lax.rem(at, thirds)) if kind == 0 else (at, 0)
            lefts = jnp.concatenate(
                [left[:, pl.ds(aligned(f * fold + k * 128), 128)] for f in range(n)], axis=1
            )
            for h in range(2):
                product = tn(lefts, right[:, pl.ds(aligned((2 * j + h) * ch), ch)]).astype(BF16)
                for f in range(n):
                    block = product[f * 128 : (f + 1) * 128].reshape(rep, 128 // rep, ch)
                    mine_g[slot, h, :, f * part : (f + 1) * part, :] = block
        else:
            left, right = (act, dy) if kind == 2 else (att, dab)
            for q in range(rep):
                cols = left[:, pl.ds(aligned(at * 256), 256)]
                product = tn(cols, right[:, q * ch : (q + 1) * ch]).astype(BF16)
                for h in range(2):
                    mine_g[slot, h, q] = product[h * 128 : (h + 1) * 128]

    def within(c, low, high):
        return jnp.logical_and(c >= low, c < high)

    def tick(t, carry):
        c = t - (2 * steps + 2)
        for kind in range(4):
            @pl.when(within(c, starts[kind], starts[kind + 1]))
            def _():
                for copy in out_copies(c, kind):
                    copy.wait()

        c_out = t - (2 * steps + 1)

        @pl.when(within(c_out, 0, total))
        def _():
            for copy in gather_copies(c_out, steps - 1):
                copy.wait()

        for kind in range(4):
            @pl.when(within(c_out, starts[kind], starts[kind + 1]))
            def _():
                for copy in out_copies(c_out, kind):
                    copy.start()

        for j in reversed(range(1, steps)):
            c_ag = t - (steps + 1 + j)

            @pl.when(within(c_ag, 0, total))
            def _():
                for copy in gather_copies(c_ag, j - 1):
                    copy.wait()
                for copy in gather_copies(c_ag, j):
                    copy.start()

        c_z = t - (steps + 1)

        @pl.when(within(c_z, 0, columns_end))
        def _():
            for copy in across_copies(c_z):
                copy.wait()

        @pl.when(within(c_z, 0, total))
        def _():
            for copy in gather_copies(c_z, 0):
                copy.start()

        for j in reversed(range(steps)):
            c_rs = t - (j + 1)
            slot, two = lax.rem(c_rs, g_slots), lax.rem(c_rs, 2)

            @pl.when(within(c_rs, 0, total))
            def _():
                for h, i, copy in scatter_copies(c_rs, j):
                    copy.wait()
                for h, bits in enumerate(orders):
                    for i in range(rep >> (j + 1)):
                        piece = flips(mine, bits[j + 1 :], i)
                        value = mine_g[slot, h, piece].astype(F32) + got[j][two, h, i].astype(F32)
                        if j < steps - 1:
                            mine_g[slot, h, piece] = value.astype(BF16)
                        else:
                            reduced[h] = value.astype(BF16)
                if j < steps - 1:
                    for h, i, copy in scatter_copies(c_rs, j + 1):
                        copy.start()

            if j == steps - 1:
                at = lax.rem(c_rs, slots)

                @pl.when(within(c_rs, 0, columns_end))
                def _():
                    for copy in across_copies(c_rs):
                        copy.start()
                    rows = pl.ds(pl.multiple_of(me * part, part), part)
                    whole[at, :, mine, rows, :] = reduced[:, rows, :]

                @pl.when(within(c_rs, columns_end, total))
                def _():
                    whole[at, :, mine] = reduced[...]

        for kind in range(4):
            @pl.when(within(t, starts[kind], starts[kind + 1]))
            def _():
                compute(t, kind)

        @pl.when(t < total)
        def _():
            for h, i, copy in scatter_copies(t, 0):
                copy.start()

        pack_tick(t)
        return carry

    lax.fori_loop(0, total + 2 * steps + 3, tick, 0)


def run_grads(n, rep, xn, hn, dy, dab, att, act, dgu, dqkv, small):
    tokens, width = xn.shape
    ch = att.shape[-1]
    hidden = act.shape[-1]
    kcols = (dqkv.shape[-1] - ch) // 2
    fold = width // n
    steps = rep.bit_length() - 1
    hbm = pl.BlockSpec(memory_space=pltpu.HBM)

    def owned(columns):
        return jax.ShapeDtypeStruct((fold // 128, rep, 128 // rep, columns * n), BF16)

    shaped = [
        owned(ch), owned(kcols), owned(kcols), jax.ShapeDtypeStruct((ch, width), BF16),
        owned(hidden), owned(hidden), jax.ShapeDtypeStruct((hidden, width), BF16),
    ]
    lanes = -(-sum(value.shape[-1] for value in small) // (128 * n)) * 128
    vm = pl.BlockSpec(memory_space=pltpu.VMEM)
    operands = (xn, hn, dy, dab, att, act, dgu, dqkv)
    scratch = [pltpu.VMEM(value.shape, BF16) for value in operands] + [
        pltpu.VMEM((steps + 1, 2, rep, 128, ch), BF16),
        pltpu.VMEM((2, 128, ch), BF16),
        pltpu.VMEM((steps + 3, 2, rep, 128, ch), BF16),
        pltpu.VMEM((n, 1, lanes), F32),
        pltpu.VMEM((n - 1, 1, lanes), F32),
        pltpu.VMEM((steps, 1, lanes), F32),
        pltpu.VMEM((steps, 1, lanes), F32),
        *[pltpu.VMEM((2, 2, rep >> (j + 1), 128, ch), BF16) for j in range(steps)],
        pltpu.SemaphoreType.DMA((len(operands),)),
        pltpu.SemaphoreType.DMA((steps, 2, 2, rep // 2)),
        pltpu.SemaphoreType.DMA((steps, 2, 2, rep // 2)),
        pltpu.SemaphoreType.DMA((2, n - 1)),
        pltpu.SemaphoreType.DMA((2, n - 1)),
        pltpu.SemaphoreType.DMA((steps, 2, 2, rep // 2)),
        pltpu.SemaphoreType.DMA((steps, 2, 2, rep // 2)),
        pltpu.SemaphoreType.DMA((2, n, 3)),
        pltpu.SemaphoreType.DMA((n - 1,)),
        pltpu.SemaphoreType.DMA((n - 1,)),
        pltpu.SemaphoreType.DMA((steps,)),
        pltpu.SemaphoreType.DMA((steps,)),
    ]
    *results, sums = pl.pallas_call(
        functools.partial(grad_kernel, n, rep),
        out_shape=shaped + [jax.ShapeDtypeStruct((1, lanes), F32)],
        in_specs=[hbm] * len(operands) + [vm] * len(small),
        out_specs=[hbm] * len(shaped) + [vm],
        scratch_shapes=scratch,
        compiler_params=pltpu.CompilerParams(
            collective_id=1, has_side_effects=True, vmem_limit_bytes=67043328
        ),
        name="grads",
    )(*operands, *small)
    return [value.reshape(-1, value.shape[-1]).astype(F32) for value in results], sums


def per_device(tokens_in, cotangent, ln1, wq, wk, wv, qn, kn, wo, ln2, wg, wu, wd):
    n, rep = lax.axis_size("fsdp"), lax.axis_size("replica")

    (
        y, dx, xn, hn, dy, dab, att, act, dgu, dqkv, *small,
    ) = run_layer(
        n, rep, tokens_in, cotangent, ln1, ln2, qn, kn,
        wq[0], wk[0], wv[0], wg[0], wu[0], wo[0], wd[0],
    )

    def flat(value):
        return value.reshape(-1, value.shape[-1])

    xn, hn, dy, dab, att, act, dgu, dqkv = map(flat, (xn, hn, dy, dab, att, act, dgu, dqkv))

    grads, sums = run_grads(n, rep, xn, hn, dy, dab, att, act, dgu, dqkv, small)
    g_wq, g_wk, g_wv, g_wo, g_wg, g_wu, g_wd = grads
    owned, at = [], 0
    for gain in (ln1, ln2, qn, kn):
        owned.append(sums[0, at : at + gain.shape[1]])
        at += gain.shape[1]
    g_ln1, g_ln2, g_qn, g_kn = owned
    results = (y, dx, g_ln1, g_wq, g_wk, g_wv, g_qn, g_kn, g_wo, g_ln2, g_wg, g_wu, g_wd)
    return tuple(value[None] for value in results)


def solution(mesh):
    rows = P("section", "fsdp", None)
    gain = P("section", "fsdp")
    tokens = P(("fsdp", "replica"), None)
    stacked = P("section", ("fsdp", "replica"), None)
    weights = (gain, rows, rows, rows, gain, gain, rows, gain, rows, rows, rows)
    return jax.shard_map(
        per_device,
        mesh=mesh,
        in_specs=(tokens, tokens, *weights),
        out_specs=(stacked, stacked, *weights),
        check_vma=False,
    )
```

```python
import functools
import math
import types

import jax
import jax.numpy as jnp
from jax import lax
from jax.experimental import pallas as pl
from jax.experimental.pallas import tpu as pltpu
from jax.sharding import PartitionSpec as P

LEN = 128
EPS = 1e-06
F32 = jnp.float32
BF16 = jnp.bfloat16
MESH = pl.DeviceIdType.MESH
TILE = 512


def rope_tables(length, half_dim):
    freq = jnp.exp(jnp.arange(half_dim, dtype=F32) * (-math.log(1000000.0) / half_dim))
    angle = jnp.arange(length, dtype=F32)[:, None] * freq[None, :]
    cosine, sine = jnp.cos(angle), jnp.sin(angle)
    return (
        jnp.concatenate([cosine, cosine], axis=1),
        jnp.concatenate([-sine, sine], axis=1),
    )


def nn(left, right):
    return jnp.dot(left, right, preferred_element_type=F32)


def nt(left, right):
    return lax.dot_general(left, right, (((1,), (1,)), ((), ())), preferred_element_type=F32)


def tn(left, right):
    return lax.dot_general(left, right, (((0,), (0,)), ((), ())), preferred_element_type=F32)


def mean_last(value):
    return jnp.mean(value, axis=-1, keepdims=True)


def tiles(total):
    return [(at, min(TILE, total - at)) for at in range(0, total, TILE)]


def flip(value, bit):
    return value + (1 - 2 * (value // 2**bit % 2)) * 2**bit


def flips(value, bits, subset):
    for at, bit in enumerate(bits):
        if subset >> at & 1:
            value = flip(value, bit)
    return value


def grad_plan(n, qcols, hidden, width):
    blocks = width // n // 128
    thirds = hidden // qcols
    return blocks, thirds, (blocks * thirds, hidden // 256, qcols // 256, blocks)


def rem(value, by):
    return value % by if isinstance(value, int) else lax.rem(value, by)


def within(value, low, high):
    if isinstance(value, int):
        return low <= value < high
    return jnp.logical_and(value >= low, value < high)


def when(condition):
    if isinstance(condition, bool):
        return lambda work: work() if condition else None
    return pl.when(condition)


def remote(src, dst, send, recv, where):
    return pltpu.make_async_remote_copy(
        src_ref=src, dst_ref=dst, send_sem=send, recv_sem=recv,
        device_id=where, device_id_type=MESH,
    )


def grad_stream(r, n, rep, ours, whole):
    me = lax.axis_index("fsdp")
    mine = lax.axis_index("replica")
    steps = rep.bit_length() - 1
    g_slots, slots = steps + 1, steps + 3
    ch = r.att.shape[-1]
    part = 128 // n
    width = r.xn.shape[-1]
    tokens = r.xn.shape[0] * r.xn.shape[1]
    fold = width // n
    hidden = r.act.shape[-1]
    kcols = r.gk_h.shape[-1] // n
    thirds = grad_plan(n, ch, hidden, width)[1]
    counts = grad_plan(n, ch, hidden, width)[2]
    starts = [sum(counts[:k]) for k in range(len(counts) + 1)]
    total = starts[-1]
    orders = (tuple(range(steps)), tuple(reversed(range(steps))))
    got = [getattr(r, f"got{j}") for j in range(steps)]

    def lanes(h):
        return pl.ds(h * ch, ch)

    def scatter_copies(c, j):
        slot, two = rem(c, g_slots), rem(c, 2)
        for h, bits in enumerate(orders):
            partner = flip(mine, bits[j])
            for i in range(rep >> (j + 1)):
                piece = flips(partner, bits[j + 1 :], i)
                yield remote(
                    ours(slot).at[piece, :, lanes(h)], got[j].at[two, h, i],
                    r.grs_send.at[j, two, h, i], r.grs_recv.at[j, two, h, i],
                    {"replica": partner},
                )

    def across_copies(c):
        slot, two = rem(c, slots), rem(c, 2)
        for d in range(1, n):
            to = lax.rem(me + d, n)
            yield remote(
                r.reduced.at[pl.ds(to * part, part), :],
                whole(slot).at[mine, pl.ds(me * part, part), :],
                r.gz_send.at[two, d - 1], r.gz_recv.at[two, d - 1], {"fsdp": to},
            )

    def gather_copies(c, j):
        slot, two = rem(c, slots), rem(c, 2)
        for h, order in enumerate(orders):
            bits = order[::-1]
            partner = flip(mine, bits[j])
            for i in range(1 << j):
                ref = whole(slot).at[flips(mine, bits[:j], i), :, lanes(h)]
                yield remote(
                    ref, ref, r.gag_send.at[j, two, h, i], r.gag_recv.at[j, two, h, i],
                    {"replica": partner},
                )

    def aligned(at):
        return pl.multiple_of(at, 128)

    def out_copies(c, kind):
        slot, two = rem(c, slots), rem(c, 2)
        at = c - starts[kind]
        for f in range(n):
            rows = pl.ds(f * part, part)
            if kind == 0:
                k, j = at // thirds, rem(at, thirds)
                cols = pl.ds(aligned(f * hidden + j * ch), ch)
                pairs = [
                    (whole(slot).at[:, rows, lanes(h)], dst.at[k, :, :, cols])
                    for h, dst in enumerate((r.gg_h, r.gu_h))
                ]
            elif kind == 3:
                cols = pl.ds(f * kcols, kcols)
                pairs = [
                    (whole(slot).at[:, rows, lanes(0)], r.gq_h.at[at, :, :, pl.ds(f * ch, ch)]),
                    (whole(slot).at[:, rows, pl.ds(ch, kcols)], r.gk_h.at[at, :, :, cols]),
                    (whole(slot).at[:, rows, pl.ds(ch + kcols, kcols)], r.gv_h.at[at, :, :, cols]),
                ]
            else:
                dst = r.gd_h if kind == 1 else r.go_h
                pairs = [
                    (
                        whole(slot).at[f, :, lanes(h)],
                        dst.at[pl.ds(aligned(at * 256 + h * 128), 128), pl.ds(f * ch, ch)],
                    )
                    for h in range(2)
                ]
            for i, (src, to) in enumerate(pairs):
                yield pltpu.make_async_copy(src, to, r.gout_sem.at[two, f, i])

    def columns_of(ref, at, size):
        return ref[:, :, pl.ds(at, size)].reshape(tokens, size)

    def compute(c, kind):
        to = ours(rem(c, g_slots))
        at = c - starts[kind]
        if kind in (0, 3):
            left, right = (r.hn, r.dgu) if kind == 0 else (r.xn, r.dqkv)
            k, j = (at // thirds, rem(at, thirds)) if kind == 0 else (at, 0)
            lefts = jnp.concatenate(
                [columns_of(left, aligned(f * fold + k * 128), 128) for f in range(n)], axis=1
            )
            for h in range(2):
                product = tn(lefts, columns_of(right, aligned((2 * j + h) * ch), ch)).astype(BF16)
                for f in range(n):
                    block = product[f * 128 : (f + 1) * 128].reshape(rep, 128 // rep, ch)
                    to[:, f * part : (f + 1) * part, h * ch : (h + 1) * ch] = block
        else:
            left, right = (r.act, r.dy) if kind == 1 else (r.att, r.dab)
            lefts = columns_of(left, aligned(at * 256), 256)
            for q in range(rep):
                product = tn(lefts, columns_of(right, q * ch, ch)).astype(BF16)
                for h in range(2):
                    to[q, :, h * ch : (h + 1) * ch] = product[h * 128 : (h + 1) * 128]

    def tick(t, kinds=(0, 1, 2, 3)):
        def is_kind(c, kind):
            return within(c, starts[kind], starts[kind + 1])

        c_done = t - (2 * steps + 2)
        for kind in kinds:
            @when(is_kind(c_done, kind))
            def _():
                for copy in out_copies(c_done, kind):
                    copy.wait()

        c_out = t - (2 * steps + 1)

        @when(within(c_out, 0, total))
        def _():
            for copy in gather_copies(c_out, steps - 1):
                copy.wait()

        for kind in kinds:
            @when(is_kind(c_out, kind))
            def _():
                for copy in out_copies(c_out, kind):
                    copy.start()

        for j in reversed(range(1, steps)):
            c_ag = t - (steps + 1 + j)

            @when(within(c_ag, 0, total))
            def _():
                for copy in gather_copies(c_ag, j - 1):
                    copy.wait()
                for copy in gather_copies(c_ag, j):
                    copy.start()

        c_z = t - (steps + 1)
        for kind in kinds:
            @when(is_kind(c_z, kind))
            def _():
                if kind in (0, 3):
                    for copy in across_copies(c_z):
                        copy.wait()
                else:
                    for d in range(1, n):
                        pl.semaphore_wait(r.gsig.at[rem(c_z, 2), d - 1], 1)

        @when(within(c_z, 0, total))
        def _():
            for copy in gather_copies(c_z, 0):
                copy.start()

        for j in reversed(range(steps)):
            c_rs = t - (j + 1)

            @when(within(c_rs, 0, total))
            def _():
                for copy in scatter_copies(c_rs, j):
                    copy.wait()
                for h, bits in enumerate(orders):
                    half = slice(h * ch, (h + 1) * ch)
                    for i in range(rep >> (j + 1)):
                        piece = flips(mine, bits[j + 1 :], i)
                        value = ours(rem(c_rs, g_slots))[piece, :, half].astype(F32)
                        value = (value + got[j][rem(c_rs, 2), h, i].astype(F32)).astype(BF16)
                        if j < steps - 1:
                            ours(rem(c_rs, g_slots))[piece, :, half] = value
                        else:
                            r.reduced[:, half] = value
                if j < steps - 1:
                    for copy in scatter_copies(c_rs, j + 1):
                        copy.start()

            if j == steps - 1:
                for kind in kinds:
                    @when(is_kind(c_rs, kind))
                    def _():
                        to = whole(rem(c_rs, slots))
                        if kind in (0, 3):
                            for copy in across_copies(c_rs):
                                copy.start()
                            rows = pl.ds(pl.multiple_of(me * part, part), part)
                            to[mine, rows, :] = r.reduced[rows, :]
                        else:
                            for d in range(1, n):
                                pl.semaphore_signal(
                                    r.gsig.at[rem(c_rs, 2), d - 1], inc=1,
                                    device_id={"fsdp": lax.rem(me + d, n)}, device_id_type=MESH,
                                )
                            to[mine] = r.reduced[...]

        for kind in kinds:
            @when(is_kind(t, kind))
            def _():
                compute(t, kind)

        @when(within(t, 0, total))
        def _():
            for copy in scatter_copies(t, 0):
                copy.start()

    def pack_across(d):
        to = lax.rem(me + d, n)
        return remote(
            r.pack.at[to], r.pack_z.at[d - 1], r.pz_send.at[d - 1], r.pz_recv.at[d - 1], {"fsdp": to}
        )

    def pack_swap(j):
        return remote(
            r.pack_r.at[j], r.pack_in.at[j], r.pr_send.at[j], r.pr_recv.at[j],
            {"replica": flip(mine, j)},
        )

    def pack_fill(dgains):
        r.pack[...] = jnp.zeros_like(r.pack)
        at = 0
        for value in dgains:
            size = value.shape[-1] // n
            for f in range(n):
                r.pack[f, :, at : at + size] = value[:, f * size : (f + 1) * size]
            at += size

    def pack_start():
        for d in range(1, n):
            pack_across(d).start()

    def pack_tick(t):
        for j in range(steps + 1):
            @pl.when(t == 2 * j + 2)
            def _():
                if j == 0:
                    value = r.pack[me]
                    for d in range(1, n):
                        pack_across(d).wait()
                        value = value + r.pack_z[d - 1]
                else:
                    pack_swap(j - 1).wait()
                    value = r.pack_r[j - 1] + r.pack_in[j - 1]
                if j < steps:
                    r.pack_r[j] = value
                    pack_swap(j).start()
                else:
                    r.sums[...] = value

    def finish(first):
        def step(t, carry):
            tick(t)
            pack_tick(t - first)
            return carry

        lax.fori_loop(first, total + 2 * steps + 3, step, 0)

    return types.SimpleNamespace(
        tick=tick, pack_fill=pack_fill, pack_start=pack_start, finish=finish
    )


def stream_scratch(n, rep, ch, lanes):
    steps = rep.bit_length() - 1
    dma = pltpu.SemaphoreType.DMA
    swap = dma((steps, 2, 2, rep // 2))
    return {
        "reduced": pltpu.VMEM((128, 2 * ch), BF16),
        "pack": pltpu.VMEM((n, 1, lanes), F32),
        "pack_z": pltpu.VMEM((n - 1, 1, lanes), F32),
        "pack_r": pltpu.VMEM((steps, 1, lanes), F32),
        "pack_in": pltpu.VMEM((steps, 1, lanes), F32),
        **{
            f"got{j}": pltpu.VMEM((2, 2, rep >> (j + 1), 128, ch), BF16) for j in range(steps)
        },
        "grs_send": swap, "grs_recv": swap,
        "gz_send": dma((2, n - 1)), "gz_recv": dma((2, n - 1)),
        "gag_send": swap, "gag_recv": swap,
        "gout_sem": dma((2, n, 3)),
        "pz_send": dma((n - 1,)), "pz_recv": dma((n - 1,)),
        "pr_send": dma((steps,)), "pr_recv": dma((steps,)),
        "gsig": pltpu.SemaphoreType.REGULAR((2, n - 1)),
    }


def stream_outputs(n, rep, ch, hidden, width, lanes):
    kcols = ch // 2

    def owned(columns):
        return jax.ShapeDtypeStruct((width // n // 128, rep, 128 // rep, columns * n), BF16)

    return {
        "gq_h": owned(ch), "gk_h": owned(kcols), "gv_h": owned(kcols),
        "go_h": jax.ShapeDtypeStruct((ch, width), BF16),
        "gg_h": owned(hidden), "gu_h": owned(hidden),
        "gd_h": jax.ShapeDtypeStruct((hidden, width), BF16),
        "sums": jax.ShapeDtypeStruct((1, lanes), F32),
    }


def named(body, names, *args):
    def kernel(*refs):
        body(types.SimpleNamespace(**dict(zip(names, refs))), *args)

    return kernel


def call(body, args, inputs, outputs, scratch, in_vmem, out_vmem, name, collective):
    vm = pl.BlockSpec(memory_space=pltpu.VMEM)
    hbm = pl.BlockSpec(memory_space=pltpu.HBM)
    results = pl.pallas_call(
        named(body, [*inputs, *outputs, *scratch], *args),
        out_shape=list(outputs.values()),
        in_specs=[vm if key in in_vmem else hbm for key in inputs],
        out_specs=[vm if key in out_vmem else hbm for key in outputs],
        scratch_shapes=list(scratch.values()),
        compiler_params=pltpu.CompilerParams(
            collective_id=collective, has_side_effects=True, vmem_limit_bytes=67043328
        ),
        name=name,
    )(*inputs.values())
    return dict(zip(outputs, results))


def greet(n, rep, me, mine):
    barrier = pltpu.get_barrier_semaphore()
    for d in range(1, n):
        pl.semaphore_signal(
            barrier, inc=1, device_id={"fsdp": lax.rem(me + d, n)}, device_id_type=MESH
        )
    for bit in range(rep.bit_length() - 1):
        pl.semaphore_signal(
            barrier, inc=1, device_id={"replica": flip(mine, bit)}, device_id_type=MESH
        )
    return barrier


def grad_kernel(r, n, rep):
    me = lax.axis_index("fsdp")
    mine = lax.axis_index("replica")
    barrier = greet(n, rep, me, mine)
    loads = []
    for k, key in enumerate(("hn", "dgu", "act", "dy", "att", "dab", "xn", "dqkv")):
        loads.append(
            pltpu.make_async_copy(getattr(r, key + "_h"), getattr(r, key), r.in_sem.at[k])
        )
        loads[-1].start()
    stream = grad_stream(r, n, rep, lambda slot: r.ours.at[slot], lambda slot: r.whole.at[slot])
    stream.pack_fill((r.dln1, r.dln2, r.dqn, r.dkn))
    pl.semaphore_wait(barrier, n - 1 + rep.bit_length() - 1)
    for load in loads:
        load.wait()
    stream.pack_start()
    stream.finish(0)


def layer_kernel(r, n, rep, hd, fused):
    sec = lax.axis_index("section")
    me = lax.axis_index("fsdp")
    mine = lax.axis_index("replica")
    wq_h, wk_h, wv_h, wg_h, wu_h = r.wq_h, r.wk_h, r.wv_h, r.wg_h, r.wu_h
    cosine, sine, wall, wo, wd, ln1, ln2, qn, kn, gains = (
        r.cosine, r.sine, r.wall, r.wo, r.wd, r.ln1, r.ln2, r.qn, r.kn, r.gains
    )
    xin, xn_all, hn_all, dy_all, qkv, qkvb, att, hres, gate, up, act, dgu, dqkv = (
        r.xin, r.xn, r.hn, r.dy, r.qkv, r.qkvb, r.att, r.hres, r.gate, r.up, r.act, r.dgu, r.dqkv
    )
    dab_all = r.dab if fused else r.hn
    dob, yv, sbuf, rbuf, turn = r.dob, r.yv, r.sbuf, r.rbuf, r.turn
    dln1, dln2, dqn, dkn = r.dln1, r.dln2, r.dqn, r.dkn
    zw_send, zw_recv, gw_send, gw_recv, own_sem = r.zw_send, r.zw_recv, r.gw_send, r.gw_recv, r.own_sem
    ag_send, ag_recv, rs_send, rs_recv = r.ag_send, r.ag_recv, r.rs_send, r.rs_recv
    steps = rep.bit_length() - 1
    rows, width = xin.shape
    ch = att.shape[-1]
    qcols = ch
    kcols = (qkvb.shape[-1] - qcols) // 2
    hidden = act.shape[-1]
    chunks = wall.shape[0]
    share = wall.shape[3]
    kfold = rep * share
    scale = 1.0 / math.sqrt(hd)
    orders = (tuple(range(steps)), tuple(reversed(range(steps))))

    barrier = greet(n, rep, me, mine)
    pl.semaphore_signal(barrier, inc=1, device_id={"section": 1 - sec}, device_id_type=MESH)
    load_o = pltpu.make_async_copy(r.wo_h, wo, r.w_sem.at[0])
    load_d = pltpu.make_async_copy(r.wd_h, wd, r.w_sem.at[1])
    load_x = pltpu.make_async_copy(r.tok, xin, r.w_sem.at[2])
    load_y = pltpu.make_async_copy(r.cot, dy_all.at[me], r.w_sem.at[3])

    @pl.when(sec == 0)
    def _():
        load_x.start()

    @pl.when(sec == 1)
    def _():
        load_y.start()

    load_o.start()
    load_d.start()

    at = 0
    gain_at = []
    gains[me] = jnp.zeros_like(gains[me])
    for value in (r.ln1_own, r.ln2_own, r.qn_own, r.kn_own):
        size = value.shape[-1]
        gains[me, :, at : at + size] = value[...].astype(F32)
        gain_at.append((at, size))
        at += size
    pl.semaphore_wait(barrier, n + steps)

    def gain_copy(d):
        return remote(
            gains.at[me], gains.at[me], r.gain_send.at[d - 1], r.gain_recv.at[d - 1],
            {"fsdp": lax.rem(me + d, n)},
        )

    for d in range(1, n):
        gain_copy(d).start()

    def slabs(c, to):
        rows_in = pl.ds(pl.multiple_of(mine * share, share), share)
        if isinstance(c, int) and c == 0:
            return (
                (wq_h.at[rows_in, pl.ds(to * ch, ch)], pl.ds(0, ch)),
                (wk_h.at[rows_in, pl.ds(to * kcols, kcols)], pl.ds(ch, kcols)),
                (wv_h.at[rows_in, pl.ds(to * kcols, kcols)], pl.ds(ch + kcols, kcols)),
            )
        cols = pl.ds(pl.multiple_of(to * hidden + (c - 1) * ch, 128), ch)
        return (
            (wg_h.at[rows_in, cols], pl.ds(0, ch)),
            (wu_h.at[rows_in, cols], pl.ds(ch, ch)),
        )

    def slab_copies(c):
        for i, (src, lanes) in enumerate(slabs(c, me)):
            yield pltpu.make_async_copy(src, wall.at[c, me, mine, :, lanes], own_sem.at[c, i])
        for d in range(1, n):
            to = lax.rem(me + d, n)
            for i, (src, lanes) in enumerate(slabs(c, to)):
                yield remote(
                    src, wall.at[c, me, mine, :, lanes],
                    zw_send.at[c, d - 1, i], zw_recv.at[c, d - 1, i], {"fsdp": to},
                )

    def slab_gathers(c, j):
        for h, order in enumerate(orders):
            bits = order[::-1]
            partner = flip(mine, bits[j])
            for i in range(1 << j):
                piece = flips(mine, bits[:j], i)
                ref = wall.at[c, :, piece, :, pl.ds(h * ch, ch)]
                yield remote(
                    ref, ref, gw_send.at[j, c, h, i], gw_recv.at[j, c, h, i], {"replica": partner}
                )

    def prepare(c, j):
        for copy in slab_copies(c) if j == 0 else slab_gathers(c, j - 1):
            copy.wait()
        if j < steps:
            for copy in slab_gathers(c, j):
                copy.start()

    events = [
        (t - j, j) for t in range(1, chunks + steps) for j in range(steps) if 1 <= t - j < chunks
    ]
    events.sort(key=lambda event: (event[0] + event[1], -event[1]))
    places = n - 1
    ahead = 3

    def prepare_at(*at):
        for first in (0, 1):
            @pl.when(sec == first)
            def _():
                for k in at:
                    if k + ahead * first < len(events):
                        prepare(*events[k + ahead * first])

    bits = n.bit_length() - 1
    piece = width // n

    def low(m):
        return (m & -m).bit_length() - 1

    def across(s):
        return sum((me // 2**j + s // 2**j) % 2 * 2**j for j in range(bits))

    def spread(buf, c, m, j):
        ref = buf.at[flips(me, range(bits), m)]
        return remote(
            ref, ref, ag_send.at[c, m + 2**j], ag_recv.at[c, m + 2**j], {"fsdp": flip(me, j)}
        )

    def spread_start(buf, c):
        for j in range(bits):
            spread(buf, c, 0, j).start()

    def spread_done(buf, c):
        for m in range(n):
            for j in range(bits if m == 0 else low(m)):
                spread(buf, c, m, j).wait_send()

    def fold(c, m, k, j):
        cols = pl.ds(k * piece, piece)
        return remote(
            sbuf.at[c % 2, m, :, cols], rbuf.at[c % 2, m - 1, :, cols],
            rs_send.at[c, m, k], rs_recv.at[c, m, k], {"fsdp": flip(me, j)},
        )

    def each_pair(buf, c, work):
        def hear(s):
            ref = buf.at[across(s)]
            remote(
                ref, ref, ag_send.at[c, s], ag_recv.at[c, s], {"fsdp": flip(me, 0)}
            ).wait_recv()

        def step(q, carry):
            hear(2 * q + 1)

            def relay():
                for m in range(2, n, 2):
                    @pl.when(2 * q + 2 == m)
                    def _():
                        hear(m)
                        for j in range(low(m)):
                            spread(buf, c, m, j).start()

            def ship(k, value):
                for i in range(2):
                    part = value[i * rows : (i + 1) * rows].astype(BF16)
                    sbuf[c % 2, 2 * q + (me + i) % 2, :, k * piece : (k + 1) * piece] = part
                fold(c, 2 * q + 1, k, 0).start()

            work(q, across(2 * q) // 2 * 2, relay, ship)
            return carry

        lax.fori_loop(0, n // 2, step, 0)

    def settle_through(c):
        own, heard = sbuf.at[c % 2], rbuf.at[c % 2]
        for m in sorted(range(2, n, 2), key=low):
            for k in range(n):
                cols = slice(k * piece, (k + 1) * piece)
                value = own[m, :, cols].astype(F32)
                for j in range(low(m)):
                    fold(c, m + 2**j, k, j).wait_recv()
                    value = value + heard[m + 2**j - 1, :, cols].astype(F32)
                own[m, :, cols] = value.astype(BF16)
                fold(c, m, k, low(m)).start()

    def settle_own(c):
        for j in range(bits):
            for k in range(n):
                fold(c, 2**j, k, j).wait_recv()
        for m in range(1, n):
            for k in range(n):
                fold(c, m, k, low(m)).wait_send()

    def pair_of(buf, base):
        value = buf[pl.ds(base, 2)]
        return value.reshape(2 * rows, value.shape[-1])

    def summed(c, at):
        total = sbuf[c % 2, 0, at].astype(F32)
        for j in range(bits):
            total = total + rbuf[c % 2, 2**j - 1, at].astype(F32)
        return total

    def by_rows(work):
        height = 32

        def step(i, carry):
            work(pl.ds(pl.multiple_of(i * height, height), height))
            return carry

        lax.fori_loop(0, rows // height, step, 0)

    outs = {}
    put_keys = ("y", "dx", "xn", "hn", "dy", "dab", "att", "act", "dgu", "dqkv")

    def put(key, src):
        if hasattr(r, key + "_h"):
            copy = pltpu.make_async_copy(src, getattr(r, key + "_h"), r.out_sem.at[put_keys.index(key)])
            copy.start()
            outs[key] = copy

    def put_done(*keys):
        for key in keys:
            if key in outs:
                outs.pop(key).wait()

    def swap(value):
        return pltpu.roll(value, hd // 2, 1)

    def hand(src, dst, to, k):
        return pltpu.make_async_remote_copy(
            src_ref=src,
            dst_ref=dst,
            send_sem=r.hand_send.at[k],
            recv_sem=r.hand_recv.at[k],
            device_id={"section": to},
            device_id_type=MESH,
        )

    @pl.when(sec == 1)
    def _():
        pl.semaphore_wait(turn, 1)

    for copy in slab_copies(0):
        copy.start()
    for d in range(1, n):
        gain_copy(d).wait()
    for k, full in enumerate((ln1, ln2, qn, kn)):
        at, size = gain_at[k]
        for f in range(n):
            full[:, f * size : (f + 1) * size] = gains[f, :, at : at + size]

    @pl.when(sec == 1)
    def _():
        for j in range(steps + 1):
            prepare(0, j)
            for c in [j + 1] if j < steps else range(j + 1, chunks):
                for copy in slab_copies(c):
                    copy.start()
        for event in events[:ahead]:
            prepare(*event)
        hand(yv, xin, 0, 0).wait_recv()

    @pl.when(sec == 0)
    def _():
        load_x.wait()

    @by_rows
    def _(at):
        x32 = xin[at].astype(F32)
        r1 = lax.rsqrt(mean_last(x32 * x32) + EPS)
        xn_all[me, at] = (x32 * r1 * ln1[...]).astype(BF16)

    spread_start(xn_all, 0)

    @pl.when(sec == 0)
    def _():
        for c in range(1, chunks):
            for copy in slab_copies(c):
                copy.start()
        for j in range(steps + 1):
            prepare(0, j)

    load_o.wait()
    load_d.wait()

    def masked_scores(qh, kh):
        raw = nt(qh, kh) * scale
        at_row = lax.broadcasted_iota(jnp.int32, raw.shape, 0)
        at_col = lax.broadcasted_iota(jnp.int32, raw.shape, 1)
        raw = jnp.where(at_row >= at_col, raw, -jnp.inf)
        top = jnp.max(raw, axis=-1, keepdims=True)
        lse = top + jnp.log(jnp.sum(jnp.exp(raw - top), axis=-1, keepdims=True))
        return jnp.exp(raw - lse)

    def attend_block(s):
        for at in range(0, qcols + kcols, hd):
            field = qkv[s, :, at : at + hd]
            gain = qn[...] if at < qcols else kn[...]
            factor = lax.rsqrt(mean_last(field * field) + EPS)
            normed = field * factor * gain
            turned = normed * cosine[...] + swap(normed) * sine[...]
            qkvb[s, :, at : at + hd] = turned.astype(BF16)
        qkvb[s, :, qcols + kcols :] = qkv[s, :, qcols + kcols :].astype(BF16)
        for j in range(qcols // hd):
            kv = j * kcols // qcols
            kat = qcols + kv * hd
            vat = qcols + kcols + kv * hd
            probs = masked_scores(qkvb[s, :, j * hd : (j + 1) * hd], qkvb[s, :, kat : kat + hd])
            attended = nn(probs.astype(BF16), qkvb[s, :, vat : vat + hd])
            att[s, :, j * hd : (j + 1) * hd] = attended.astype(BF16)
    def both(base, work):
        lax.fori_loop(0, 2, lambda i, carry: work(base + i) or carry, 0)

    def attend(q, base, relay, ship):
        for k in range(places):
            if k % 2 == 0:
                @pl.when(q == k // 2)
                def _():
                    prepare_at(k)

        a = pair_of(xn_all, base)
        for at, size in tiles(2 * ch):
            w = wall[0, :, :, :, at : at + size].reshape(width, size)
            qkv[pl.ds(base, 2), :, at : at + size] = nn(a, w).reshape(2, rows, size)
        relay()
        both(base, attend_block)
        for k in range(places):
            if k % 2 == 1:
                @pl.when(q == k // 2)
                def _():
                    prepare_at(k)

        a = pair_of(att, base)
        for k in range(n):
            ship(k, nn(a, wo[:, k * piece : (k + 1) * piece]))

    each_pair(xn_all, 0, attend)
    settle_through(0)
    prepare_at(places, places + 1)
    settle_own(0)

    @by_rows
    def _(at):
        h = xin[at].astype(F32) + summed(0, at)
        hres[at] = h
        r2 = lax.rsqrt(mean_last(h * h) + EPS)
        hn_all[me, at] = (h * r2 * ln2[...]).astype(BF16)

    spread_start(hn_all, 1)
    put("xn", xn_all)
    put("att", att)

    prepare_at(*range(places + 2, len(events)))
    for c in range(1, chunks):
        prepare(c, steps)

    @pl.when(sec == 0)
    def _():
        pl.semaphore_signal(turn, inc=1, device_id={"section": 1}, device_id_type=MESH)

    def feed(q, base, relay, ship):
        a = pair_of(hn_all, base)
        here = pl.ds(base, 2)
        for at in range(0, hidden, ch):
            j = 1 + at // ch
            g = nn(a, wall[j, :, :, :, :ch].reshape(width, ch))
            u = nn(a, wall[j, :, :, :, ch:].reshape(width, ch))
            gate[here, :, at : at + ch] = g.reshape(2, rows, ch)
            up[here, :, at : at + ch] = u.reshape(2, rows, ch)
            value = (g * jax.nn.sigmoid(g) * u).astype(BF16)
            act[here, :, at : at + ch] = value.reshape(2, rows, ch)
        relay()

        @pl.when(jnp.logical_and(sec == 1, q == 0))
        def _():
            load_y.wait()
            spread_start(dy_all, 2)

        a = pair_of(act, base)
        for k in range(n):
            ship(k, nn(a, wd[:, k * piece : (k + 1) * piece]))

    each_pair(hn_all, 1, feed)

    def write_y():
        @by_rows
        def _(at):
            yv[at] = (hres[at] + summed(1, at)).astype(BF16)

    put("hn", hn_all)
    put("act", act)

    @pl.when(sec == 0)
    def _():
        settle_through(1)
        settle_own(1)
        write_y()
        hand(yv, xin, 1, 0).start()
        hand(yv, dy_all.at[me], 1, 1).wait_recv()
        spread_start(dy_all, 2)

    spread_done(hn_all, 1)
    put_done("hn")

    def feed_back(q, base, relay, ship):
        a = pair_of(dy_all, base)
        here = pl.ds(base, 2)
        for at in range(0, hidden, ch):
            dact = nt(a, wd[at : at + ch, :])
            g = gate[here, :, at : at + ch].reshape(2 * rows, ch)
            u = up[here, :, at : at + ch].reshape(2 * rows, ch)
            sig = jax.nn.sigmoid(g)
            dg = (dact * u * sig * (1.0 + g * (1.0 - sig))).astype(BF16)
            du = (dact * g * sig).astype(BF16)
            dgu[here, :, 2 * at : 2 * at + ch] = dg.reshape(2, rows, ch)
            dgu[here, :, 2 * at + ch : 2 * at + 2 * ch] = du.reshape(2, rows, ch)
        relay()

        @pl.when(jnp.logical_and(sec == 1, q == n // 2 - 1))
        def _():
            settle_through(1)

        a = pair_of(dgu, base)
        for f in range(n):
            total = jnp.zeros((2 * rows, kfold), F32)
            for j in range(1, chunks):
                w = wall[j, f].reshape(kfold, 2 * ch)
                total = total + nt(a[:, 2 * (j - 1) * ch : 2 * j * ch], w)
            ship(f, total)

    each_pair(dy_all, 2, feed_back)

    if fused:
        g_slots = steps + 1

        def place(slot):
            return wall.at[1 + slot // n, slot % n]

        view = types.SimpleNamespace(**{**vars(r), "hn": hn_all, "dab": dab_all})
        stream = grad_stream(
            view, n, rep, place, lambda slot: place(slot + g_slots)
        )
        for d in range(1, n):
            pl.semaphore_signal(
                r.freed, inc=1, device_id={"fsdp": lax.rem(me + d, n)}, device_id_type=MESH
            )

    def early_tick(t):
        if fused:
            stream.tick(t, (0,))

    def early(low, high):
        if fused:
            pl.semaphore_wait(r.freed, n - 1)
            lax.fori_loop(low, high, lambda t, carry: early_tick(t) or carry, 0)

    early_tick(0)
    settle_through(2)
    early_tick(1)

    @pl.when(sec == 1)
    def _():
        settle_own(1)
        write_y()

    settle_own(2)
    dln2[...] = jnp.zeros_like(dln2)
    dln1[...] = jnp.zeros_like(dln1)

    @by_rows
    def _(at):
        dhn = summed(2, at)
        h = hres[at]
        r2 = lax.rsqrt(mean_last(h * h) + EPS)
        u = dhn * ln2[...]
        dh = dy_all[me, at].astype(F32) + (r2 * u - h * r2 * r2 * r2 * mean_last(u * h))
        dln2[...] += jnp.sum(dhn * h * r2, axis=0, keepdims=True)
        hres[at] = dh
        dab_all[me, at] = dh.astype(BF16)

    spread_start(dab_all, 3)
    early(2, 4)

    put("y", yv)
    put("dy", dy_all)
    put("dgu", dgu)

    dqn[...] = jnp.zeros_like(dqn)
    dkn[...] = jnp.zeros_like(dkn)

    def head_back(s, at, grad, gain, dgain):
        field = qkv[s, :, at : at + hd]
        factor = lax.rsqrt(mean_last(field * field) + EPS)
        grad = grad * cosine[...] - swap(grad) * sine[...]
        v = grad * gain
        back = factor * v - field * factor * factor * factor * mean_last(v * field)
        dgain[...] += jnp.sum(grad * field * factor, axis=0, keepdims=True)
        dqkv[s, :, at : at + hd] = back.astype(BF16)

    def attend_back_block(i, s):
        for kv in range(kcols // hd):
            kat = qcols + kv * hd
            vat = qcols + kcols + kv * hd
            kh = qkvb[s, :, kat : kat + hd]
            vh = qkvb[s, :, vat : vat + hd]
            dk = jnp.zeros((rows, hd), F32)
            dv = jnp.zeros((rows, hd), F32)
            for j in range(kv * qcols // kcols, (kv + 1) * qcols // kcols):
                qh = qkvb[s, :, j * hd : (j + 1) * hd]
                dh_out = dob[i, :, j * hd : (j + 1) * hd]
                probs = masked_scores(qh, kh)
                dv = dv + tn(probs.astype(BF16), dh_out)
                dp = nt(dh_out, vh)
                delta = jnp.sum(probs * dp, axis=-1, keepdims=True)
                ds = (probs * (dp - delta) * scale).astype(BF16)
                dk = dk + tn(ds, qh)
                head_back(s, j * hd, nn(ds, kh), qn[...], dqn)
            head_back(s, kat, dk, kn[...], dkn)
            dqkv[s, :, vat : vat + hd] = dv.astype(BF16)
    def attend_back(q, base, relay, ship):
        early_tick(4 + 2 * q)
        a = pair_of(dab_all, base)
        for at, size in tiles(qcols):
            dout = nt(a, wo[at : at + size, :]).astype(BF16)
            dob[:, :, at : at + size] = dout.reshape(2, rows, size)
        relay()
        early_tick(5 + 2 * q)
        lax.fori_loop(0, 2, lambda i, carry: attend_back_block(i, base + i) or carry, 0)
        a = pair_of(dqkv, base)
        for f in range(n):
            w = wall[0, f].reshape(kfold, 2 * ch)
            ship(f, nt(a, w))

    each_pair(dab_all, 3, attend_back)
    early_tick(4 + n)
    settle_through(3)
    early_tick(5 + n)
    settle_own(3)
    put_done("y")

    @pl.when(sec == 0)
    def _():
        hand(yv, xin, 1, 0).wait_send()

    @by_rows
    def _(at):
        dxn = summed(3, at)
        x32 = xin[at].astype(F32)
        r1 = lax.rsqrt(mean_last(x32 * x32) + EPS)
        u = dxn * ln1[...]
        dx = hres[at] + (r1 * u - x32 * r1 * r1 * r1 * mean_last(u * x32))
        dln1[...] += jnp.sum(dxn * x32 * r1, axis=0, keepdims=True)
        yv[at] = dx.astype(BF16)
        hres[at] = dx

    @pl.when(sec == 1)
    def _():
        hand(yv, dy_all.at[me], 0, 1).start()

    put("dx", hres)
    put("dab", dab_all)
    put("dqkv", dqkv)
    if fused:
        stream.pack_fill((dln1, dln2, dqn, dkn))
        stream.pack_start()
        stream.finish(6 + n)
    for c, buf in ((0, xn_all), (2, dy_all), (3, dab_all)):
        spread_done(buf, c)

    @pl.when(sec == 1)
    def _():
        hand(yv, dy_all.at[me], 0, 1).wait_send()

    put_done(*list(outs))


def run_layer(n, rep, fused, lanes, tok, cot, ln1, ln2, qn, kn, wq, wk, wv, wg, wu, wo, wd):
    rows, width = tok.shape
    hd = n * qn.shape[-1]
    qcols = wo.shape[0]
    qkvcols = 2 * qcols
    steps = rep.bit_length() - 1
    chunks = 1 + wd.shape[0] // qcols
    hidden = wd.shape[0]
    cosine, sine = rope_tables(rows, hd // 2)
    inputs = {
        "tok": tok, "cot": cot, "ln1_own": ln1, "ln2_own": ln2, "qn_own": qn, "kn_own": kn,
        "cosine": cosine, "sine": sine, "wq_h": wq, "wk_h": wk, "wv_h": wv, "wg_h": wg, "wu_h": wu,
        "wo_h": wo, "wd_h": wd,
    }
    in_vmem = ("ln1_own", "ln2_own", "qn_own", "kn_own", "cosine", "sine")
    single = {"dln1": (1, width), "dln2": (1, width), "dqn": (1, hd), "dkn": (1, hd)}
    outputs = {
        "y_h": jax.ShapeDtypeStruct((rows, width), BF16),
        "dx_h": jax.ShapeDtypeStruct((rows, width), F32),
    }
    saved = {
        "xn": width, "hn": width, "dy": width, "dab": width, "att": qcols, "act": hidden,
        "dgu": 2 * hidden, "dqkv": qkvcols,
    }
    dma = pltpu.SemaphoreType.DMA
    scratch = {
        "wall": pltpu.VMEM((chunks, n, rep, width // (n * rep), qkvcols), BF16),
        "wo": pltpu.VMEM(wo.shape, BF16),
        "wd": pltpu.VMEM(wd.shape, BF16),
        "ln1": pltpu.VMEM((1, width), F32),
        "ln2": pltpu.VMEM((1, width), F32),
        "qn": pltpu.VMEM((1, hd), F32),
        "kn": pltpu.VMEM((1, hd), F32),
        "gains": pltpu.VMEM((n, 1, lanes), F32),
        "xin": pltpu.VMEM((rows, width), BF16),
        **{
            key: pltpu.VMEM((n, rows, size), BF16)
            for key, size in saved.items() if fused or key != "dab"
        },
        "qkv": pltpu.VMEM((n, rows, qkvcols), F32),
        "qkvb": pltpu.VMEM((n, rows, qkvcols), BF16),
        "hres": pltpu.VMEM((rows, width), F32),
        "gate": pltpu.VMEM((n, rows, hidden), F32),
        "up": pltpu.VMEM((n, rows, hidden), F32),
        "dob": pltpu.VMEM((2, rows, qcols), BF16),
        "yv": pltpu.VMEM((rows, width), BF16),
        "sbuf": pltpu.VMEM((2, n, rows, width), BF16),
        "rbuf": pltpu.VMEM((2, n - 1, rows, width), BF16),
        "w_sem": dma((4,)),
        "zw_send": dma((chunks, n - 1, 3)),
        "zw_recv": dma((chunks, n - 1, 3)),
        "gw_send": dma((steps, chunks, 2, rep // 2)),
        "gw_recv": dma((steps, chunks, 2, rep // 2)),
        "own_sem": dma((chunks, 3)),
        "gain_send": dma((n - 1,)),
        "gain_recv": dma((n - 1,)),
        "turn": pltpu.SemaphoreType.REGULAR,
        "out_sem": dma((10,)),
        "ag_send": dma((4, n)),
        "ag_recv": dma((4, n)),
        "rs_send": dma((4, n, n)),
        "rs_recv": dma((4, n, n)),
        "hand_send": dma((2,)),
        "hand_recv": dma((2,)),
    }
    if fused:
        outputs |= stream_outputs(n, rep, qcols, hidden, width, lanes)
        scratch |= {key: pltpu.VMEM(shape, F32) for key, shape in single.items()}
        scratch |= stream_scratch(n, rep, qcols, lanes)
        scratch["freed"] = pltpu.SemaphoreType.REGULAR
    else:
        outputs |= {
            key + "_h": jax.ShapeDtypeStruct((n, rows, size), BF16) for key, size in saved.items()
        }
        outputs |= {key: jax.ShapeDtypeStruct(shape, F32) for key, shape in single.items()}
    out_vmem = (*single, "sums")
    return call(
        layer_kernel, (n, rep, hd, fused), inputs, outputs, scratch, in_vmem, out_vmem, "layer", 0
    )


def run_grads(n, rep, saved, lanes):
    steps = rep.bit_length() - 1
    ch, hidden, width = (saved[key].shape[-1] for key in ("att_h", "act_h", "xn_h"))
    inputs = {key: value for key, value in saved.items() if key not in ("y_h", "dx_h")}
    scratch = {
        key[:-2]: pltpu.VMEM(value.shape, BF16) for key, value in inputs.items() if key[-2:] == "_h"
    }
    scratch["ours"] = pltpu.VMEM((steps + 1, rep, 128, 2 * ch), BF16)
    scratch["whole"] = pltpu.VMEM((steps + 3, rep, 128, 2 * ch), BF16)
    scratch["in_sem"] = pltpu.SemaphoreType.DMA((8,))
    scratch |= stream_scratch(n, rep, ch, lanes)
    outputs = stream_outputs(n, rep, ch, hidden, width, lanes)
    small = ("dln1", "dln2", "dqn", "dkn")
    return call(grad_kernel, (n, rep), inputs, outputs, scratch, small, ("sums",), "grads", 1)


def per_device(tokens_in, cotangent, ln1, wq, wk, wv, qn, kn, wo, ln2, wg, wu, wd):
    n, rep = lax.axis_size("fsdp"), lax.axis_size("replica")

    lanes = -(-2 * (ln1.shape[-1] + qn.shape[-1]) // 128) * 128
    thirds = grad_plan(n, wo.shape[1], wd.shape[1], wo.shape[2])[1]
    fused = (2 * rep.bit_length() + 2) <= n * thirds and wq.shape[1] == n * 128
    done = run_layer(
        n, rep, fused, lanes, tokens_in, cotangent, ln1, ln2, qn, kn,
        wq[0], wk[0], wv[0], wg[0], wu[0], wo[0], wd[0],
    )
    y, dx = done["y_h"], done["dx_h"]
    if not fused:
        done = run_grads(n, rep, done, lanes)
    g_wq, g_wk, g_wv, g_wo, g_wg, g_wu, g_wd = (
        done[key].reshape(-1, done[key].shape[-1]).astype(F32)
        for key in ("gq_h", "gk_h", "gv_h", "go_h", "gg_h", "gu_h", "gd_h")
    )
    sums = done["sums"]
    owned, at = [], 0
    for gain in (ln1, ln2, qn, kn):
        owned.append(sums[0, at : at + gain.shape[1]])
        at += gain.shape[1]
    g_ln1, g_ln2, g_qn, g_kn = owned
    results = (y, dx, g_ln1, g_wq, g_wk, g_wv, g_qn, g_kn, g_wo, g_ln2, g_wg, g_wu, g_wd)
    return tuple(value[None] for value in results)


def solution(mesh):
    rows = P("section", "fsdp", None)
    gain = P("section", "fsdp")
    tokens = P(("fsdp", "replica"), None)
    stacked = P("section", ("fsdp", "replica"), None)
    weights = (gain, rows, rows, rows, gain, gain, rows, gain, rows, rows, rows)
    return jax.shard_map(
        per_device,
        mesh=mesh,
        in_specs=(tokens, tokens, *weights),
        out_specs=(stacked, stacked, *weights),
        check_vma=False,
    )
```

```python
import functools
import math
import types

import jax
import jax.numpy as jnp
from jax import lax
from jax.experimental import pallas as pl
from jax.experimental.pallas import tpu as pltpu
from jax.sharding import PartitionSpec as P

LEN = 128
EPS = 1e-06
F32 = jnp.float32
BF16 = jnp.bfloat16
MESH = pl.DeviceIdType.MESH
TILE = 512


def rope_tables(length, half_dim):
    freq = jnp.exp(jnp.arange(half_dim, dtype=F32) * (-math.log(1000000.0) / half_dim))
    angle = jnp.arange(length, dtype=F32)[:, None] * freq[None, :]
    cosine, sine = jnp.cos(angle), jnp.sin(angle)
    return (
        jnp.concatenate([cosine, cosine], axis=1),
        jnp.concatenate([-sine, sine], axis=1),
    )


def nn(left, right):
    return jnp.dot(left, right, preferred_element_type=F32)


def nt(left, right):
    return lax.dot_general(left, right, (((1,), (1,)), ((), ())), preferred_element_type=F32)


def tn(left, right):
    return lax.dot_general(left, right, (((0,), (0,)), ((), ())), preferred_element_type=F32)


def mean_last(value):
    return jnp.mean(value, axis=-1, keepdims=True)


def tiles(total):
    return [(at, min(TILE, total - at)) for at in range(0, total, TILE)]


def flip(value, bit):
    return value + (1 - 2 * (value // 2**bit % 2)) * 2**bit


def flips(value, bits, subset):
    for at, bit in enumerate(bits):
        if subset >> at & 1:
            value = flip(value, bit)
    return value


def grad_plan(n, qcols, hidden, width):
    blocks = width // n // 128
    thirds = hidden // qcols
    return blocks, thirds, (hidden // 256, blocks * thirds, qcols // 256, blocks)


def rem(value, by):
    return value % by if isinstance(value, int) else lax.rem(value, by)


def within(value, low, high):
    if isinstance(value, int):
        return low <= value < high
    return jnp.logical_and(value >= low, value < high)


def when(condition):
    if isinstance(condition, bool):
        return lambda work: work() if condition else None
    return pl.when(condition)


def remote(src, dst, send, recv, where):
    return pltpu.make_async_remote_copy(
        src_ref=src, dst_ref=dst, send_sem=send, recv_sem=recv,
        device_id=where, device_id_type=MESH,
    )


def grad_stream(r, n, rep, ours, whole):
    me = lax.axis_index("fsdp")
    mine = lax.axis_index("replica")
    steps = rep.bit_length() - 1
    g_slots, slots = steps + 1, steps + 3
    ch = r.att.shape[-1]
    part = 128 // n
    width = r.xn.shape[-1]
    tokens = r.xn.shape[0] * r.xn.shape[1]
    fold = width // n
    hidden = r.act.shape[-1]
    kcols = r.gk_h.shape[-1] // n
    thirds = grad_plan(n, ch, hidden, width)[1]
    counts = grad_plan(n, ch, hidden, width)[2]
    starts = [sum(counts[:k]) for k in range(len(counts) + 1)]
    total = starts[-1]
    orders = (tuple(range(steps)), tuple(reversed(range(steps))))
    got = [getattr(r, f"got{j}") for j in range(steps)]

    def lanes(h):
        return pl.ds(h * ch, ch)

    def scatter_copies(c, j):
        slot, two = rem(c, g_slots), rem(c, 2)
        for h, bits in enumerate(orders):
            partner = flip(mine, bits[j])
            for i in range(rep >> (j + 1)):
                piece = flips(partner, bits[j + 1 :], i)
                yield remote(
                    ours(slot).at[piece, :, lanes(h)], got[j].at[two, h, i],
                    r.grs_send.at[j, two, h, i], r.grs_recv.at[j, two, h, i],
                    {"replica": partner},
                )

    def across_copies(c):
        slot, two = rem(c, slots), rem(c, 2)
        for d in range(1, n):
            to = lax.rem(me + d, n)
            yield remote(
                r.reduced.at[pl.ds(to * part, part), :],
                whole(slot).at[mine, pl.ds(me * part, part), :],
                r.gz_send.at[two, d - 1], r.gz_recv.at[two, d - 1], {"fsdp": to},
            )

    def gather_copies(c, j):
        slot, two = rem(c, slots), rem(c, 2)
        for h, order in enumerate(orders):
            bits = order[::-1]
            partner = flip(mine, bits[j])
            for i in range(1 << j):
                ref = whole(slot).at[flips(mine, bits[:j], i), :, lanes(h)]
                yield remote(
                    ref, ref, r.gag_send.at[j, two, h, i], r.gag_recv.at[j, two, h, i],
                    {"replica": partner},
                )

    def aligned(at):
        return pl.multiple_of(at, 128)

    def out_copies(c, kind):
        slot, two = rem(c, slots), rem(c, 2)
        at = c - starts[kind]
        for f in range(n):
            rows = pl.ds(f * part, part)
            if kind == 1:
                k, j = at // thirds, rem(at, thirds)
                cols = pl.ds(aligned(f * hidden + j * ch), ch)
                pairs = [
                    (whole(slot).at[:, rows, lanes(h)], dst.at[k, :, :, cols])
                    for h, dst in enumerate((r.gg_h, r.gu_h))
                ]
            elif kind == 3:
                cols = pl.ds(f * kcols, kcols)
                pairs = [
                    (whole(slot).at[:, rows, lanes(0)], r.gq_h.at[at, :, :, pl.ds(f * ch, ch)]),
                    (whole(slot).at[:, rows, pl.ds(ch, kcols)], r.gk_h.at[at, :, :, cols]),
                    (whole(slot).at[:, rows, pl.ds(ch + kcols, kcols)], r.gv_h.at[at, :, :, cols]),
                ]
            else:
                dst = r.gd_h if kind == 0 else r.go_h
                pairs = [
                    (
                        whole(slot).at[f, :, lanes(h)],
                        dst.at[pl.ds(aligned(at * 256 + h * 128), 128), pl.ds(f * ch, ch)],
                    )
                    for h in range(2)
                ]
            for i, (src, to) in enumerate(pairs):
                yield pltpu.make_async_copy(src, to, r.gout_sem.at[two, f, i])

    def columns_of(ref, at, size):
        return ref[:, :, pl.ds(at, size)].reshape(tokens, size)

    def compute(c, kind):
        to = ours(rem(c, g_slots))
        at = c - starts[kind]
        if kind in (1, 3):
            left, right = (r.hn, r.dgu) if kind == 1 else (r.xn, r.dqkv)
            k, j = (at // thirds, rem(at, thirds)) if kind == 1 else (at, 0)
            lefts = jnp.concatenate(
                [columns_of(left, aligned(f * fold + k * 128), 128) for f in range(n)], axis=1
            )
            for h in range(2):
                product = tn(lefts, columns_of(right, aligned((2 * j + h) * ch), ch)).astype(BF16)
                for f in range(n):
                    block = product[f * 128 : (f + 1) * 128].reshape(rep, 128 // rep, ch)
                    to[:, f * part : (f + 1) * part, h * ch : (h + 1) * ch] = block
        else:
            left, right = (r.act, r.dy) if kind == 0 else (r.att, r.dab)
            lefts = columns_of(left, aligned(at * 256), 256)
            for q in range(rep):
                product = tn(lefts, columns_of(right, q * ch, ch)).astype(BF16)
                for h in range(2):
                    to[q, :, h * ch : (h + 1) * ch] = product[h * 128 : (h + 1) * 128]

    def tick(t, kinds=(0, 1, 2, 3)):
        def is_kind(c, kind):
            return within(c, starts[kind], starts[kind + 1])

        c_done = t - (2 * steps + 2)
        for kind in kinds:
            @when(is_kind(c_done, kind))
            def _():
                for copy in out_copies(c_done, kind):
                    copy.wait()

        c_out = t - (2 * steps + 1)

        @when(within(c_out, 0, total))
        def _():
            for copy in gather_copies(c_out, steps - 1):
                copy.wait()

        for kind in kinds:
            @when(is_kind(c_out, kind))
            def _():
                for copy in out_copies(c_out, kind):
                    copy.start()

        for j in reversed(range(1, steps)):
            c_ag = t - (steps + 1 + j)

            @when(within(c_ag, 0, total))
            def _():
                for copy in gather_copies(c_ag, j - 1):
                    copy.wait()
                for copy in gather_copies(c_ag, j):
                    copy.start()

        c_z = t - (steps + 1)
        for kind in kinds:
            @when(is_kind(c_z, kind))
            def _():
                if kind in (1, 3):
                    for copy in across_copies(c_z):
                        copy.wait()
                else:
                    for d in range(1, n):
                        pl.semaphore_wait(r.gsig.at[rem(c_z, 2), d - 1], 1)

        @when(within(c_z, 0, total))
        def _():
            for copy in gather_copies(c_z, 0):
                copy.start()

        for j in reversed(range(steps)):
            c_rs = t - (j + 1)

            @when(within(c_rs, 0, total))
            def _():
                for copy in scatter_copies(c_rs, j):
                    copy.wait()
                for h, bits in enumerate(orders):
                    half = slice(h * ch, (h + 1) * ch)
                    for i in range(rep >> (j + 1)):
                        piece = flips(mine, bits[j + 1 :], i)
                        value = ours(rem(c_rs, g_slots))[piece, :, half].astype(F32)
                        value = (value + got[j][rem(c_rs, 2), h, i].astype(F32)).astype(BF16)
                        if j < steps - 1:
                            ours(rem(c_rs, g_slots))[piece, :, half] = value
                        else:
                            r.reduced[:, half] = value
                if j < steps - 1:
                    for copy in scatter_copies(c_rs, j + 1):
                        copy.start()

            if j == steps - 1:
                for kind in kinds:
                    @when(is_kind(c_rs, kind))
                    def _():
                        to = whole(rem(c_rs, slots))
                        if kind in (1, 3):
                            for copy in across_copies(c_rs):
                                copy.start()
                            rows = pl.ds(pl.multiple_of(me * part, part), part)
                            to[mine, rows, :] = r.reduced[rows, :]
                        else:
                            for d in range(1, n):
                                pl.semaphore_signal(
                                    r.gsig.at[rem(c_rs, 2), d - 1], inc=1,
                                    device_id={"fsdp": lax.rem(me + d, n)}, device_id_type=MESH,
                                )
                            to[mine] = r.reduced[...]

        for kind in kinds:
            @when(is_kind(t, kind))
            def _():
                compute(t, kind)

        @when(within(t, 0, total))
        def _():
            for copy in scatter_copies(t, 0):
                copy.start()

    def pack_across(d):
        to = lax.rem(me + d, n)
        return remote(
            r.pack.at[to], r.pack_z.at[d - 1], r.pz_send.at[d - 1], r.pz_recv.at[d - 1], {"fsdp": to}
        )

    def pack_swap(j):
        return remote(
            r.pack_r.at[j], r.pack_in.at[j], r.pr_send.at[j], r.pr_recv.at[j],
            {"replica": flip(mine, j)},
        )

    def pack_fill(dgains):
        r.pack[...] = jnp.zeros_like(r.pack)
        at = 0
        for value in dgains:
            size = value.shape[-1] // n
            for f in range(n):
                r.pack[f, :, at : at + size] = value[:, f * size : (f + 1) * size]
            at += size

    def pack_start():
        for d in range(1, n):
            pack_across(d).start()

    def pack_tick(t):
        for j in range(steps + 1):
            @pl.when(t == 2 * j + 2)
            def _():
                if j == 0:
                    value = r.pack[me]
                    for d in range(1, n):
                        pack_across(d).wait()
                        value = value + r.pack_z[d - 1]
                else:
                    pack_swap(j - 1).wait()
                    value = r.pack_r[j - 1] + r.pack_in[j - 1]
                if j < steps:
                    r.pack_r[j] = value
                    pack_swap(j).start()
                else:
                    r.sums[...] = value

    def finish(first):
        def step(t, carry):
            tick(t)
            pack_tick(t - first)
            return carry

        lax.fori_loop(first, total + 2 * steps + 3, step, 0)

    return types.SimpleNamespace(
        tick=tick, pack_fill=pack_fill, pack_start=pack_start, finish=finish
    )


def stream_scratch(n, rep, ch, lanes):
    steps = rep.bit_length() - 1
    dma = pltpu.SemaphoreType.DMA
    swap = dma((steps, 2, 2, rep // 2))
    return {
        "reduced": pltpu.VMEM((128, 2 * ch), BF16),
        "pack": pltpu.VMEM((n, 1, lanes), F32),
        "pack_z": pltpu.VMEM((n - 1, 1, lanes), F32),
        "pack_r": pltpu.VMEM((steps, 1, lanes), F32),
        "pack_in": pltpu.VMEM((steps, 1, lanes), F32),
        **{
            f"got{j}": pltpu.VMEM((2, 2, rep >> (j + 1), 128, ch), BF16) for j in range(steps)
        },
        "grs_send": swap, "grs_recv": swap,
        "gz_send": dma((2, n - 1)), "gz_recv": dma((2, n - 1)),
        "gag_send": swap, "gag_recv": swap,
        "gout_sem": dma((2, n, 3)),
        "pz_send": dma((n - 1,)), "pz_recv": dma((n - 1,)),
        "pr_send": dma((steps,)), "pr_recv": dma((steps,)),
        "gsig": pltpu.SemaphoreType.REGULAR((2, n - 1)),
    }


def stream_outputs(n, rep, ch, hidden, width, lanes):
    kcols = ch // 2

    def owned(columns):
        return jax.ShapeDtypeStruct((width // n // 128, rep, 128 // rep, columns * n), BF16)

    return {
        "gq_h": owned(ch), "gk_h": owned(kcols), "gv_h": owned(kcols),
        "go_h": jax.ShapeDtypeStruct((ch, width), BF16),
        "gg_h": owned(hidden), "gu_h": owned(hidden),
        "gd_h": jax.ShapeDtypeStruct((hidden, width), BF16),
        "sums": jax.ShapeDtypeStruct((1, lanes), F32),
    }


def named(body, names, *args):
    def kernel(*refs):
        body(types.SimpleNamespace(**dict(zip(names, refs))), *args)

    return kernel


def call(body, args, inputs, outputs, scratch, in_vmem, out_vmem, name, collective):
    vm = pl.BlockSpec(memory_space=pltpu.VMEM)
    hbm = pl.BlockSpec(memory_space=pltpu.HBM)
    results = pl.pallas_call(
        named(body, [*inputs, *outputs, *scratch], *args),
        out_shape=list(outputs.values()),
        in_specs=[vm if key in in_vmem else hbm for key in inputs],
        out_specs=[vm if key in out_vmem else hbm for key in outputs],
        scratch_shapes=list(scratch.values()),
        compiler_params=pltpu.CompilerParams(
            collective_id=collective, has_side_effects=True, vmem_limit_bytes=67043328
        ),
        name=name,
    )(*inputs.values())
    return dict(zip(outputs, results))


def greet(n, rep, me, mine):
    barrier = pltpu.get_barrier_semaphore()
    for d in range(1, n):
        pl.semaphore_signal(
            barrier, inc=1, device_id={"fsdp": lax.rem(me + d, n)}, device_id_type=MESH
        )
    for bit in range(rep.bit_length() - 1):
        pl.semaphore_signal(
            barrier, inc=1, device_id={"replica": flip(mine, bit)}, device_id_type=MESH
        )
    return barrier


def grad_kernel(r, n, rep):
    me = lax.axis_index("fsdp")
    mine = lax.axis_index("replica")
    barrier = greet(n, rep, me, mine)
    loads = []
    for k, key in enumerate(("act", "dy", "hn", "dgu", "att", "dab", "xn", "dqkv")):
        loads.append(
            pltpu.make_async_copy(getattr(r, key + "_h"), getattr(r, key), r.in_sem.at[k])
        )
        loads[-1].start()
    stream = grad_stream(r, n, rep, lambda slot: r.ours.at[slot], lambda slot: r.whole.at[slot])
    stream.pack_fill((r.dln1, r.dln2, r.dqn, r.dkn))
    pl.semaphore_wait(barrier, n - 1 + rep.bit_length() - 1)
    for load in loads:
        load.wait()
    stream.pack_start()
    stream.finish(0)


def layer_kernel(r, n, rep, hd, fused):
    sec = lax.axis_index("section")
    me = lax.axis_index("fsdp")
    mine = lax.axis_index("replica")
    wq_h, wk_h, wv_h, wg_h, wu_h = r.wq_h, r.wk_h, r.wv_h, r.wg_h, r.wu_h
    cosine, sine, wall, wo, wd, ln1, ln2, qn, kn, gains = (
        r.cosine, r.sine, r.wall, r.wo, r.wd, r.ln1, r.ln2, r.qn, r.kn, r.gains
    )
    xin, xn_all, hn_all, dy_all, qkv, qkvb, att, hres, gate, up, act, dgu, dqkv = (
        r.xin, r.xn, r.hn, r.dy, r.qkv, r.qkvb, r.att, r.hres, r.gate, r.up, r.act, r.dgu, r.dqkv
    )
    dab_all = r.dab if fused else r.hn
    dob, yv, sbuf, rbuf, turn = r.dob, r.yv, r.sbuf, r.rbuf, r.turn
    dln1, dln2, dqn, dkn = r.dln1, r.dln2, r.dqn, r.dkn
    zw_send, zw_recv, gw_send, gw_recv, own_sem = r.zw_send, r.zw_recv, r.gw_send, r.gw_recv, r.own_sem
    ag_send, ag_recv, rs_send, rs_recv = r.ag_send, r.ag_recv, r.rs_send, r.rs_recv
    steps = rep.bit_length() - 1
    rows, width = xin.shape
    ch = att.shape[-1]
    qcols = ch
    kcols = (qkvb.shape[-1] - qcols) // 2
    hidden = act.shape[-1]
    chunks = wall.shape[0]
    share = wall.shape[3]
    kfold = rep * share
    scale = 1.0 / math.sqrt(hd)
    orders = (tuple(range(steps)), tuple(reversed(range(steps))))

    barrier = greet(n, rep, me, mine)
    pl.semaphore_signal(barrier, inc=1, device_id={"section": 1 - sec}, device_id_type=MESH)
    load_o = pltpu.make_async_copy(r.wo_h, wo, r.w_sem.at[0])
    load_d = pltpu.make_async_copy(r.wd_h, wd, r.w_sem.at[1])
    load_x = pltpu.make_async_copy(r.tok, xin, r.w_sem.at[2])
    load_y = pltpu.make_async_copy(r.cot, dy_all.at[me], r.w_sem.at[3])

    @pl.when(sec == 0)
    def _():
        load_x.start()

    @pl.when(sec == 1)
    def _():
        load_y.start()

    load_o.start()
    load_d.start()

    at = 0
    gain_at = []
    gains[me] = jnp.zeros_like(gains[me])
    for value in (r.ln1_own, r.ln2_own, r.qn_own, r.kn_own):
        size = value.shape[-1]
        gains[me, :, at : at + size] = value[...].astype(F32)
        gain_at.append((at, size))
        at += size
    pl.semaphore_wait(barrier, n + steps)

    def gain_copy(d):
        return remote(
            gains.at[me], gains.at[me], r.gain_send.at[d - 1], r.gain_recv.at[d - 1],
            {"fsdp": lax.rem(me + d, n)},
        )

    for d in range(1, n):
        gain_copy(d).start()

    def slabs(c, to):
        rows_in = pl.ds(pl.multiple_of(mine * share, share), share)
        if isinstance(c, int) and c == 0:
            return (
                (wq_h.at[rows_in, pl.ds(to * ch, ch)], pl.ds(0, ch)),
                (wk_h.at[rows_in, pl.ds(to * kcols, kcols)], pl.ds(ch, kcols)),
                (wv_h.at[rows_in, pl.ds(to * kcols, kcols)], pl.ds(ch + kcols, kcols)),
            )
        cols = pl.ds(pl.multiple_of(to * hidden + (c - 1) * ch, 128), ch)
        return (
            (wg_h.at[rows_in, cols], pl.ds(0, ch)),
            (wu_h.at[rows_in, cols], pl.ds(ch, ch)),
        )

    def slab_copies(c):
        for i, (src, lanes) in enumerate(slabs(c, me)):
            yield pltpu.make_async_copy(src, wall.at[c, me, mine, :, lanes], own_sem.at[c, i])
        for d in range(1, n):
            to = lax.rem(me + d, n)
            for i, (src, lanes) in enumerate(slabs(c, to)):
                yield remote(
                    src, wall.at[c, me, mine, :, lanes],
                    zw_send.at[c, d - 1, i], zw_recv.at[c, d - 1, i], {"fsdp": to},
                )

    def slab_gathers(c, j):
        for h, order in enumerate(orders):
            bits = order[::-1]
            partner = flip(mine, bits[j])
            for i in range(1 << j):
                piece = flips(mine, bits[:j], i)
                ref = wall.at[c, :, piece, :, pl.ds(h * ch, ch)]
                yield remote(
                    ref, ref, gw_send.at[j, c, h, i], gw_recv.at[j, c, h, i], {"replica": partner}
                )

    def prepare(c, j):
        for copy in slab_copies(c) if j == 0 else slab_gathers(c, j - 1):
            copy.wait()
        if j < steps:
            for copy in slab_gathers(c, j):
                copy.start()

    events = [
        (t - j, j) for t in range(2, chunks + steps) for j in range(steps) if 2 <= t - j < chunks
    ]
    events.sort(key=lambda event: (event[0] + event[1], -event[1]))
    places = [events[3 * k : 3 * k + 1] for k in range(n // 2 - 1)]
    middles = [events[3 * k + 1 : 3 * k + 3] for k in range(n // 2 - 1)]
    leftover = events[3 * (n // 2 - 1) :]

    def prepare_all(some):
        for event in some:
            prepare(*event)

    def prepare_first():
        for j in range(steps + 1):
            prepare(0, j)
            if j > 0:
                prepare(1, j - 1)

    bits = n.bit_length() - 1
    piece = width // n

    def low(m):
        return (m & -m).bit_length() - 1

    def across(s):
        return sum((me // 2**j + s // 2**j) % 2 * 2**j for j in range(bits))

    def spread(buf, c, m, j):
        ref = buf.at[flips(me, range(bits), m)]
        return remote(
            ref, ref, ag_send.at[c, m + 2**j], ag_recv.at[c, m + 2**j], {"fsdp": flip(me, j)}
        )

    def spread_start(buf, c):
        for j in range(bits):
            spread(buf, c, 0, j).start()

    def spread_done(buf, c):
        for m in range(n):
            for j in range(bits if m == 0 else low(m)):
                spread(buf, c, m, j).wait_send()

    def fold(c, m, k, j):
        cols = pl.ds(k * piece, piece)
        return remote(
            sbuf.at[c % 2, m, :, cols], rbuf.at[c % 2, m - 1, :, cols],
            rs_send.at[c, m, k], rs_recv.at[c, m, k], {"fsdp": flip(me, j)},
        )

    def each_pair(buf, c, work):
        def hear(s):
            ref = buf.at[across(s)]
            remote(
                ref, ref, ag_send.at[c, s], ag_recv.at[c, s], {"fsdp": flip(me, 0)}
            ).wait_recv()

        def step(q, carry):
            hear(2 * q + 1)

            def relay():
                for m in range(2, n, 2):
                    @pl.when(2 * q + 2 == m)
                    def _():
                        hear(m)
                        for j in range(low(m)):
                            spread(buf, c, m, j).start()

            def ship(k, value):
                for i in range(2):
                    part = value[i * rows : (i + 1) * rows].astype(BF16)
                    sbuf[c % 2, 2 * q + (me + i) % 2, :, k * piece : (k + 1) * piece] = part
                fold(c, 2 * q + 1, k, 0).start()

            work(q, across(2 * q) // 2 * 2, relay, ship)
            return carry

        lax.fori_loop(0, n // 2, step, 0)

    def settle_through(c):
        own, heard = sbuf.at[c % 2], rbuf.at[c % 2]
        for m in sorted(range(2, n, 2), key=low):
            for k in range(n):
                cols = slice(k * piece, (k + 1) * piece)
                value = own[m, :, cols].astype(F32)
                for j in range(low(m)):
                    fold(c, m + 2**j, k, j).wait_recv()
                    value = value + heard[m + 2**j - 1, :, cols].astype(F32)
                own[m, :, cols] = value.astype(BF16)
                fold(c, m, k, low(m)).start()

    def settle_own(c):
        for j in range(bits):
            for k in range(n):
                fold(c, 2**j, k, j).wait_recv()
        for m in range(1, n):
            for k in range(n):
                fold(c, m, k, low(m)).wait_send()

    def pair_of(buf, base):
        value = buf[pl.ds(base, 2)]
        return value.reshape(2 * rows, value.shape[-1])

    def summed(c, at):
        total = sbuf[c % 2, 0, at].astype(F32)
        for j in range(bits):
            total = total + rbuf[c % 2, 2**j - 1, at].astype(F32)
        return total

    def by_rows(work):
        height = 32

        def step(i, carry):
            work(pl.ds(pl.multiple_of(i * height, height), height))
            return carry

        lax.fori_loop(0, rows // height, step, 0)

    outs = {}
    put_keys = ("y", "dx", "xn", "hn", "dy", "dab", "att", "act", "dgu", "dqkv")

    def put(key, src):
        if hasattr(r, key + "_h"):
            copy = pltpu.make_async_copy(src, getattr(r, key + "_h"), r.out_sem.at[put_keys.index(key)])
            copy.start()
            outs[key] = copy

    def put_done(*keys):
        for key in keys:
            if key in outs:
                outs.pop(key).wait()

    def swap(value):
        return pltpu.roll(value, hd // 2, 1)

    def hand(src, dst, to, k):
        return pltpu.make_async_remote_copy(
            src_ref=src,
            dst_ref=dst,
            send_sem=r.hand_send.at[k],
            recv_sem=r.hand_recv.at[k],
            device_id={"section": to},
            device_id_type=MESH,
        )

    @pl.when(sec == 1)
    def _():
        pl.semaphore_wait(turn, 1)

    for c in range(2):
        for copy in slab_copies(c):
            copy.start()
    for d in range(1, n):
        gain_copy(d).wait()
    for k, full in enumerate((ln1, ln2, qn, kn)):
        at, size = gain_at[k]
        for f in range(n):
            full[:, f * size : (f + 1) * size] = gains[f, :, at : at + size]

    @pl.when(sec == 1)
    def _():
        prepare_first()
        hand(yv, xin, 0, 0).wait_recv()

    @pl.when(sec == 0)
    def _():
        load_x.wait()

    @by_rows
    def _(at):
        x32 = xin[at].astype(F32)
        r1 = lax.rsqrt(mean_last(x32 * x32) + EPS)
        xn_all[me, at] = (x32 * r1 * ln1[...]).astype(BF16)

    spread_start(xn_all, 0)
    for c in range(2, chunks):
        for copy in slab_copies(c):
            copy.start()

    @pl.when(sec == 0)
    def _():
        prepare_first()

    load_o.wait()
    load_d.wait()

    def masked_scores(qh, kh):
        raw = nt(qh, kh) * scale
        at_row = lax.broadcasted_iota(jnp.int32, raw.shape, 0)
        at_col = lax.broadcasted_iota(jnp.int32, raw.shape, 1)
        raw = jnp.where(at_row >= at_col, raw, -jnp.inf)
        top = jnp.max(raw, axis=-1, keepdims=True)
        lse = top + jnp.log(jnp.sum(jnp.exp(raw - top), axis=-1, keepdims=True))
        return jnp.exp(raw - lse)

    def attend_block(s):
        for at in range(0, qcols + kcols, hd):
            field = qkv[s, :, at : at + hd]
            gain = qn[...] if at < qcols else kn[...]
            factor = lax.rsqrt(mean_last(field * field) + EPS)
            normed = field * factor * gain
            turned = normed * cosine[...] + swap(normed) * sine[...]
            qkvb[s, :, at : at + hd] = turned.astype(BF16)
        qkvb[s, :, qcols + kcols :] = qkv[s, :, qcols + kcols :].astype(BF16)
        for j in range(qcols // hd):
            kv = j * kcols // qcols
            kat = qcols + kv * hd
            vat = qcols + kcols + kv * hd
            probs = masked_scores(qkvb[s, :, j * hd : (j + 1) * hd], qkvb[s, :, kat : kat + hd])
            attended = nn(probs.astype(BF16), qkvb[s, :, vat : vat + hd])
            att[s, :, j * hd : (j + 1) * hd] = attended.astype(BF16)
    def both(base, work):
        lax.fori_loop(0, 2, lambda i, carry: work(base + i) or carry, 0)

    def attend(q, base, relay, ship):
        for k, some in enumerate(places):
            @pl.when(q == k + 1)
            def _():
                prepare_all(some)

        a = pair_of(xn_all, base)
        for at, size in tiles(2 * ch):
            w = wall[0, :, :, :, at : at + size].reshape(width, size)
            qkv[pl.ds(base, 2), :, at : at + size] = nn(a, w).reshape(2, rows, size)
        relay()
        both(base, attend_block)
        for k, some in enumerate(middles):
            @pl.when(q == k + 1)
            def _():
                prepare_all(some)

        a = pair_of(att, base)
        for k in range(n):
            ship(k, nn(a, wo[:, k * piece : (k + 1) * piece]))

    each_pair(xn_all, 0, attend)
    settle_through(0)
    prepare_all(leftover[:1])
    settle_own(0)

    @by_rows
    def _(at):
        h = xin[at].astype(F32) + summed(0, at)
        hres[at] = h
        r2 = lax.rsqrt(mean_last(h * h) + EPS)
        hn_all[me, at] = (h * r2 * ln2[...]).astype(BF16)

    spread_start(hn_all, 1)
    put("xn", xn_all)
    put("att", att)

    prepare_all(leftover[1:])
    for c in range(1, chunks):
        prepare(c, steps)

    @pl.when(sec == 0)
    def _():
        pl.semaphore_signal(turn, inc=1, device_id={"section": 1}, device_id_type=MESH)

    def feed(q, base, relay, ship):
        a = pair_of(hn_all, base)
        here = pl.ds(base, 2)
        for at in range(0, hidden, ch):
            j = 1 + at // ch
            g = nn(a, wall[j, :, :, :, :ch].reshape(width, ch))
            u = nn(a, wall[j, :, :, :, ch:].reshape(width, ch))
            gate[here, :, at : at + ch] = g.astype(BF16).reshape(2, rows, ch)
            up[here, :, at : at + ch] = u.astype(BF16).reshape(2, rows, ch)
            value = (g * jax.nn.sigmoid(g) * u).astype(BF16)
            act[here, :, at : at + ch] = value.reshape(2, rows, ch)
        relay()

        @pl.when(jnp.logical_and(sec == 1, q == 0))
        def _():
            load_y.wait()
            spread_start(dy_all, 2)

        a = pair_of(act, base)
        for k in range(n):
            ship(k, nn(a, wd[:, k * piece : (k + 1) * piece]))

    each_pair(hn_all, 1, feed)

    def write_y():
        @by_rows
        def _(at):
            yv[at] = (hres[at] + summed(1, at)).astype(BF16)

    put("hn", hn_all)
    put("act", act)

    @pl.when(sec == 0)
    def _():
        settle_through(1)
        settle_own(1)
        write_y()
        hand(yv, xin, 1, 0).start()
        hand(yv, dy_all.at[me], 1, 1).wait_recv()
        spread_start(dy_all, 2)

    spread_done(hn_all, 1)
    put_done("hn")

    if fused:
        def place(slot):
            return wall.at[1 + slot // n, slot % n]

        view = types.SimpleNamespace(**{**vars(r), "hn": hn_all, "dab": dab_all})
        stream = grad_stream(view, n, rep, lambda slot: r.ours.at[slot], place)

    def early_tick(t):
        if fused:
            stream.tick(t, (0, 1))

    def early(low, high):
        if fused:
            lax.fori_loop(low, high, lambda t, carry: early_tick(t) or carry, 0)

    def feed_back(q, base, relay, ship):
        @pl.when(q == n // 2 - 1)
        def _():
            early_tick(0)

        a = pair_of(dy_all, base)
        here = pl.ds(base, 2)
        for at in range(0, hidden, ch):
            dact = nt(a, wd[at : at + ch, :])
            g = gate[here, :, at : at + ch].reshape(2 * rows, ch).astype(F32)
            u = up[here, :, at : at + ch].reshape(2 * rows, ch).astype(F32)
            sig = jax.nn.sigmoid(g)
            dg = (dact * u * sig * (1.0 + g * (1.0 - sig))).astype(BF16)
            du = (dact * g * sig).astype(BF16)
            dgu[here, :, 2 * at : 2 * at + ch] = dg.reshape(2, rows, ch)
            dgu[here, :, 2 * at + ch : 2 * at + 2 * ch] = du.reshape(2, rows, ch)
        relay()

        @pl.when(jnp.logical_and(sec == 1, q == n // 2 - 1))
        def _():
            settle_through(1)

        @pl.when(q == n // 2 - 1)
        def _():
            early_tick(1)

        a = pair_of(dgu, base)
        for f in range(n):
            total = jnp.zeros((2 * rows, kfold), F32)
            for j in range(1, chunks):
                w = wall[j, f].reshape(kfold, 2 * ch)
                total = total + nt(a[:, 2 * (j - 1) * ch : 2 * j * ch], w)
            ship(f, total)

    each_pair(dy_all, 2, feed_back)


    if fused:
        for where in [{"fsdp": lax.rem(me + d, n)} for d in range(1, n)] + [
            {"replica": flip(mine, bit)} for bit in range(steps)
        ]:
            pl.semaphore_signal(r.freed, inc=1, device_id=where, device_id_type=MESH)
    early_tick(2)
    settle_through(2)
    if fused:
        pl.semaphore_wait(r.freed, n - 1 + steps)
    early_tick(3)

    @pl.when(sec == 1)
    def _():
        settle_own(1)
        write_y()

    settle_own(2)
    dln2[...] = jnp.zeros_like(dln2)
    dln1[...] = jnp.zeros_like(dln1)

    @by_rows
    def _(at):
        dhn = summed(2, at)
        h = hres[at]
        r2 = lax.rsqrt(mean_last(h * h) + EPS)
        u = dhn * ln2[...]
        dh = dy_all[me, at].astype(F32) + (r2 * u - h * r2 * r2 * r2 * mean_last(u * h))
        dln2[...] += jnp.sum(dhn * h * r2, axis=0, keepdims=True)
        hres[at] = dh
        dab_all[me, at] = dh.astype(BF16)

    spread_start(dab_all, 3)
    early(4, 6)

    put("y", yv)
    put("dy", dy_all)
    put("dgu", dgu)

    dqn[...] = jnp.zeros_like(dqn)
    dkn[...] = jnp.zeros_like(dkn)

    def head_back(s, at, grad, gain, dgain):
        field = qkv[s, :, at : at + hd]
        factor = lax.rsqrt(mean_last(field * field) + EPS)
        grad = grad * cosine[...] - swap(grad) * sine[...]
        v = grad * gain
        back = factor * v - field * factor * factor * factor * mean_last(v * field)
        dgain[...] += jnp.sum(grad * field * factor, axis=0, keepdims=True)
        dqkv[s, :, at : at + hd] = back.astype(BF16)

    def attend_back_block(i, s):
        for kv in range(kcols // hd):
            kat = qcols + kv * hd
            vat = qcols + kcols + kv * hd
            kh = qkvb[s, :, kat : kat + hd]
            vh = qkvb[s, :, vat : vat + hd]
            dk = jnp.zeros((rows, hd), F32)
            dv = jnp.zeros((rows, hd), F32)
            for j in range(kv * qcols // kcols, (kv + 1) * qcols // kcols):
                qh = qkvb[s, :, j * hd : (j + 1) * hd]
                dh_out = dob[i, :, j * hd : (j + 1) * hd]
                probs = masked_scores(qh, kh)
                dv = dv + tn(probs.astype(BF16), dh_out)
                dp = nt(dh_out, vh)
                delta = jnp.sum(probs * dp, axis=-1, keepdims=True)
                ds = (probs * (dp - delta) * scale).astype(BF16)
                dk = dk + tn(ds, qh)
                head_back(s, j * hd, nn(ds, kh), qn[...], dqn)
            head_back(s, kat, dk, kn[...], dkn)
            dqkv[s, :, vat : vat + hd] = dv.astype(BF16)
    def attend_back(q, base, relay, ship):
        early_tick(6 + 2 * q)
        a = pair_of(dab_all, base)
        for at, size in tiles(qcols):
            dout = nt(a, wo[at : at + size, :]).astype(BF16)
            dob[:, :, at : at + size] = dout.reshape(2, rows, size)
        relay()
        early_tick(7 + 2 * q)
        lax.fori_loop(0, 2, lambda i, carry: attend_back_block(i, base + i) or carry, 0)
        a = pair_of(dqkv, base)
        for f in range(n):
            w = wall[0, f].reshape(kfold, 2 * ch)
            ship(f, nt(a, w))

    each_pair(dab_all, 3, attend_back)
    early_tick(6 + n)
    settle_through(3)
    early_tick(7 + n)
    settle_own(3)
    put_done("y")

    @pl.when(sec == 0)
    def _():
        hand(yv, xin, 1, 0).wait_send()

    @by_rows
    def _(at):
        dxn = summed(3, at)
        x32 = xin[at].astype(F32)
        r1 = lax.rsqrt(mean_last(x32 * x32) + EPS)
        u = dxn * ln1[...]
        dx = hres[at] + (r1 * u - x32 * r1 * r1 * r1 * mean_last(u * x32))
        dln1[...] += jnp.sum(dxn * x32 * r1, axis=0, keepdims=True)
        yv[at] = dx.astype(BF16)
        hres[at] = dx

    @pl.when(sec == 1)
    def _():
        hand(yv, dy_all.at[me], 0, 1).start()

    put("dx", hres)
    put("dab", dab_all)
    put("dqkv", dqkv)
    if fused:
        stream.pack_fill((dln1, dln2, dqn, dkn))
        stream.pack_start()
        stream.finish(8 + n)
    for c, buf in ((0, xn_all), (2, dy_all), (3, dab_all)):
        spread_done(buf, c)

    @pl.when(sec == 1)
    def _():
        hand(yv, dy_all.at[me], 0, 1).wait_send()

    put_done(*list(outs))


def run_layer(n, rep, fused, lanes, tok, cot, ln1, ln2, qn, kn, wq, wk, wv, wg, wu, wo, wd):
    rows, width = tok.shape
    hd = n * qn.shape[-1]
    qcols = wo.shape[0]
    qkvcols = 2 * qcols
    steps = rep.bit_length() - 1
    chunks = 1 + wd.shape[0] // qcols
    hidden = wd.shape[0]
    cosine, sine = rope_tables(rows, hd // 2)
    inputs = {
        "tok": tok, "cot": cot, "ln1_own": ln1, "ln2_own": ln2, "qn_own": qn, "kn_own": kn,
        "cosine": cosine, "sine": sine, "wq_h": wq, "wk_h": wk, "wv_h": wv, "wg_h": wg, "wu_h": wu,
        "wo_h": wo, "wd_h": wd,
    }
    in_vmem = ("ln1_own", "ln2_own", "qn_own", "kn_own", "cosine", "sine")
    single = {"dln1": (1, width), "dln2": (1, width), "dqn": (1, hd), "dkn": (1, hd)}
    outputs = {
        "y_h": jax.ShapeDtypeStruct((rows, width), BF16),
        "dx_h": jax.ShapeDtypeStruct((rows, width), F32),
    }
    saved = {
        "xn": width, "hn": width, "dy": width, "dab": width, "att": qcols, "act": hidden,
        "dgu": 2 * hidden, "dqkv": qkvcols,
    }
    dma = pltpu.SemaphoreType.DMA
    scratch = {
        "wall": pltpu.VMEM((chunks, n, rep, width // (n * rep), qkvcols), BF16),
        "wo": pltpu.VMEM(wo.shape, BF16),
        "wd": pltpu.VMEM(wd.shape, BF16),
        "ln1": pltpu.VMEM((1, width), F32),
        "ln2": pltpu.VMEM((1, width), F32),
        "qn": pltpu.VMEM((1, hd), F32),
        "kn": pltpu.VMEM((1, hd), F32),
        "gains": pltpu.VMEM((n, 1, lanes), F32),
        "xin": pltpu.VMEM((rows, width), BF16),
        **{
            key: pltpu.VMEM((n, rows, size), BF16)
            for key, size in saved.items() if fused or key != "dab"
        },
        "qkv": pltpu.VMEM((n, rows, qkvcols), F32),
        "qkvb": pltpu.VMEM((n, rows, qkvcols), BF16),
        "hres": pltpu.VMEM((rows, width), F32),
        "gate": pltpu.VMEM((n, rows, hidden), BF16),
        "up": pltpu.VMEM((n, rows, hidden), BF16),
        "dob": pltpu.VMEM((2, rows, qcols), BF16),
        "yv": pltpu.VMEM((rows, width), BF16),
        "sbuf": pltpu.VMEM((2, n, rows, width), BF16),
        "rbuf": pltpu.VMEM((2, n - 1, rows, width), BF16),
        "w_sem": dma((4,)),
        "zw_send": dma((chunks, n - 1, 3)),
        "zw_recv": dma((chunks, n - 1, 3)),
        "gw_send": dma((steps, chunks, 2, rep // 2)),
        "gw_recv": dma((steps, chunks, 2, rep // 2)),
        "own_sem": dma((chunks, 3)),
        "gain_send": dma((n - 1,)),
        "gain_recv": dma((n - 1,)),
        "turn": pltpu.SemaphoreType.REGULAR,
        "out_sem": dma((10,)),
        "ag_send": dma((4, n)),
        "ag_recv": dma((4, n)),
        "rs_send": dma((4, n, n)),
        "rs_recv": dma((4, n, n)),
        "hand_send": dma((2,)),
        "hand_recv": dma((2,)),
    }
    if fused:
        outputs |= stream_outputs(n, rep, qcols, hidden, width, lanes)
        scratch |= {key: pltpu.VMEM(shape, F32) for key, shape in single.items()}
        scratch |= stream_scratch(n, rep, qcols, lanes)
        scratch["freed"] = pltpu.SemaphoreType.REGULAR
        scratch["ours"] = pltpu.VMEM((steps + 1, rep, 128, 2 * qcols), BF16)
    else:
        outputs |= {
            key + "_h": jax.ShapeDtypeStruct((n, rows, size), BF16) for key, size in saved.items()
        }
        outputs |= {key: jax.ShapeDtypeStruct(shape, F32) for key, shape in single.items()}
    out_vmem = (*single, "sums")
    return call(
        layer_kernel, (n, rep, hd, fused), inputs, outputs, scratch, in_vmem, out_vmem, "layer", 0
    )


def run_grads(n, rep, saved, lanes):
    steps = rep.bit_length() - 1
    ch, hidden, width = (saved[key].shape[-1] for key in ("att_h", "act_h", "xn_h"))
    inputs = {key: value for key, value in saved.items() if key not in ("y_h", "dx_h")}
    scratch = {
        key[:-2]: pltpu.VMEM(value.shape, BF16) for key, value in inputs.items() if key[-2:] == "_h"
    }
    scratch["ours"] = pltpu.VMEM((steps + 1, rep, 128, 2 * ch), BF16)
    scratch["whole"] = pltpu.VMEM((steps + 3, rep, 128, 2 * ch), BF16)
    scratch["in_sem"] = pltpu.SemaphoreType.DMA((8,))
    scratch |= stream_scratch(n, rep, ch, lanes)
    outputs = stream_outputs(n, rep, ch, hidden, width, lanes)
    small = ("dln1", "dln2", "dqn", "dkn")
    return call(grad_kernel, (n, rep), inputs, outputs, scratch, small, ("sums",), "grads", 1)


def per_device(tokens_in, cotangent, ln1, wq, wk, wv, qn, kn, wo, ln2, wg, wu, wd):
    n, rep = lax.axis_size("fsdp"), lax.axis_size("replica")

    lanes = -(-2 * (ln1.shape[-1] + qn.shape[-1]) // 128) * 128
    thirds = grad_plan(n, wo.shape[1], wd.shape[1], wo.shape[2])[1]
    fused = (2 * rep.bit_length() + 2) <= n * thirds and wq.shape[1] == n * 128
    done = run_layer(
        n, rep, fused, lanes, tokens_in, cotangent, ln1, ln2, qn, kn,
        wq[0], wk[0], wv[0], wg[0], wu[0], wo[0], wd[0],
    )
    y, dx = done["y_h"], done["dx_h"]
    if not fused:
        done = run_grads(n, rep, done, lanes)
    g_wq, g_wk, g_wv, g_wo, g_wg, g_wu, g_wd = (
        done[key].reshape(-1, done[key].shape[-1]).astype(F32)
        for key in ("gq_h", "gk_h", "gv_h", "go_h", "gg_h", "gu_h", "gd_h")
    )
    sums = done["sums"]
    owned, at = [], 0
    for gain in (ln1, ln2, qn, kn):
        owned.append(sums[0, at : at + gain.shape[1]])
        at += gain.shape[1]
    g_ln1, g_ln2, g_qn, g_kn = owned
    results = (y, dx, g_ln1, g_wq, g_wk, g_wv, g_qn, g_kn, g_wo, g_ln2, g_wg, g_wu, g_wd)
    return tuple(value[None] for value in results)


def solution(mesh):
    rows = P("section", "fsdp", None)
    gain = P("section", "fsdp")
    tokens = P(("fsdp", "replica"), None)
    stacked = P("section", ("fsdp", "replica"), None)
    weights = (gain, rows, rows, rows, gain, gain, rows, gain, rows, rows, rows)
    return jax.shard_map(
        per_device,
        mesh=mesh,
        in_specs=(tokens, tokens, *weights),
        out_specs=(stacked, stacked, *weights),
        check_vma=False,
    )
```

```python
import functools
import math
import types

import jax
import jax.numpy as jnp
from jax import lax
from jax.experimental import pallas as pl
from jax.experimental.pallas import tpu as pltpu
from jax.sharding import PartitionSpec as P

LEN = 128
EPS = 1e-06
F32 = jnp.float32
BF16 = jnp.bfloat16
MESH = pl.DeviceIdType.MESH
TILE = 512


def rope_tables(length, half_dim):
    freq = jnp.exp(jnp.arange(half_dim, dtype=F32) * (-math.log(1000000.0) / half_dim))
    angle = jnp.arange(length, dtype=F32)[:, None] * freq[None, :]
    cosine, sine = jnp.cos(angle), jnp.sin(angle)
    return (
        jnp.concatenate([cosine, cosine], axis=1),
        jnp.concatenate([-sine, sine], axis=1),
    )


def nn(left, right):
    return jnp.dot(left, right, preferred_element_type=F32)


def nt(left, right):
    return lax.dot_general(left, right, (((1,), (1,)), ((), ())), preferred_element_type=F32)


def tn(left, right):
    return lax.dot_general(left, right, (((0,), (0,)), ((), ())), preferred_element_type=F32)


def mean_last(value):
    return jnp.mean(value, axis=-1, keepdims=True)


def tiles(total):
    return [(at, min(TILE, total - at)) for at in range(0, total, TILE)]


def flip(value, bit):
    return value + (1 - 2 * (value // 2**bit % 2)) * 2**bit


def flips(value, bits, subset):
    for at, bit in enumerate(bits):
        if subset >> at & 1:
            value = flip(value, bit)
    return value


def grad_plan(n, qcols, hidden, width):
    blocks = width // n // 128
    thirds = hidden // qcols
    return blocks, thirds, (hidden // 256, blocks * thirds, qcols // 256, blocks)


def rem(value, by):
    return value % by if isinstance(value, int) else lax.rem(value, by)


def within(value, low, high):
    if isinstance(value, int):
        return low <= value < high
    return jnp.logical_and(value >= low, value < high)


def when(condition):
    if isinstance(condition, bool):
        return lambda work: work() if condition else None
    return pl.when(condition)


def remote(src, dst, send, recv, where):
    return pltpu.make_async_remote_copy(
        src_ref=src, dst_ref=dst, send_sem=send, recv_sem=recv,
        device_id=where, device_id_type=MESH,
    )


def grad_stream(r, n, rep, ours, whole):
    me = lax.axis_index("fsdp")
    mine = lax.axis_index("replica")
    steps = rep.bit_length() - 1
    g_slots, slots = steps + 1, steps + 3
    ch = r.att.shape[-1]
    part = 128 // n
    width = r.xn.shape[-1]
    tokens = r.xn.shape[0] * r.xn.shape[1]
    fold = width // n
    hidden = r.act.shape[-1]
    kcols = r.gk_h.shape[-1] // n
    thirds = grad_plan(n, ch, hidden, width)[1]
    counts = grad_plan(n, ch, hidden, width)[2]
    starts = [sum(counts[:k]) for k in range(len(counts) + 1)]
    total = starts[-1]
    orders = (tuple(range(steps)), tuple(reversed(range(steps))))
    got = [getattr(r, f"got{j}") for j in range(steps)]

    def lanes(h):
        return pl.ds(h * ch, ch)

    def scatter_copies(c, j):
        slot, two = rem(c, g_slots), rem(c, 2)
        for h, bits in enumerate(orders):
            partner = flip(mine, bits[j])
            for i in range(rep >> (j + 1)):
                piece = flips(partner, bits[j + 1 :], i)
                yield remote(
                    ours(slot).at[piece, :, lanes(h)], got[j].at[two, h, i],
                    r.grs_send.at[j, two, h, i], r.grs_recv.at[j, two, h, i],
                    {"replica": partner},
                )

    def across_copies(c):
        slot, two = rem(c, slots), rem(c, 2)
        for d in range(1, n):
            to = lax.rem(me + d, n)
            yield remote(
                r.reduced.at[pl.ds(to * part, part), :],
                whole(slot).at[mine, pl.ds(me * part, part), :],
                r.gz_send.at[two, d - 1], r.gz_recv.at[two, d - 1], {"fsdp": to},
            )

    def gather_copies(c, j):
        slot, two = rem(c, slots), rem(c, 2)
        for h, order in enumerate(orders):
            bits = order[::-1]
            partner = flip(mine, bits[j])
            for i in range(1 << j):
                ref = whole(slot).at[flips(mine, bits[:j], i), :, lanes(h)]
                yield remote(
                    ref, ref, r.gag_send.at[j, two, h, i], r.gag_recv.at[j, two, h, i],
                    {"replica": partner},
                )

    def aligned(at):
        return pl.multiple_of(at, 128)

    def out_copies(c, kind):
        slot, two = rem(c, slots), rem(c, 2)
        at = c - starts[kind]
        for f in range(n):
            rows = pl.ds(f * part, part)
            if kind == 1:
                k, j = at // thirds, rem(at, thirds)
                cols = pl.ds(aligned(f * hidden + j * ch), ch)
                pairs = [
                    (whole(slot).at[:, rows, lanes(h)], dst.at[k, :, :, cols])
                    for h, dst in enumerate((r.gg_h, r.gu_h))
                ]
            elif kind == 3:
                cols = pl.ds(f * kcols, kcols)
                pairs = [
                    (whole(slot).at[:, rows, lanes(0)], r.gq_h.at[at, :, :, pl.ds(f * ch, ch)]),
                    (whole(slot).at[:, rows, pl.ds(ch, kcols)], r.gk_h.at[at, :, :, cols]),
                    (whole(slot).at[:, rows, pl.ds(ch + kcols, kcols)], r.gv_h.at[at, :, :, cols]),
                ]
            else:
                dst = r.gd_h if kind == 0 else r.go_h
                pairs = [
                    (
                        whole(slot).at[f, :, lanes(h)],
                        dst.at[pl.ds(aligned(at * 256 + h * 128), 128), pl.ds(f * ch, ch)],
                    )
                    for h in range(2)
                ]
            for i, (src, to) in enumerate(pairs):
                yield pltpu.make_async_copy(src, to, r.gout_sem.at[two, f, i])

    def columns_of(ref, at, size):
        return ref[:, :, pl.ds(at, size)].reshape(tokens, size)

    def compute(c, kind):
        to = ours(rem(c, g_slots))
        at = c - starts[kind]
        if kind in (1, 3):
            left, right = (r.hn, r.dgu) if kind == 1 else (r.xn, r.dqkv)
            k, j = (at // thirds, rem(at, thirds)) if kind == 1 else (at, 0)
            lefts = jnp.concatenate(
                [columns_of(left, aligned(f * fold + k * 128), 128) for f in range(n)], axis=1
            )
            for h in range(2):
                product = tn(lefts, columns_of(right, aligned((2 * j + h) * ch), ch)).astype(BF16)
                for f in range(n):
                    block = product[f * 128 : (f + 1) * 128].reshape(rep, 128 // rep, ch)
                    to[:, f * part : (f + 1) * part, h * ch : (h + 1) * ch] = block
        else:
            left, right = (r.act, r.dy) if kind == 0 else (r.att, r.dab)
            lefts = columns_of(left, aligned(at * 256), 256)
            for q in range(rep):
                product = tn(lefts, columns_of(right, q * ch, ch)).astype(BF16)
                for h in range(2):
                    to[q, :, h * ch : (h + 1) * ch] = product[h * 128 : (h + 1) * 128]

    def tick(t, kinds=(0, 1, 2, 3)):
        def is_kind(c, kind):
            return within(c, starts[kind], starts[kind + 1])

        c_done = t - (2 * steps + 2)
        for kind in kinds:
            @when(is_kind(c_done, kind))
            def _():
                for copy in out_copies(c_done, kind):
                    copy.wait()

        c_out = t - (2 * steps + 1)

        @when(within(c_out, 0, total))
        def _():
            for copy in gather_copies(c_out, steps - 1):
                copy.wait()

        for kind in kinds:
            @when(is_kind(c_out, kind))
            def _():
                for copy in out_copies(c_out, kind):
                    copy.start()

        for j in reversed(range(1, steps)):
            c_ag = t - (steps + 1 + j)

            @when(within(c_ag, 0, total))
            def _():
                for copy in gather_copies(c_ag, j - 1):
                    copy.wait()
                for copy in gather_copies(c_ag, j):
                    copy.start()

        c_z = t - (steps + 1)
        for kind in kinds:
            @when(is_kind(c_z, kind))
            def _():
                if kind in (1, 3):
                    for copy in across_copies(c_z):
                        copy.wait()
                else:
                    for d in range(1, n):
                        pl.semaphore_wait(r.gsig.at[rem(c_z, 2), d - 1], 1)

        @when(within(c_z, 0, total))
        def _():
            for copy in gather_copies(c_z, 0):
                copy.start()

        for j in reversed(range(steps)):
            c_rs = t - (j + 1)

            @when(within(c_rs, 0, total))
            def _():
                for copy in scatter_copies(c_rs, j):
                    copy.wait()
                for h, bits in enumerate(orders):
                    half = slice(h * ch, (h + 1) * ch)
                    for i in range(rep >> (j + 1)):
                        piece = flips(mine, bits[j + 1 :], i)
                        value = ours(rem(c_rs, g_slots))[piece, :, half].astype(F32)
                        value = (value + got[j][rem(c_rs, 2), h, i].astype(F32)).astype(BF16)
                        if j < steps - 1:
                            ours(rem(c_rs, g_slots))[piece, :, half] = value
                        else:
                            r.reduced[:, half] = value
                if j < steps - 1:
                    for copy in scatter_copies(c_rs, j + 1):
                        copy.start()

            if j == steps - 1:
                for kind in kinds:
                    @when(is_kind(c_rs, kind))
                    def _():
                        to = whole(rem(c_rs, slots))
                        if kind in (1, 3):
                            for copy in across_copies(c_rs):
                                copy.start()
                            rows = pl.ds(pl.multiple_of(me * part, part), part)
                            to[mine, rows, :] = r.reduced[rows, :]
                        else:
                            for d in range(1, n):
                                pl.semaphore_signal(
                                    r.gsig.at[rem(c_rs, 2), d - 1], inc=1,
                                    device_id={"fsdp": lax.rem(me + d, n)}, device_id_type=MESH,
                                )
                            to[mine] = r.reduced[...]

        @when(within(t, 0, total))
        def _():
            for copy in scatter_copies(t, 0):
                copy.start()

        for kind in kinds:
            @when(is_kind(t + 1, kind))
            def _():
                compute(t + 1, kind)

    def pack_across(d):
        to = lax.rem(me + d, n)
        return remote(
            r.pack.at[to], r.pack_z.at[d - 1], r.pz_send.at[d - 1], r.pz_recv.at[d - 1], {"fsdp": to}
        )

    def pack_swap(j):
        return remote(
            r.pack_r.at[j], r.pack_in.at[j], r.pr_send.at[j], r.pr_recv.at[j],
            {"replica": flip(mine, j)},
        )

    def pack_fill(dgains):
        r.pack[...] = jnp.zeros_like(r.pack)
        at = 0
        for value in dgains:
            size = value.shape[-1] // n
            for f in range(n):
                r.pack[f, :, at : at + size] = value[:, f * size : (f + 1) * size]
            at += size

    def pack_start():
        for d in range(1, n):
            pack_across(d).start()

    def pack_tick(t):
        for j in range(steps + 1):
            @pl.when(t == 2 * j + 2)
            def _():
                if j == 0:
                    value = r.pack[me]
                    for d in range(1, n):
                        pack_across(d).wait()
                        value = value + r.pack_z[d - 1]
                else:
                    pack_swap(j - 1).wait()
                    value = r.pack_r[j - 1] + r.pack_in[j - 1]
                if j < steps:
                    r.pack_r[j] = value
                    pack_swap(j).start()
                else:
                    r.sums[...] = value

    def finish(first):
        def step(t, carry):
            tick(t)
            pack_tick(t - first)
            return carry

        lax.fori_loop(first, total + 2 * steps + 3, step, 0)

    return types.SimpleNamespace(
        tick=tick, prime=lambda kind: compute(0, kind), pack_fill=pack_fill, pack_start=pack_start, finish=finish
    )


def stream_scratch(n, rep, ch, lanes):
    steps = rep.bit_length() - 1
    dma = pltpu.SemaphoreType.DMA
    swap = dma((steps, 2, 2, rep // 2))
    return {
        "reduced": pltpu.VMEM((128, 2 * ch), BF16),
        "pack": pltpu.VMEM((n, 1, lanes), F32),
        "pack_z": pltpu.VMEM((n - 1, 1, lanes), F32),
        "pack_r": pltpu.VMEM((steps, 1, lanes), F32),
        "pack_in": pltpu.VMEM((steps, 1, lanes), F32),
        **{
            f"got{j}": pltpu.VMEM((2, 2, rep >> (j + 1), 128, ch), BF16) for j in range(steps)
        },
        "grs_send": swap, "grs_recv": swap,
        "gz_send": dma((2, n - 1)), "gz_recv": dma((2, n - 1)),
        "gag_send": swap, "gag_recv": swap,
        "gout_sem": dma((2, n, 3)),
        "pz_send": dma((n - 1,)), "pz_recv": dma((n - 1,)),
        "pr_send": dma((steps,)), "pr_recv": dma((steps,)),
        "gsig": pltpu.SemaphoreType.REGULAR((2, n - 1)),
    }


def stream_outputs(n, rep, ch, hidden, width, lanes):
    kcols = ch // 2

    def owned(columns):
        return jax.ShapeDtypeStruct((width // n // 128, rep, 128 // rep, columns * n), BF16)

    return {
        "gq_h": owned(ch), "gk_h": owned(kcols), "gv_h": owned(kcols),
        "go_h": jax.ShapeDtypeStruct((ch, width), BF16),
        "gg_h": owned(hidden), "gu_h": owned(hidden),
        "gd_h": jax.ShapeDtypeStruct((hidden, width), BF16),
        "sums": jax.ShapeDtypeStruct((1, lanes), F32),
    }


def named(body, names, *args):
    def kernel(*refs):
        body(types.SimpleNamespace(**dict(zip(names, refs))), *args)

    return kernel


def call(body, args, inputs, outputs, scratch, in_vmem, out_vmem, name, collective):
    vm = pl.BlockSpec(memory_space=pltpu.VMEM)
    hbm = pl.BlockSpec(memory_space=pltpu.HBM)
    results = pl.pallas_call(
        named(body, [*inputs, *outputs, *scratch], *args),
        out_shape=list(outputs.values()),
        in_specs=[vm if key in in_vmem else hbm for key in inputs],
        out_specs=[vm if key in out_vmem else hbm for key in outputs],
        scratch_shapes=list(scratch.values()),
        compiler_params=pltpu.CompilerParams(
            collective_id=collective, has_side_effects=True, vmem_limit_bytes=67043328
        ),
        name=name,
    )(*inputs.values())
    return dict(zip(outputs, results))


def greet(n, rep, me, mine):
    barrier = pltpu.get_barrier_semaphore()
    for d in range(1, n):
        pl.semaphore_signal(
            barrier, inc=1, device_id={"fsdp": lax.rem(me + d, n)}, device_id_type=MESH
        )
    for bit in range(rep.bit_length() - 1):
        pl.semaphore_signal(
            barrier, inc=1, device_id={"replica": flip(mine, bit)}, device_id_type=MESH
        )
    return barrier


def grad_kernel(r, n, rep):
    me = lax.axis_index("fsdp")
    mine = lax.axis_index("replica")
    barrier = greet(n, rep, me, mine)
    loads = []
    for k, key in enumerate(("act", "dy", "hn", "dgu", "att", "dab", "xn", "dqkv")):
        loads.append(
            pltpu.make_async_copy(getattr(r, key + "_h"), getattr(r, key), r.in_sem.at[k])
        )
        loads[-1].start()
    stream = grad_stream(r, n, rep, lambda slot: r.ours.at[slot], lambda slot: r.whole.at[slot])
    stream.pack_fill((r.dln1, r.dln2, r.dqn, r.dkn))
    pl.semaphore_wait(barrier, n - 1 + rep.bit_length() - 1)
    for load in loads:
        load.wait()
    stream.pack_start()
    stream.prime(0)
    stream.finish(0)


def layer_kernel(r, n, rep, hd, fused):
    sec = lax.axis_index("section")
    me = lax.axis_index("fsdp")
    mine = lax.axis_index("replica")
    wq_h, wk_h, wv_h, wg_h, wu_h = r.wq_h, r.wk_h, r.wv_h, r.wg_h, r.wu_h
    cosine, sine, wall, wo, wd, ln1, ln2, qn, kn, gains = (
        r.cosine, r.sine, r.wall, r.wo, r.wd, r.ln1, r.ln2, r.qn, r.kn, r.gains
    )
    xin, xn_all, hn_all, dy_all, qkv, qkvb, att, hres, gate, up, act, dgu, dqkv = (
        r.xin, r.xn, r.hn, r.dy, r.qkv, r.qkvb, r.att, r.hres, r.gate, r.up, r.act, r.dgu, r.dqkv
    )
    dab_all = r.dab if fused else r.hn
    dob, yv, sbuf, rbuf, turn = r.dob, r.yv, r.sbuf, r.rbuf, r.turn
    dln1, dln2, dqn, dkn = r.dln1, r.dln2, r.dqn, r.dkn
    zw_send, zw_recv, gw_send, gw_recv, own_sem = r.zw_send, r.zw_recv, r.gw_send, r.gw_recv, r.own_sem
    ag_send, ag_recv, rs_send, rs_recv = r.ag_send, r.ag_recv, r.rs_send, r.rs_recv
    steps = rep.bit_length() - 1
    rows, width = xin.shape
    ch = att.shape[-1]
    qcols = ch
    kcols = (qkvb.shape[-1] - qcols) // 2
    hidden = act.shape[-1]
    chunks = wall.shape[0]
    share = wall.shape[3]
    kfold = rep * share
    scale = 1.0 / math.sqrt(hd)
    orders = (tuple(range(steps)), tuple(reversed(range(steps))))

    barrier = greet(n, rep, me, mine)
    pl.semaphore_signal(barrier, inc=1, device_id={"section": 1 - sec}, device_id_type=MESH)
    load_o = pltpu.make_async_copy(r.wo_h, wo, r.w_sem.at[0])
    load_d = pltpu.make_async_copy(r.wd_h, wd, r.w_sem.at[1])
    load_x = pltpu.make_async_copy(r.tok, xin, r.w_sem.at[2])
    load_y = pltpu.make_async_copy(r.cot, dy_all.at[me], r.w_sem.at[3])

    @pl.when(sec == 0)
    def _():
        load_x.start()

    @pl.when(sec == 1)
    def _():
        load_y.start()

    load_o.start()
    load_d.start()

    at = 0
    gain_at = []
    gains[me] = jnp.zeros_like(gains[me])
    for value in (r.ln1_own, r.ln2_own, r.qn_own, r.kn_own):
        size = value.shape[-1]
        gains[me, :, at : at + size] = value[...].astype(F32)
        gain_at.append((at, size))
        at += size
    pl.semaphore_wait(barrier, n + steps)

    def gain_copy(d):
        return remote(
            gains.at[me], gains.at[me], r.gain_send.at[d - 1], r.gain_recv.at[d - 1],
            {"fsdp": lax.rem(me + d, n)},
        )

    for d in range(1, n):
        gain_copy(d).start()

    def slabs(c, to):
        rows_in = pl.ds(pl.multiple_of(mine * share, share), share)
        if isinstance(c, int) and c == 0:
            return (
                (wq_h.at[rows_in, pl.ds(to * ch, ch)], pl.ds(0, ch)),
                (wk_h.at[rows_in, pl.ds(to * kcols, kcols)], pl.ds(ch, kcols)),
                (wv_h.at[rows_in, pl.ds(to * kcols, kcols)], pl.ds(ch + kcols, kcols)),
            )
        cols = pl.ds(pl.multiple_of(to * hidden + (c - 1) * ch, 128), ch)
        return (
            (wg_h.at[rows_in, cols], pl.ds(0, ch)),
            (wu_h.at[rows_in, cols], pl.ds(ch, ch)),
        )

    def slab_copies(c):
        for i, (src, lanes) in enumerate(slabs(c, me)):
            yield pltpu.make_async_copy(src, wall.at[c, me, mine, :, lanes], own_sem.at[c, i])
        for d in range(1, n):
            to = lax.rem(me + d, n)
            for i, (src, lanes) in enumerate(slabs(c, to)):
                yield remote(
                    src, wall.at[c, me, mine, :, lanes],
                    zw_send.at[c, d - 1, i], zw_recv.at[c, d - 1, i], {"fsdp": to},
                )

    def slab_gathers(c, j):
        for h, order in enumerate(orders):
            bits = order[::-1]
            partner = flip(mine, bits[j])
            for i in range(1 << j):
                piece = flips(mine, bits[:j], i)
                ref = wall.at[c, :, piece, :, pl.ds(h * ch, ch)]
                yield remote(
                    ref, ref, gw_send.at[j, c, h, i], gw_recv.at[j, c, h, i], {"replica": partner}
                )

    def prepare(c, j):
        for copy in slab_copies(c) if j == 0 else slab_gathers(c, j - 1):
            copy.wait()
        if j < steps:
            for copy in slab_gathers(c, j):
                copy.start()

    events = [
        (t - j, j) for t in range(2, chunks + steps) for j in range(steps) if 2 <= t - j < chunks
    ]
    events.sort(key=lambda event: (event[0] + event[1], -event[1]))
    places = [events[3 * k : 3 * k + 1] for k in range(n // 2 - 1)]
    middles = [events[3 * k + 1 : 3 * k + 3] for k in range(n // 2 - 1)]
    leftover = events[3 * (n // 2 - 1) :]

    def prepare_all(some):
        for event in some:
            prepare(*event)

    def prepare_first():
        for j in range(steps + 1):
            prepare(0, j)
            if j > 0:
                prepare(1, j - 1)

    bits = n.bit_length() - 1
    piece = width // n

    def low(m):
        return (m & -m).bit_length() - 1

    def across(s):
        return sum((me // 2**j + s // 2**j) % 2 * 2**j for j in range(bits))

    def spread(buf, c, m, j):
        ref = buf.at[flips(me, range(bits), m)]
        return remote(
            ref, ref, ag_send.at[c, m + 2**j], ag_recv.at[c, m + 2**j], {"fsdp": flip(me, j)}
        )

    def spread_start(buf, c):
        for j in range(bits):
            spread(buf, c, 0, j).start()

    def spread_done(buf, c):
        for m in range(n):
            for j in range(bits if m == 0 else low(m)):
                spread(buf, c, m, j).wait_send()

    def fold(c, m, k, j):
        cols = pl.ds(k * piece, piece)
        return remote(
            sbuf.at[c % 2, m, :, cols], rbuf.at[c % 2, m - 1, :, cols],
            rs_send.at[c, m, k], rs_recv.at[c, m, k], {"fsdp": flip(me, j)},
        )

    def each_pair(buf, c, work):
        def hear(s):
            ref = buf.at[across(s)]
            remote(
                ref, ref, ag_send.at[c, s], ag_recv.at[c, s], {"fsdp": flip(me, 0)}
            ).wait_recv()

        def step(q, carry):
            hear(2 * q + 1)

            def relay():
                for m in range(2, n, 2):
                    @pl.when(2 * q + 2 == m)
                    def _():
                        hear(m)
                        for j in range(low(m)):
                            spread(buf, c, m, j).start()

            def ship(k, value):
                for i in range(2):
                    part = value[i * rows : (i + 1) * rows].astype(BF16)
                    sbuf[c % 2, 2 * q + (me + i) % 2, :, k * piece : (k + 1) * piece] = part
                fold(c, 2 * q + 1, k, 0).start()

            work(q, across(2 * q) // 2 * 2, relay, ship)
            return carry

        lax.fori_loop(0, n // 2, step, 0)

    def settle_through(c):
        own, heard = sbuf.at[c % 2], rbuf.at[c % 2]
        for m in sorted(range(2, n, 2), key=low):
            for k in range(n):
                cols = slice(k * piece, (k + 1) * piece)
                value = own[m, :, cols].astype(F32)
                for j in range(low(m)):
                    fold(c, m + 2**j, k, j).wait_recv()
                    value = value + heard[m + 2**j - 1, :, cols].astype(F32)
                own[m, :, cols] = value.astype(BF16)
                fold(c, m, k, low(m)).start()

    def settle_own(c):
        for j in range(bits):
            for k in range(n):
                fold(c, 2**j, k, j).wait_recv()
        for m in range(1, n):
            for k in range(n):
                fold(c, m, k, low(m)).wait_send()

    def pair_of(buf, base):
        value = buf[pl.ds(base, 2)]
        return value.reshape(2 * rows, value.shape[-1])

    def summed(c, at):
        total = sbuf[c % 2, 0, at].astype(F32)
        for j in range(bits):
            total = total + rbuf[c % 2, 2**j - 1, at].astype(F32)
        return total

    def by_rows(work):
        height = 32

        def step(i, carry):
            work(pl.ds(pl.multiple_of(i * height, height), height))
            return carry

        lax.fori_loop(0, rows // height, step, 0)

    outs = {}
    put_keys = ("y", "dx", "xn", "hn", "dy", "dab", "att", "act", "dgu", "dqkv")

    def put(key, src):
        if hasattr(r, key + "_h"):
            copy = pltpu.make_async_copy(src, getattr(r, key + "_h"), r.out_sem.at[put_keys.index(key)])
            copy.start()
            outs[key] = copy

    def put_done(*keys):
        for key in keys:
            if key in outs:
                outs.pop(key).wait()

    def swap(value):
        return pltpu.roll(value, hd // 2, 1)

    def hand(src, dst, to, k):
        return pltpu.make_async_remote_copy(
            src_ref=src,
            dst_ref=dst,
            send_sem=r.hand_send.at[k],
            recv_sem=r.hand_recv.at[k],
            device_id={"section": to},
            device_id_type=MESH,
        )

    @pl.when(sec == 1)
    def _():
        pl.semaphore_wait(turn, 1)

    for c in range(2):
        for copy in slab_copies(c):
            copy.start()
    for d in range(1, n):
        gain_copy(d).wait()
    for k, full in enumerate((ln1, ln2, qn, kn)):
        at, size = gain_at[k]
        for f in range(n):
            full[:, f * size : (f + 1) * size] = gains[f, :, at : at + size]

    @pl.when(sec == 1)
    def _():
        prepare_first()
        hand(yv, xin, 0, 0).wait_recv()

    @pl.when(sec == 0)
    def _():
        load_x.wait()

    @by_rows
    def _(at):
        x32 = xin[at].astype(F32)
        r1 = lax.rsqrt(mean_last(x32 * x32) + EPS)
        xn_all[me, at] = (x32 * r1 * ln1[...]).astype(BF16)

    spread_start(xn_all, 0)
    for c in range(2, chunks):
        for copy in slab_copies(c):
            copy.start()

    @pl.when(sec == 0)
    def _():
        prepare_first()

    load_o.wait()
    load_d.wait()

    def masked_scores(qh, kh):
        raw = nt(qh, kh) * scale
        at_row = lax.broadcasted_iota(jnp.int32, raw.shape, 0)
        at_col = lax.broadcasted_iota(jnp.int32, raw.shape, 1)
        raw = jnp.where(at_row >= at_col, raw, -jnp.inf)
        top = jnp.max(raw, axis=-1, keepdims=True)
        lse = top + jnp.log(jnp.sum(jnp.exp(raw - top), axis=-1, keepdims=True))
        return jnp.exp(raw - lse)

    def attend_block(s):
        for at in range(0, qcols + kcols, hd):
            field = qkv[s, :, at : at + hd]
            gain = qn[...] if at < qcols else kn[...]
            factor = lax.rsqrt(mean_last(field * field) + EPS)
            normed = field * factor * gain
            turned = normed * cosine[...] + swap(normed) * sine[...]
            qkvb[s, :, at : at + hd] = turned.astype(BF16)
        qkvb[s, :, qcols + kcols :] = qkv[s, :, qcols + kcols :].astype(BF16)
        for j in range(qcols // hd):
            kv = j * kcols // qcols
            kat = qcols + kv * hd
            vat = qcols + kcols + kv * hd
            probs = masked_scores(qkvb[s, :, j * hd : (j + 1) * hd], qkvb[s, :, kat : kat + hd])
            attended = nn(probs.astype(BF16), qkvb[s, :, vat : vat + hd])
            att[s, :, j * hd : (j + 1) * hd] = attended.astype(BF16)
    def both(base, work):
        lax.fori_loop(0, 2, lambda i, carry: work(base + i) or carry, 0)

    def attend(q, base, relay, ship):
        for k, some in enumerate(places):
            @pl.when(q == k + 1)
            def _():
                prepare_all(some)

        a = pair_of(xn_all, base)
        for at, size in tiles(2 * ch):
            w = wall[0, :, :, :, at : at + size].reshape(width, size)
            qkv[pl.ds(base, 2), :, at : at + size] = nn(a, w).reshape(2, rows, size)
        relay()
        both(base, attend_block)
        for k, some in enumerate(middles):
            @pl.when(q == k + 1)
            def _():
                prepare_all(some)

        a = pair_of(att, base)
        for k in range(n):
            ship(k, nn(a, wo[:, k * piece : (k + 1) * piece]))

    each_pair(xn_all, 0, attend)
    settle_through(0)
    prepare_all(leftover[:1])
    settle_own(0)

    @by_rows
    def _(at):
        h = xin[at].astype(F32) + summed(0, at)
        hres[at] = h
        r2 = lax.rsqrt(mean_last(h * h) + EPS)
        hn_all[me, at] = (h * r2 * ln2[...]).astype(BF16)

    spread_start(hn_all, 1)
    put("xn", xn_all)
    put("att", att)

    prepare_all(leftover[1:])
    for c in range(1, chunks):
        prepare(c, steps)

    @pl.when(sec == 0)
    def _():
        pl.semaphore_signal(turn, inc=1, device_id={"section": 1}, device_id_type=MESH)

    def feed(q, base, relay, ship):
        a = pair_of(hn_all, base)
        here = pl.ds(base, 2)
        for at in range(0, hidden, ch):
            j = 1 + at // ch
            g = nn(a, wall[j, :, :, :, :ch].reshape(width, ch))
            u = nn(a, wall[j, :, :, :, ch:].reshape(width, ch))
            gate[here, :, at : at + ch] = g.astype(BF16).reshape(2, rows, ch)
            up[here, :, at : at + ch] = u.astype(BF16).reshape(2, rows, ch)
            value = (g * jax.nn.sigmoid(g) * u).astype(BF16)
            act[here, :, at : at + ch] = value.reshape(2, rows, ch)
        relay()

        @pl.when(jnp.logical_and(sec == 1, q == 0))
        def _():
            load_y.wait()
            spread_start(dy_all, 2)

        a = pair_of(act, base)
        for k in range(n):
            ship(k, nn(a, wd[:, k * piece : (k + 1) * piece]))

    each_pair(hn_all, 1, feed)

    def write_y():
        @by_rows
        def _(at):
            yv[at] = (hres[at] + summed(1, at)).astype(BF16)

    put("hn", hn_all)
    put("act", act)

    @pl.when(sec == 0)
    def _():
        settle_through(1)
        settle_own(1)
        write_y()
        hand(yv, xin, 1, 0).start()
        hand(yv, dy_all.at[me], 1, 1).wait_recv()
        spread_start(dy_all, 2)

    spread_done(hn_all, 1)
    put_done("hn")

    if fused:
        def place(slot):
            return wall.at[1 + slot // n, slot % n]

        view = types.SimpleNamespace(**{**vars(r), "hn": hn_all, "dab": dab_all})
        stream = grad_stream(view, n, rep, lambda slot: r.ours.at[slot], place)

    def early_tick(t):
        if fused:
            stream.tick(t, (0, 1))

    def early(low, high):
        if fused:
            lax.fori_loop(low, high, lambda t, carry: early_tick(t) or carry, 0)

    def feed_back(q, base, relay, ship):
        @pl.when(q == n // 2 - 1)
        def _():
            if fused:
                stream.prime(0)
            early_tick(0)

        a = pair_of(dy_all, base)
        here = pl.ds(base, 2)
        for at in range(0, hidden, ch):
            dact = nt(a, wd[at : at + ch, :])
            g = gate[here, :, at : at + ch].reshape(2 * rows, ch).astype(F32)
            u = up[here, :, at : at + ch].reshape(2 * rows, ch).astype(F32)
            sig = jax.nn.sigmoid(g)
            dg = (dact * u * sig * (1.0 + g * (1.0 - sig))).astype(BF16)
            du = (dact * g * sig).astype(BF16)
            dgu[here, :, 2 * at : 2 * at + ch] = dg.reshape(2, rows, ch)
            dgu[here, :, 2 * at + ch : 2 * at + 2 * ch] = du.reshape(2, rows, ch)
        relay()

        @pl.when(jnp.logical_and(sec == 1, q == n // 2 - 1))
        def _():
            settle_through(1)

        @pl.when(q == n // 2 - 1)
        def _():
            early_tick(1)

        a = pair_of(dgu, base)
        for f in range(n):
            total = jnp.zeros((2 * rows, kfold), F32)
            for j in range(1, chunks):
                w = wall[j, f].reshape(kfold, 2 * ch)
                total = total + nt(a[:, 2 * (j - 1) * ch : 2 * j * ch], w)
            ship(f, total)

    each_pair(dy_all, 2, feed_back)


    if fused:
        for where in [{"fsdp": lax.rem(me + d, n)} for d in range(1, n)] + [
            {"replica": flip(mine, bit)} for bit in range(steps)
        ]:
            pl.semaphore_signal(r.freed, inc=1, device_id=where, device_id_type=MESH)
    early_tick(2)
    settle_through(2)
    if fused:
        pl.semaphore_wait(r.freed, n - 1 + steps)
    early_tick(3)

    @pl.when(sec == 1)
    def _():
        settle_own(1)
        write_y()

    settle_own(2)
    dln2[...] = jnp.zeros_like(dln2)
    dln1[...] = jnp.zeros_like(dln1)

    @by_rows
    def _(at):
        dhn = summed(2, at)
        h = hres[at]
        r2 = lax.rsqrt(mean_last(h * h) + EPS)
        u = dhn * ln2[...]
        dh = dy_all[me, at].astype(F32) + (r2 * u - h * r2 * r2 * r2 * mean_last(u * h))
        dln2[...] += jnp.sum(dhn * h * r2, axis=0, keepdims=True)
        hres[at] = dh
        dab_all[me, at] = dh.astype(BF16)

    spread_start(dab_all, 3)
    early(4, 6)

    put("y", yv)
    put("dy", dy_all)
    put("dgu", dgu)

    dqn[...] = jnp.zeros_like(dqn)
    dkn[...] = jnp.zeros_like(dkn)

    def head_back(s, at, grad, gain, dgain):
        field = qkv[s, :, at : at + hd]
        factor = lax.rsqrt(mean_last(field * field) + EPS)
        grad = grad * cosine[...] - swap(grad) * sine[...]
        v = grad * gain
        back = factor * v - field * factor * factor * factor * mean_last(v * field)
        dgain[...] += jnp.sum(grad * field * factor, axis=0, keepdims=True)
        dqkv[s, :, at : at + hd] = back.astype(BF16)

    def attend_back_block(i, s):
        for kv in range(kcols // hd):
            kat = qcols + kv * hd
            vat = qcols + kcols + kv * hd
            kh = qkvb[s, :, kat : kat + hd]
            vh = qkvb[s, :, vat : vat + hd]
            dk = jnp.zeros((rows, hd), F32)
            dv = jnp.zeros((rows, hd), F32)
            for j in range(kv * qcols // kcols, (kv + 1) * qcols // kcols):
                qh = qkvb[s, :, j * hd : (j + 1) * hd]
                dh_out = dob[i, :, j * hd : (j + 1) * hd]
                probs = masked_scores(qh, kh)
                dv = dv + tn(probs.astype(BF16), dh_out)
                dp = nt(dh_out, vh)
                delta = jnp.sum(probs * dp, axis=-1, keepdims=True)
                ds = (probs * (dp - delta) * scale).astype(BF16)
                dk = dk + tn(ds, qh)
                head_back(s, j * hd, nn(ds, kh), qn[...], dqn)
            head_back(s, kat, dk, kn[...], dkn)
            dqkv[s, :, vat : vat + hd] = dv.astype(BF16)
    def attend_back(q, base, relay, ship):
        early_tick(6 + 2 * q)
        a = pair_of(dab_all, base)
        for at, size in tiles(qcols):
            dout = nt(a, wo[at : at + size, :]).astype(BF16)
            dob[:, :, at : at + size] = dout.reshape(2, rows, size)
        relay()
        early_tick(7 + 2 * q)
        lax.fori_loop(0, 2, lambda i, carry: attend_back_block(i, base + i) or carry, 0)
        a = pair_of(dqkv, base)
        for f in range(n):
            w = wall[0, f].reshape(kfold, 2 * ch)
            ship(f, nt(a, w))

    each_pair(dab_all, 3, attend_back)
    early_tick(6 + n)
    settle_through(3)
    early_tick(7 + n)
    settle_own(3)
    put_done("y")

    @pl.when(sec == 0)
    def _():
        hand(yv, xin, 1, 0).wait_send()

    @by_rows
    def _(at):
        dxn = summed(3, at)
        x32 = xin[at].astype(F32)
        r1 = lax.rsqrt(mean_last(x32 * x32) + EPS)
        u = dxn * ln1[...]
        dx = hres[at] + (r1 * u - x32 * r1 * r1 * r1 * mean_last(u * x32))
        dln1[...] += jnp.sum(dxn * x32 * r1, axis=0, keepdims=True)
        yv[at] = dx.astype(BF16)
        hres[at] = dx

    @pl.when(sec == 1)
    def _():
        hand(yv, dy_all.at[me], 0, 1).start()

    put("dx", hres)
    put("dab", dab_all)
    put("dqkv", dqkv)
    if fused:
        stream.pack_fill((dln1, dln2, dqn, dkn))
        stream.pack_start()
        stream.finish(8 + n)
    for c, buf in ((0, xn_all), (2, dy_all), (3, dab_all)):
        spread_done(buf, c)

    @pl.when(sec == 1)
    def _():
        hand(yv, dy_all.at[me], 0, 1).wait_send()

    put_done(*list(outs))


def run_layer(n, rep, fused, lanes, tok, cot, ln1, ln2, qn, kn, wq, wk, wv, wg, wu, wo, wd):
    rows, width = tok.shape
    hd = n * qn.shape[-1]
    qcols = wo.shape[0]
    qkvcols = 2 * qcols
    steps = rep.bit_length() - 1
    chunks = 1 + wd.shape[0] // qcols
    hidden = wd.shape[0]
    cosine, sine = rope_tables(rows, hd // 2)
    inputs = {
        "tok": tok, "cot": cot, "ln1_own": ln1, "ln2_own": ln2, "qn_own": qn, "kn_own": kn,
        "cosine": cosine, "sine": sine, "wq_h": wq, "wk_h": wk, "wv_h": wv, "wg_h": wg, "wu_h": wu,
        "wo_h": wo, "wd_h": wd,
    }
    in_vmem = ("ln1_own", "ln2_own", "qn_own", "kn_own", "cosine", "sine")
    single = {"dln1": (1, width), "dln2": (1, width), "dqn": (1, hd), "dkn": (1, hd)}
    outputs = {
        "y_h": jax.ShapeDtypeStruct((rows, width), BF16),
        "dx_h": jax.ShapeDtypeStruct((rows, width), F32),
    }
    saved = {
        "xn": width, "hn": width, "dy": width, "dab": width, "att": qcols, "act": hidden,
        "dgu": 2 * hidden, "dqkv": qkvcols,
    }
    dma = pltpu.SemaphoreType.DMA
    scratch = {
        "wall": pltpu.VMEM((chunks, n, rep, width // (n * rep), qkvcols), BF16),
        "wo": pltpu.VMEM(wo.shape, BF16),
        "wd": pltpu.VMEM(wd.shape, BF16),
        "ln1": pltpu.VMEM((1, width), F32),
        "ln2": pltpu.VMEM((1, width), F32),
        "qn": pltpu.VMEM((1, hd), F32),
        "kn": pltpu.VMEM((1, hd), F32),
        "gains": pltpu.VMEM((n, 1, lanes), F32),
        "xin": pltpu.VMEM((rows, width), BF16),
        **{
            key: pltpu.VMEM((n, rows, size), BF16)
            for key, size in saved.items() if fused or key != "dab"
        },
        "qkv": pltpu.VMEM((n, rows, qkvcols), F32),
        "qkvb": pltpu.VMEM((n, rows, qkvcols), BF16),
        "hres": pltpu.VMEM((rows, width), F32),
        "gate": pltpu.VMEM((n, rows, hidden), BF16),
        "up": pltpu.VMEM((n, rows, hidden), BF16),
        "dob": pltpu.VMEM((2, rows, qcols), BF16),
        "yv": pltpu.VMEM((rows, width), BF16),
        "sbuf": pltpu.VMEM((2, n, rows, width), BF16),
        "rbuf": pltpu.VMEM((2, n - 1, rows, width), BF16),
        "w_sem": dma((4,)),
        "zw_send": dma((chunks, n - 1, 3)),
        "zw_recv": dma((chunks, n - 1, 3)),
        "gw_send": dma((steps, chunks, 2, rep // 2)),
        "gw_recv": dma((steps, chunks, 2, rep // 2)),
        "own_sem": dma((chunks, 3)),
        "gain_send": dma((n - 1,)),
        "gain_recv": dma((n - 1,)),
        "turn": pltpu.SemaphoreType.REGULAR,
        "out_sem": dma((10,)),
        "ag_send": dma((4, n)),
        "ag_recv": dma((4, n)),
        "rs_send": dma((4, n, n)),
        "rs_recv": dma((4, n, n)),
        "hand_send": dma((2,)),
        "hand_recv": dma((2,)),
    }
    if fused:
        outputs |= stream_outputs(n, rep, qcols, hidden, width, lanes)
        scratch |= {key: pltpu.VMEM(shape, F32) for key, shape in single.items()}
        scratch |= stream_scratch(n, rep, qcols, lanes)
        scratch["freed"] = pltpu.SemaphoreType.REGULAR
        scratch["ours"] = pltpu.VMEM((steps + 1, rep, 128, 2 * qcols), BF16)
    else:
        outputs |= {
            key + "_h": jax.ShapeDtypeStruct((n, rows, size), BF16) for key, size in saved.items()
        }
        outputs |= {key: jax.ShapeDtypeStruct(shape, F32) for key, shape in single.items()}
    out_vmem = (*single, "sums")
    return call(
        layer_kernel, (n, rep, hd, fused), inputs, outputs, scratch, in_vmem, out_vmem, "layer", 0
    )


def run_grads(n, rep, saved, lanes):
    steps = rep.bit_length() - 1
    ch, hidden, width = (saved[key].shape[-1] for key in ("att_h", "act_h", "xn_h"))
    inputs = {key: value for key, value in saved.items() if key not in ("y_h", "dx_h")}
    scratch = {
        key[:-2]: pltpu.VMEM(value.shape, BF16) for key, value in inputs.items() if key[-2:] == "_h"
    }
    scratch["ours"] = pltpu.VMEM((steps + 1, rep, 128, 2 * ch), BF16)
    scratch["whole"] = pltpu.VMEM((steps + 3, rep, 128, 2 * ch), BF16)
    scratch["in_sem"] = pltpu.SemaphoreType.DMA((8,))
    scratch |= stream_scratch(n, rep, ch, lanes)
    outputs = stream_outputs(n, rep, ch, hidden, width, lanes)
    small = ("dln1", "dln2", "dqn", "dkn")
    return call(grad_kernel, (n, rep), inputs, outputs, scratch, small, ("sums",), "grads", 1)


def write_results(sources, sums, gains, y, dx):
    steps = 16

    moved = [*sources, y, dx]

    def rows_of(value):
        return pl.BlockSpec((value.shape[0] // steps, value.shape[1]), lambda i: (i, 0))

    def all_of(columns):
        return pl.BlockSpec((1, columns), lambda i: (0, 0))

    kinds = [F32] * len(sources) + [BF16, F32]

    def kernel(*refs):
        ins, outs = refs[: len(moved) + 1], refs[len(moved) + 1 :]
        for src, dst in zip(ins, outs[: len(moved)]):
            dst[...] = src[...].astype(dst.dtype)
        at = 0
        for size, dst in zip(gains, outs[len(moved) :]):
            dst[...] = ins[-1][:, at : at + size]
            at += size

    return pl.pallas_call(
        kernel,
        grid=(steps,),
        out_shape=[jax.ShapeDtypeStruct(v.shape, kind) for v, kind in zip(moved, kinds)]
        + [jax.ShapeDtypeStruct((1, size), F32) for size in gains],
        in_specs=[rows_of(value) for value in moved] + [all_of(sums.shape[1])],
        out_specs=[rows_of(value) for value in moved] + [all_of(size) for size in gains],
        compiler_params=pltpu.CompilerParams(vmem_limit_bytes=67043328),
        name="results",
    )(*moved, sums)


def per_device(tokens_in, cotangent, ln1, wq, wk, wv, qn, kn, wo, ln2, wg, wu, wd):
    n, rep = lax.axis_size("fsdp"), lax.axis_size("replica")

    lanes = -(-2 * (ln1.shape[-1] + qn.shape[-1]) // 128) * 128
    thirds = grad_plan(n, wo.shape[1], wd.shape[1], wo.shape[2])[1]
    fused = (2 * rep.bit_length() + 2) <= n * thirds and wq.shape[1] == n * 128
    done = run_layer(
        n, rep, fused, lanes, tokens_in, cotangent, ln1, ln2, qn, kn,
        wq[0], wk[0], wv[0], wg[0], wu[0], wo[0], wd[0],
    )
    y, dx = done["y_h"], done["dx_h"]
    if not fused:
        done = run_grads(n, rep, done, lanes)
    sources = [
        done[key].reshape(-1, done[key].shape[-1])
        for key in ("gq_h", "gk_h", "gv_h", "go_h", "gg_h", "gu_h", "gd_h")
    ]
    gains = [gain.shape[1] for gain in (ln1, ln2, qn, kn)]
    (
        g_wq, g_wk, g_wv, g_wo, g_wg, g_wu, g_wd, y, dx, *owned
    ) = write_results(sources, done["sums"], gains, y, dx)
    g_ln1, g_ln2, g_qn, g_kn = (value[0] for value in owned)
    results = (y, dx, g_ln1, g_wq, g_wk, g_wv, g_qn, g_kn, g_wo, g_ln2, g_wg, g_wu, g_wd)
    return tuple(value[None] for value in results)


def solution(mesh):
    rows = P("section", "fsdp", None)
    gain = P("section", "fsdp")
    tokens = P(("fsdp", "replica"), None)
    stacked = P("section", ("fsdp", "replica"), None)
    weights = (gain, rows, rows, rows, gain, gain, rows, gain, rows, rows, rows)
    return jax.shard_map(
        per_device,
        mesh=mesh,
        in_specs=(tokens, tokens, *weights),
        out_specs=(stacked, stacked, *weights),
        check_vma=False,
    )
```

```python
import functools
import math
import types

import jax
import jax.numpy as jnp
from jax import lax
from jax.experimental import pallas as pl
from jax.experimental.pallas import tpu as pltpu
from jax.sharding import PartitionSpec as P

LEN = 128
EPS = 1e-06
F32 = jnp.float32
BF16 = jnp.bfloat16
MESH = pl.DeviceIdType.MESH
TILE = 512


def rope_tables(length, half_dim):
    freq = jnp.exp(jnp.arange(half_dim, dtype=F32) * (-math.log(1000000.0) / half_dim))
    angle = jnp.arange(length, dtype=F32)[:, None] * freq[None, :]
    cosine, sine = jnp.cos(angle), jnp.sin(angle)
    return (
        jnp.concatenate([cosine, cosine], axis=1),
        jnp.concatenate([-sine, sine], axis=1),
    )


def nn(left, right):
    return jnp.dot(left, right, preferred_element_type=F32)


def nt(left, right):
    return lax.dot_general(left, right, (((1,), (1,)), ((), ())), preferred_element_type=F32)


def tn(left, right):
    return lax.dot_general(left, right, (((0,), (0,)), ((), ())), preferred_element_type=F32)


def mean_last(value):
    return jnp.mean(value, axis=-1, keepdims=True)


def tiles(total):
    return [(at, min(TILE, total - at)) for at in range(0, total, TILE)]


def flip(value, bit):
    return value + (1 - 2 * (value // 2**bit % 2)) * 2**bit


def flips(value, bits, subset):
    for at, bit in enumerate(bits):
        if subset >> at & 1:
            value = flip(value, bit)
    return value


def grad_plan(n, qcols, hidden, width):
    blocks = width // n // 128
    thirds = hidden // qcols
    return blocks, thirds, (hidden // 256, blocks * thirds, qcols // 256, blocks)


def rem(value, by):
    return value % by if isinstance(value, int) else lax.rem(value, by)


def within(value, low, high):
    if isinstance(value, int):
        return low <= value < high
    return jnp.logical_and(value >= low, value < high)


def both(first, second):
    if isinstance(first, bool):
        return second if first else False
    return jnp.logical_and(first, second)


def when(condition):
    if isinstance(condition, bool):
        return lambda work: work() if condition else None
    return pl.when(condition)


def remote(src, dst, send, recv, where):
    return pltpu.make_async_remote_copy(
        src_ref=src, dst_ref=dst, send_sem=send, recv_sem=recv,
        device_id=where, device_id_type=MESH,
    )


def grad_stream(r, n, rep, ours, whole, far=None):
    me = lax.axis_index("fsdp")
    mine = lax.axis_index("replica")
    steps = rep.bit_length() - 1
    g_slots, slots = steps + 1, steps + 3
    ch = r.att.shape[-1]
    part = 128 // n
    width = r.xn.shape[-1]
    tokens = r.xn.shape[0] * r.xn.shape[1]
    fold = width // n
    hidden = r.act.shape[-1]
    kcols = r.gk_h.shape[-1] // n
    thirds = grad_plan(n, ch, hidden, width)[1]
    counts = grad_plan(n, ch, hidden, width)[2]
    starts = [sum(counts[:k]) for k in range(len(counts) + 1)]
    total = starts[-1]
    orders = (tuple(range(steps)), tuple(reversed(range(steps))))
    got = [getattr(r, f"got{j}") for j in range(steps)]
    strip = ch // rep

    def lanes(h):
        return pl.ds(h * ch, ch)

    def scatter_copies(c, j):
        slot, two = rem(c, g_slots), rem(c, 2)
        for h, bits in enumerate(orders):
            partner = flip(mine, bits[j])
            for i in range(rep >> (j + 1)):
                piece = flips(partner, bits[j + 1 :], i)
                yield remote(
                    ours(slot).at[piece, :, lanes(h)], got[j].at[two, h, i],
                    r.grs_send.at[j, two, h, i], r.grs_recv.at[j, two, h, i],
                    {"replica": partner},
                )

    def owner_part(owner, apart):
        if apart:
            return slice(None), pl.ds(aligned(owner * 2 * strip), 2 * strip)
        return pl.ds(pl.multiple_of(owner * part, part), part), slice(None)

    def across_copies(c, apart):
        slot, two = rem(c, slots), rem(c, 2)
        for d in range(1, n):
            to = lax.rem(me + d, n)
            yield remote(
                r.reduced.at[owner_part(to, apart)],
                whole(slot).at[(mine, *owner_part(me, apart))],
                r.gz_send.at[two, d - 1], r.gz_recv.at[two, d - 1], {"fsdp": to},
            )

    def gather_copies(c, j):
        slot, three = rem(c, slots), rem(c, 3)
        for h, order in enumerate(orders):
            bits = order[::-1]
            partner = flip(mine, bits[j])
            for i in range(1 << j):
                ref = whole(slot).at[flips(mine, bits[:j], i), :, lanes(h)]
                yield remote(
                    ref, ref, r.gag_send.at[j, three, h, i], r.gag_recv.at[j, three, h, i],
                    {"replica": partner},
                )

    def aligned(at):
        return pl.multiple_of(at, 128)

    def out_copies(c, kind, apart):
        slot, two = rem(c, slots), rem(c, 2)
        at = c - starts[kind]
        for f in range(n):
            rows = pl.ds(f * part, part)
            if kind == 1:
                k, j = at // thirds, rem(at, thirds)
                pairs = []
                for h, dst in enumerate((r.gg_h, r.gu_h)):
                    for q in range(rep):
                        if apart:
                            src = whole(slot).at[q, :, pl.ds((2 * f + h) * strip, strip)]
                            cols = pl.ds(aligned(f * hidden + j * ch + q * strip), strip)
                            to = dst.at[k, :, cols]
                        else:
                            src = whole(slot).at[q, rows, lanes(h)]
                            cols = pl.ds(aligned(f * hidden + j * ch), ch)
                            to = dst.at[k, pl.ds(q * (128 // rep), 128 // rep), cols]
                        pairs.append((src, to))
            elif kind == 3:
                cols = pl.ds(f * kcols, kcols)
                pairs = [
                    (whole(slot).at[:, rows, lanes(0)], r.gq_h.at[at, :, :, pl.ds(f * ch, ch)]),
                    (whole(slot).at[:, rows, pl.ds(ch, kcols)], r.gk_h.at[at, :, :, cols]),
                    (whole(slot).at[:, rows, pl.ds(ch + kcols, kcols)], r.gv_h.at[at, :, :, cols]),
                ]
            else:
                dst = r.gd_h if kind == 0 else r.go_h
                pairs = [
                    (
                        whole(slot).at[f, :, lanes(h)],
                        dst.at[pl.ds(aligned(at * 256 + h * 128), 128), pl.ds(f * ch, ch)],
                    )
                    for h in range(2)
                ]
            for i, (src, to) in enumerate(pairs):
                yield pltpu.make_async_copy(src, to, r.gout_sem.at[two, f, i])

    def columns_of(ref, at, size):
        return ref[:, :, pl.ds(at, size)].reshape(tokens, size)

    def compute(c, kind):
        to = ours(rem(c, g_slots))
        at = c - starts[kind]
        if kind in (1, 3):
            left, right = (r.hn, r.dgu) if kind == 1 else (r.xn, r.dqkv)
            k, j = (at // thirds, rem(at, thirds)) if kind == 1 else (at, 0)
            lefts = jnp.concatenate(
                [columns_of(left, aligned(f * fold + k * 128), 128) for f in range(n)], axis=1
            )
            for h in range(2):
                product = tn(lefts, columns_of(right, aligned((2 * j + h) * ch), ch)).astype(BF16)
                for f in range(n):
                    block = product[f * 128 : (f + 1) * 128].reshape(rep, 128 // rep, ch)
                    to[:, f * part : (f + 1) * part, h * ch : (h + 1) * ch] = block
        else:
            left, right = (r.act, r.dy) if kind == 0 else (r.att, r.dab)
            lefts = columns_of(left, aligned(at * 256), 256)
            for q in range(rep):
                product = tn(lefts, columns_of(right, q * ch, ch)).astype(BF16)
                for h in range(2):
                    to[q, :, h * ch : (h + 1) * ch] = product[h * 128 : (h + 1) * 128]

    def full_product(c):
        at = c - starts[1]
        k, j = at // thirds, rem(at, thirds)

        @when(at == 0)
        def _():
            far.ready()

        @when(j == 0)
        def _():
            loads = [
                pltpu.make_async_copy(
                    r.hn_far.at[:, block, :, pl.ds(aligned(f * fold + k * 128), 128)],
                    far.left(block).at[:, :, pl.ds(f * 128, 128)], r.far_load.at[block, f],
                )
                for block in range(n) for f in range(n)
            ]
            for load in loads:
                load.start()
            for load in loads:
                load.wait()

            def owner_rows(f, carry):
                rows = pl.ds(pl.multiple_of(f * 128, 128), 128)
                product = jnp.zeros((128, thirds * 2 * strip), F32)
                for block in range(n):
                    left = far.left(block)[:, :, rows].reshape(rep * 128, 128)
                    right = far.right(block)[:, :, : thirds * 2 * strip]
                    product = product + tn(left, right.reshape(rep * 128, thirds * 2 * strip))
                for third in range(thirds):
                    value = product[:, third * 2 * strip : (third + 1) * 2 * strip].astype(BF16)
                    far.held[third, :, pl.ds(aligned(f * 2 * strip), 2 * strip)] = value
                return carry

            lax.fori_loop(0, n, owner_rows, 0)

        r.reduced[...] = far.held[j]

    def tick(t, kinds=(0, 1, 2, 3)):
        def is_kind(c, kind):
            return within(c, starts[kind], starts[kind + 1])

        def cases(c):
            for kind in kinds:
                hit = is_kind(c, kind)
                if far is None or kind != 1:
                    yield hit, kind, False
                else:
                    yield both(hit, jnp.logical_not(far.here)), kind, False
                    yield both(hit, far.here), kind, True

        def exchanged(c):
            hit = within(c, 0, total)
            apart = is_kind(c, 1)
            if far is None or apart is False:
                return hit
            if apart is True:
                return both(hit, jnp.logical_not(far.here))
            return jnp.logical_and(hit, jnp.logical_not(jnp.logical_and(apart, far.here)))

        c_done = t - (2 * steps + 2)
        for hit, kind, apart in cases(c_done):
            @when(hit)
            def _():
                for copy in out_copies(c_done, kind, apart):
                    copy.wait()

        for j in reversed(range(1, steps)):
            c_ag = t - (steps + 1 + j)

            @when(within(c_ag, 0, total))
            def _():
                for copy in gather_copies(c_ag, j - 1):
                    copy.wait()
                for copy in gather_copies(c_ag, j):
                    copy.start()

        c_z = t - (steps + 1)
        for hit, kind, apart in cases(c_z):
            @when(hit)
            def _():
                if kind in (1, 3):
                    for copy in across_copies(c_z, apart):
                        copy.wait()
                else:
                    for d in range(1, n):
                        pl.semaphore_wait(r.gsig.at[rem(c_z, 2), d - 1], 1)

        @when(within(c_z, 0, total))
        def _():
            for copy in gather_copies(c_z, 0):
                copy.start()

        for j in reversed(range(steps)):
            c_rs = t - (j + 1)

            @when(exchanged(c_rs))
            def _():
                for copy in scatter_copies(c_rs, j):
                    copy.wait()
                for h, bits in enumerate(orders):
                    half = slice(h * ch, (h + 1) * ch)
                    for i in range(rep >> (j + 1)):
                        piece = flips(mine, bits[j + 1 :], i)
                        value = ours(rem(c_rs, g_slots))[piece, :, half].astype(F32)
                        value = (value + got[j][rem(c_rs, 2), h, i].astype(F32)).astype(BF16)
                        if j < steps - 1:
                            ours(rem(c_rs, g_slots))[piece, :, half] = value
                        else:
                            r.reduced[:, half] = value
                if j < steps - 1:
                    for copy in scatter_copies(c_rs, j + 1):
                        copy.start()

            if j == steps - 1:
                for hit, kind, apart in cases(c_rs):
                    @when(hit)
                    def _():
                        to = whole(rem(c_rs, slots))
                        if apart:
                            full_product(c_rs)
                        if kind in (1, 3):
                            for copy in across_copies(c_rs, apart):
                                copy.start()
                            own = owner_part(me, apart)
                            to[(mine, *own)] = r.reduced[own]
                        else:
                            for d in range(1, n):
                                pl.semaphore_signal(
                                    r.gsig.at[rem(c_rs, 2), d - 1], inc=1,
                                    device_id={"fsdp": lax.rem(me + d, n)}, device_id_type=MESH,
                                )
                            to[mine] = r.reduced[...]

        @when(exchanged(t))
        def _():
            for copy in scatter_copies(t, 0):
                copy.start()

        for hit, kind, apart in cases(t + 1):
            if not apart:
                @when(hit)
                def _():
                    compute(t + 1, kind)

        c_out = t - (2 * steps + 1)

        @when(within(c_out, 0, total))
        def _():
            for copy in gather_copies(c_out, steps - 1):
                copy.wait()

        for hit, kind, apart in cases(c_out):
            @when(hit)
            def _():
                for copy in out_copies(c_out, kind, apart):
                    copy.start()

    def pack_across(d):
        to = lax.rem(me + d, n)
        return remote(
            r.pack.at[to], r.pack_z.at[d - 1], r.pz_send.at[d - 1], r.pz_recv.at[d - 1], {"fsdp": to}
        )

    def pack_swap(j):
        return remote(
            r.pack_r.at[j], r.pack_in.at[j], r.pr_send.at[j], r.pr_recv.at[j],
            {"replica": flip(mine, j)},
        )

    def pack_fill(dgains):
        r.pack[...] = jnp.zeros_like(r.pack)
        at = 0
        for value in dgains:
            size = value.shape[-1] // n
            for f in range(n):
                r.pack[f, :, at : at + size] = value[:, f * size : (f + 1) * size]
            at += size

    def pack_start():
        for d in range(1, n):
            pack_across(d).start()

    def pack_tick(t):
        for j in range(steps + 1):
            @pl.when(t == 2 * j + 2)
            def _():
                if j == 0:
                    value = r.pack[me]
                    for d in range(1, n):
                        pack_across(d).wait()
                        value = value + r.pack_z[d - 1]
                else:
                    pack_swap(j - 1).wait()
                    value = r.pack_r[j - 1] + r.pack_in[j - 1]
                if j < steps:
                    r.pack_r[j] = value
                    pack_swap(j).start()
                else:
                    r.sums[...] = value

    def finish(first):
        def step(t, carry):
            tick(t)
            pack_tick(t - first)
            return carry

        lax.fori_loop(first, total + 2 * steps + 3, step, 0)

    return types.SimpleNamespace(
        tick=tick, prime=lambda kind: compute(0, kind), pack_fill=pack_fill, pack_start=pack_start, finish=finish
    )


def stream_scratch(n, rep, ch, lanes):
    steps = rep.bit_length() - 1
    dma = pltpu.SemaphoreType.DMA
    swap = dma((steps, 2, 2, rep // 2))
    return {
        "reduced": pltpu.VMEM((128, 2 * ch), BF16),
        "pack": pltpu.VMEM((n, 1, lanes), F32),
        "pack_z": pltpu.VMEM((n - 1, 1, lanes), F32),
        "pack_r": pltpu.VMEM((steps, 1, lanes), F32),
        "pack_in": pltpu.VMEM((steps, 1, lanes), F32),
        **{
            f"got{j}": pltpu.VMEM((2, 2, rep >> (j + 1), 128, ch), BF16) for j in range(steps)
        },
        "grs_send": swap, "grs_recv": swap,
        "gz_send": dma((2, n - 1)), "gz_recv": dma((2, n - 1)),
        "gag_send": dma((steps, 3, 2, rep // 2)), "gag_recv": dma((steps, 3, 2, rep // 2)),
        "gout_sem": dma((2, n, 2 * rep)),
        "pz_send": dma((n - 1,)), "pz_recv": dma((n - 1,)),
        "pr_send": dma((steps,)), "pr_recv": dma((steps,)),
        "gsig": pltpu.SemaphoreType.REGULAR((2, n - 1)),
    }


def stream_outputs(n, rep, ch, hidden, width, lanes):
    kcols = ch // 2

    def owned(columns):
        return jax.ShapeDtypeStruct((width // n // 128, rep, 128 // rep, columns * n), BF16)

    return {
        "gq_h": owned(ch), "gk_h": owned(kcols), "gv_h": owned(kcols),
        "go_h": jax.ShapeDtypeStruct((ch, width), BF16),
        "gg_h": jax.ShapeDtypeStruct((width // n // 128, 128, hidden * n), BF16),
        "gu_h": jax.ShapeDtypeStruct((width // n // 128, 128, hidden * n), BF16),
        "gd_h": jax.ShapeDtypeStruct((hidden, width), BF16),
        "sums": jax.ShapeDtypeStruct((1, lanes), F32),
    }


def named(body, names, *args):
    def kernel(*refs):
        body(types.SimpleNamespace(**dict(zip(names, refs))), *args)

    return kernel


def call(body, args, inputs, outputs, scratch, in_vmem, out_vmem, name, collective):
    vm = pl.BlockSpec(memory_space=pltpu.VMEM)
    hbm = pl.BlockSpec(memory_space=pltpu.HBM)
    results = pl.pallas_call(
        named(body, [*inputs, *outputs, *scratch], *args),
        out_shape=list(outputs.values()),
        in_specs=[vm if key in in_vmem else hbm for key in inputs],
        out_specs=[vm if key in out_vmem else hbm for key in outputs],
        scratch_shapes=list(scratch.values()),
        compiler_params=pltpu.CompilerParams(
            collective_id=collective, has_side_effects=True, vmem_limit_bytes=67043328
        ),
        name=name,
    )(*inputs.values())
    return dict(zip(outputs, results))


def peer(mine, rep, m):
    return flips(mine, range(rep.bit_length() - 1), m)


def greet(n, rep, me, mine):
    barrier = pltpu.get_barrier_semaphore()
    for d in range(1, n):
        pl.semaphore_signal(
            barrier, inc=1, device_id={"fsdp": lax.rem(me + d, n)}, device_id_type=MESH
        )
    for m in range(1, rep):
        pl.semaphore_signal(
            barrier, inc=1, device_id={"replica": peer(mine, rep, m)}, device_id_type=MESH
        )
    return barrier


def grad_kernel(r, n, rep):
    me = lax.axis_index("fsdp")
    mine = lax.axis_index("replica")
    barrier = greet(n, rep, me, mine)
    loads = []
    for k, key in enumerate(("act", "dy", "hn", "dgu", "att", "dab", "xn", "dqkv")):
        loads.append(
            pltpu.make_async_copy(getattr(r, key + "_h"), getattr(r, key), r.in_sem.at[k])
        )
        loads[-1].start()
    stream = grad_stream(r, n, rep, lambda slot: r.ours.at[slot], lambda slot: r.whole.at[slot])
    stream.pack_fill((r.dln1, r.dln2, r.dqn, r.dkn))
    pl.semaphore_wait(barrier, n - 1 + rep - 1)
    for load in loads:
        load.wait()
    stream.pack_start()
    stream.prime(0)
    stream.finish(0)


def layer_kernel(r, n, rep, hd, fused):
    sec = lax.axis_index("section")
    me = lax.axis_index("fsdp")
    mine = lax.axis_index("replica")
    wq_h, wk_h, wv_h, wg_h, wu_h = r.wq_h, r.wk_h, r.wv_h, r.wg_h, r.wu_h
    cosine, sine, wall, wo, wd, ln1, ln2, qn, kn, gains = (
        r.cosine, r.sine, r.wall, r.wo, r.wd, r.ln1, r.ln2, r.qn, r.kn, r.gains
    )
    xin, xn_all, hn_all, dy_all, qkv, qkvb, att, hres, gate, up, act, dgu, dqkv = (
        r.xin, r.xn, r.hn, r.dy, r.qkv, r.qkvb, r.att, r.hres, r.gate, r.up, r.act, r.dgu, r.dqkv
    )
    dab_all = r.dab if fused else r.hn
    dob, yv, sbuf, rbuf, turn = r.dob, r.yv, r.sbuf, r.rbuf, r.turn
    dln1, dln2, dqn, dkn = r.dln1, r.dln2, r.dqn, r.dkn
    zw_send, zw_recv, gw_send, gw_recv, own_sem = r.zw_send, r.zw_recv, r.gw_send, r.gw_recv, r.own_sem
    ag_send, ag_recv, rs_send, rs_recv = r.ag_send, r.ag_recv, r.rs_send, r.rs_recv
    steps = rep.bit_length() - 1
    rows, width = xin.shape
    ch = att.shape[-1]
    qcols = ch
    kcols = (qkvb.shape[-1] - qcols) // 2
    hidden = act.shape[-1]
    chunks = wall.shape[0]
    share = wall.shape[3]
    kfold = rep * share
    scale = 1.0 / math.sqrt(hd)
    orders = (tuple(range(steps)), tuple(reversed(range(steps))))

    barrier = greet(n, rep, me, mine)
    pl.semaphore_signal(barrier, inc=1, device_id={"section": 1 - sec}, device_id_type=MESH)
    load_o = pltpu.make_async_copy(r.wo_h, wo, r.w_sem.at[0])
    load_d = pltpu.make_async_copy(r.wd_h, wd, r.w_sem.at[1])
    load_x = pltpu.make_async_copy(r.tok, xin, r.w_sem.at[2])
    load_y = pltpu.make_async_copy(r.cot, dy_all.at[me], r.w_sem.at[3])

    @pl.when(sec == 0)
    def _():
        load_x.start()

    @pl.when(sec == 1)
    def _():
        load_y.start()

    load_o.start()
    load_d.start()

    at = 0
    gain_at = []
    gains[me] = jnp.zeros_like(gains[me])
    for value in (r.ln1_own, r.ln2_own, r.qn_own, r.kn_own):
        size = value.shape[-1]
        gains[me, :, at : at + size] = value[...].astype(F32)
        gain_at.append((at, size))
        at += size
    pl.semaphore_wait(barrier, n + rep - 1)

    def gain_copy(d):
        return remote(
            gains.at[me], gains.at[me], r.gain_send.at[d - 1], r.gain_recv.at[d - 1],
            {"fsdp": lax.rem(me + d, n)},
        )

    for d in range(1, n):
        gain_copy(d).start()

    def slabs(c, to):
        rows_in = pl.ds(pl.multiple_of(mine * share, share), share)
        if isinstance(c, int) and c == 0:
            return (
                (wq_h.at[rows_in, pl.ds(to * ch, ch)], pl.ds(0, ch)),
                (wk_h.at[rows_in, pl.ds(to * kcols, kcols)], pl.ds(ch, kcols)),
                (wv_h.at[rows_in, pl.ds(to * kcols, kcols)], pl.ds(ch + kcols, kcols)),
            )
        cols = pl.ds(pl.multiple_of(to * hidden + (c - 1) * ch, 128), ch)
        return (
            (wg_h.at[rows_in, cols], pl.ds(0, ch)),
            (wu_h.at[rows_in, cols], pl.ds(ch, ch)),
        )

    def slab_copies(c):
        for i, (src, lanes) in enumerate(slabs(c, me)):
            yield pltpu.make_async_copy(src, wall.at[c, me, mine, :, lanes], own_sem.at[c, i])
        for d in range(1, n):
            to = lax.rem(me + d, n)
            for i, (src, lanes) in enumerate(slabs(c, to)):
                yield remote(
                    src, wall.at[c, me, mine, :, lanes],
                    zw_send.at[c, d - 1, i], zw_recv.at[c, d - 1, i], {"fsdp": to},
                )

    def slab_gathers(c, j):
        for h, order in enumerate(orders):
            bits = order[::-1]
            partner = flip(mine, bits[j])
            for i in range(1 << j):
                piece = flips(mine, bits[:j], i)
                ref = wall.at[c, :, piece, :, pl.ds(h * ch, ch)]
                yield remote(
                    ref, ref, gw_send.at[j, c, h, i], gw_recv.at[j, c, h, i], {"replica": partner}
                )

    def prepare(c, j):
        for copy in slab_copies(c) if j == 0 else slab_gathers(c, j - 1):
            copy.wait()
        if j < steps:
            for copy in slab_gathers(c, j):
                copy.start()

    events = [
        (t - j, j) for t in range(2, chunks + steps) for j in range(steps) if 2 <= t - j < chunks
    ]
    events.sort(key=lambda event: (event[0] + event[1], -event[1]))
    places = [events[3 * k : 3 * k + 1] for k in range(n // 2 - 1)]
    middles = [events[3 * k + 1 : 3 * k + 3] for k in range(n // 2 - 1)]
    leftover = events[3 * (n // 2 - 1) :]

    def prepare_all(some):
        for event in some:
            prepare(*event)

    def prepare_first():
        for j in range(steps + 1):
            prepare(0, j)
            if j > 0:
                prepare(1, j - 1)

    bits = n.bit_length() - 1
    piece = width // n

    def low(m):
        return (m & -m).bit_length() - 1

    def across(s):
        return sum((me // 2**j + s // 2**j) % 2 * 2**j for j in range(bits))

    def spread(buf, c, m, j):
        ref = buf.at[flips(me, range(bits), m)]
        return remote(
            ref, ref, ag_send.at[c, m + 2**j], ag_recv.at[c, m + 2**j], {"fsdp": flip(me, j)}
        )

    def spread_start(buf, c):
        for j in range(bits):
            spread(buf, c, 0, j).start()

    def spread_done(buf, c):
        for m in range(n):
            for j in range(bits if m == 0 else low(m)):
                spread(buf, c, m, j).wait_send()

    def fold(c, m, k, j):
        cols = pl.ds(k * piece, piece)
        return remote(
            sbuf.at[c % 2, m, :, cols], rbuf.at[c % 2, m - 1, :, cols],
            rs_send.at[c, m, k], rs_recv.at[c, m, k], {"fsdp": flip(me, j)},
        )

    def each_pair(buf, c, work):
        def hear(s):
            ref = buf.at[across(s)]
            remote(
                ref, ref, ag_send.at[c, s], ag_recv.at[c, s], {"fsdp": flip(me, 0)}
            ).wait_recv()

        def step(q, carry):
            hear(2 * q + 1)

            def relay():
                for m in range(2, n, 2):
                    @pl.when(2 * q + 2 == m)
                    def _():
                        hear(m)
                        for j in range(low(m)):
                            spread(buf, c, m, j).start()

            def ship(k, value):
                for i in range(2):
                    part = value[i * rows : (i + 1) * rows].astype(BF16)
                    sbuf[c % 2, 2 * q + (me + i) % 2, :, k * piece : (k + 1) * piece] = part
                fold(c, 2 * q + 1, k, 0).start()

            work(q, across(2 * q) // 2 * 2, relay, ship)
            return carry

        lax.fori_loop(0, n // 2, step, 0)

    def settle_through(c):
        own, heard = sbuf.at[c % 2], rbuf.at[c % 2]
        for m in sorted(range(2, n, 2), key=low):
            for k in range(n):
                cols = slice(k * piece, (k + 1) * piece)
                value = own[m, :, cols].astype(F32)
                for j in range(low(m)):
                    fold(c, m + 2**j, k, j).wait_recv()
                    value = value + heard[m + 2**j - 1, :, cols].astype(F32)
                own[m, :, cols] = value.astype(BF16)
                fold(c, m, k, low(m)).start()

    def settle_own(c):
        for j in range(bits):
            for k in range(n):
                fold(c, 2**j, k, j).wait_recv()
        for m in range(1, n):
            for k in range(n):
                fold(c, m, k, low(m)).wait_send()

    def pair_of(buf, base):
        value = buf[pl.ds(base, 2)]
        return value.reshape(2 * rows, value.shape[-1])

    def summed(c, at):
        total = sbuf[c % 2, 0, at].astype(F32)
        for j in range(bits):
            total = total + rbuf[c % 2, 2**j - 1, at].astype(F32)
        return total

    def by_rows(work):
        height = 32

        def step(i, carry):
            work(pl.ds(pl.multiple_of(i * height, height), height))
            return carry

        lax.fori_loop(0, rows // height, step, 0)

    outs = {}
    put_keys = ("y", "dx", "xn", "hn", "dy", "dab", "att", "act", "dgu", "dqkv")

    def put(key, src):
        if hasattr(r, key + "_h"):
            copy = pltpu.make_async_copy(src, getattr(r, key + "_h"), r.out_sem.at[put_keys.index(key)])
            copy.start()
            outs[key] = copy

    def put_done(*keys):
        for key in keys:
            if key in outs:
                outs.pop(key).wait()

    def swap(value):
        return pltpu.roll(value, hd // 2, 1)

    def hand(src, dst, to, k):
        return pltpu.make_async_remote_copy(
            src_ref=src,
            dst_ref=dst,
            send_sem=r.hand_send.at[k],
            recv_sem=r.hand_recv.at[k],
            device_id={"section": to},
            device_id_type=MESH,
        )

    @pl.when(sec == 1)
    def _():
        pl.semaphore_wait(turn, 1)

    for c in range(2):
        for copy in slab_copies(c):
            copy.start()
    for d in range(1, n):
        gain_copy(d).wait()
    for k, full in enumerate((ln1, ln2, qn, kn)):
        at, size = gain_at[k]
        for f in range(n):
            full[:, f * size : (f + 1) * size] = gains[f, :, at : at + size]

    @pl.when(sec == 1)
    def _():
        prepare_first()
        hand(yv, xin, 0, 0).wait_recv()

    @pl.when(sec == 0)
    def _():
        load_x.wait()

    @by_rows
    def _(at):
        x32 = xin[at].astype(F32)
        r1 = lax.rsqrt(mean_last(x32 * x32) + EPS)
        xn_all[me, at] = (x32 * r1 * ln1[...]).astype(BF16)

    spread_start(xn_all, 0)
    for c in range(2, chunks):
        for copy in slab_copies(c):
            copy.start()

    @pl.when(sec == 0)
    def _():
        prepare_first()

    load_o.wait()
    load_d.wait()

    def masked_scores(qh, kh):
        raw = nt(qh, kh) * scale
        at_row = lax.broadcasted_iota(jnp.int32, raw.shape, 0)
        at_col = lax.broadcasted_iota(jnp.int32, raw.shape, 1)
        raw = jnp.where(at_row >= at_col, raw, -jnp.inf)
        top = jnp.max(raw, axis=-1, keepdims=True)
        lse = top + jnp.log(jnp.sum(jnp.exp(raw - top), axis=-1, keepdims=True))
        return jnp.exp(raw - lse)

    def attend_block(s):
        for at in range(0, qcols + kcols, hd):
            field = qkv[s, :, at : at + hd]
            gain = qn[...] if at < qcols else kn[...]
            factor = lax.rsqrt(mean_last(field * field) + EPS)
            normed = field * factor * gain
            turned = normed * cosine[...] + swap(normed) * sine[...]
            qkvb[s, :, at : at + hd] = turned.astype(BF16)
        qkvb[s, :, qcols + kcols :] = qkv[s, :, qcols + kcols :].astype(BF16)
        for j in range(qcols // hd):
            kv = j * kcols // qcols
            kat = qcols + kv * hd
            vat = qcols + kcols + kv * hd
            probs = masked_scores(qkvb[s, :, j * hd : (j + 1) * hd], qkvb[s, :, kat : kat + hd])
            attended = nn(probs.astype(BF16), qkvb[s, :, vat : vat + hd])
            att[s, :, j * hd : (j + 1) * hd] = attended.astype(BF16)
    def both(base, work):
        lax.fori_loop(0, 2, lambda i, carry: work(base + i) or carry, 0)

    def attend(q, base, relay, ship):
        for k, some in enumerate(places):
            @pl.when(q == k + 1)
            def _():
                prepare_all(some)

        a = pair_of(xn_all, base)
        for at, size in tiles(2 * ch):
            w = wall[0, :, :, :, at : at + size].reshape(width, size)
            qkv[pl.ds(base, 2), :, at : at + size] = nn(a, w).reshape(2, rows, size)
        relay()
        both(base, attend_block)
        for k, some in enumerate(middles):
            @pl.when(q == k + 1)
            def _():
                prepare_all(some)

        a = pair_of(att, base)
        for k in range(n):
            ship(k, nn(a, wo[:, k * piece : (k + 1) * piece]))

    each_pair(xn_all, 0, attend)
    settle_through(0)
    prepare_all(leftover[:1])
    settle_own(0)

    @by_rows
    def _(at):
        h = xin[at].astype(F32) + summed(0, at)
        hres[at] = h
        r2 = lax.rsqrt(mean_last(h * h) + EPS)
        hn_all[me, at] = (h * r2 * ln2[...]).astype(BF16)

    spread_start(hn_all, 1)
    put("xn", xn_all)
    put("att", att)

    prepare_all(leftover[1:])
    for c in range(1, chunks):
        prepare(c, steps)

    @pl.when(sec == 0)
    def _():
        pl.semaphore_signal(turn, inc=1, device_id={"section": 1}, device_id_type=MESH)

    if fused:
        @pl.when(sec == 1)
        def _():
            pl.semaphore_signal(r.later, inc=1, device_id={"section": 0}, device_id_type=MESH)

    def feed(q, base, relay, ship):
        a = pair_of(hn_all, base)
        here = pl.ds(base, 2)
        for at in range(0, hidden, ch):
            j = 1 + at // ch
            g = nn(a, wall[j, :, :, :, :ch].reshape(width, ch))
            u = nn(a, wall[j, :, :, :, ch:].reshape(width, ch))
            gate[here, :, at : at + ch] = g.astype(BF16).reshape(2, rows, ch)
            up[here, :, at : at + ch] = u.astype(BF16).reshape(2, rows, ch)
            value = (g * jax.nn.sigmoid(g) * u).astype(BF16)
            act[here, :, at : at + ch] = value.reshape(2, rows, ch)
        relay()

        @pl.when(jnp.logical_and(sec == 1, q == 0))
        def _():
            load_y.wait()
            spread_start(dy_all, 2)

        a = pair_of(act, base)
        for k in range(n):
            ship(k, nn(a, wd[:, k * piece : (k + 1) * piece]))

    each_pair(hn_all, 1, feed)

    def write_y():
        @by_rows
        def _(at):
            yv[at] = (hres[at] + summed(1, at)).astype(BF16)

    if fused:
        def place(slot):
            return wall.at[1 + slot // n, slot % n]

        view = types.SimpleNamespace(**{**vars(r), "hn": hn_all, "dab": dab_all})
        strip = ch // rep

        def far_out():
            yield pltpu.make_async_copy(hn_all, r.hn_far.at[mine], r.far_own.at[2 * chunks])
            for m in range(1, rep):
                yield remote(
                    hn_all, r.hn_far.at[mine], r.far_send.at[m - 1, 0], r.far_recv.at[m - 1, 0],
                    {"replica": peer(mine, rep, m)},
                )

        def strips_out():
            for k in range(2 * (chunks - 1)):
                to = wall.at[chunks - 1, :, mine, :, pl.ds(k * strip, strip)]
                own = pl.ds(pl.multiple_of(k * ch + mine * strip, strip), strip)
                yield pltpu.make_async_copy(dgu.at[:, :, own], to, r.far_own.at[k])
                for m in range(1, rep):
                    other = peer(mine, rep, m)
                    cols = pl.ds(pl.multiple_of(k * ch + other * strip, strip), strip)
                    yield remote(
                        dgu.at[:, :, cols], to, r.far_send.at[m - 1, k + 1],
                        r.far_recv.at[m - 1, k + 1], {"replica": other},
                    )

        def far_ready():
            for copy in (*far_out(), *strips_out()):
                copy.wait()

        far = types.SimpleNamespace(
            here=sec == 0,
            ready=far_ready,
            left=lambda block: wall.at[2, 2 + block // 2, :, :, pl.ds(block % 2 * n * 128, n * 128)],
            right=lambda block: wall.at[chunks - 1, block],
            held=wall.at[2, 1],
        )
        stream = grad_stream(view, n, rep, lambda slot: r.ours.at[slot], place, far)

    put("hn", hn_all)
    put("act", act)

    @pl.when(sec == 0)
    def _():
        settle_through(1)
        settle_own(1)
        write_y()
        hand(yv, xin, 1, 0).start()
        if fused:
            pl.semaphore_wait(r.later, 1)
            for copy in far_out():
                copy.start()
        hand(yv, dy_all.at[me], 1, 1).wait_recv()
        spread_start(dy_all, 2)

    spread_done(hn_all, 1)
    put_done("hn")

    def early_tick(t):
        if fused:
            stream.tick(t, (0, 1))

    def early(low, high):
        if fused:
            lax.fori_loop(low, high, lambda t, carry: early_tick(t) or carry, 0)

    def feed_back(q, base, relay, ship):
        @pl.when(q == n // 2 - 1)
        def _():
            if fused:
                stream.prime(0)
            early_tick(0)

        a = pair_of(dy_all, base)
        here = pl.ds(base, 2)
        for at in range(0, hidden, ch):
            dact = nt(a, wd[at : at + ch, :])
            g = gate[here, :, at : at + ch].reshape(2 * rows, ch).astype(F32)
            u = up[here, :, at : at + ch].reshape(2 * rows, ch).astype(F32)
            sig = jax.nn.sigmoid(g)
            dg = (dact * u * sig * (1.0 + g * (1.0 - sig))).astype(BF16)
            du = (dact * g * sig).astype(BF16)
            dgu[here, :, 2 * at : 2 * at + ch] = dg.reshape(2, rows, ch)
            dgu[here, :, 2 * at + ch : 2 * at + 2 * ch] = du.reshape(2, rows, ch)
        relay()

        @pl.when(jnp.logical_and(sec == 1, q == n // 2 - 1))
        def _():
            settle_through(1)

        @pl.when(q == n // 2 - 1)
        def _():
            early_tick(1)

        a = pair_of(dgu, base)
        for f in range(n):
            total = jnp.zeros((2 * rows, kfold), F32)
            for j in range(1, chunks):
                w = wall[j, f].reshape(kfold, 2 * ch)
                total = total + nt(a[:, 2 * (j - 1) * ch : 2 * j * ch], w)
            ship(f, total)

    each_pair(dy_all, 2, feed_back)


    if fused:
        for where in [{"fsdp": lax.rem(me + d, n)} for d in range(1, n)] + [
            {"replica": peer(mine, rep, m)} for m in range(1, rep)
        ]:
            pl.semaphore_signal(r.freed, inc=1, device_id=where, device_id_type=MESH)
    early_tick(2)
    settle_through(2)
    if fused:
        pl.semaphore_wait(r.freed, n - 1 + rep - 1)

        @pl.when(sec == 0)
        def _():
            for copy in strips_out():
                copy.start()
    early_tick(3)

    @pl.when(sec == 1)
    def _():
        settle_own(1)
        write_y()

    settle_own(2)
    dln2[...] = jnp.zeros_like(dln2)
    dln1[...] = jnp.zeros_like(dln1)

    @by_rows
    def _(at):
        dhn = summed(2, at)
        h = hres[at]
        r2 = lax.rsqrt(mean_last(h * h) + EPS)
        u = dhn * ln2[...]
        dh = dy_all[me, at].astype(F32) + (r2 * u - h * r2 * r2 * r2 * mean_last(u * h))
        dln2[...] += jnp.sum(dhn * h * r2, axis=0, keepdims=True)
        hres[at] = dh
        dab_all[me, at] = dh.astype(BF16)

    spread_start(dab_all, 3)
    early(4, 6)

    put("y", yv)
    put("dy", dy_all)
    put("dgu", dgu)

    dqn[...] = jnp.zeros_like(dqn)
    dkn[...] = jnp.zeros_like(dkn)

    def head_back(s, at, grad, gain, dgain):
        field = qkv[s, :, at : at + hd]
        factor = lax.rsqrt(mean_last(field * field) + EPS)
        grad = grad * cosine[...] - swap(grad) * sine[...]
        v = grad * gain
        back = factor * v - field * factor * factor * factor * mean_last(v * field)
        dgain[...] += jnp.sum(grad * field * factor, axis=0, keepdims=True)
        dqkv[s, :, at : at + hd] = back.astype(BF16)

    def attend_back_block(i, s):
        for kv in range(kcols // hd):
            kat = qcols + kv * hd
            vat = qcols + kcols + kv * hd
            kh = qkvb[s, :, kat : kat + hd]
            vh = qkvb[s, :, vat : vat + hd]
            dk = jnp.zeros((rows, hd), F32)
            dv = jnp.zeros((rows, hd), F32)
            for j in range(kv * qcols // kcols, (kv + 1) * qcols // kcols):
                qh = qkvb[s, :, j * hd : (j + 1) * hd]
                dh_out = dob[i, :, j * hd : (j + 1) * hd]
                probs = masked_scores(qh, kh)
                dv = dv + tn(probs.astype(BF16), dh_out)
                dp = nt(dh_out, vh)
                delta = jnp.sum(probs * dp, axis=-1, keepdims=True)
                ds = (probs * (dp - delta) * scale).astype(BF16)
                dk = dk + tn(ds, qh)
                head_back(s, j * hd, nn(ds, kh), qn[...], dqn)
            head_back(s, kat, dk, kn[...], dkn)
            dqkv[s, :, vat : vat + hd] = dv.astype(BF16)
    def attend_back(q, base, relay, ship):
        a = pair_of(dab_all, base)
        for at, size in tiles(qcols):
            dout = nt(a, wo[at : at + size, :]).astype(BF16)
            dob[:, :, at : at + size] = dout.reshape(2, rows, size)
        relay()
        early(6 + 2 * q, 8 + 2 * q)
        lax.fori_loop(0, 2, lambda i, carry: attend_back_block(i, base + i) or carry, 0)
        a = pair_of(dqkv, base)
        for f in range(n):
            w = wall[0, f].reshape(kfold, 2 * ch)
            ship(f, nt(a, w))

    each_pair(dab_all, 3, attend_back)
    early_tick(6 + n)
    settle_through(3)
    early_tick(7 + n)
    settle_own(3)
    put_done("y")

    @pl.when(sec == 0)
    def _():
        hand(yv, xin, 1, 0).wait_send()

    @by_rows
    def _(at):
        dxn = summed(3, at)
        x32 = xin[at].astype(F32)
        r1 = lax.rsqrt(mean_last(x32 * x32) + EPS)
        u = dxn * ln1[...]
        dx = hres[at] + (r1 * u - x32 * r1 * r1 * r1 * mean_last(u * x32))
        dln1[...] += jnp.sum(dxn * x32 * r1, axis=0, keepdims=True)
        yv[at] = dx.astype(BF16)
        hres[at] = dx

    @pl.when(sec == 1)
    def _():
        hand(yv, dy_all.at[me], 0, 1).start()

    put("dx", hres)
    put("dab", dab_all)
    put("dqkv", dqkv)
    if fused:
        stream.pack_fill((dln1, dln2, dqn, dkn))
        stream.pack_start()
        stream.finish(8 + n)
    for c, buf in ((0, xn_all), (2, dy_all), (3, dab_all)):
        spread_done(buf, c)

    @pl.when(sec == 1)
    def _():
        hand(yv, dy_all.at[me], 0, 1).wait_send()

    put_done(*list(outs))


def run_layer(n, rep, fused, lanes, tok, cot, ln1, ln2, qn, kn, wq, wk, wv, wg, wu, wo, wd):
    rows, width = tok.shape
    hd = n * qn.shape[-1]
    qcols = wo.shape[0]
    qkvcols = 2 * qcols
    steps = rep.bit_length() - 1
    chunks = 1 + wd.shape[0] // qcols
    hidden = wd.shape[0]
    cosine, sine = rope_tables(rows, hd // 2)
    inputs = {
        "tok": tok, "cot": cot, "ln1_own": ln1, "ln2_own": ln2, "qn_own": qn, "kn_own": kn,
        "cosine": cosine, "sine": sine, "wq_h": wq, "wk_h": wk, "wv_h": wv, "wg_h": wg, "wu_h": wu,
        "wo_h": wo, "wd_h": wd,
    }
    in_vmem = ("ln1_own", "ln2_own", "qn_own", "kn_own", "cosine", "sine")
    single = {"dln1": (1, width), "dln2": (1, width), "dqn": (1, hd), "dkn": (1, hd)}
    outputs = {
        "y_h": jax.ShapeDtypeStruct((rows, width), BF16),
        "dx_h": jax.ShapeDtypeStruct((rows, width), F32),
    }
    saved = {
        "xn": width, "hn": width, "dy": width, "dab": width, "att": qcols, "act": hidden,
        "dgu": 2 * hidden, "dqkv": qkvcols,
    }
    dma = pltpu.SemaphoreType.DMA
    scratch = {
        "wall": pltpu.VMEM((chunks, n, rep, width // (n * rep), qkvcols), BF16),
        "wo": pltpu.VMEM(wo.shape, BF16),
        "wd": pltpu.VMEM(wd.shape, BF16),
        "ln1": pltpu.VMEM((1, width), F32),
        "ln2": pltpu.VMEM((1, width), F32),
        "qn": pltpu.VMEM((1, hd), F32),
        "kn": pltpu.VMEM((1, hd), F32),
        "gains": pltpu.VMEM((n, 1, lanes), F32),
        "xin": pltpu.VMEM((rows, width), BF16),
        **{
            key: pltpu.VMEM((n, rows, size), BF16)
            for key, size in saved.items() if fused or key != "dab"
        },
        "qkv": pltpu.VMEM((n, rows, qkvcols), F32),
        "qkvb": pltpu.VMEM((n, rows, qkvcols), BF16),
        "hres": pltpu.VMEM((rows, width), F32),
        "gate": pltpu.VMEM((n, rows, hidden), BF16),
        "up": pltpu.VMEM((n, rows, hidden), BF16),
        "dob": pltpu.VMEM((2, rows, qcols), BF16),
        "yv": pltpu.VMEM((rows, width), BF16),
        "sbuf": pltpu.VMEM((2, n, rows, width), BF16),
        "rbuf": pltpu.VMEM((2, n - 1, rows, width), BF16),
        "w_sem": dma((4,)),
        "zw_send": dma((chunks, n - 1, 3)),
        "zw_recv": dma((chunks, n - 1, 3)),
        "gw_send": dma((steps, chunks, 2, rep // 2)),
        "gw_recv": dma((steps, chunks, 2, rep // 2)),
        "own_sem": dma((chunks, 3)),
        "gain_send": dma((n - 1,)),
        "gain_recv": dma((n - 1,)),
        "turn": pltpu.SemaphoreType.REGULAR,
        "out_sem": dma((10,)),
        "ag_send": dma((4, n)),
        "ag_recv": dma((4, n)),
        "rs_send": dma((4, n, n)),
        "rs_recv": dma((4, n, n)),
        "hand_send": dma((2,)),
        "hand_recv": dma((2,)),
    }
    if fused:
        outputs |= stream_outputs(n, rep, qcols, hidden, width, lanes)
        scratch |= {key: pltpu.VMEM(shape, F32) for key, shape in single.items()}
        scratch |= stream_scratch(n, rep, qcols, lanes)
        outputs["hn_far"] = jax.ShapeDtypeStruct((rep, n, rows, width), BF16)
        scratch["freed"] = pltpu.SemaphoreType.REGULAR
        scratch["later"] = pltpu.SemaphoreType.REGULAR
        scratch["far_own"] = dma((2 * chunks + 1,))
        scratch["far_send"] = dma((rep - 1, 2 * chunks))
        scratch["far_recv"] = dma((rep - 1, 2 * chunks))
        scratch["far_load"] = dma((n, n))
        scratch["ours"] = pltpu.VMEM((steps + 1, rep, 128, 2 * qcols), BF16)
    else:
        outputs |= {
            key + "_h": jax.ShapeDtypeStruct((n, rows, size), BF16) for key, size in saved.items()
        }
        outputs |= {key: jax.ShapeDtypeStruct(shape, F32) for key, shape in single.items()}
    out_vmem = (*single, "sums")
    return call(
        layer_kernel, (n, rep, hd, fused), inputs, outputs, scratch, in_vmem, out_vmem, "layer", 0
    )


def run_grads(n, rep, saved, lanes):
    steps = rep.bit_length() - 1
    ch, hidden, width = (saved[key].shape[-1] for key in ("att_h", "act_h", "xn_h"))
    inputs = {key: value for key, value in saved.items() if key not in ("y_h", "dx_h")}
    scratch = {
        key[:-2]: pltpu.VMEM(value.shape, BF16) for key, value in inputs.items() if key[-2:] == "_h"
    }
    scratch["ours"] = pltpu.VMEM((steps + 1, rep, 128, 2 * ch), BF16)
    scratch["whole"] = pltpu.VMEM((steps + 3, rep, 128, 2 * ch), BF16)
    scratch["in_sem"] = pltpu.SemaphoreType.DMA((8,))
    scratch |= stream_scratch(n, rep, ch, lanes)
    outputs = stream_outputs(n, rep, ch, hidden, width, lanes)
    small = ("dln1", "dln2", "dqn", "dkn")
    return call(grad_kernel, (n, rep), inputs, outputs, scratch, small, ("sums",), "grads", 1)


def write_results(sources, sums, gains, y, dx):
    steps = 16

    moved = [*sources, y, dx]

    def rows_of(value):
        return pl.BlockSpec((value.shape[0] // steps, value.shape[1]), lambda i: (i, 0))

    def all_of(columns):
        return pl.BlockSpec((1, columns), lambda i: (0, 0))

    kinds = [F32] * len(sources) + [BF16, F32]

    def kernel(*refs):
        ins, outs = refs[: len(moved) + 1], refs[len(moved) + 1 :]
        for src, dst in zip(ins, outs[: len(moved)]):
            dst[...] = src[...].astype(dst.dtype)
        at = 0
        for size, dst in zip(gains, outs[len(moved) :]):
            dst[...] = ins[-1][:, at : at + size]
            at += size

    return pl.pallas_call(
        kernel,
        grid=(steps,),
        out_shape=[jax.ShapeDtypeStruct(v.shape, kind) for v, kind in zip(moved, kinds)]
        + [jax.ShapeDtypeStruct((1, size), F32) for size in gains],
        in_specs=[rows_of(value) for value in moved] + [all_of(sums.shape[1])],
        out_specs=[rows_of(value) for value in moved] + [all_of(size) for size in gains],
        compiler_params=pltpu.CompilerParams(vmem_limit_bytes=67043328),
        name="results",
    )(*moved, sums)


def per_device(tokens_in, cotangent, ln1, wq, wk, wv, qn, kn, wo, ln2, wg, wu, wd):
    n, rep = lax.axis_size("fsdp"), lax.axis_size("replica")

    lanes = -(-2 * (ln1.shape[-1] + qn.shape[-1]) // 128) * 128
    thirds = grad_plan(n, wo.shape[1], wd.shape[1], wo.shape[2])[1]
    fused = (2 * rep.bit_length() + 2) <= n * thirds and wq.shape[1] == n * 128
    fused = fused and n == rep == 4 and thirds == 3
    done = run_layer(
        n, rep, fused, lanes, tokens_in, cotangent, ln1, ln2, qn, kn,
        wq[0], wk[0], wv[0], wg[0], wu[0], wo[0], wd[0],
    )
    y, dx = done["y_h"], done["dx_h"]
    if not fused:
        done = run_grads(n, rep, done, lanes)
    sources = [
        done[key].reshape(-1, done[key].shape[-1])
        for key in ("gq_h", "gk_h", "gv_h", "go_h", "gg_h", "gu_h", "gd_h")
    ]
    gains = [gain.shape[1] for gain in (ln1, ln2, qn, kn)]
    (
        g_wq, g_wk, g_wv, g_wo, g_wg, g_wu, g_wd, y, dx, *owned
    ) = write_results(sources, done["sums"], gains, y, dx)
    g_ln1, g_ln2, g_qn, g_kn = (value[0] for value in owned)
    results = (y, dx, g_ln1, g_wq, g_wk, g_wv, g_qn, g_kn, g_wo, g_ln2, g_wg, g_wu, g_wd)
    return tuple(value[None] for value in results)


def solution(mesh):
    rows = P("section", "fsdp", None)
    gain = P("section", "fsdp")
    tokens = P(("fsdp", "replica"), None)
    stacked = P("section", ("fsdp", "replica"), None)
    weights = (gain, rows, rows, rows, gain, gain, rows, gain, rows, rows, rows)
    return jax.shard_map(
        per_device,
        mesh=mesh,
        in_specs=(tokens, tokens, *weights),
        out_specs=(stacked, stacked, *weights),
        check_vma=False,
    )
```

```python
import functools
import math
import types

import jax
import jax.numpy as jnp
from jax import lax
from jax.experimental import pallas as pl
from jax.experimental.pallas import tpu as pltpu
from jax.sharding import PartitionSpec as P

LEN = 128
EPS = 1e-06
F32 = jnp.float32
BF16 = jnp.bfloat16
MESH = pl.DeviceIdType.MESH
TILE = 512


def rope_tables(length, half_dim):
    freq = jnp.exp(jnp.arange(half_dim, dtype=F32) * (-math.log(1000000.0) / half_dim))
    angle = jnp.arange(length, dtype=F32)[:, None] * freq[None, :]
    cosine, sine = jnp.cos(angle), jnp.sin(angle)
    return (
        jnp.concatenate([cosine, cosine], axis=1),
        jnp.concatenate([-sine, sine], axis=1),
    )


def nn(left, right):
    return jnp.dot(left, right, preferred_element_type=F32)


def nt(left, right):
    return lax.dot_general(left, right, (((1,), (1,)), ((), ())), preferred_element_type=F32)


def tn(left, right):
    return lax.dot_general(left, right, (((0,), (0,)), ((), ())), preferred_element_type=F32)


def mean_last(value):
    return jnp.mean(value, axis=-1, keepdims=True)


def tiles(total):
    return [(at, min(TILE, total - at)) for at in range(0, total, TILE)]


def flip(value, bit):
    return value + (1 - 2 * (value // 2**bit % 2)) * 2**bit


def flips(value, bits, subset):
    for at, bit in enumerate(bits):
        if subset >> at & 1:
            value = flip(value, bit)
    return value


def grad_plan(n, qcols, hidden, width):
    blocks = width // n // 128
    thirds = hidden // qcols
    return blocks, thirds, (hidden // 256, blocks * thirds, qcols // 256, blocks)


def rem(value, by):
    return value % by if isinstance(value, int) else lax.rem(value, by)


def within(value, low, high):
    if isinstance(value, int):
        return low <= value < high
    return jnp.logical_and(value >= low, value < high)


def both(first, second):
    if isinstance(first, bool):
        return second if first else False
    return jnp.logical_and(first, second)


def when(condition):
    if isinstance(condition, bool):
        return lambda work: work() if condition else None
    return pl.when(condition)


def remote(src, dst, send, recv, where):
    return pltpu.make_async_remote_copy(
        src_ref=src, dst_ref=dst, send_sem=send, recv_sem=recv,
        device_id=where, device_id_type=MESH,
    )


def grad_stream(r, n, rep, ours, whole, far=None):
    me = lax.axis_index("fsdp")
    mine = lax.axis_index("replica")
    steps = rep.bit_length() - 1
    g_slots, slots = steps + 1, steps + 3
    ch = r.att.shape[-1]
    part = 128 // n
    width = r.xn.shape[-1]
    tokens = r.xn.shape[0] * r.xn.shape[1]
    fold = width // n
    hidden = r.act.shape[-1]
    kcols = r.gk_h.shape[-1] // n
    thirds = grad_plan(n, ch, hidden, width)[1]
    counts = grad_plan(n, ch, hidden, width)[2]
    starts = [sum(counts[:k]) for k in range(len(counts) + 1)]
    total = starts[-1]
    orders = (tuple(range(steps)), tuple(reversed(range(steps))))
    got = [getattr(r, f"got{j}") for j in range(steps)]
    strip = ch // rep

    def lanes(h):
        return pl.ds(h * ch, ch)

    def scatter_copies(c, j):
        slot, two = rem(c, g_slots), rem(c, 2)
        for h, bits in enumerate(orders):
            partner = flip(mine, bits[j])
            for i in range(rep >> (j + 1)):
                piece = flips(partner, bits[j + 1 :], i)
                yield remote(
                    ours(slot).at[piece, :, lanes(h)], got[j].at[two, h, i],
                    r.grs_send.at[j, two, h, i], r.grs_recv.at[j, two, h, i],
                    {"replica": partner},
                )

    def owner_part(owner, apart):
        if apart:
            return slice(None), pl.ds(aligned(owner * 2 * strip), 2 * strip)
        return pl.ds(pl.multiple_of(owner * part, part), part), slice(None)

    def across_copies(c, apart):
        slot, two = rem(c, slots), rem(c, 2)
        for d in range(1, n):
            to = lax.rem(me + d, n)
            yield remote(
                r.reduced.at[owner_part(to, apart)],
                whole(slot).at[(mine, *owner_part(me, apart))],
                r.gz_send.at[two, d - 1], r.gz_recv.at[two, d - 1], {"fsdp": to},
            )

    def gather_copies(c, j):
        slot, three = rem(c, slots), rem(c, 3)
        for h, order in enumerate(orders):
            bits = order[::-1]
            partner = flip(mine, bits[j])
            for i in range(1 << j):
                ref = whole(slot).at[flips(mine, bits[:j], i), :, lanes(h)]
                yield remote(
                    ref, ref, r.gag_send.at[j, three, h, i], r.gag_recv.at[j, three, h, i],
                    {"replica": partner},
                )

    def aligned(at):
        return pl.multiple_of(at, 128)

    def out_copies(c, kind, apart):
        slot, two = rem(c, slots), rem(c, 2)
        at = c - starts[kind]
        for f in range(n):
            rows = pl.ds(f * part, part)
            if kind == 1:
                k, j = at // thirds, rem(at, thirds)
                pairs = []
                for h, dst in enumerate((r.gg_h, r.gu_h)):
                    for q in range(rep):
                        if apart:
                            src = whole(slot).at[q, :, pl.ds((2 * f + h) * strip, strip)]
                            cols = pl.ds(aligned(f * hidden + j * ch + q * strip), strip)
                            to = dst.at[k, :, cols]
                        else:
                            src = whole(slot).at[q, rows, lanes(h)]
                            cols = pl.ds(aligned(f * hidden + j * ch), ch)
                            to = dst.at[k, pl.ds(q * (128 // rep), 128 // rep), cols]
                        pairs.append((src, to))
            elif kind == 3:
                cols = pl.ds(f * kcols, kcols)
                pairs = [
                    (whole(slot).at[:, rows, lanes(0)], r.gq_h.at[at, :, :, pl.ds(f * ch, ch)]),
                    (whole(slot).at[:, rows, pl.ds(ch, kcols)], r.gk_h.at[at, :, :, cols]),
                    (whole(slot).at[:, rows, pl.ds(ch + kcols, kcols)], r.gv_h.at[at, :, :, cols]),
                ]
            else:
                dst = r.gd_h if kind == 0 else r.go_h
                pairs = [
                    (
                        whole(slot).at[f, :, lanes(h)],
                        dst.at[pl.ds(aligned(at * 256 + h * 128), 128), pl.ds(f * ch, ch)],
                    )
                    for h in range(2)
                ]
            for i, (src, to) in enumerate(pairs):
                yield pltpu.make_async_copy(src, to, r.gout_sem.at[two, f, i])

    def columns_of(ref, at, size):
        return ref[:, :, pl.ds(at, size)].reshape(tokens, size)

    def compute(c, kind):
        to = ours(rem(c, g_slots))
        at = c - starts[kind]
        if kind in (1, 3):
            left, right = (r.hn, r.dgu) if kind == 1 else (r.xn, r.dqkv)
            k, j = (at // thirds, rem(at, thirds)) if kind == 1 else (at, 0)
            lefts = jnp.concatenate(
                [columns_of(left, aligned(f * fold + k * 128), 128) for f in range(n)], axis=1
            )
            for h in range(2):
                product = tn(lefts, columns_of(right, aligned((2 * j + h) * ch), ch)).astype(BF16)
                for f in range(n):
                    block = product[f * 128 : (f + 1) * 128].reshape(rep, 128 // rep, ch)
                    to[:, f * part : (f + 1) * part, h * ch : (h + 1) * ch] = block
        else:
            left, right = (r.act, r.dy) if kind == 0 else (r.att, r.dab)
            lefts = columns_of(left, aligned(at * 256), 256)
            for q in range(rep):
                product = tn(lefts, columns_of(right, q * ch, ch)).astype(BF16)
                for h in range(2):
                    to[q, :, h * ch : (h + 1) * ch] = product[h * 128 : (h + 1) * 128]

    def full_product(c):
        at = c - starts[1]
        k, j = at // thirds, rem(at, thirds)

        @when(at == 0)
        def _():
            far.ready()

        @when(j == 0)
        def _():
            loads = [
                pltpu.make_async_copy(
                    r.hn_far.at[:, block, :, pl.ds(aligned(f * fold + k * 128), 128)],
                    far.left(block).at[:, :, pl.ds(f * 128, 128)], r.far_load.at[block, f],
                )
                for block in range(n) for f in range(n)
            ]
            for load in loads:
                load.start()
            for load in loads:
                load.wait()

            def owner_rows(f, carry):
                rows = pl.ds(pl.multiple_of(f * 128, 128), 128)
                product = jnp.zeros((128, thirds * 2 * strip), F32)
                for block in range(n):
                    left = far.left(block)[:, :, rows].reshape(rep * 128, 128)
                    right = far.right(block)[:, :, : thirds * 2 * strip]
                    product = product + tn(left, right.reshape(rep * 128, thirds * 2 * strip))
                for third in range(thirds):
                    value = product[:, third * 2 * strip : (third + 1) * 2 * strip].astype(BF16)
                    far.held[third, :, pl.ds(aligned(f * 2 * strip), 2 * strip)] = value
                return carry

            lax.fori_loop(0, n, owner_rows, 0)

        r.reduced[...] = far.held[j]

    def tick(t, kinds=(0, 1, 2, 3)):
        def is_kind(c, kind):
            return within(c, starts[kind], starts[kind + 1])

        def cases(c):
            for kind in kinds:
                hit = is_kind(c, kind)
                if far is None or kind != 1:
                    yield hit, kind, False
                else:
                    yield both(hit, jnp.logical_not(far.here)), kind, False
                    yield both(hit, far.here), kind, True

        def exchanged(c):
            hit = within(c, 0, total)
            apart = is_kind(c, 1)
            if far is None or apart is False:
                return hit
            if apart is True:
                return both(hit, jnp.logical_not(far.here))
            return jnp.logical_and(hit, jnp.logical_not(jnp.logical_and(apart, far.here)))

        c_done = t - (2 * steps + 2)
        for hit, kind, apart in cases(c_done):
            @when(hit)
            def _():
                for copy in out_copies(c_done, kind, apart):
                    copy.wait()

        for j in reversed(range(1, steps)):
            c_ag = t - (steps + 1 + j)

            @when(within(c_ag, 0, total))
            def _():
                for copy in gather_copies(c_ag, j - 1):
                    copy.wait()
                for copy in gather_copies(c_ag, j):
                    copy.start()

        c_z = t - (steps + 1)
        for hit, kind, apart in cases(c_z):
            @when(hit)
            def _():
                if kind in (1, 3):
                    for copy in across_copies(c_z, apart):
                        copy.wait()
                else:
                    for d in range(1, n):
                        pl.semaphore_wait(r.gsig.at[rem(c_z, 2), d - 1], 1)

        @when(within(c_z, 0, total))
        def _():
            for copy in gather_copies(c_z, 0):
                copy.start()

        for j in reversed(range(steps)):
            c_rs = t - (j + 1)

            @when(exchanged(c_rs))
            def _():
                for copy in scatter_copies(c_rs, j):
                    copy.wait()
                for h, bits in enumerate(orders):
                    half = slice(h * ch, (h + 1) * ch)
                    for i in range(rep >> (j + 1)):
                        piece = flips(mine, bits[j + 1 :], i)
                        value = ours(rem(c_rs, g_slots))[piece, :, half].astype(F32)
                        value = (value + got[j][rem(c_rs, 2), h, i].astype(F32)).astype(BF16)
                        if j < steps - 1:
                            ours(rem(c_rs, g_slots))[piece, :, half] = value
                        else:
                            r.reduced[:, half] = value
                if j < steps - 1:
                    for copy in scatter_copies(c_rs, j + 1):
                        copy.start()

            if j == steps - 1:
                for hit, kind, apart in cases(c_rs):
                    @when(hit)
                    def _():
                        to = whole(rem(c_rs, slots))
                        if apart:
                            full_product(c_rs)
                        if kind in (1, 3):
                            for copy in across_copies(c_rs, apart):
                                copy.start()
                            own = owner_part(me, apart)
                            to[(mine, *own)] = r.reduced[own]
                        else:
                            for d in range(1, n):
                                pl.semaphore_signal(
                                    r.gsig.at[rem(c_rs, 2), d - 1], inc=1,
                                    device_id={"fsdp": lax.rem(me + d, n)}, device_id_type=MESH,
                                )
                            to[mine] = r.reduced[...]

        @when(exchanged(t))
        def _():
            for copy in scatter_copies(t, 0):
                copy.start()

        for hit, kind, apart in cases(t + 1):
            if not apart:
                @when(hit)
                def _():
                    compute(t + 1, kind)

        c_out = t - (2 * steps + 1)

        @when(within(c_out, 0, total))
        def _():
            for copy in gather_copies(c_out, steps - 1):
                copy.wait()

        for hit, kind, apart in cases(c_out):
            @when(hit)
            def _():
                for copy in out_copies(c_out, kind, apart):
                    copy.start()

    def pack_across(d):
        to = lax.rem(me + d, n)
        return remote(
            r.pack.at[to], r.pack_z.at[d - 1], r.pz_send.at[d - 1], r.pz_recv.at[d - 1], {"fsdp": to}
        )

    def pack_swap(j):
        return remote(
            r.pack_r.at[j], r.pack_in.at[j], r.pr_send.at[j], r.pr_recv.at[j],
            {"replica": flip(mine, j)},
        )

    def pack_fill(dgains):
        r.pack[...] = jnp.zeros_like(r.pack)
        at = 0
        for value in dgains:
            size = value.shape[-1] // n
            for f in range(n):
                r.pack[f, :, at : at + size] = value[:, f * size : (f + 1) * size]
            at += size

    def pack_start():
        for d in range(1, n):
            pack_across(d).start()

    def pack_tick(t):
        for j in range(steps + 1):
            @pl.when(t == 2 * j + 2)
            def _():
                if j == 0:
                    value = r.pack[me]
                    for d in range(1, n):
                        pack_across(d).wait()
                        value = value + r.pack_z[d - 1]
                else:
                    pack_swap(j - 1).wait()
                    value = r.pack_r[j - 1] + r.pack_in[j - 1]
                if j < steps:
                    r.pack_r[j] = value
                    pack_swap(j).start()
                else:
                    r.sums[...] = value

    def finish(first):
        def step(t, carry):
            tick(t)
            pack_tick(t - first)
            return carry

        lax.fori_loop(first, total + 2 * steps + 3, step, 0)

    return types.SimpleNamespace(
        tick=tick, prime=lambda kind: compute(0, kind), pack_fill=pack_fill, pack_start=pack_start, finish=finish
    )


def stream_scratch(n, rep, ch, lanes):
    steps = rep.bit_length() - 1
    dma = pltpu.SemaphoreType.DMA
    swap = dma((steps, 2, 2, rep // 2))
    return {
        "reduced": pltpu.VMEM((128, 2 * ch), BF16),
        "pack": pltpu.VMEM((n, 1, lanes), F32),
        "pack_z": pltpu.VMEM((n - 1, 1, lanes), F32),
        "pack_r": pltpu.VMEM((steps, 1, lanes), F32),
        "pack_in": pltpu.VMEM((steps, 1, lanes), F32),
        **{
            f"got{j}": pltpu.VMEM((2, 2, rep >> (j + 1), 128, ch), BF16) for j in range(steps)
        },
        "grs_send": swap, "grs_recv": swap,
        "gz_send": dma((2, n - 1)), "gz_recv": dma((2, n - 1)),
        "gag_send": dma((steps, 3, 2, rep // 2)), "gag_recv": dma((steps, 3, 2, rep // 2)),
        "gout_sem": dma((2, n, 2 * rep)),
        "pz_send": dma((n - 1,)), "pz_recv": dma((n - 1,)),
        "pr_send": dma((steps,)), "pr_recv": dma((steps,)),
        "gsig": pltpu.SemaphoreType.REGULAR((2, n - 1)),
    }


def stream_outputs(n, rep, ch, hidden, width, lanes):
    kcols = ch // 2

    def owned(columns):
        return jax.ShapeDtypeStruct((width // n // 128, rep, 128 // rep, columns * n), BF16)

    return {
        "gq_h": owned(ch), "gk_h": owned(kcols), "gv_h": owned(kcols),
        "go_h": jax.ShapeDtypeStruct((ch, width), BF16),
        "gg_h": jax.ShapeDtypeStruct((width // n // 128, 128, hidden * n), BF16),
        "gu_h": jax.ShapeDtypeStruct((width // n // 128, 128, hidden * n), BF16),
        "gd_h": jax.ShapeDtypeStruct((hidden, width), BF16),
        "sums": jax.ShapeDtypeStruct((1, lanes), F32),
    }


def named(body, names, *args):
    def kernel(*refs):
        body(types.SimpleNamespace(**dict(zip(names, refs))), *args)

    return kernel


def call(body, args, inputs, outputs, scratch, in_vmem, out_vmem, name, collective):
    vm = pl.BlockSpec(memory_space=pltpu.VMEM)
    hbm = pl.BlockSpec(memory_space=pltpu.HBM)
    results = pl.pallas_call(
        named(body, [*inputs, *outputs, *scratch], *args),
        out_shape=list(outputs.values()),
        in_specs=[vm if key in in_vmem else hbm for key in inputs],
        out_specs=[vm if key in out_vmem else hbm for key in outputs],
        scratch_shapes=list(scratch.values()),
        compiler_params=pltpu.CompilerParams(
            collective_id=collective, has_side_effects=True, vmem_limit_bytes=67043328
        ),
        name=name,
    )(*inputs.values())
    return dict(zip(outputs, results))


def peer(mine, rep, m):
    return flips(mine, range(rep.bit_length() - 1), m)


def greet(n, rep, me, mine):
    barrier = pltpu.get_barrier_semaphore()
    for d in range(1, n):
        pl.semaphore_signal(
            barrier, inc=1, device_id={"fsdp": lax.rem(me + d, n)}, device_id_type=MESH
        )
    for m in range(1, rep):
        pl.semaphore_signal(
            barrier, inc=1, device_id={"replica": peer(mine, rep, m)}, device_id_type=MESH
        )
    return barrier


def grad_kernel(r, n, rep):
    me = lax.axis_index("fsdp")
    mine = lax.axis_index("replica")
    barrier = greet(n, rep, me, mine)
    loads = []
    for k, key in enumerate(("act", "dy", "hn", "dgu", "att", "dab", "xn", "dqkv")):
        loads.append(
            pltpu.make_async_copy(getattr(r, key + "_h"), getattr(r, key), r.in_sem.at[k])
        )
        loads[-1].start()
    stream = grad_stream(r, n, rep, lambda slot: r.ours.at[slot], lambda slot: r.whole.at[slot])
    stream.pack_fill((r.dln1, r.dln2, r.dqn, r.dkn))
    pl.semaphore_wait(barrier, n - 1 + rep - 1)
    for load in loads:
        load.wait()
    stream.pack_start()
    stream.prime(0)
    stream.finish(0)


def layer_kernel(r, n, rep, hd, fused):
    sec = lax.axis_index("section")
    me = lax.axis_index("fsdp")
    mine = lax.axis_index("replica")
    wq_h, wk_h, wv_h, wg_h, wu_h = r.wq_h, r.wk_h, r.wv_h, r.wg_h, r.wu_h
    cosine, sine, wall, wo, wd, ln1, ln2, qn, kn, gains = (
        r.cosine, r.sine, r.wall, r.wo, r.wd, r.ln1, r.ln2, r.qn, r.kn, r.gains
    )
    xin, xn_all, hn_all, dy_all, qkv, qkvb, att, hres, gate, up, act, dgu, dqkv = (
        r.xin, r.xn, r.hn, r.dy, r.qkv, r.qkvb, r.att, r.hres, r.gate, r.up, r.act, r.dgu, r.dqkv
    )
    dab_all = r.dab if fused else r.hn
    dob, yv, sbuf, rbuf, turn = r.dob, r.yv, r.sbuf, r.rbuf, r.turn
    dln1, dln2, dqn, dkn = r.dln1, r.dln2, r.dqn, r.dkn
    zw_send, zw_recv, gw_send, gw_recv, own_sem = r.zw_send, r.zw_recv, r.gw_send, r.gw_recv, r.own_sem
    ag_send, ag_recv, rs_send, rs_recv = r.ag_send, r.ag_recv, r.rs_send, r.rs_recv
    steps = rep.bit_length() - 1
    rows, width = xin.shape
    ch = att.shape[-1]
    qcols = ch
    kcols = (qkvb.shape[-1] - qcols) // 2
    hidden = act.shape[-1]
    chunks = wall.shape[0]
    share = wall.shape[3]
    kfold = rep * share
    scale = 1.0 / math.sqrt(hd)
    orders = (tuple(range(steps)), tuple(reversed(range(steps))))

    barrier = greet(n, rep, me, mine)
    pl.semaphore_signal(barrier, inc=1, device_id={"section": 1 - sec}, device_id_type=MESH)
    load_o = pltpu.make_async_copy(r.wo_h, wo, r.w_sem.at[0])
    load_d = pltpu.make_async_copy(r.wd_h, wd, r.w_sem.at[1])
    load_x = pltpu.make_async_copy(r.tok, xin, r.w_sem.at[2])
    load_y = pltpu.make_async_copy(r.cot, dy_all.at[me], r.w_sem.at[3])

    @pl.when(sec == 0)
    def _():
        load_x.start()

    @pl.when(sec == 1)
    def _():
        load_y.start()

    load_o.start()
    load_d.start()

    at = 0
    gain_at = []
    gains[me] = jnp.zeros_like(gains[me])
    for value in (r.ln1_own, r.ln2_own, r.qn_own, r.kn_own):
        size = value.shape[-1]
        gains[me, :, at : at + size] = value[...].astype(F32)
        gain_at.append((at, size))
        at += size
    pl.semaphore_wait(barrier, n + rep - 1)

    def gain_copy(d):
        return remote(
            gains.at[me], gains.at[me], r.gain_send.at[d - 1], r.gain_recv.at[d - 1],
            {"fsdp": lax.rem(me + d, n)},
        )

    for d in range(1, n):
        gain_copy(d).start()

    def slabs(c, to):
        rows_in = pl.ds(pl.multiple_of(mine * share, share), share)
        if isinstance(c, int) and c == 0:
            return (
                (wq_h.at[rows_in, pl.ds(to * ch, ch)], pl.ds(0, ch)),
                (wk_h.at[rows_in, pl.ds(to * kcols, kcols)], pl.ds(ch, kcols)),
                (wv_h.at[rows_in, pl.ds(to * kcols, kcols)], pl.ds(ch + kcols, kcols)),
            )
        cols = pl.ds(pl.multiple_of(to * hidden + (c - 1) * ch, 128), ch)
        return (
            (wg_h.at[rows_in, cols], pl.ds(0, ch)),
            (wu_h.at[rows_in, cols], pl.ds(ch, ch)),
        )

    def slab_copies(c):
        for i, (src, lanes) in enumerate(slabs(c, me)):
            yield pltpu.make_async_copy(src, wall.at[c, me, mine, :, lanes], own_sem.at[c, i])
        for d in range(1, n):
            to = lax.rem(me + d, n)
            for i, (src, lanes) in enumerate(slabs(c, to)):
                yield remote(
                    src, wall.at[c, me, mine, :, lanes],
                    zw_send.at[c, d - 1, i], zw_recv.at[c, d - 1, i], {"fsdp": to},
                )

    def slab_gathers(c, j):
        for h, order in enumerate(orders):
            bits = order[::-1]
            partner = flip(mine, bits[j])
            for i in range(1 << j):
                piece = flips(mine, bits[:j], i)
                ref = wall.at[c, :, piece, :, pl.ds(h * ch, ch)]
                yield remote(
                    ref, ref, gw_send.at[j, c, h, i], gw_recv.at[j, c, h, i], {"replica": partner}
                )

    def prepare(c, j):
        for copy in slab_copies(c) if j == 0 else slab_gathers(c, j - 1):
            copy.wait()
        if j < steps:
            for copy in slab_gathers(c, j):
                copy.start()

    events = [
        (t - j, j) for t in range(2, chunks + steps) for j in range(steps) if 2 <= t - j < chunks
    ]
    events.sort(key=lambda event: (event[0] + event[1], -event[1]))
    places = [events[3 * k : 3 * k + 1] for k in range(n // 2 - 1)]
    middles = [events[3 * k + 1 : 3 * k + 3] for k in range(n // 2 - 1)]
    leftover = events[3 * (n // 2 - 1) :]

    def prepare_all(some):
        for event in some:
            prepare(*event)

    def prepare_first():
        for j in range(steps + 1):
            prepare(0, j)
            if j > 0:
                prepare(1, j - 1)

    bits = n.bit_length() - 1
    piece = width // n

    def low(m):
        return (m & -m).bit_length() - 1

    def across(s):
        return sum((me // 2**j + s // 2**j) % 2 * 2**j for j in range(bits))

    def spread(buf, c, m, j):
        ref = buf.at[flips(me, range(bits), m)]
        return remote(
            ref, ref, ag_send.at[c, m + 2**j], ag_recv.at[c, m + 2**j], {"fsdp": flip(me, j)}
        )

    def spread_start(buf, c):
        for j in range(bits):
            spread(buf, c, 0, j).start()

    def spread_done(buf, c):
        for m in range(n):
            for j in range(bits if m == 0 else low(m)):
                spread(buf, c, m, j).wait_send()

    def fold(c, m, k, j):
        cols = pl.ds(k * piece, piece)
        return remote(
            sbuf.at[c % 2, m, :, cols], rbuf.at[c % 2, m - 1, :, cols],
            rs_send.at[c, m, k], rs_recv.at[c, m, k], {"fsdp": flip(me, j)},
        )

    def each_pair(buf, c, work):
        def hear(s):
            ref = buf.at[across(s)]
            remote(
                ref, ref, ag_send.at[c, s], ag_recv.at[c, s], {"fsdp": flip(me, 0)}
            ).wait_recv()

        def step(q, carry):
            hear(2 * q + 1)

            def relay():
                for m in range(2, n, 2):
                    @pl.when(2 * q + 2 == m)
                    def _():
                        hear(m)
                        for j in range(low(m)):
                            spread(buf, c, m, j).start()

            def ship(k, value):
                for i in range(2):
                    part = value[i * rows : (i + 1) * rows].astype(BF16)
                    sbuf[c % 2, 2 * q + (me + i) % 2, :, k * piece : (k + 1) * piece] = part
                fold(c, 2 * q + 1, k, 0).start()

            work(q, across(2 * q) // 2 * 2, relay, ship)
            return carry

        lax.fori_loop(0, n // 2, step, 0)

    def settle_through(c):
        own, heard = sbuf.at[c % 2], rbuf.at[c % 2]
        for m in sorted(range(2, n, 2), key=low):
            for k in range(n):
                cols = slice(k * piece, (k + 1) * piece)
                value = own[m, :, cols].astype(F32)
                for j in range(low(m)):
                    fold(c, m + 2**j, k, j).wait_recv()
                    value = value + heard[m + 2**j - 1, :, cols].astype(F32)
                own[m, :, cols] = value.astype(BF16)
                fold(c, m, k, low(m)).start()

    def settle_own(c):
        for j in range(bits):
            for k in range(n):
                fold(c, 2**j, k, j).wait_recv()
        for m in range(1, n):
            for k in range(n):
                fold(c, m, k, low(m)).wait_send()

    def pair_of(buf, base):
        value = buf[pl.ds(base, 2)]
        return value.reshape(2 * rows, value.shape[-1])

    def summed(c, at):
        total = sbuf[c % 2, 0, at].astype(F32)
        for j in range(bits):
            total = total + rbuf[c % 2, 2**j - 1, at].astype(F32)
        return total

    def by_rows(work):
        height = 32

        def step(i, carry):
            work(pl.ds(pl.multiple_of(i * height, height), height))
            return carry

        lax.fori_loop(0, rows // height, step, 0)

    outs = {}
    put_keys = ("y", "dx", "xn", "hn", "dy", "dab", "att", "act", "dgu", "dqkv")

    def put(key, src):
        if hasattr(r, key + "_h"):
            copy = pltpu.make_async_copy(src, getattr(r, key + "_h"), r.out_sem.at[put_keys.index(key)])
            copy.start()
            outs[key] = copy

    def put_done(*keys):
        for key in keys:
            if key in outs:
                outs.pop(key).wait()

    def swap(value):
        return pltpu.roll(value, hd // 2, 1)

    def hand(src, dst, to, k):
        return pltpu.make_async_remote_copy(
            src_ref=src,
            dst_ref=dst,
            send_sem=r.hand_send.at[k],
            recv_sem=r.hand_recv.at[k],
            device_id={"section": to},
            device_id_type=MESH,
        )

    @pl.when(sec == 1)
    def _():
        pl.semaphore_wait(turn, 1)

    for c in range(2):
        for copy in slab_copies(c):
            copy.start()
    for d in range(1, n):
        gain_copy(d).wait()
    for k, full in enumerate((ln1, ln2, qn, kn)):
        at, size = gain_at[k]
        for f in range(n):
            full[:, f * size : (f + 1) * size] = gains[f, :, at : at + size]

    @pl.when(sec == 1)
    def _():
        prepare_first()
        hand(yv, xin, 0, 0).wait_recv()

    @pl.when(sec == 0)
    def _():
        load_x.wait()

    @by_rows
    def _(at):
        x32 = xin[at].astype(F32)
        r1 = lax.rsqrt(mean_last(x32 * x32) + EPS)
        xn_all[me, at] = (x32 * r1 * ln1[...]).astype(BF16)

    spread_start(xn_all, 0)
    for c in range(2, chunks):
        for copy in slab_copies(c):
            copy.start()

    @pl.when(sec == 0)
    def _():
        prepare_first()

    load_o.wait()
    load_d.wait()

    def masked_scores(qh, kh):
        raw = nt(qh, kh) * scale
        at_row = lax.broadcasted_iota(jnp.int32, raw.shape, 0)
        at_col = lax.broadcasted_iota(jnp.int32, raw.shape, 1)
        raw = jnp.where(at_row >= at_col, raw, -jnp.inf)
        top = jnp.max(raw, axis=-1, keepdims=True)
        lse = top + jnp.log(jnp.sum(jnp.exp(raw - top), axis=-1, keepdims=True))
        return jnp.exp(raw - lse)

    def attend_block(s):
        for at in range(0, qcols + kcols, hd):
            field = qkv[s, :, at : at + hd]
            gain = qn[...] if at < qcols else kn[...]
            factor = lax.rsqrt(mean_last(field * field) + EPS)
            normed = field * factor * gain
            turned = normed * cosine[...] + swap(normed) * sine[...]
            qkvb[s, :, at : at + hd] = turned.astype(BF16)
        qkvb[s, :, qcols + kcols :] = qkv[s, :, qcols + kcols :].astype(BF16)
        for j in range(qcols // hd):
            kv = j * kcols // qcols
            kat = qcols + kv * hd
            vat = qcols + kcols + kv * hd
            probs = masked_scores(qkvb[s, :, j * hd : (j + 1) * hd], qkvb[s, :, kat : kat + hd])
            attended = nn(probs.astype(BF16), qkvb[s, :, vat : vat + hd])
            att[s, :, j * hd : (j + 1) * hd] = attended.astype(BF16)
    def both(base, work):
        lax.fori_loop(0, 2, lambda i, carry: work(base + i) or carry, 0)

    def attend(q, base, relay, ship):
        for k, some in enumerate(places):
            @pl.when(q == k + 1)
            def _():
                prepare_all(some)

        a = pair_of(xn_all, base)
        for at, size in tiles(2 * ch):
            w = wall[0, :, :, :, at : at + size].reshape(width, size)
            qkv[pl.ds(base, 2), :, at : at + size] = nn(a, w).reshape(2, rows, size)
        relay()
        both(base, attend_block)
        for k, some in enumerate(middles):
            @pl.when(q == k + 1)
            def _():
                prepare_all(some)

        a = pair_of(att, base)
        for k in range(n):
            ship(k, nn(a, wo[:, k * piece : (k + 1) * piece]))

    each_pair(xn_all, 0, attend)
    settle_through(0)
    prepare_all(leftover[:1])
    settle_own(0)

    @by_rows
    def _(at):
        h = xin[at].astype(F32) + summed(0, at)
        hres[at] = h
        r2 = lax.rsqrt(mean_last(h * h) + EPS)
        hn_all[me, at] = (h * r2 * ln2[...]).astype(BF16)

    spread_start(hn_all, 1)
    put("xn", xn_all)
    put("att", att)

    prepare_all(leftover[1:])
    for c in range(1, chunks):
        prepare(c, steps)

    @pl.when(sec == 0)
    def _():
        pl.semaphore_signal(turn, inc=1, device_id={"section": 1}, device_id_type=MESH)

    if fused:
        @pl.when(sec == 1)
        def _():
            pl.semaphore_signal(r.later, inc=1, device_id={"section": 0}, device_id_type=MESH)

    def feed(q, base, relay, ship):
        a = pair_of(hn_all, base)
        here = pl.ds(base, 2)
        for at in range(0, hidden, ch):
            j = 1 + at // ch
            g = nn(a, wall[j, :, :, :, :ch].reshape(width, ch))
            u = nn(a, wall[j, :, :, :, ch:].reshape(width, ch))
            gate[here, :, at : at + ch] = g.astype(BF16).reshape(2, rows, ch)
            up[here, :, at : at + ch] = u.astype(BF16).reshape(2, rows, ch)
            value = (g * jax.nn.sigmoid(g) * u).astype(BF16)
            act[here, :, at : at + ch] = value.reshape(2, rows, ch)
        relay()

        @pl.when(jnp.logical_and(sec == 1, q == 0))
        def _():
            load_y.wait()
            spread_start(dy_all, 2)

        a = pair_of(act, base)
        for k in range(n):
            ship(k, nn(a, wd[:, k * piece : (k + 1) * piece]))

    each_pair(hn_all, 1, feed)

    def write_y():
        @by_rows
        def _(at):
            yv[at] = (hres[at] + summed(1, at)).astype(BF16)

    if fused:
        def place(slot):
            return wall.at[1 + slot // n, slot % n]

        view = types.SimpleNamespace(**{**vars(r), "hn": hn_all, "dab": dab_all})
        strip = ch // rep

        def far_out():
            yield pltpu.make_async_copy(hn_all, r.hn_far.at[mine], r.far_own.at[2 * chunks])
            for m in range(1, rep):
                yield remote(
                    hn_all, r.hn_far.at[mine], r.far_send.at[m - 1, 0], r.far_recv.at[m - 1, 0],
                    {"replica": peer(mine, rep, m)},
                )

        def strips_out():
            for k in range(2 * (chunks - 1)):
                to = wall.at[chunks - 1, :, mine, :, pl.ds(k * strip, strip)]
                own = pl.ds(pl.multiple_of(k * ch + mine * strip, strip), strip)
                yield pltpu.make_async_copy(dgu.at[:, :, own], to, r.far_own.at[k])
                for m in range(1, rep):
                    other = peer(mine, rep, m)
                    cols = pl.ds(pl.multiple_of(k * ch + other * strip, strip), strip)
                    yield remote(
                        dgu.at[:, :, cols], to, r.far_send.at[m - 1, k + 1],
                        r.far_recv.at[m - 1, k + 1], {"replica": other},
                    )

        def far_ready():
            for copy in (*far_out(), *strips_out()):
                copy.wait()

        far = types.SimpleNamespace(
            here=sec == 0,
            ready=far_ready,
            left=lambda block: wall.at[2, 2 + block // 2, :, :, pl.ds(block % 2 * n * 128, n * 128)],
            right=lambda block: wall.at[chunks - 1, block],
            held=wall.at[2, 1],
        )
        stream = grad_stream(view, n, rep, lambda slot: r.ours.at[slot], place, far)

    put("hn", hn_all)
    put("act", act)

    @pl.when(sec == 0)
    def _():
        settle_through(1)
        settle_own(1)
        write_y()
        hand(yv, xin, 1, 0).start()
        if fused:
            pl.semaphore_wait(r.later, 1)
            for copy in far_out():
                copy.start()
        hand(yv, dy_all.at[me], 1, 1).wait_recv()
        spread_start(dy_all, 2)

    spread_done(hn_all, 1)
    put_done("hn")

    def early_tick(t):
        if fused:
            stream.tick(t, (0, 1))

    def early(low, high):
        if fused:
            lax.fori_loop(low, high, lambda t, carry: early_tick(t) or carry, 0)

    def feed_back(q, base, relay, ship):
        @pl.when(q == n // 2 - 1)
        def _():
            if fused:
                stream.prime(0)
            early_tick(0)

        a = pair_of(dy_all, base)
        here = pl.ds(base, 2)
        for at in range(0, hidden, ch):
            dact = nt(a, wd[at : at + ch, :])
            g = gate[here, :, at : at + ch].reshape(2 * rows, ch).astype(F32)
            u = up[here, :, at : at + ch].reshape(2 * rows, ch).astype(F32)
            sig = jax.nn.sigmoid(g)
            dg = (dact * u * sig * (1.0 + g * (1.0 - sig))).astype(BF16)
            du = (dact * g * sig).astype(BF16)
            dgu[here, :, 2 * at : 2 * at + ch] = dg.reshape(2, rows, ch)
            dgu[here, :, 2 * at + ch : 2 * at + 2 * ch] = du.reshape(2, rows, ch)
        relay()

        @pl.when(jnp.logical_and(sec == 1, q == n // 2 - 1))
        def _():
            settle_through(1)

        @pl.when(q == n // 2 - 1)
        def _():
            early_tick(1)

        a = pair_of(dgu, base)
        for f in range(n):
            total = jnp.zeros((2 * rows, kfold), F32)
            for j in range(1, chunks):
                w = wall[j, f].reshape(kfold, 2 * ch)
                total = total + nt(a[:, 2 * (j - 1) * ch : 2 * j * ch], w)
            ship(f, total)

    each_pair(dy_all, 2, feed_back)


    if fused:
        for where in [{"fsdp": lax.rem(me + d, n)} for d in range(1, n)] + [
            {"replica": peer(mine, rep, m)} for m in range(1, rep)
        ]:
            pl.semaphore_signal(r.freed, inc=1, device_id=where, device_id_type=MESH)
    early_tick(2)
    settle_through(2)
    if fused:
        pl.semaphore_wait(r.freed, n - 1 + rep - 1)

        @pl.when(sec == 0)
        def _():
            for copy in strips_out():
                copy.start()
    early_tick(3)

    @pl.when(sec == 1)
    def _():
        settle_own(1)
        write_y()

    settle_own(2)
    dln2[...] = jnp.zeros_like(dln2)
    dln1[...] = jnp.zeros_like(dln1)

    @by_rows
    def _(at):
        dhn = summed(2, at)
        h = hres[at]
        r2 = lax.rsqrt(mean_last(h * h) + EPS)
        u = dhn * ln2[...]
        dh = dy_all[me, at].astype(F32) + (r2 * u - h * r2 * r2 * r2 * mean_last(u * h))
        dln2[...] += jnp.sum(dhn * h * r2, axis=0, keepdims=True)
        hres[at] = dh
        dab_all[me, at] = dh.astype(BF16)

    spread_start(dab_all, 3)
    early(4, 6)

    put("y", yv)
    put("dy", dy_all)
    put("dgu", dgu)

    dqn[...] = jnp.zeros_like(dqn)
    dkn[...] = jnp.zeros_like(dkn)

    def head_back(s, at, grad, gain, dgain):
        field = qkv[s, :, at : at + hd]
        factor = lax.rsqrt(mean_last(field * field) + EPS)
        grad = grad * cosine[...] - swap(grad) * sine[...]
        v = grad * gain
        back = factor * v - field * factor * factor * factor * mean_last(v * field)
        dgain[...] += jnp.sum(grad * field * factor, axis=0, keepdims=True)
        dqkv[s, :, at : at + hd] = back.astype(BF16)

    def attend_back_block(i, s):
        for kv in range(kcols // hd):
            kat = qcols + kv * hd
            vat = qcols + kcols + kv * hd
            kh = qkvb[s, :, kat : kat + hd]
            vh = qkvb[s, :, vat : vat + hd]
            dk = jnp.zeros((rows, hd), F32)
            dv = jnp.zeros((rows, hd), F32)
            for j in range(kv * qcols // kcols, (kv + 1) * qcols // kcols):
                qh = qkvb[s, :, j * hd : (j + 1) * hd]
                dh_out = dob[i, :, j * hd : (j + 1) * hd]
                probs = masked_scores(qh, kh)
                dv = dv + tn(probs.astype(BF16), dh_out)
                dp = nt(dh_out, vh)
                delta = jnp.sum(probs * dp, axis=-1, keepdims=True)
                ds = (probs * (dp - delta) * scale).astype(BF16)
                dk = dk + tn(ds, qh)
                head_back(s, j * hd, nn(ds, kh), qn[...], dqn)
            head_back(s, kat, dk, kn[...], dkn)
            dqkv[s, :, vat : vat + hd] = dv.astype(BF16)
    def attend_back(q, base, relay, ship):
        a = pair_of(dab_all, base)
        for at, size in tiles(qcols):
            dout = nt(a, wo[at : at + size, :]).astype(BF16)
            dob[:, :, at : at + size] = dout.reshape(2, rows, size)
        relay()
        early(6 + 2 * q, 8 + 2 * q)
        lax.fori_loop(0, 2, lambda i, carry: attend_back_block(i, base + i) or carry, 0)
        a = pair_of(dqkv, base)
        for f in range(n):
            w = wall[0, f].reshape(kfold, 2 * ch)
            ship(f, nt(a, w))

    each_pair(dab_all, 3, attend_back)
    early_tick(6 + n)
    settle_through(3)
    early_tick(7 + n)
    settle_own(3)
    put_done("y")

    @pl.when(sec == 0)
    def _():
        hand(yv, xin, 1, 0).wait_send()

    @by_rows
    def _(at):
        dxn = summed(3, at)
        x32 = xin[at].astype(F32)
        r1 = lax.rsqrt(mean_last(x32 * x32) + EPS)
        u = dxn * ln1[...]
        dx = hres[at] + (r1 * u - x32 * r1 * r1 * r1 * mean_last(u * x32))
        dln1[...] += jnp.sum(dxn * x32 * r1, axis=0, keepdims=True)
        yv[at] = dx.astype(BF16)
        hres[at] = dx

    @pl.when(sec == 1)
    def _():
        hand(yv, dy_all.at[me], 0, 1).start()

    put("dx", hres)
    put("dab", dab_all)
    put("dqkv", dqkv)
    if fused:
        stream.pack_fill((dln1, dln2, dqn, dkn))
        stream.pack_start()
        stream.finish(8 + n)
    for c, buf in ((0, xn_all), (2, dy_all), (3, dab_all)):
        spread_done(buf, c)

    @pl.when(sec == 1)
    def _():
        hand(yv, dy_all.at[me], 0, 1).wait_send()

    put_done(*list(outs))


def run_layer(n, rep, fused, lanes, tok, cot, ln1, ln2, qn, kn, wq, wk, wv, wg, wu, wo, wd):
    rows, width = tok.shape
    hd = n * qn.shape[-1]
    qcols = wo.shape[0]
    qkvcols = 2 * qcols
    steps = rep.bit_length() - 1
    chunks = 1 + wd.shape[0] // qcols
    hidden = wd.shape[0]
    cosine, sine = rope_tables(rows, hd // 2)
    inputs = {
        "tok": tok, "cot": cot, "ln1_own": ln1, "ln2_own": ln2, "qn_own": qn, "kn_own": kn,
        "cosine": cosine, "sine": sine, "wq_h": wq, "wk_h": wk, "wv_h": wv, "wg_h": wg, "wu_h": wu,
        "wo_h": wo, "wd_h": wd,
    }
    in_vmem = ("ln1_own", "ln2_own", "qn_own", "kn_own", "cosine", "sine")
    single = {"dln1": (1, width), "dln2": (1, width), "dqn": (1, hd), "dkn": (1, hd)}
    outputs = {
        "y_h": jax.ShapeDtypeStruct((rows, width), BF16),
        "dx_h": jax.ShapeDtypeStruct((rows, width), F32),
    }
    saved = {
        "xn": width, "hn": width, "dy": width, "dab": width, "att": qcols, "act": hidden,
        "dgu": 2 * hidden, "dqkv": qkvcols,
    }
    dma = pltpu.SemaphoreType.DMA
    scratch = {
        "wall": pltpu.VMEM((chunks, n, rep, width // (n * rep), qkvcols), BF16),
        "wo": pltpu.VMEM(wo.shape, BF16),
        "wd": pltpu.VMEM(wd.shape, BF16),
        "ln1": pltpu.VMEM((1, width), F32),
        "ln2": pltpu.VMEM((1, width), F32),
        "qn": pltpu.VMEM((1, hd), F32),
        "kn": pltpu.VMEM((1, hd), F32),
        "gains": pltpu.VMEM((n, 1, lanes), F32),
        "xin": pltpu.VMEM((rows, width), BF16),
        **{
            key: pltpu.VMEM((n, rows, size), BF16)
            for key, size in saved.items() if fused or key != "dab"
        },
        "qkv": pltpu.VMEM((n, rows, qkvcols), F32),
        "qkvb": pltpu.VMEM((n, rows, qkvcols), BF16),
        "hres": pltpu.VMEM((rows, width), F32),
        "gate": pltpu.VMEM((n, rows, hidden), BF16),
        "up": pltpu.VMEM((n, rows, hidden), BF16),
        "dob": pltpu.VMEM((2, rows, qcols), BF16),
        "yv": pltpu.VMEM((rows, width), BF16),
        "sbuf": pltpu.VMEM((2, n, rows, width), BF16),
        "rbuf": pltpu.VMEM((2, n - 1, rows, width), BF16),
        "w_sem": dma((4,)),
        "zw_send": dma((chunks, n - 1, 3)),
        "zw_recv": dma((chunks, n - 1, 3)),
        "gw_send": dma((steps, chunks, 2, rep // 2)),
        "gw_recv": dma((steps, chunks, 2, rep // 2)),
        "own_sem": dma((chunks, 3)),
        "gain_send": dma((n - 1,)),
        "gain_recv": dma((n - 1,)),
        "turn": pltpu.SemaphoreType.REGULAR,
        "out_sem": dma((10,)),
        "ag_send": dma((4, n)),
        "ag_recv": dma((4, n)),
        "rs_send": dma((4, n, n)),
        "rs_recv": dma((4, n, n)),
        "hand_send": dma((2,)),
        "hand_recv": dma((2,)),
    }
    if fused:
        outputs |= stream_outputs(n, rep, qcols, hidden, width, lanes)
        scratch |= {key: pltpu.VMEM(shape, F32) for key, shape in single.items()}
        scratch |= stream_scratch(n, rep, qcols, lanes)
        outputs["hn_far"] = jax.ShapeDtypeStruct((rep, n, rows, width), BF16)
        scratch["freed"] = pltpu.SemaphoreType.REGULAR
        scratch["later"] = pltpu.SemaphoreType.REGULAR
        scratch["far_own"] = dma((2 * chunks + 1,))
        scratch["far_send"] = dma((rep - 1, 2 * chunks))
        scratch["far_recv"] = dma((rep - 1, 2 * chunks))
        scratch["far_load"] = dma((n, n))
        scratch["ours"] = pltpu.VMEM((steps + 1, rep, 128, 2 * qcols), BF16)
    else:
        outputs |= {
            key + "_h": jax.ShapeDtypeStruct((n, rows, size), BF16) for key, size in saved.items()
        }
        outputs |= {key: jax.ShapeDtypeStruct(shape, F32) for key, shape in single.items()}
    out_vmem = (*single, "sums")
    return call(
        layer_kernel, (n, rep, hd, fused), inputs, outputs, scratch, in_vmem, out_vmem, "layer", 0
    )


def run_grads(n, rep, saved, lanes):
    steps = rep.bit_length() - 1
    ch, hidden, width = (saved[key].shape[-1] for key in ("att_h", "act_h", "xn_h"))
    inputs = {key: value for key, value in saved.items() if key not in ("y_h", "dx_h")}
    scratch = {
        key[:-2]: pltpu.VMEM(value.shape, BF16) for key, value in inputs.items() if key[-2:] == "_h"
    }
    scratch["ours"] = pltpu.VMEM((steps + 1, rep, 128, 2 * ch), BF16)
    scratch["whole"] = pltpu.VMEM((steps + 3, rep, 128, 2 * ch), BF16)
    scratch["in_sem"] = pltpu.SemaphoreType.DMA((8,))
    scratch |= stream_scratch(n, rep, ch, lanes)
    outputs = stream_outputs(n, rep, ch, hidden, width, lanes)
    small = ("dln1", "dln2", "dqn", "dkn")
    return call(grad_kernel, (n, rep), inputs, outputs, scratch, small, ("sums",), "grads", 1)


def write_results(sources, sums, gains, y, dx):
    steps = 8

    moved = [*sources, y, dx]

    def rows_of(value):
        return pl.BlockSpec((value.shape[0] // steps, value.shape[1]), lambda i: (i, 0))

    def all_of(columns):
        return pl.BlockSpec((1, columns), lambda i: (0, 0))

    kinds = [F32] * len(sources) + [BF16, F32]

    def kernel(*refs):
        ins, outs = refs[: len(moved) + 1], refs[len(moved) + 1 :]
        for src, dst in zip(ins, outs[: len(moved)]):
            dst[...] = src[...].astype(dst.dtype)
        at = 0
        for size, dst in zip(gains, outs[len(moved) :]):
            dst[...] = ins[-1][:, at : at + size]
            at += size

    return pl.pallas_call(
        kernel,
        grid=(steps,),
        out_shape=[jax.ShapeDtypeStruct(v.shape, kind) for v, kind in zip(moved, kinds)]
        + [jax.ShapeDtypeStruct((1, size), F32) for size in gains],
        in_specs=[rows_of(value) for value in moved] + [all_of(sums.shape[1])],
        out_specs=[rows_of(value) for value in moved] + [all_of(size) for size in gains],
        compiler_params=pltpu.CompilerParams(vmem_limit_bytes=67043328),
        name="results",
    )(*moved, sums)


def per_device(tokens_in, cotangent, ln1, wq, wk, wv, qn, kn, wo, ln2, wg, wu, wd):
    n, rep = lax.axis_size("fsdp"), lax.axis_size("replica")

    lanes = -(-2 * (ln1.shape[-1] + qn.shape[-1]) // 128) * 128
    thirds = grad_plan(n, wo.shape[1], wd.shape[1], wo.shape[2])[1]
    fused = (2 * rep.bit_length() + 2) <= n * thirds and wq.shape[1] == n * 128
    fused = fused and n == rep == 4 and thirds == 3
    done = run_layer(
        n, rep, fused, lanes, tokens_in, cotangent, ln1, ln2, qn, kn,
        wq[0], wk[0], wv[0], wg[0], wu[0], wo[0], wd[0],
    )
    y, dx = done["y_h"], done["dx_h"]
    if not fused:
        done = run_grads(n, rep, done, lanes)
    sources = [
        done[key].reshape(-1, done[key].shape[-1])
        for key in ("gq_h", "gk_h", "gv_h", "go_h", "gg_h", "gu_h", "gd_h")
    ]
    gains = [gain.shape[1] for gain in (ln1, ln2, qn, kn)]
    (
        g_wq, g_wk, g_wv, g_wo, g_wg, g_wu, g_wd, y, dx, *owned
    ) = write_results(sources, done["sums"], gains, y, dx)
    g_ln1, g_ln2, g_qn, g_kn = (value[0] for value in owned)
    results = (y, dx, g_ln1, g_wq, g_wk, g_wv, g_qn, g_kn, g_wo, g_ln2, g_wg, g_wu, g_wd)
    return tuple(value[None] for value in results)


def solution(mesh):
    rows = P("section", "fsdp", None)
    gain = P("section", "fsdp")
    tokens = P(("fsdp", "replica"), None)
    stacked = P("section", ("fsdp", "replica"), None)
    weights = (gain, rows, rows, rows, gain, gain, rows, gain, rows, rows, rows)
    return jax.shard_map(
        per_device,
        mesh=mesh,
        in_specs=(tokens, tokens, *weights),
        out_specs=(stacked, stacked, *weights),
        check_vma=False,
    )
```
